32 devices in a mesh: wide: 8 (over z, x), narrow: 4 (over y, core).
Axes of the slice: x: 2, y: 2, z: 4, core: 2. Of those that a mesh axis runs over, the one named last changes fastest.
Arguments:
- text_in: bfloat16 [2, 32, 4, 108, 768], P(None, ('wide', 'narrow')), may hold values from -6 to 6
- memory_in: bfloat16 [2, 32, 10, 768], P(None, ('wide', 'narrow')), may hold values from -6 to 6
- counts: int32 [2, 32], P(None, ('wide', 'narrow')), may hold values from 2 to 4
- last_len: int32 [2, 32], P(None, ('wide', 'narrow')), may hold values from 1 to 108
- cot_text: bfloat16 [2, 32, 4, 108, 768], P(None, ('wide', 'narrow')), may hold values from -6 to 6
- cot_memory: bfloat16 [2, 32, 10, 768], P(None, ('wide', 'narrow')), may hold values from -6 to 6
- qkv_weight: bfloat16 [2, 3, 768, 768], P(None, None, 'wide', 'narrow'), may hold values from -0.21875 to 0.21875
- out_weight: bfloat16 [2, 768, 768], P(None, 'wide', 'narrow'), may hold values from -0.875 to 0.875
- up_weight: bfloat16 [2, 768, 3072], P(None, 'wide', 'narrow'), may hold values from -0.21875 to 0.21875
- down_weight: bfloat16 [2, 3072, 768], P(None, 'wide', 'narrow'), may hold values from -0.109375 to 0.109375
- biases: bfloat16 [2, 4, 768], P(None, 'narrow', 'wide'), may hold values from -3 to 3
- up_bias: bfloat16 [2, 3072], P(None, ('wide', 'narrow')), may hold values from -3 to 3
- norm_params: bfloat16 [2, 4, 768], P(None, 'narrow', 'wide'), may hold values from -1.2 to 1.5, as said below
Outputs:
- text_out: bfloat16 [2, 32, 4, 108, 768], P(None, ('wide', 'narrow'))
- memory_out: bfloat16 [2, 32, 10, 768], P(None, ('wide', 'narrow'))
- text_grad: bfloat16 [2, 32, 4, 108, 768], P(None, ('wide', 'narrow'))
- memory_grad: bfloat16 [2, 32, 10, 768], P(None, ('wide', 'narrow'))
- grad_qkv: float32 [2, 3, 768, 768], P(None, None, 'wide', 'narrow')
- grad_out: float32 [2, 768, 768], P(None, 'wide', 'narrow')
- grad_up: float32 [2, 768, 3072], P(None, 'wide', 'narrow')
- grad_down: float32 [2, 3072, 768], P(None, 'wide', 'narrow')
- grad_biases: float32 [2, 4, 768], P(None, 'narrow', 'wide')
- grad_up_bias: float32 [2, 3072], P(None, ('wide', 'narrow'))
- grad_norm: float32 [2, 4, 768], P(None, 'narrow', 'wide')
The draws below stay inside these ranges and needn't reach their ends.
Inputs may be any that keep to these rules, and one draw needn't show every extreme that they name: `norm_params`: rows 0 and 2 of each layer are positive gains, rows 1 and 3 shifts.
All inputs are finite; a program needn't handle non-finite values.
Results may differ from the reference program's by a relative error of at most 0.03.
Values may be sent and summed in bfloat16 or wider, within the bound.
A program may use at most 448 MiB of HBM per device.

```python
import math
import jax
import jax.numpy as jnp
from jax import lax

D = 768
HEADS = 12
HD = 64
FF = 3072
MEM = 10
TEXT = 108
SEGS = 4
MB = 2
LAYERS = 2
ITEMS = 32


def draw_norm_params(key, part):
    gain_key, shift_key = jax.random.split(jax.random.fold_in(key, 17))
    gains = jax.random.uniform(gain_key, (LAYERS, 2, D), jnp.float32, 0.5, 1.5)
    shifts = jnp.clip(0.3 * jax.random.normal(shift_key, (LAYERS, 2, D), jnp.float32), -1.2, 1.2)
    stacked = jnp.stack([gains[:, 0], shifts[:, 0], gains[:, 1], shifts[:, 1]], axis=1)
    return stacked.astype(jnp.bfloat16)


def set_ends(values, own_key, low, high):
    spot = [jax.random.randint(jax.random.fold_in(own_key, axis), (), 0, length) for axis, length in enumerate(values.shape)]
    longest = values.shape.index(max(values.shape))
    neighbour = spot[:longest] + [(spot[longest] + 1) % values.shape[longest]] + spot[longest + 1:]
    return values.at[tuple(spot)].set(low).at[tuple(neighbour)].set(high)


def spiked(values, rng, source, target, parts, factor):
    owner, partner = [(jnp.arange(values.shape[position]) // (values.shape[position] // parts)).reshape([-1 if axis == position else 1 for axis in range(values.ndim)]) for position in (source, target)]
    chosen = jax.random.permutation(rng, parts)[partner]
    strong = (owner == chosen) | (owner == (partner + parts // 2) % parts)
    return jnp.where(strong, factor * values, values)


def level_of(key, extent, cuts, least, high):
    gain, own = 1.0, jax.random.fold_in(key, 6)
    for dim, parts in cuts:
        steps = jnp.exp(jax.random.uniform(jax.random.fold_in(own, dim), (parts,), jnp.float32, least / len(cuts), high / len(cuts)))
        gain = gain * jnp.repeat(steps, extent[dim] // parts).reshape([-1 if axis == dim else 1 for axis in range(len(extent))])
    return gain


def centred(stream_key, dims, deviation, most, cuts=(), kind=jnp.bfloat16):
    level = level_of(stream_key, dims, cuts, -0.22, 0.18) if cuts else 1.0
    values = jax.random.normal(stream_key, dims, jnp.float32) * deviation * level
    return jnp.minimum(jnp.maximum(values, -most), most).astype(kind)


def noise_with(rng, extent, deviation, reach, cuts, heavy, kind=jnp.bfloat16):
    entries = deviation * jax.random.normal(rng, extent, jnp.float32)
    if cuts:
        entries = entries * level_of(rng, extent, cuts, -0.22, 0.18)
    return jnp.clip(spiked(entries, jax.random.fold_in(rng, 3), *heavy), -reach, reach).astype(kind)


def setup_inputs(seed: int = 0) -> dict:
    streams_of = jax.random.split(jax.random.key(seed), 14)
    return {
        "text_in": centred(streams_of[0], (MB, ITEMS, SEGS, TEXT, D), 1.0, 6.0, ((1, 32),)),
        "memory_in": centred(streams_of[1], (MB, ITEMS, MEM, D), 1.0, 6.0, ((1, 32),)),
        "counts": set_ends(jax.random.randint(streams_of[2], (MB, ITEMS), 2, SEGS + 1), jax.random.fold_in(streams_of[2], 1), 2, SEGS).astype(jnp.int32),
        "last_len": set_ends(jax.random.randint(streams_of[3], (MB, ITEMS), 1, TEXT + 1), jax.random.fold_in(streams_of[3], 1), 1, TEXT).astype(jnp.int32),
        "cot_text": noise_with(streams_of[4], (MB, ITEMS, SEGS, TEXT, D), 1.0, 6.0, ((1, 32),), (1, 4, 32, 2.75)),
        "cot_memory": centred(streams_of[5], (MB, ITEMS, MEM, D), 1.0, 6.0, ((1, 32),)),
        "qkv_weight": centred(streams_of[6], (LAYERS, 3, D, D), D ** -0.5, 0.21875, ((2, 8), (3, 4))),
        "out_weight": centred(streams_of[7], (LAYERS, D, D), (D // 16) ** -0.5, 0.875, ((1, 8), (2, 4))),
        "up_weight": centred(streams_of[8], (LAYERS, D, FF), D ** -0.5, 0.21875, ((1, 8), (2, 4))),
        "down_weight": centred(streams_of[9], (LAYERS, FF, D), FF ** -0.5, 0.109375, ((1, 8), (2, 4))),
        "biases": centred(streams_of[10], (LAYERS, 4, D), 0.5, 3.0, ((1, 4), (2, 8))),
        "up_bias": centred(streams_of[11], (LAYERS, FF), 0.5, 3.0, ((1, 32),)),
        "norm_params": draw_norm_params(jax.random.fold_in(streams_of[13], 71), 0),
    }


highest = lax.Precision.HIGHEST
eps = 1e-12

@jax.custom_vjp
def low(v):
    return lax.optimization_barrier(v.astype(jnp.bfloat16)).astype(jnp.float32)

@jax.custom_vjp
def low_back(v):
    return v

def low_keep(v):
    return (low(v), None)

def low_pass(kept, grad):
    return (grad,)

def back_keep(v):
    return (v, None)

def back_low(kept, grad):
    return (low(grad),)
low.defvjp(low_keep, low_pass)
low_back.defvjp(back_keep, back_low)

def norm_rows(stream, norm_gain, norm_shift):
    center = stream - lax.optimization_barrier(jnp.mean(stream, axis=-1, keepdims=True))
    spread = lax.optimization_barrier(jnp.mean(center * center, axis=-1, keepdims=True))
    return center * lax.rsqrt(spread + eps) * norm_gain + norm_shift

def layer_step(stream, key_valid, weights):
    triple, output_w, expand_w, reduce_w, shifts, inner_b, norm_gains = weights
    group_size, seg_rows, model_width = stream.shape
    rows_low = low(stream)

    def project(matrix, offset):
        return low(low_back(jnp.einsum('gsd,de->gse', rows_low, matrix, precision=highest) + offset))
    query_rows = project(triple[0], shifts[0])
    key_rows = project(triple[1], jnp.zeros((model_width,), jnp.float32))
    value_rows = project(triple[2], shifts[1])
    head_shape = (group_size, seg_rows, HEADS, HD)
    scores = jnp.einsum('gqhd,gkhd->ghqk', query_rows.reshape(head_shape), key_rows.reshape(head_shape), precision=highest) * HD ** (-0.5)
    scores = low_back(scores)
    scores = jnp.where(key_valid[:, None, None, :], scores, -1e+30)
    attn_probs = jax.nn.softmax(scores, axis=-1)
    context = jnp.einsum('ghqk,gkhd->gqhd', low(attn_probs), value_rows.reshape(head_shape), precision=highest)
    context = low(low_back(context.reshape(group_size, seg_rows, model_width)))
    attn_out = low_back(jnp.einsum('gsd,de->gse', context, output_w, precision=highest) + shifts[2])
    normed = norm_rows(stream + attn_out, norm_gains[0], norm_gains[1])
    inner_pre = low_back(jnp.einsum('gsd,df->gsf', low(normed), expand_w, precision=highest) + inner_b)
    hidden = low(jax.nn.gelu(inner_pre, approximate=False))
    ffn_out = low_back(jnp.einsum('gsf,fd->gsd', hidden, reduce_w, precision=highest) + shifts[3])
    return norm_rows(normed + ffn_out, norm_gains[2], norm_gains[3])

def run_group(text_group, memory_group, count_group, length_group, weights):
    positions = jnp.arange(TEXT, dtype=jnp.int32)
    memory_ones = jnp.ones((count_group.shape[0], MEM), dtype=jnp.bool_)

    def seg_step(memory, inputs):
        text_seg, seg_index = inputs
        whole_seg = seg_index < count_group - 1
        last_seg = seg_index == count_group - 1
        text_valid = whole_seg[:, None] | last_seg[:, None] & (positions[None, :] < length_group[:, None])
        active = seg_index < count_group
        key_valid = jnp.concatenate([memory_ones, text_valid, memory_ones], axis=1)
        stream = jnp.concatenate([memory, text_seg, memory], axis=1)
        for layer_index in range(LAYERS):
            layer_weights = tuple((w[layer_index] for w in weights))
            stream = layer_step(stream, key_valid, layer_weights)
        text_result = jnp.where(text_valid[:, :, None], stream[:, MEM:MEM + TEXT], jnp.zeros((), jnp.float32))
        memory_next = jnp.where(active[:, None, None], stream[:, MEM + TEXT:], memory)
        return (memory_next, text_result)
    seg_ids = jnp.arange(SEGS, dtype=jnp.int32)
    memory_end, text_results = lax.scan(seg_step, memory_group, (jnp.moveaxis(text_group, 1, 0), seg_ids))
    return (jnp.moveaxis(text_results, 0, 1), memory_end)

def reference(text_in, memory_in, counts, last_len, cot_text, cot_memory, qkv_weight, out_weight, up_weight, down_weight, biases, up_bias, norm_params):
    seg_rows = TEXT + 2 * MEM
    total_items = MB * ITEMS
    group_size = math.gcd(total_items, max(1, 4096 // (SEGS * seg_rows)))
    group_count = total_items // group_size

    def regroup(array):
        return array.reshape((group_count, group_size) + array.shape[2:])
    count_groups = regroup(counts)
    length_groups = regroup(last_len)
    checked = jax.checkpoint(run_group)

    def forward(text_all, memory_all, weights):

        def scan_body(carry, inputs):
            text_group, memory_group, count_group, length_group = inputs
            return (carry, checked(text_group, memory_group, count_group, length_group, weights))
        start = jnp.zeros((), jnp.float32)
        _, (text_results, memory_results) = lax.scan(scan_body, start, (regroup(text_all), regroup(memory_all), count_groups, length_groups))
        return (text_results.reshape(text_all.shape), memory_results.reshape(memory_all.shape))
    weights = (qkv_weight.astype(jnp.float32), out_weight.astype(jnp.float32), up_weight.astype(jnp.float32), down_weight.astype(jnp.float32), biases.astype(jnp.float32), up_bias.astype(jnp.float32), norm_params.astype(jnp.float32))
    primal, pullback = jax.vjp(forward, text_in.astype(jnp.float32), memory_in.astype(jnp.float32), weights)
    text_grad, memory_grad, weight_grads = pullback((cot_text.astype(jnp.float32), cot_memory.astype(jnp.float32)))
    return (primal[0].astype(jnp.bfloat16), primal[1].astype(jnp.bfloat16), text_grad.astype(jnp.bfloat16), memory_grad.astype(jnp.bfloat16), weight_grads[0], weight_grads[1], weight_grads[2], weight_grads[3], weight_grads[4], weight_grads[5], weight_grads[6])
```

```python
import functools

import jax
import jax.numpy as jnp
from jax import lax
from jax.experimental import pallas as pl
from jax.experimental.pallas import tpu as pltpu
from jax.sharding import PartitionSpec as P

HEADS = 12
HD = 64
MEM = 10
TEXT = 108
SEGS = 4
MB = 2
LAYERS = 2
SEG = TEXT + 2 * MEM
TAIL = 104
ROWS = MB * SEG
EPS = 1e-12
BF = jnp.bfloat16
F32 = jnp.float32
NEG = -1e30
RSQRT2 = 0.7071067811865476
RSQRT2PI = 0.3989422804014327
VMEM_LIMIT = 66_000_000
FT = 512


def dot(a, b):
    return lax.dot_general(a, b, (((1,), (0,)), ((), ())), preferred_element_type=F32)


def dot_rt(a, b):
    return lax.dot_general(a, b, (((1,), (1,)), ((), ())), preferred_element_type=F32)


def dot_lt(a, b):
    return lax.dot_general(a, b, (((0,), (0,)), ((), ())), preferred_element_type=F32)


def row_ids(shape):
    return lax.broadcasted_iota(jnp.int32, shape, 0)


def lane_ids(shape):
    return lax.broadcasted_iota(jnp.int32, shape, 1)


def valid_rows(seg, count, length):
    return jnp.where(seg < count - 1, TEXT, jnp.where(seg == count - 1, length, 0))


def colsum(v):
    rows, cols = v.shape
    return jnp.sum(v.reshape(rows // 8, 8, cols), axis=0)


def fwd_kernel(
    counts, lens, text, mem0, wqkv, wo, wup, wdn, bias, ubias, norm,
    text_out, mem_out, a_out, qkv_out, p_out, c_out, y_out, g_out, gp_out, xh1_out, xh2_out, rs_out,
    x_ref, mem_ref, y_ref, acc_ref,
):
    seg = pl.program_id(0)
    layer = pl.program_id(1)
    d = x_ref.shape[-1]

    @pl.when((seg == 0) & (layer == 0))
    def _():
        mem_ref[...] = mem0[...]

    @pl.when(layer == 0)
    def _():
        for i in range(MB):
            x_ref[i * SEG : i * SEG + TEXT, :] = text[i, 0].astype(F32)
            tail = slice(i * SEG + TAIL, (i + 1) * SEG)
            now = x_ref[tail, :]
            x_ref[tail, :] = jnp.where(row_ids(now.shape) < TEXT - TAIL, now, mem_ref[i])

    xb = x_ref[...].astype(BF)
    a_out[0] = xb
    qkv_out[0, :, 0:d] = (dot(xb, wqkv[layer, 0]) + bias[layer, 0:1, :]).astype(BF)
    qkv_out[0, :, d : 2 * d] = dot(xb, wqkv[layer, 1]).astype(BF)
    qkv_out[0, :, 2 * d : 3 * d] = (dot(xb, wqkv[layer, 2]) + bias[layer, 1:2, :]).astype(BF)

    low_half = lane_ids((SEG, 128)) < HD
    lanes = lane_ids((1, SEG))
    for i in range(MB):
        vr = valid_rows(seg, counts[i], lens[i])
        keep = (lanes < vr) | (lanes >= TEXT)
        r0 = i * SEG
        for pair in range(HEADS // 2):
            c0 = pair * 128
            q = qkv_out[0, r0 : r0 + SEG, c0 : c0 + 128]
            k = qkv_out[0, r0 : r0 + SEG, d + c0 : d + c0 + 128]
            v = qkv_out[0, r0 : r0 + SEG, 2 * d + c0 : 2 * d + c0 + 128]
            zero = jnp.zeros_like(q)
            q2 = jnp.concatenate([jnp.where(low_half, q, zero), jnp.where(low_half, zero, q)], axis=0)
            s = dot_rt(q2, k) * (HD ** -0.5)
            s = jnp.where(keep, s, NEG)
            e = jnp.exp(s - jnp.max(s, axis=-1, keepdims=True))
            p = (e / jnp.sum(e, axis=-1, keepdims=True)).astype(BF)
            u0 = (i * (HEADS // 2) + pair) * 2 * SEG
            p_out[0, u0 : u0 + 2 * SEG, :] = p
            c2 = dot(p, v)
            c_out[0, r0 : r0 + SEG, c0 : c0 + 128] = jnp.where(low_half, c2[:SEG], c2[SEG:]).astype(BF)

    def norm_to(h, gain, shift, xh_out, rs_index):
        center = h - jnp.mean(h, axis=-1, keepdims=True)
        rs = lax.rsqrt(jnp.mean(center * center, axis=-1, keepdims=True) + EPS)
        xh = center * rs
        xh_out[0] = xh
        rs_out[0, rs_index] = jnp.broadcast_to(rs, (ROWS, 128))
        return xh * gain + shift

    h1 = x_ref[...] + (dot(c_out[0], wo[layer]) + bias[layer, 2:3, :])
    y = norm_to(h1, norm[layer, 0:1, :], norm[layer, 1:2, :], xh1_out, 0)
    y_ref[...] = y
    y_out[0] = y.astype(BF)

    acc_ref[...] = jnp.zeros_like(acc_ref)
    ff = wup.shape[-1]

    def ffn_step(j, carry):
        cols = pl.ds(pl.multiple_of(j * FT, FT), FT)
        u = dot(y_out[0], wup[layer, :, cols]) + ubias[layer, :, cols]
        cdf = 0.5 * (1.0 + lax.erf(u * RSQRT2))
        g = (u * cdf).astype(BF)
        g_out[0, :, cols] = g
        gp_out[0, :, cols] = (cdf + u * (jnp.exp(-0.5 * (u * u)) * RSQRT2PI)).astype(BF)
        acc_ref[...] += dot(g, wdn[layer, cols, :])
        return carry

    lax.fori_loop(0, ff // FT, ffn_step, 0)
    h2 = y_ref[...] + (acc_ref[...] + bias[layer, 3:4, :])
    x_ref[...] = norm_to(h2, norm[layer, 2:3, :], norm[layer, 3:4, :], xh2_out, 1)

    @pl.when(layer == LAYERS - 1)
    def _():
        for i in range(MB):
            vr = valid_rows(seg, counts[i], lens[i])
            body = x_ref[i * SEG : i * SEG + TEXT, :]
            text_out[i, 0] = jnp.where(row_ids(body.shape) < vr, body, 0.0).astype(BF)
            tail = x_ref[i * SEG + TAIL : (i + 1) * SEG, :]
            both = jnp.where(row_ids(tail.shape) >= TEXT - TAIL + MEM, tail, pltpu.roll(tail, SEG - TAIL - MEM, axis=0))
            mem_ref[i] = jnp.where(seg < counts[i], both, mem_ref[i])
        mem_out[...] = mem_ref[...]


def whole(shape):
    return pl.BlockSpec(shape, lambda *_: (0,) * len(shape), pipeline_mode=pl.Buffered(1))


def saved(rows, cols):
    return pl.BlockSpec((1, rows, cols), lambda s, l: (l, s, 0))


def forward_local(text, mem, counts, lens, weights):
    wqkv, wo, wup, wdn, bias, ubias, norm = weights
    d, ff = wup.shape[1:]
    mem0 = jnp.concatenate([jnp.zeros((MB, TEXT - TAIL, d), F32), mem.astype(F32), mem.astype(F32)], axis=1)
    total = SEGS * ROWS
    units = MB * HEADS * SEG
    smem = pl.BlockSpec(memory_space=pltpu.SMEM)
    outs = pl.pallas_call(
        fwd_kernel,
        grid=(SEGS, LAYERS),
        in_specs=[
            smem, smem,
            pl.BlockSpec((MB, 1, TEXT, d), lambda s, l: (0, s, 0, 0)),
            whole(mem0.shape), whole(wqkv.shape), whole(wo.shape), whole(wup.shape), whole(wdn.shape),
            whole(bias.shape), whole((LAYERS, 1, ff)), whole(norm.shape),
        ],
        out_specs=[
            pl.BlockSpec((MB, 1, TEXT, d), lambda s, l: (0, s, 0, 0)),
            whole(mem0.shape),
            saved(ROWS, d), saved(ROWS, 3 * d), saved(units, 128), saved(ROWS, d), saved(ROWS, d),
            saved(ROWS, ff), saved(ROWS, ff), saved(ROWS, d), saved(ROWS, d),
            pl.BlockSpec((1, 2, ROWS, 128), lambda s, l: (l, 0, s, 0)),
        ],
        out_shape=[
            jax.ShapeDtypeStruct((MB, SEGS, TEXT, d), BF),
            jax.ShapeDtypeStruct(mem0.shape, F32),
            jax.ShapeDtypeStruct((LAYERS, total, d), BF),
            jax.ShapeDtypeStruct((LAYERS, total, 3 * d), BF),
            jax.ShapeDtypeStruct((LAYERS, SEGS * units, 128), BF),
            jax.ShapeDtypeStruct((LAYERS, total, d), BF),
            jax.ShapeDtypeStruct((LAYERS, total, d), BF),
            jax.ShapeDtypeStruct((LAYERS, total, ff), BF),
            jax.ShapeDtypeStruct((LAYERS, total, ff), BF),
            jax.ShapeDtypeStruct((LAYERS, total, d), F32),
            jax.ShapeDtypeStruct((LAYERS, total, d), F32),
            jax.ShapeDtypeStruct((LAYERS, 2, total, 128), F32),
        ],
        scratch_shapes=[
            pltpu.VMEM((ROWS, d), F32), pltpu.VMEM(mem0.shape, F32),
            pltpu.VMEM((ROWS, d), F32), pltpu.VMEM((ROWS, d), F32),
        ],
        compiler_params=pltpu.CompilerParams(
            dimension_semantics=("arbitrary", "arbitrary"), vmem_limit_bytes=VMEM_LIMIT
        ),
        name="rmt_forward",
    )(counts, lens, text, mem0, wqkv, wo, wup, wdn, bias.astype(F32), ubias.astype(F32)[:, None, :], norm.astype(F32))
    text_out, mem_end = outs[:2]
    return text_out, mem_end[:, TEXT - TAIL + MEM :].astype(BF), outs[2:]


def bwd_kernel(
    counts, lens, cot, gm0, qkv, p_in, gp_in, xh1_in, xh2_in, rs_in, wqkv, wo, wup, wdn, norm,
    tg_out, gm_out, dqkv_out, dao_out, du_out, df_out, gb_out, gub_out, gn_out,
    g_ref, gm_ref, t_ref, acc_ref, dc_ref,
):
    seg = SEGS - 1 - pl.program_id(0)
    step = pl.program_id(1)
    layer = LAYERS - 1 - step
    d = g_ref.shape[-1]

    @pl.when((seg == SEGS - 1) & (step == 0))
    def _():
        gm_ref[...] = gm0[...]
        gb_out[...] = jnp.zeros_like(gb_out)
        gub_out[...] = jnp.zeros_like(gub_out)
        gn_out[...] = jnp.zeros_like(gn_out)

    @pl.when(step == 0)
    def _():
        for i in range(MB):
            vr = valid_rows(seg, counts[i], lens[i])
            ct = cot[i, 0].astype(F32)
            g_ref[i * SEG : i * SEG + TEXT, :] = jnp.where(row_ids(ct.shape) < vr, ct, 0.0)
            tail = slice(i * SEG + TAIL, (i + 1) * SEG)
            now = g_ref[tail, :]
            rows = row_ids(now.shape)
            mem_part = jnp.where((rows >= TEXT - TAIL + MEM) & (seg < counts[i]), gm_ref[i], 0.0)
            g_ref[tail, :] = jnp.where(rows < TEXT - TAIL, now, mem_part)

    def norm_back(gout, xh, rs, gain, slot):
        gn_out[layer, slot] += colsum(gout * xh)
        gn_out[layer, slot + 1] += colsum(gout)
        t = gout * gain
        return rs * (t - jnp.mean(t, axis=-1, keepdims=True) - xh * jnp.mean(t * xh, axis=-1, keepdims=True))

    dh2 = norm_back(g_ref[...], xh2_in[0], rs_in[0, 1][:, :1], norm[layer, 2:3, :], 2)
    t_ref[...] = dh2
    df = dh2.astype(BF)
    df_out[0] = df
    gb_out[layer, 3] += colsum(df.astype(F32))
    acc_ref[...] = jnp.zeros_like(acc_ref)
    ff = wup.shape[-1]

    def ffn_step(j, carry):
        cols = pl.ds(pl.multiple_of(j * FT, FT), FT)
        dg = dot_rt(df_out[0], wdn[layer, cols, :])
        du = (dg * gp_in[0, :, cols].astype(F32)).astype(BF)
        du_out[0, :, cols] = du
        gub_out[layer, :, cols] += colsum(du.astype(F32))
        acc_ref[...] += dot_rt(du, wup[layer, :, cols])
        return carry

    lax.fori_loop(0, ff // FT, ffn_step, 0)
    dh1 = norm_back(t_ref[...] + acc_ref[...], xh1_in[0], rs_in[0, 0][:, :1], norm[layer, 0:1, :], 0)
    t_ref[...] = dh1
    dao = dh1.astype(BF)
    dao_out[0] = dao
    gb_out[layer, 2] += colsum(dao.astype(F32))
    dc_ref[...] = dot_rt(dao, wo[layer]).astype(BF)

    low_half = lane_ids((SEG, 128)) < HD
    scale = HD ** -0.5
    for i in range(MB):
        r0 = i * SEG
        for pair in range(HEADS // 2):
            c0 = pair * 128
            q = qkv[0, r0 : r0 + SEG, c0 : c0 + 128]
            k = qkv[0, r0 : r0 + SEG, d + c0 : d + c0 + 128]
            v = qkv[0, r0 : r0 + SEG, 2 * d + c0 : 2 * d + c0 + 128]
            dc = dc_ref[r0 : r0 + SEG, c0 : c0 + 128]
            zero = jnp.zeros_like(q)
            q2 = jnp.concatenate([jnp.where(low_half, q, zero), jnp.where(low_half, zero, q)], axis=0)
            dc2 = jnp.concatenate([jnp.where(low_half, dc, zero), jnp.where(low_half, zero, dc)], axis=0)
            u0 = (i * (HEADS // 2) + pair) * 2 * SEG
            pb = p_in[0, u0 : u0 + 2 * SEG, :]
            p = pb.astype(F32)
            pdp = p * dot_rt(dc2, v)
            ds = (pdp - p * jnp.sum(pdp, axis=-1, keepdims=True)).astype(BF)
            dq2 = dot(ds, k)
            dq = (jnp.where(low_half, dq2[:SEG], dq2[SEG:]) * scale).astype(BF)
            dk = (dot_lt(ds, q2) * scale).astype(BF)
            dv = dot_lt(pb, dc2).astype(BF)
            dqkv_out[0, r0 : r0 + SEG, c0 : c0 + 128] = dq
            dqkv_out[0, r0 : r0 + SEG, d + c0 : d + c0 + 128] = dk
            dqkv_out[0, r0 : r0 + SEG, 2 * d + c0 : 2 * d + c0 + 128] = dv

    gb_out[layer, 0] += colsum(dqkv_out[0, :, 0:d].astype(F32))
    gb_out[layer, 1] += colsum(dqkv_out[0, :, 2 * d : 3 * d].astype(F32))
    g_ref[...] = (
        t_ref[...]
        + dot_rt(dqkv_out[0, :, 0:d], wqkv[layer, 0])
        + dot_rt(dqkv_out[0, :, d : 2 * d], wqkv[layer, 1])
        + dot_rt(dqkv_out[0, :, 2 * d : 3 * d], wqkv[layer, 2])
    )

    @pl.when(layer == 0)
    def _():
        for i in range(MB):
            tg_out[i, 0] = g_ref[i * SEG : i * SEG + TEXT, :].astype(BF)
            tail = g_ref[i * SEG + TAIL : (i + 1) * SEG, :]
            back = tail + pltpu.roll(tail, MEM, axis=0)
            gm_ref[i] = jnp.where(seg < counts[i], 0.0, gm_ref[i]) + back
        gm_out[...] = gm_ref[...]


def backward_local(cot, cot_mem, counts, lens, kept, weights):
    wqkv, wo, wup, wdn, _, _, norm = weights
    _, qkv, p_all, _, _, _, gp, xh1, xh2, rs = kept
    d, ff = wup.shape[1:]
    gm0 = jnp.concatenate([jnp.zeros((MB, TEXT - TAIL + MEM, d), F32), cot_mem.astype(F32)], axis=1)
    total = SEGS * ROWS
    units = MB * HEADS * SEG
    smem = pl.BlockSpec(memory_space=pltpu.SMEM)

    def kept_spec(rows, cols):
        return pl.BlockSpec((1, rows, cols), lambda s, l: (LAYERS - 1 - l, SEGS - 1 - s, 0))

    outs = pl.pallas_call(
        bwd_kernel,
        grid=(SEGS, LAYERS),
        in_specs=[
            smem, smem,
            pl.BlockSpec((MB, 1, TEXT, d), lambda s, l: (0, SEGS - 1 - s, 0, 0)),
            whole(gm0.shape),
            kept_spec(ROWS, 3 * d), kept_spec(units, 128), kept_spec(ROWS, ff), kept_spec(ROWS, d), kept_spec(ROWS, d),
            pl.BlockSpec((1, 2, ROWS, 128), lambda s, l: (LAYERS - 1 - l, 0, SEGS - 1 - s, 0)),
            whole(wqkv.shape), whole(wo.shape), whole(wup.shape), whole(wdn.shape), whole(norm.shape),
        ],
        out_specs=[
            pl.BlockSpec((MB, 1, TEXT, d), lambda s, l: (0, SEGS - 1 - s, 0, 0)),
            whole(gm0.shape),
            kept_spec(ROWS, 3 * d), kept_spec(ROWS, d), kept_spec(ROWS, ff), kept_spec(ROWS, d),
            whole((LAYERS, 4, 8, d)), whole((LAYERS, 8, ff)), whole((LAYERS, 4, 8, d)),
        ],
        out_shape=[
            jax.ShapeDtypeStruct((MB, SEGS, TEXT, d), BF),
            jax.ShapeDtypeStruct(gm0.shape, F32),
            jax.ShapeDtypeStruct((LAYERS, total, 3 * d), BF),
            jax.ShapeDtypeStruct((LAYERS, total, d), BF),
            jax.ShapeDtypeStruct((LAYERS, total, ff), BF),
            jax.ShapeDtypeStruct((LAYERS, total, d), BF),
            jax.ShapeDtypeStruct((LAYERS, 4, 8, d), F32),
            jax.ShapeDtypeStruct((LAYERS, 8, ff), F32),
            jax.ShapeDtypeStruct((LAYERS, 4, 8, d), F32),
        ],
        scratch_shapes=[
            pltpu.VMEM((ROWS, d), F32), pltpu.VMEM(gm0.shape, F32),
            pltpu.VMEM((ROWS, d), F32), pltpu.VMEM((ROWS, d), F32), pltpu.VMEM((ROWS, d), BF),
        ],
        compiler_params=pltpu.CompilerParams(
            dimension_semantics=("arbitrary", "arbitrary"), vmem_limit_bytes=VMEM_LIMIT
        ),
        name="rmt_backward",
    )(counts, lens, cot, gm0, qkv, p_all, gp, xh1, xh2, rs, wqkv, wo, wup, wdn, norm.astype(F32))
    tg, gm = outs[:2]
    small = (outs[6].sum(axis=2), outs[7].sum(axis=1), outs[8].sum(axis=2))
    return tg, gm[:, TEXT - TAIL + MEM :].astype(BF), outs[2:6], small


def weight_grads(kept, grads):
    a, _, _, c, y, g = kept[:6]
    dqkv, dao, du, df = grads
    d = a.shape[-1]

    def per_layer(lhs, rhs):
        return jnp.stack([dot_lt(lhs[l], rhs[l]).astype(BF) for l in range(LAYERS)])

    gq = jnp.stack([
        jnp.stack([dot_lt(a[l], dqkv[l, :, j * d : (j + 1) * d]).astype(BF) for j in range(3)]) for l in range(LAYERS)
    ])
    return gq, per_layer(c, dao), per_layer(y, du), per_layer(g, df)


def gather_weights(pieces):
    wqkv, wo, wup, wdn, bias, ubias, norm = pieces
    narrow = [(wqkv, 3), (wo, 2), (wup, 2), (wdn, 2), (bias, 1), (norm, 1)]
    wqkv, wo, wup, wdn, bias, norm = (lax.all_gather(w, "narrow", axis=k, tiled=True) for w, k in narrow)
    wide = [(wqkv, 2), (wo, 1), (wup, 1), (wdn, 1), (bias, 2), (norm, 2)]
    wqkv, wo, wup, wdn, bias, norm = (lax.all_gather(w, "wide", axis=k, tiled=True) for w, k in wide)
    ubias = lax.all_gather(ubias, ("wide", "narrow"), axis=1, tiled=True)
    return wqkv, wo, wup, wdn, bias, ubias, norm


def scatter_two(grad, row_axis, col_axis):
    low = lax.psum_scatter(grad.astype(BF), "narrow", scatter_dimension=col_axis, tiled=True)
    return lax.psum_scatter(low.astype(F32), "wide", scatter_dimension=row_axis, tiled=True)


def scatter_grads(big, small):
    gq, go, gup, gdn = big
    gb, gub, gn = small
    big = (scatter_two(gq, 2, 3), scatter_two(go, 1, 2), scatter_two(gup, 1, 2), scatter_two(gdn, 1, 2))
    gub = lax.psum_scatter(gub, ("wide", "narrow"), scatter_dimension=1, tiled=True)

    def small_two(g):
        return lax.psum_scatter(
            lax.psum_scatter(g, "narrow", scatter_dimension=1, tiled=True), "wide", scatter_dimension=2, tiled=True
        )

    return big + (small_two(gb), gub, small_two(gn))


def shards(
    text_in, memory_in, counts, last_len, cot_text, cot_memory,
    qkv_weight, out_weight, up_weight, down_weight, biases, up_bias, norm_params,
):
    text, cot = text_in[:, 0], cot_text[:, 0]
    mem, cot_mem = memory_in[:, 0], cot_memory[:, 0]
    cnt, lens = counts[:, 0], last_len[:, 0]
    weights = gather_weights((qkv_weight, out_weight, up_weight, down_weight, biases, up_bias, norm_params))
    text_out, mem_out, kept = forward_local(text, mem, cnt, lens, weights)
    text_grad, mem_grad, grads, small = backward_local(cot, cot_mem, cnt, lens, kept, weights)
    grads = scatter_grads(weight_grads(kept, grads), small)
    return (text_out[:, None], mem_out[:, None], text_grad[:, None], mem_grad[:, None]) + grads


def solution(mesh):
    items = ("wide", "narrow")
    act5 = P(None, items, None, None, None)
    act4 = P(None, items, None, None)
    ids = P(None, items)
    split = P(None, "wide", "narrow")
    small = P(None, "narrow", "wide")
    params = (P(None, None, "wide", "narrow"), split, split, split, small, ids, small)
    return jax.shard_map(
        shards,
        mesh=mesh,
        in_specs=(act5, act4, ids, ids, act5, act4) + params,
        out_specs=(act5, act4, act5, act4) + params,
        check_vma=False,
    )
```

```python
import functools

import jax
import jax.numpy as jnp
from jax import lax
from jax.experimental import pallas as pl
from jax.experimental.pallas import tpu as pltpu
from jax.sharding import PartitionSpec as P

HEADS = 12
HD = 64
MEM = 10
TEXT = 108
SEGS = 4
MB = 2
LAYERS = 2
SEG = TEXT + 2 * MEM
TAIL = 104
ROWS = MB * SEG
EPS = 1e-12
BF = jnp.bfloat16
F32 = jnp.float32
NEG = -1e30
RSQRT2 = 0.7071067811865476
RSQRT2PI = 0.3989422804014327
VMEM_LIMIT = 66_000_000
FT = 512


def dot(a, b):
    return lax.dot_general(a, b, (((1,), (0,)), ((), ())), preferred_element_type=F32)


def dot_rt(a, b):
    return lax.dot_general(a, b, (((1,), (1,)), ((), ())), preferred_element_type=F32)


def dot_lt(a, b):
    return lax.dot_general(a, b, (((0,), (0,)), ((), ())), preferred_element_type=F32)


def row_ids(shape):
    return lax.broadcasted_iota(jnp.int32, shape, 0)


def lane_ids(shape):
    return lax.broadcasted_iota(jnp.int32, shape, 1)


def valid_rows(seg, count, length):
    return jnp.where(seg < count - 1, TEXT, jnp.where(seg == count - 1, length, 0))


def colsum(v):
    rows, cols = v.shape
    return jnp.sum(v.reshape(rows // 8, 8, cols), axis=0)


def fwd_kernel(
    counts, lens, text, mem0, wqkv, wo, wup, wdn, bias, ubias, norm,
    text_out, mem_out, a_out, qkv_out, p_out, c_out, y_out, g_out, gp_out, xh1_out, xh2_out, rs_out,
    x_ref, mem_ref, y_ref, acc_ref,
):
    seg = pl.program_id(0)
    layer = pl.program_id(1)
    d = x_ref.shape[-1]

    @pl.when((seg == 0) & (layer == 0))
    def _():
        mem_ref[...] = mem0[...]

    @pl.when(layer == 0)
    def _():
        for i in range(MB):
            x_ref[i * SEG : i * SEG + TEXT, :] = text[i, 0].astype(F32)
            tail = slice(i * SEG + TAIL, (i + 1) * SEG)
            now = x_ref[tail, :]
            x_ref[tail, :] = jnp.where(row_ids(now.shape) < TEXT - TAIL, now, mem_ref[i])

    xb = x_ref[...].astype(BF)
    a_out[0] = xb
    qkv_out[0, :, 0:d] = (dot(xb, wqkv[layer, 0]) + bias[layer, 0:1, :]).astype(BF)
    qkv_out[0, :, d : 2 * d] = dot(xb, wqkv[layer, 1]).astype(BF)
    qkv_out[0, :, 2 * d : 3 * d] = (dot(xb, wqkv[layer, 2]) + bias[layer, 1:2, :]).astype(BF)

    low_half = lane_ids((SEG, 128)) < HD
    lanes = lane_ids((1, SEG))
    for i in range(MB):
        vr = valid_rows(seg, counts[i], lens[i])
        keep = (lanes < vr) | (lanes >= TEXT)
        r0 = i * SEG
        for pair in range(HEADS // 2):
            c0 = pair * 128
            q = qkv_out[0, r0 : r0 + SEG, c0 : c0 + 128]
            k = qkv_out[0, r0 : r0 + SEG, d + c0 : d + c0 + 128]
            v = qkv_out[0, r0 : r0 + SEG, 2 * d + c0 : 2 * d + c0 + 128]
            zero = jnp.zeros_like(q)
            q2 = jnp.concatenate([jnp.where(low_half, q, zero), jnp.where(low_half, zero, q)], axis=0)
            s = dot_rt(q2, k) * (HD ** -0.5)
            s = jnp.where(keep, s, NEG)
            e = jnp.exp(s - jnp.max(s, axis=-1, keepdims=True))
            p = (e / jnp.sum(e, axis=-1, keepdims=True)).astype(BF)
            u0 = (i * (HEADS // 2) + pair) * 2 * SEG
            p_out[0, u0 : u0 + 2 * SEG, :] = p
            c2 = dot(p, v)
            c_out[0, r0 : r0 + SEG, c0 : c0 + 128] = jnp.where(low_half, c2[:SEG], c2[SEG:]).astype(BF)

    def norm_to(h, gain, shift, xh_out, rs_index):
        center = h - jnp.mean(h, axis=-1, keepdims=True)
        rs = lax.rsqrt(jnp.mean(center * center, axis=-1, keepdims=True) + EPS)
        xh = center * rs
        xh_out[0] = xh
        rs_out[0, rs_index] = jnp.broadcast_to(rs, (ROWS, 128))
        return xh * gain + shift

    h1 = x_ref[...] + (dot(c_out[0], wo[layer]) + bias[layer, 2:3, :])
    y = norm_to(h1, norm[layer, 0:1, :], norm[layer, 1:2, :], xh1_out, 0)
    y_ref[...] = y
    y_out[0] = y.astype(BF)

    acc_ref[...] = jnp.zeros_like(acc_ref)
    ff = wup.shape[-1]

    def ffn_step(j, carry):
        cols = pl.ds(pl.multiple_of(j * FT, FT), FT)
        u = dot(y_out[0], wup[layer, :, cols]) + ubias[layer, :, cols]
        cdf = 0.5 * (1.0 + lax.erf(u * RSQRT2))
        g = (u * cdf).astype(BF)
        g_out[0, :, cols] = g
        gp_out[0, :, cols] = (cdf + u * (jnp.exp(-0.5 * (u * u)) * RSQRT2PI)).astype(BF)
        acc_ref[...] += dot(g, wdn[layer, cols, :])
        return carry

    lax.fori_loop(0, ff // FT, ffn_step, 0)
    h2 = y_ref[...] + (acc_ref[...] + bias[layer, 3:4, :])
    x_ref[...] = norm_to(h2, norm[layer, 2:3, :], norm[layer, 3:4, :], xh2_out, 1)

    @pl.when(layer == LAYERS - 1)
    def _():
        for i in range(MB):
            vr = valid_rows(seg, counts[i], lens[i])
            body = x_ref[i * SEG : i * SEG + TEXT, :]
            text_out[i, 0] = jnp.where(row_ids(body.shape) < vr, body, 0.0).astype(BF)
            tail = x_ref[i * SEG + TAIL : (i + 1) * SEG, :]
            both = jnp.where(row_ids(tail.shape) >= TEXT - TAIL + MEM, tail, pltpu.roll(tail, SEG - TAIL - MEM, axis=0))
            mem_ref[i] = jnp.where(seg < counts[i], both, mem_ref[i])
        mem_out[...] = mem_ref[...]


def whole(shape):
    return pl.BlockSpec(shape, lambda *_: (0,) * len(shape), pipeline_mode=pl.Buffered(1))


def saved(rows, cols):
    return pl.BlockSpec((1, rows, cols), lambda s, l: (l, s, 0))


def forward_local(text, mem, counts, lens, weights):
    wqkv, wo, wup, wdn, bias, ubias, norm = weights
    d, ff = wup.shape[1:]
    mem0 = jnp.concatenate([jnp.zeros((MB, TEXT - TAIL, d), F32), mem.astype(F32), mem.astype(F32)], axis=1)
    total = SEGS * ROWS
    units = MB * HEADS * SEG
    smem = pl.BlockSpec(memory_space=pltpu.SMEM)
    outs = pl.pallas_call(
        fwd_kernel,
        grid=(SEGS, LAYERS),
        in_specs=[
            smem, smem,
            pl.BlockSpec((MB, 1, TEXT, d), lambda s, l: (0, s, 0, 0)),
            whole(mem0.shape), whole(wqkv.shape), whole(wo.shape), whole(wup.shape), whole(wdn.shape),
            whole(bias.shape), whole((LAYERS, 1, ff)), whole(norm.shape),
        ],
        out_specs=[
            pl.BlockSpec((MB, 1, TEXT, d), lambda s, l: (0, s, 0, 0)),
            whole(mem0.shape),
            saved(ROWS, d), saved(ROWS, 3 * d), saved(units, 128), saved(ROWS, d), saved(ROWS, d),
            saved(ROWS, ff), saved(ROWS, ff), saved(ROWS, d), saved(ROWS, d),
            pl.BlockSpec((1, 2, ROWS, 128), lambda s, l: (l, 0, s, 0)),
        ],
        out_shape=[
            jax.ShapeDtypeStruct((MB, SEGS, TEXT, d), BF),
            jax.ShapeDtypeStruct(mem0.shape, F32),
            jax.ShapeDtypeStruct((LAYERS, total, d), BF),
            jax.ShapeDtypeStruct((LAYERS, total, 3 * d), BF),
            jax.ShapeDtypeStruct((LAYERS, SEGS * units, 128), BF),
            jax.ShapeDtypeStruct((LAYERS, total, d), BF),
            jax.ShapeDtypeStruct((LAYERS, total, d), BF),
            jax.ShapeDtypeStruct((LAYERS, total, ff), BF),
            jax.ShapeDtypeStruct((LAYERS, total, ff), BF),
            jax.ShapeDtypeStruct((LAYERS, total, d), F32),
            jax.ShapeDtypeStruct((LAYERS, total, d), F32),
            jax.ShapeDtypeStruct((LAYERS, 2, total, 128), F32),
        ],
        scratch_shapes=[
            pltpu.VMEM((ROWS, d), F32), pltpu.VMEM(mem0.shape, F32),
            pltpu.VMEM((ROWS, d), F32), pltpu.VMEM((ROWS, d), F32),
        ],
        compiler_params=pltpu.CompilerParams(
            dimension_semantics=("arbitrary", "arbitrary"), vmem_limit_bytes=VMEM_LIMIT
        ),
        name="rmt_forward",
    )(counts, lens, text, mem0, wqkv, wo, wup, wdn, bias.astype(F32), ubias.astype(F32)[:, None, :], norm.astype(F32))
    text_out, mem_end = outs[:2]
    return text_out, mem_end[:, TEXT - TAIL + MEM :].astype(BF), outs[2:]


def bwd_kernel(
    counts, lens, cot, gm0, qkv, p_in, gp_in, xh1_in, xh2_in, rs_in, wqkv, wo, wup, wdn, norm,
    tg_out, gm_out, dqkv_out, dao_out, du_out, df_out, gb_out, gub_out, gn_out,
    g_ref, gm_ref, t_ref, acc_ref, dc_ref,
):
    seg = SEGS - 1 - pl.program_id(0)
    step = pl.program_id(1)
    layer = LAYERS - 1 - step
    d = g_ref.shape[-1]

    @pl.when((seg == SEGS - 1) & (step == 0))
    def _():
        gm_ref[...] = gm0[...]
        gb_out[...] = jnp.zeros_like(gb_out)
        gub_out[...] = jnp.zeros_like(gub_out)
        gn_out[...] = jnp.zeros_like(gn_out)

    @pl.when(step == 0)
    def _():
        for i in range(MB):
            vr = valid_rows(seg, counts[i], lens[i])
            ct = cot[i, 0].astype(F32)
            g_ref[i * SEG : i * SEG + TEXT, :] = jnp.where(row_ids(ct.shape) < vr, ct, 0.0)
            tail = slice(i * SEG + TAIL, (i + 1) * SEG)
            now = g_ref[tail, :]
            rows = row_ids(now.shape)
            mem_part = jnp.where((rows >= TEXT - TAIL + MEM) & (seg < counts[i]), gm_ref[i], 0.0)
            g_ref[tail, :] = jnp.where(rows < TEXT - TAIL, now, mem_part)

    def norm_back(gout, xh, rs, gain, slot):
        gn_out[layer, slot] += colsum(gout * xh)
        gn_out[layer, slot + 1] += colsum(gout)
        t = gout * gain
        return rs * (t - jnp.mean(t, axis=-1, keepdims=True) - xh * jnp.mean(t * xh, axis=-1, keepdims=True))

    dh2 = norm_back(g_ref[...], xh2_in[0], rs_in[0, 1][:, :1], norm[layer, 2:3, :], 2)
    t_ref[...] = dh2
    df = dh2.astype(BF)
    df_out[0] = df
    gb_out[layer, 3] += colsum(df.astype(F32))
    acc_ref[...] = jnp.zeros_like(acc_ref)
    ff = wup.shape[-1]

    def ffn_step(j, carry):
        cols = pl.ds(pl.multiple_of(j * FT, FT), FT)
        dg = dot_rt(df_out[0], wdn[layer, cols, :])
        du = (dg * gp_in[0, :, cols].astype(F32)).astype(BF)
        du_out[0, :, cols] = du
        gub_out[layer, :, cols] += colsum(du.astype(F32))
        acc_ref[...] += dot_rt(du, wup[layer, :, cols])
        return carry

    lax.fori_loop(0, ff // FT, ffn_step, 0)
    dh1 = norm_back(t_ref[...] + acc_ref[...], xh1_in[0], rs_in[0, 0][:, :1], norm[layer, 0:1, :], 0)
    t_ref[...] = dh1
    dao = dh1.astype(BF)
    dao_out[0] = dao
    gb_out[layer, 2] += colsum(dao.astype(F32))
    dc_ref[...] = dot_rt(dao, wo[layer]).astype(BF)

    low_half = lane_ids((SEG, 128)) < HD
    scale = HD ** -0.5
    for i in range(MB):
        r0 = i * SEG
        for pair in range(HEADS // 2):
            c0 = pair * 128
            q = qkv[0, r0 : r0 + SEG, c0 : c0 + 128]
            k = qkv[0, r0 : r0 + SEG, d + c0 : d + c0 + 128]
            v = qkv[0, r0 : r0 + SEG, 2 * d + c0 : 2 * d + c0 + 128]
            dc = dc_ref[r0 : r0 + SEG, c0 : c0 + 128]
            zero = jnp.zeros_like(q)
            q2 = jnp.concatenate([jnp.where(low_half, q, zero), jnp.where(low_half, zero, q)], axis=0)
            dc2 = jnp.concatenate([jnp.where(low_half, dc, zero), jnp.where(low_half, zero, dc)], axis=0)
            u0 = (i * (HEADS // 2) + pair) * 2 * SEG
            pb = p_in[0, u0 : u0 + 2 * SEG, :]
            p = pb.astype(F32)
            pdp = p * dot_rt(dc2, v)
            ds = (pdp - p * jnp.sum(pdp, axis=-1, keepdims=True)).astype(BF)
            dq2 = dot(ds, k)
            dq = (jnp.where(low_half, dq2[:SEG], dq2[SEG:]) * scale).astype(BF)
            dk = (dot_lt(ds, q2) * scale).astype(BF)
            dv = dot_lt(pb, dc2).astype(BF)
            dqkv_out[0, r0 : r0 + SEG, c0 : c0 + 128] = dq
            dqkv_out[0, r0 : r0 + SEG, d + c0 : d + c0 + 128] = dk
            dqkv_out[0, r0 : r0 + SEG, 2 * d + c0 : 2 * d + c0 + 128] = dv

    gb_out[layer, 0] += colsum(dqkv_out[0, :, 0:d].astype(F32))
    gb_out[layer, 1] += colsum(dqkv_out[0, :, 2 * d : 3 * d].astype(F32))
    g_ref[...] = (
        t_ref[...]
        + dot_rt(dqkv_out[0, :, 0:d], wqkv[layer, 0])
        + dot_rt(dqkv_out[0, :, d : 2 * d], wqkv[layer, 1])
        + dot_rt(dqkv_out[0, :, 2 * d : 3 * d], wqkv[layer, 2])
    )

    @pl.when(layer == 0)
    def _():
        for i in range(MB):
            tg_out[i, 0] = g_ref[i * SEG : i * SEG + TEXT, :].astype(BF)
            tail = g_ref[i * SEG + TAIL : (i + 1) * SEG, :]
            back = tail + pltpu.roll(tail, MEM, axis=0)
            gm_ref[i] = jnp.where(seg < counts[i], 0.0, gm_ref[i]) + back
        gm_out[...] = gm_ref[...]


def backward_local(cot, cot_mem, counts, lens, kept, weights):
    wqkv, wo, wup, wdn, _, _, norm = weights
    _, qkv, p_all, _, _, _, gp, xh1, xh2, rs = kept
    d, ff = wup.shape[1:]
    gm0 = jnp.concatenate([jnp.zeros((MB, TEXT - TAIL + MEM, d), F32), cot_mem.astype(F32)], axis=1)
    total = SEGS * ROWS
    units = MB * HEADS * SEG
    smem = pl.BlockSpec(memory_space=pltpu.SMEM)

    def kept_spec(rows, cols):
        return pl.BlockSpec((1, rows, cols), lambda s, l: (LAYERS - 1 - l, SEGS - 1 - s, 0))

    outs = pl.pallas_call(
        bwd_kernel,
        grid=(SEGS, LAYERS),
        in_specs=[
            smem, smem,
            pl.BlockSpec((MB, 1, TEXT, d), lambda s, l: (0, SEGS - 1 - s, 0, 0)),
            whole(gm0.shape),
            kept_spec(ROWS, 3 * d), kept_spec(units, 128), kept_spec(ROWS, ff), kept_spec(ROWS, d), kept_spec(ROWS, d),
            pl.BlockSpec((1, 2, ROWS, 128), lambda s, l: (LAYERS - 1 - l, 0, SEGS - 1 - s, 0)),
            whole(wqkv.shape), whole(wo.shape), whole(wup.shape), whole(wdn.shape), whole(norm.shape),
        ],
        out_specs=[
            pl.BlockSpec((MB, 1, TEXT, d), lambda s, l: (0, SEGS - 1 - s, 0, 0)),
            whole(gm0.shape),
            kept_spec(ROWS, 3 * d), kept_spec(ROWS, d), kept_spec(ROWS, ff), kept_spec(ROWS, d),
            whole((LAYERS, 4, 8, d)), whole((LAYERS, 8, ff)), whole((LAYERS, 4, 8, d)),
        ],
        out_shape=[
            jax.ShapeDtypeStruct((MB, SEGS, TEXT, d), BF),
            jax.ShapeDtypeStruct(gm0.shape, F32),
            jax.ShapeDtypeStruct((LAYERS, total, 3 * d), BF),
            jax.ShapeDtypeStruct((LAYERS, total, d), BF),
            jax.ShapeDtypeStruct((LAYERS, total, ff), BF),
            jax.ShapeDtypeStruct((LAYERS, total, d), BF),
            jax.ShapeDtypeStruct((LAYERS, 4, 8, d), F32),
            jax.ShapeDtypeStruct((LAYERS, 8, ff), F32),
            jax.ShapeDtypeStruct((LAYERS, 4, 8, d), F32),
        ],
        scratch_shapes=[
            pltpu.VMEM((ROWS, d), F32), pltpu.VMEM(gm0.shape, F32),
            pltpu.VMEM((ROWS, d), F32), pltpu.VMEM((ROWS, d), F32), pltpu.VMEM((ROWS, d), BF),
        ],
        compiler_params=pltpu.CompilerParams(
            dimension_semantics=("arbitrary", "arbitrary"), vmem_limit_bytes=VMEM_LIMIT
        ),
        name="rmt_backward",
    )(counts, lens, cot, gm0, qkv, p_all, gp, xh1, xh2, rs, wqkv, wo, wup, wdn, norm.astype(F32))
    tg, gm = outs[:2]
    small = (outs[6].sum(axis=2), outs[7].sum(axis=1), outs[8].sum(axis=2))
    return tg, gm[:, TEXT - TAIL + MEM :].astype(BF), outs[2:6], small


def weight_grads(kept, grads):
    a, _, _, c, y, g = kept[:6]
    dqkv, dao, du, df = grads

    def product(lhs, rhs):
        dims = (((1,), (1,)), ((0,), (0,)))
        return lax.dot_general(lhs, rhs, dims, preferred_element_type=F32).astype(BF)

    return product(a, dqkv), product(c, dao), product(y, du), product(g, df)


MESH = pl.DeviceIdType.MESH
ZN = 4


def multiple(v, k):
    return v if isinstance(v, int) else pl.multiple_of(v, k)


def span(start, size):
    return pl.ds(multiple(start, size if size % 128 else 128), size)


def where_am_i():
    w, n = lax.axis_index("wide"), lax.axis_index("narrow")
    z, x = lax.div(w, 2), lax.rem(w, 2)
    y, c = lax.div(n, 2), lax.rem(n, 2)
    links = {
        "p": {"wide": w, "narrow": n + 1 - 2 * c},
        "x": {"wide": w + 1 - 2 * x, "narrow": n},
        "y": {"wide": w, "narrow": lax.rem(n + 2, 4)},
        "up": {"wide": w + 2, "narrow": n},
        "down": {"wide": w - 2, "narrow": n},
    }
    return w, n, z, x, y, c, links


def enter(z, links):
    barrier = pltpu.get_barrier_semaphore()
    for name in ("p", "x", "y"):
        pl.semaphore_signal(barrier, inc=1, device_id=links[name], device_id_type=MESH)

    @pl.when(z < ZN - 1)
    def _():
        pl.semaphore_signal(barrier, inc=1, device_id=links["up"], device_id_type=MESH)

    @pl.when(z > 0)
    def _():
        pl.semaphore_signal(barrier, inc=1, device_id=links["down"], device_id_type=MESH)

    pl.semaphore_wait(barrier, 3 + jnp.minimum(z, 1) + jnp.minimum(ZN - 1 - z, 1))


class Net:
    def __init__(self, ssem, rsem, links):
        self.ssem, self.rsem, self.links = ssem, rsem, links
        self.next_send, self.next_recv = 0, 0

    def sends(self, count):
        base, self.next_send = self.next_send, self.next_send + count
        return base

    def recvs(self, count):
        base, self.next_recv = self.next_recv, self.next_recv + count
        return base

    def copy(self, link, src, dst, s, r):
        return pltpu.make_async_remote_copy(
            src_ref=src, dst_ref=dst, send_sem=self.ssem.at[s], recv_sem=self.rsem.at[r],
            device_id=self.links[link], device_id_type=MESH,
        )


def gather_kernel(
    q_in, o_in, u_in, d_in, s_in, Q, O, U, D, S,
    tq, to, tu, td, aq, ao, au, ad, ssem, rsem, lsem,
):
    w, n, z, x, y, c, links = where_am_i()
    mine, other = c, 1 - c
    net = Net(ssem, rsem, links)
    rw, cn = aq.shape[1], aq.shape[2]
    rd, cu = ad.shape[0], au.shape[1]
    half = cu // 2
    enter(z, links)

    first = [net.copy("p", src, dst, net.sends(1), net.recvs(1)) for src, dst in (
        (q_in.at[other], tq), (o_in.at[other], to), (u_in.at[other], tu), (d_in.at[other], td),
        (s_in, S.at[z, x, y, c]),
    )]
    for cp in first:
        cp.start()
    own_small = pltpu.make_async_copy(s_in, S.at[z, x, y, c], lsem.at[4])
    own_small.start()

    def join(own, got):
        a, b = own.astype(F32), got.astype(F32)
        lo, hi = jnp.where(c == 0, a, b), jnp.where(c == 0, b, a)
        return jnp.concatenate([lo, hi], axis=-1).astype(BF)

    outs = (
        (au, U.at[mine, span(rw * w, rw), span(cu * y, cu)]),
        (aq, Q.at[mine, :, span(rw * w, rw), span(cn * y, cn)]),
        (ao, O.at[mine, span(rw * w, rw), span(cn * y, cn)]),
        (ad, D.at[mine, span(rd * w, rd), span(cn * y, cn)]),
    )
    first[2].wait()
    au[...] = join(u_in[mine], tu[...])
    first[0].wait()
    for j in range(3):
        aq[j] = join(q_in[mine, j], tq[j])
    first[1].wait()
    ao[...] = join(o_in[mine], to[...])
    first[3].wait()
    ad[...] = join(d_in[mine], td[...])
    first[4].wait()
    own_small.wait()
    local = [pltpu.make_async_copy(src, dst, lsem.at[k]) for k, (src, dst) in enumerate(outs)]
    for cp in local:
        cp.start()
    for cp in local:
        cp.wait()

    def rows_a(zp):
        return span(2 * rw * zp, 2 * rw)

    def reg_a(zp, yp, layer):
        return [Q.at[layer, :, rows_a(zp), span(cn * yp, cn)], O.at[layer, rows_a(zp), span(cn * yp, cn)]]

    def blk_a(wp, yp, layer):
        rows = span(rw * wp, rw)
        return [Q.at[layer, :, rows, span(cn * yp, cn)], O.at[layer, rows, span(cn * yp, cn)]]

    def reg_d(zp, xp, layer):
        return [D.at[layer, span(rd * (2 * zp + xp), rd), :]]

    def blk_d(wp, yp, layer):
        return [D.at[layer, span(rd * wp, rd), span(cn * yp, cn)]]

    def blk_u(zp, xp, yp, layer):
        return [U.at[layer, span(rw * (2 * zp + xp), rw), span(cu * yp, cu)]]

    def blk_u1(zp, xp, yp, layer):
        return [U.at[layer, span(rw * (2 * zp + xp), rw), span(cu * yp, half)]]

    def blk_u2(zp, xp, yp, layer):
        return [U.at[layer, span(rw * (2 * zp + xp), rw), span(cu * yp + half, half)]]

    def pair_u1(zp, yp, layer):
        return [U.at[layer, rows_a(zp), span(cu * yp, half)]]

    def pair_u2(zp, xp, layer):
        return blk_u2(zp, xp, 0, layer) + blk_u2(zp, xp, 1, layer)

    class Lane:
        def __init__(self, link, sent, got, parts):
            self.link, self.sent, self.got, self.parts = link, sent, got, parts
            self.s = [net.sends(ZN) for _ in range(parts)]
            self.r = [net.recvs(ZN) for _ in range(parts)]

        def send(self, zp):
            for k, ref in enumerate(self.sent(zp)):
                net.copy(self.link, ref, ref, self.s[k] + zp, self.r[k] + zp).start()

        def recv(self, zp):
            for k, ref in enumerate(self.got(zp)):
                net.copy(self.link, ref, ref, self.s[k] + zp, self.r[k] + zp).wait_recv()

        def drain(self, zp):
            for k, ref in enumerate(self.sent(zp)):
                net.copy(self.link, ref, ref, self.s[k] + zp, self.r[k] + zp).wait_send()

    class Line:
        def __init__(self, region, parts):
            self.region, self.parts = region, parts
            self.su = [net.sends(ZN) for _ in range(parts)]
            self.sd = [net.sends(ZN) for _ in range(parts)]
            self.r = [net.recvs(ZN) for _ in range(parts)]

        def each(self, link, sems, zp, what):
            for k, ref in enumerate(self.region(zp)):
                getattr(net.copy(link, ref, ref, sems[k] + zp, self.r[k] + zp), what)()

        def own(self, what="start"):
            @pl.when(z < ZN - 1)
            def _():
                self.each("up", self.su, z, what)

            @pl.when(z > 0)
            def _():
                self.each("down", self.sd, z, what)

        def relay(self, t, what="start"):
            @pl.when(jnp.minimum(z - t, ZN - 2 - z) >= 0)
            def _():
                self.each("up", self.su, z - t, what)

            @pl.when(jnp.minimum(ZN - 1 - t - z, z - 1) >= 0)
            def _():
                self.each("down", self.sd, z + t, what)

        def recv(self, zp):
            self.each("up", self.su, zp, "wait_recv")

    line_a = Line(lambda zp: reg_a(zp, y, mine), 2)
    line_d = Line(lambda zp: reg_d(zp, x, mine), 1)
    line_u = Line(lambda zp: blk_u(zp, x, y, mine), 1)
    x1 = Lane("x", lambda zp: blk_a(w, y, mine), lambda zp: blk_a(w + 1 - 2 * x, y, mine), 2)
    y1 = Lane("y", lambda zp: blk_d(w, y, mine), lambda zp: blk_d(w, 1 - y, mine), 1)
    x_u1 = Lane("x", lambda zp: blk_u1(zp, x, y, mine), lambda zp: blk_u1(zp, 1 - x, y, mine), 1)
    y_u2 = Lane("y", lambda zp: blk_u2(zp, x, y, mine), lambda zp: blk_u2(zp, x, 1 - y, mine), 1)
    y_a = Lane("y", lambda zp: reg_a(zp, y, mine), lambda zp: reg_a(zp, 1 - y, mine), 2)
    x_d = Lane("x", lambda zp: reg_d(zp, x, mine), lambda zp: reg_d(zp, 1 - x, mine), 1)
    y_u1 = Lane("y", lambda zp: pair_u1(zp, y, mine), lambda zp: pair_u1(zp, 1 - y, mine), 1)
    x_u2 = Lane("x", lambda zp: pair_u2(zp, x, mine), lambda zp: pair_u2(zp, 1 - x, mine), 2)

    def to_partner(make, parts):
        return Lane("p", lambda zp: make(zp, mine), lambda zp: make(zp, other), parts)

    p_a = to_partner(lambda zp, l: reg_a(zp, y, l), 2)
    p_a2 = to_partner(lambda zp, l: reg_a(zp, 1 - y, l), 2)
    p_d = to_partner(lambda zp, l: reg_d(zp, x, l), 1)
    p_d2 = to_partner(lambda zp, l: reg_d(zp, 1 - x, l), 1)
    p_u1 = to_partner(lambda zp, l: pair_u1(zp, y, l), 1)
    p_u1b = to_partner(lambda zp, l: pair_u1(zp, 1 - y, l), 1)
    p_u2 = to_partner(lambda zp, l: pair_u2(zp, x, l), 2)
    p_u2b = to_partner(lambda zp, l: pair_u2(zp, 1 - x, l), 2)

    small_x = Lane("x", lambda zp: [S.at[z, x, y]], lambda zp: [S.at[z, 1 - x, y]], 1)
    small_y = Lane("y", lambda zp: [S.at[z, :, y]], lambda zp: [S.at[z, :, 1 - y]], 1)
    line_s = Line(lambda zp: [S.at[zp]], 1)

    line_u.own()
    x1.send(0)
    y1.send(0)
    small_x.send(0)
    x_u1.send(z)
    y_u2.send(z)
    small_x.recv(0)
    small_y.send(0)
    x1.recv(0)
    line_a.own()
    y_a.send(z)
    p_a.send(z)
    y1.recv(0)
    line_d.own()
    x_d.send(z)
    p_d.send(z)
    small_y.recv(0)
    line_s.own()

    def second(zp):
        x_u1.recv(zp)
        y_u1.send(zp)
        p_u1.send(zp)
        y_u2.recv(zp)
        x_u2.send(zp)
        p_u2.send(zp)

    def third(zp):
        y_a.recv(zp)
        p_a2.send(zp)
        x_d.recv(zp)
        p_d2.send(zp)
        y_u1.recv(zp)
        p_u1b.send(zp)
        x_u2.recv(zp)
        p_u2b.send(zp)

    def both_ways(t, make):
        @pl.when(z >= t)
        def _():
            make(z - t)

        @pl.when(z < ZN - t)
        def _():
            make(z + t)

    def take(line, t, *lanes):
        both_ways(t, line.recv)
        line.relay(t)
        for lane in lanes:
            both_ways(t, lane.send)

    second(z)
    for t in range(1, ZN):
        take(line_u, t, x_u1, y_u2)
        take(line_a, t, y_a, p_a)
        if t == 1:
            third(z)
        else:
            both_ways(t - 1, third)
        take(line_d, t, x_d, p_d)
        both_ways(t, second)
        take(line_s, t)
    both_ways(ZN - 1, third)

    partner = (p_a, p_a2, p_d, p_d2, p_u1, p_u1b, p_u2, p_u2b)
    for zp in range(ZN):
        for lane in partner:
            lane.recv(zp)
    for zp in range(ZN):
        for lane in partner + (x_u1, y_u2, y_a, x_d, y_u1, x_u2):
            lane.drain(zp)
    for lane in (x1, y1, small_x, small_y):
        lane.drain(0)
    for line in (line_u, line_a, line_d, line_s):
        line.own("wait_send")
        for t in range(1, ZN):
            line.relay(t, "wait_send")
    assert net.next_send <= ssem.shape[0] and net.next_recv <= rsem.shape[0]


def gather_fast(pieces):
    wqkv, wo, wup, wdn, bias, ubias, norm = pieces
    _, _, rw, cn = wqkv.shape
    rd, cu = wdn.shape[1], wup.shape[2]
    d, ff = rw * 8, rd * 8
    small = jnp.concatenate([bias[:, 0], norm[:, 0], ubias, jnp.zeros_like(ubias)], axis=0).astype(F32)
    small = jnp.pad(small, ((0, 0), (0, 128 - rw)))
    hbm = pl.BlockSpec(memory_space=pl.ANY)
    vmem = pl.BlockSpec(memory_space=pltpu.VMEM)
    Q, O, U, D, S = pl.pallas_call(
        gather_kernel,
        in_specs=[vmem] * 5,
        out_specs=[hbm] * 5,
        out_shape=[
            jax.ShapeDtypeStruct((LAYERS, 3, d, d), BF),
            jax.ShapeDtypeStruct((LAYERS, d, d), BF),
            jax.ShapeDtypeStruct((LAYERS, d, ff), BF),
            jax.ShapeDtypeStruct((LAYERS, ff, d), BF),
            jax.ShapeDtypeStruct((ZN, 2, 2, 2, 8, 128), F32),
        ],
        scratch_shapes=[
            pltpu.VMEM((3, rw, cn), BF), pltpu.VMEM((rw, cn), BF), pltpu.VMEM((rw, cu), BF), pltpu.VMEM((rd, cn), BF),
            pltpu.VMEM((3, rw, 2 * cn), BF), pltpu.VMEM((rw, 2 * cn), BF),
            pltpu.VMEM((rw, 2 * cu), BF), pltpu.VMEM((rd, 2 * cn), BF),
            pltpu.SemaphoreType.DMA((160,)), pltpu.SemaphoreType.DMA((160,)), pltpu.SemaphoreType.DMA((5,)),
        ],
        compiler_params=pltpu.CompilerParams(collective_id=1, has_side_effects=True),
        name="weight_gather",
    )(wqkv, wo, wup, wdn, small)
    S = S.reshape(8, 4, 8, 128)[..., :rw]
    rows = jnp.transpose(S, (2, 1, 0, 3)).reshape(8, 4, d)
    ub = jnp.transpose(S[:, :, 4:6], (2, 0, 1, 3)).reshape(2, ff)
    return Q, O, U, D, rows[0:2], ub, rows[2:4]


def gather_weights(pieces):
    wqkv, wo, wup, wdn, bias, ubias, norm = pieces
    narrow = [(wqkv, 3), (wo, 2), (wup, 2), (wdn, 2), (bias, 1), (norm, 1)]
    wqkv, wo, wup, wdn, bias, norm = (lax.all_gather(w, "narrow", axis=k, tiled=True) for w, k in narrow)
    wide = [(wqkv, 2), (wo, 1), (wup, 1), (wdn, 1), (bias, 2), (norm, 2)]
    wqkv, wo, wup, wdn, bias, norm = (lax.all_gather(w, "wide", axis=k, tiled=True) for w, k in wide)
    ubias = lax.all_gather(ubias, ("wide", "narrow"), axis=1, tiled=True)
    return wqkv, wo, wup, wdn, bias, ubias, norm


def scatter_two(grad, row_axis, col_axis):
    low = lax.psum_scatter(grad.astype(BF), "narrow", scatter_dimension=col_axis, tiled=True)
    return lax.psum_scatter(low.astype(F32), "wide", scatter_dimension=row_axis, tiled=True)


def scatter_grads(big, small):
    gq, go, gup, gdn = big
    gq = jnp.moveaxis(gq.reshape(gq.shape[:2] + (3, -1)), 2, 1)
    gb, gub, gn = small
    big = (scatter_two(gq, 2, 3), scatter_two(go, 1, 2), scatter_two(gup, 1, 2), scatter_two(gdn, 1, 2))
    gub = lax.psum_scatter(gub, ("wide", "narrow"), scatter_dimension=1, tiled=True)

    def small_two(g):
        return lax.psum_scatter(
            lax.psum_scatter(g, "narrow", scatter_dimension=1, tiled=True), "wide", scatter_dimension=2, tiled=True
        )

    return big + (small_two(gb), gub, small_two(gn))


def shards(
    near, text_in, memory_in, counts, last_len, cot_text, cot_memory,
    qkv_weight, out_weight, up_weight, down_weight, biases, up_bias, norm_params,
):
    text, cot = text_in[:, 0], cot_text[:, 0]
    mem, cot_mem = memory_in[:, 0], cot_memory[:, 0]
    cnt, lens = counts[:, 0], last_len[:, 0]
    gather = gather_fast if near else gather_weights
    weights = gather((qkv_weight, out_weight, up_weight, down_weight, biases, up_bias, norm_params))
    text_out, mem_out, kept = forward_local(text, mem, cnt, lens, weights)
    text_grad, mem_grad, grads, small = backward_local(cot, cot_mem, cnt, lens, kept, weights)
    grads = scatter_grads(weight_grads(kept, grads), small)
    return (text_out[:, None], mem_out[:, None], text_grad[:, None], mem_grad[:, None]) + grads


def solution(mesh):
    items = ("wide", "narrow")
    act5 = P(None, items, None, None, None)
    act4 = P(None, items, None, None)
    ids = P(None, items)
    split = P(None, "wide", "narrow")
    small = P(None, "narrow", "wide")
    params = (P(None, None, "wide", "narrow"), split, split, split, small, ids, small)
    near = (mesh.shape["wide"], mesh.shape["narrow"]) == (2 * ZN, 4)
    return jax.shard_map(
        functools.partial(shards, near),
        mesh=mesh,
        in_specs=(act5, act4, ids, ids, act5, act4) + params,
        out_specs=(act5, act4, act5, act4) + params,
        check_vma=False,
    )
```

```python
import functools

import jax
import jax.numpy as jnp
from jax import lax
from jax.experimental import pallas as pl
from jax.experimental.pallas import tpu as pltpu
from jax.sharding import PartitionSpec as P

HEADS = 12
HD = 64
MEM = 10
TEXT = 108
SEGS = 4
MB = 2
LAYERS = 2
SEG = TEXT + 2 * MEM
TAIL = 104
ROWS = MB * SEG
EPS = 1e-12
BF = jnp.bfloat16
F32 = jnp.float32
NEG = -1e30
RSQRT2 = 0.7071067811865476
RSQRT2PI = 0.3989422804014327
VMEM_LIMIT = 66_000_000
FT = 512


def dot(a, b):
    return lax.dot_general(a, b, (((1,), (0,)), ((), ())), preferred_element_type=F32)


def dot_rt(a, b):
    return lax.dot_general(a, b, (((1,), (1,)), ((), ())), preferred_element_type=F32)


def dot_lt(a, b):
    return lax.dot_general(a, b, (((0,), (0,)), ((), ())), preferred_element_type=F32)


def row_ids(shape):
    return lax.broadcasted_iota(jnp.int32, shape, 0)


def lane_ids(shape):
    return lax.broadcasted_iota(jnp.int32, shape, 1)


def valid_rows(seg, count, length):
    return jnp.where(seg < count - 1, TEXT, jnp.where(seg == count - 1, length, 0))


def colsum(v):
    rows, cols = v.shape
    return jnp.sum(v.reshape(rows // 8, 8, cols), axis=0)


def fwd_kernel(
    counts, lens, text, mem0, wqkv, wo, wup, wdn, bias, ubias, norm,
    text_out, mem_out, a_out, qkv_out, p_out, c_out, y_out, g_out, gp_out, xh1_out, xh2_out, rs_out,
    x_ref, mem_ref, y_ref, acc_ref,
):
    seg = pl.program_id(0)
    layer = pl.program_id(1)
    d = x_ref.shape[-1]

    @pl.when((seg == 0) & (layer == 0))
    def _():
        mem_ref[...] = mem0[...]

    @pl.when(layer == 0)
    def _():
        for i in range(MB):
            x_ref[i * SEG : i * SEG + TEXT, :] = text[i, 0].astype(F32)
            tail = slice(i * SEG + TAIL, (i + 1) * SEG)
            now = x_ref[tail, :]
            x_ref[tail, :] = jnp.where(row_ids(now.shape) < TEXT - TAIL, now, mem_ref[i])

    xb = x_ref[...].astype(BF)
    a_out[0] = xb
    qkv_out[0, :, 0:d] = (dot(xb, wqkv[layer, 0]) + bias[layer, 0:1, :]).astype(BF)
    qkv_out[0, :, d : 2 * d] = dot(xb, wqkv[layer, 1]).astype(BF)
    qkv_out[0, :, 2 * d : 3 * d] = (dot(xb, wqkv[layer, 2]) + bias[layer, 1:2, :]).astype(BF)

    low_half = lane_ids((SEG, 128)) < HD
    lanes = lane_ids((1, SEG))
    for i in range(MB):
        vr = valid_rows(seg, counts[i], lens[i])
        keep = (lanes < vr) | (lanes >= TEXT)
        r0 = i * SEG
        for pair in range(HEADS // 2):
            c0 = pair * 128
            q = qkv_out[0, r0 : r0 + SEG, c0 : c0 + 128]
            k = qkv_out[0, r0 : r0 + SEG, d + c0 : d + c0 + 128]
            v = qkv_out[0, r0 : r0 + SEG, 2 * d + c0 : 2 * d + c0 + 128]
            zero = jnp.zeros_like(q)
            q2 = jnp.concatenate([jnp.where(low_half, q, zero), jnp.where(low_half, zero, q)], axis=0)
            s = dot_rt(q2, k) * (HD ** -0.5)
            s = jnp.where(keep, s, NEG)
            e = jnp.exp(s - jnp.max(s, axis=-1, keepdims=True))
            p = (e / jnp.sum(e, axis=-1, keepdims=True)).astype(BF)
            u0 = (i * (HEADS // 2) + pair) * 2 * SEG
            p_out[0, u0 : u0 + 2 * SEG, :] = p
            c2 = dot(p, v)
            c_out[0, r0 : r0 + SEG, c0 : c0 + 128] = jnp.where(low_half, c2[:SEG], c2[SEG:]).astype(BF)

    def norm_to(h, gain, shift, xh_out, rs_index):
        center = h - jnp.mean(h, axis=-1, keepdims=True)
        rs = lax.rsqrt(jnp.mean(center * center, axis=-1, keepdims=True) + EPS)
        xh = center * rs
        xh_out[0] = xh
        rs_out[0, rs_index] = jnp.broadcast_to(rs, (ROWS, 128))
        return xh * gain + shift

    h1 = x_ref[...] + (dot(c_out[0], wo[layer]) + bias[layer, 2:3, :])
    y = norm_to(h1, norm[layer, 0:1, :], norm[layer, 1:2, :], xh1_out, 0)
    y_ref[...] = y
    y_out[0] = y.astype(BF)

    acc_ref[...] = jnp.zeros_like(acc_ref)
    ff = wup.shape[-1]

    def ffn_step(j, carry):
        cols = pl.ds(pl.multiple_of(j * FT, FT), FT)
        u = dot(y_out[0], wup[layer, :, cols]) + ubias[layer, :, cols]
        cdf = 0.5 * (1.0 + lax.erf(u * RSQRT2))
        g = (u * cdf).astype(BF)
        g_out[0, :, cols] = g
        gp_out[0, :, cols] = (cdf + u * (jnp.exp(-0.5 * (u * u)) * RSQRT2PI)).astype(BF)
        acc_ref[...] += dot(g, wdn[layer, cols, :])
        return carry

    lax.fori_loop(0, ff // FT, ffn_step, 0)
    h2 = y_ref[...] + (acc_ref[...] + bias[layer, 3:4, :])
    x_ref[...] = norm_to(h2, norm[layer, 2:3, :], norm[layer, 3:4, :], xh2_out, 1)

    @pl.when(layer == LAYERS - 1)
    def _():
        for i in range(MB):
            vr = valid_rows(seg, counts[i], lens[i])
            body = x_ref[i * SEG : i * SEG + TEXT, :]
            text_out[i, 0] = jnp.where(row_ids(body.shape) < vr, body, 0.0).astype(BF)
            tail = x_ref[i * SEG + TAIL : (i + 1) * SEG, :]
            both = jnp.where(row_ids(tail.shape) >= TEXT - TAIL + MEM, tail, pltpu.roll(tail, SEG - TAIL - MEM, axis=0))
            mem_ref[i] = jnp.where(seg < counts[i], both, mem_ref[i])
        mem_out[...] = mem_ref[...]


def whole(shape):
    return pl.BlockSpec(shape, lambda *_: (0,) * len(shape), pipeline_mode=pl.Buffered(1))


def saved(rows, cols):
    return pl.BlockSpec((1, rows, cols), lambda s, l: (l, s, 0))


def forward_local(text, mem, counts, lens, weights):
    wqkv, wo, wup, wdn, bias, ubias, norm = weights
    d, ff = wup.shape[1:]
    mem0 = jnp.concatenate([jnp.zeros((MB, TEXT - TAIL, d), F32), mem.astype(F32), mem.astype(F32)], axis=1)
    total = SEGS * ROWS
    units = MB * HEADS * SEG
    smem = pl.BlockSpec(memory_space=pltpu.SMEM)
    outs = pl.pallas_call(
        fwd_kernel,
        grid=(SEGS, LAYERS),
        in_specs=[
            smem, smem,
            pl.BlockSpec((MB, 1, TEXT, d), lambda s, l: (0, s, 0, 0)),
            whole(mem0.shape), whole(wqkv.shape), whole(wo.shape), whole(wup.shape), whole(wdn.shape),
            whole(bias.shape), whole((LAYERS, 1, ff)), whole(norm.shape),
        ],
        out_specs=[
            pl.BlockSpec((MB, 1, TEXT, d), lambda s, l: (0, s, 0, 0)),
            whole(mem0.shape),
            saved(ROWS, d), saved(ROWS, 3 * d), saved(units, 128), saved(ROWS, d), saved(ROWS, d),
            saved(ROWS, ff), saved(ROWS, ff), saved(ROWS, d), saved(ROWS, d),
            pl.BlockSpec((1, 2, ROWS, 128), lambda s, l: (l, 0, s, 0)),
        ],
        out_shape=[
            jax.ShapeDtypeStruct((MB, SEGS, TEXT, d), BF),
            jax.ShapeDtypeStruct(mem0.shape, F32),
            jax.ShapeDtypeStruct((LAYERS, total, d), BF),
            jax.ShapeDtypeStruct((LAYERS, total, 3 * d), BF),
            jax.ShapeDtypeStruct((LAYERS, SEGS * units, 128), BF),
            jax.ShapeDtypeStruct((LAYERS, total, d), BF),
            jax.ShapeDtypeStruct((LAYERS, total, d), BF),
            jax.ShapeDtypeStruct((LAYERS, total, ff), BF),
            jax.ShapeDtypeStruct((LAYERS, total, ff), BF),
            jax.ShapeDtypeStruct((LAYERS, total, d), F32),
            jax.ShapeDtypeStruct((LAYERS, total, d), F32),
            jax.ShapeDtypeStruct((LAYERS, 2, total, 128), F32),
        ],
        scratch_shapes=[
            pltpu.VMEM((ROWS, d), F32), pltpu.VMEM(mem0.shape, F32),
            pltpu.VMEM((ROWS, d), F32), pltpu.VMEM((ROWS, d), F32),
        ],
        compiler_params=pltpu.CompilerParams(
            dimension_semantics=("arbitrary", "arbitrary"), vmem_limit_bytes=VMEM_LIMIT
        ),
        name="rmt_forward",
    )(counts, lens, text, mem0, wqkv, wo, wup, wdn, bias.astype(F32), ubias.astype(F32)[:, None, :], norm.astype(F32))
    text_out, mem_end = outs[:2]
    return text_out, mem_end[:, TEXT - TAIL + MEM :].astype(BF), outs[2:]


def bwd_kernel(
    counts, lens, cot, gm0, qkv, p_in, gp_in, xh1_in, xh2_in, rs_in, wqkv, wo, wup, wdn, norm,
    tg_out, gm_out, dqkv_out, dao_out, du_out, df_out, gb_out, gub_out, gn_out,
    g_ref, gm_ref, t_ref, acc_ref, dc_ref,
):
    seg = SEGS - 1 - pl.program_id(0)
    step = pl.program_id(1)
    layer = LAYERS - 1 - step
    d = g_ref.shape[-1]

    @pl.when((seg == SEGS - 1) & (step == 0))
    def _():
        gm_ref[...] = gm0[...]
        gb_out[...] = jnp.zeros_like(gb_out)
        gub_out[...] = jnp.zeros_like(gub_out)
        gn_out[...] = jnp.zeros_like(gn_out)

    @pl.when(step == 0)
    def _():
        for i in range(MB):
            vr = valid_rows(seg, counts[i], lens[i])
            ct = cot[i, 0].astype(F32)
            g_ref[i * SEG : i * SEG + TEXT, :] = jnp.where(row_ids(ct.shape) < vr, ct, 0.0)
            tail = slice(i * SEG + TAIL, (i + 1) * SEG)
            now = g_ref[tail, :]
            rows = row_ids(now.shape)
            mem_part = jnp.where((rows >= TEXT - TAIL + MEM) & (seg < counts[i]), gm_ref[i], 0.0)
            g_ref[tail, :] = jnp.where(rows < TEXT - TAIL, now, mem_part)

    def norm_back(gout, xh, rs, gain, slot):
        gn_out[layer, slot] += colsum(gout * xh)
        gn_out[layer, slot + 1] += colsum(gout)
        t = gout * gain
        return rs * (t - jnp.mean(t, axis=-1, keepdims=True) - xh * jnp.mean(t * xh, axis=-1, keepdims=True))

    dh2 = norm_back(g_ref[...], xh2_in[0], rs_in[0, 1][:, :1], norm[layer, 2:3, :], 2)
    t_ref[...] = dh2
    df = dh2.astype(BF)
    df_out[0] = df
    gb_out[layer, 3] += colsum(df.astype(F32))
    acc_ref[...] = jnp.zeros_like(acc_ref)
    ff = wup.shape[-1]

    def ffn_step(j, carry):
        cols = pl.ds(pl.multiple_of(j * FT, FT), FT)
        dg = dot_rt(df_out[0], wdn[layer, cols, :])
        du = (dg * gp_in[0, :, cols].astype(F32)).astype(BF)
        du_out[0, :, cols] = du
        gub_out[layer, :, cols] += colsum(du.astype(F32))
        acc_ref[...] += dot_rt(du, wup[layer, :, cols])
        return carry

    lax.fori_loop(0, ff // FT, ffn_step, 0)
    dh1 = norm_back(t_ref[...] + acc_ref[...], xh1_in[0], rs_in[0, 0][:, :1], norm[layer, 0:1, :], 0)
    t_ref[...] = dh1
    dao = dh1.astype(BF)
    dao_out[0] = dao
    gb_out[layer, 2] += colsum(dao.astype(F32))
    dc_ref[...] = dot_rt(dao, wo[layer]).astype(BF)

    low_half = lane_ids((SEG, 128)) < HD
    scale = HD ** -0.5
    for i in range(MB):
        r0 = i * SEG
        for pair in range(HEADS // 2):
            c0 = pair * 128
            q = qkv[0, r0 : r0 + SEG, c0 : c0 + 128]
            k = qkv[0, r0 : r0 + SEG, d + c0 : d + c0 + 128]
            v = qkv[0, r0 : r0 + SEG, 2 * d + c0 : 2 * d + c0 + 128]
            dc = dc_ref[r0 : r0 + SEG, c0 : c0 + 128]
            zero = jnp.zeros_like(q)
            q2 = jnp.concatenate([jnp.where(low_half, q, zero), jnp.where(low_half, zero, q)], axis=0)
            dc2 = jnp.concatenate([jnp.where(low_half, dc, zero), jnp.where(low_half, zero, dc)], axis=0)
            u0 = (i * (HEADS // 2) + pair) * 2 * SEG
            pb = p_in[0, u0 : u0 + 2 * SEG, :]
            p = pb.astype(F32)
            pdp = p * dot_rt(dc2, v)
            ds = (pdp - p * jnp.sum(pdp, axis=-1, keepdims=True)).astype(BF)
            dq2 = dot(ds, k)
            dq = (jnp.where(low_half, dq2[:SEG], dq2[SEG:]) * scale).astype(BF)
            dk = (dot_lt(ds, q2) * scale).astype(BF)
            dv = dot_lt(pb, dc2).astype(BF)
            dqkv_out[0, r0 : r0 + SEG, c0 : c0 + 128] = dq
            dqkv_out[0, r0 : r0 + SEG, d + c0 : d + c0 + 128] = dk
            dqkv_out[0, r0 : r0 + SEG, 2 * d + c0 : 2 * d + c0 + 128] = dv

    gb_out[layer, 0] += colsum(dqkv_out[0, :, 0:d].astype(F32))
    gb_out[layer, 1] += colsum(dqkv_out[0, :, 2 * d : 3 * d].astype(F32))
    g_ref[...] = (
        t_ref[...]
        + dot_rt(dqkv_out[0, :, 0:d], wqkv[layer, 0])
        + dot_rt(dqkv_out[0, :, d : 2 * d], wqkv[layer, 1])
        + dot_rt(dqkv_out[0, :, 2 * d : 3 * d], wqkv[layer, 2])
    )

    @pl.when(layer == 0)
    def _():
        for i in range(MB):
            tg_out[i, 0] = g_ref[i * SEG : i * SEG + TEXT, :].astype(BF)
            tail = g_ref[i * SEG + TAIL : (i + 1) * SEG, :]
            back = tail + pltpu.roll(tail, MEM, axis=0)
            gm_ref[i] = jnp.where(seg < counts[i], 0.0, gm_ref[i]) + back
        gm_out[...] = gm_ref[...]


def backward_local(cot, cot_mem, counts, lens, kept, weights):
    wqkv, wo, wup, wdn, _, _, norm = weights
    _, qkv, p_all, _, _, _, gp, xh1, xh2, rs = kept
    d, ff = wup.shape[1:]
    gm0 = jnp.concatenate([jnp.zeros((MB, TEXT - TAIL + MEM, d), F32), cot_mem.astype(F32)], axis=1)
    total = SEGS * ROWS
    units = MB * HEADS * SEG
    smem = pl.BlockSpec(memory_space=pltpu.SMEM)

    def kept_spec(rows, cols):
        return pl.BlockSpec((1, rows, cols), lambda s, l: (LAYERS - 1 - l, SEGS - 1 - s, 0))

    outs = pl.pallas_call(
        bwd_kernel,
        grid=(SEGS, LAYERS),
        in_specs=[
            smem, smem,
            pl.BlockSpec((MB, 1, TEXT, d), lambda s, l: (0, SEGS - 1 - s, 0, 0)),
            whole(gm0.shape),
            kept_spec(ROWS, 3 * d), kept_spec(units, 128), kept_spec(ROWS, ff), kept_spec(ROWS, d), kept_spec(ROWS, d),
            pl.BlockSpec((1, 2, ROWS, 128), lambda s, l: (LAYERS - 1 - l, 0, SEGS - 1 - s, 0)),
            whole(wqkv.shape), whole(wo.shape), whole(wup.shape), whole(wdn.shape), whole(norm.shape),
        ],
        out_specs=[
            pl.BlockSpec((MB, 1, TEXT, d), lambda s, l: (0, SEGS - 1 - s, 0, 0)),
            whole(gm0.shape),
            kept_spec(ROWS, 3 * d), kept_spec(ROWS, d), kept_spec(ROWS, ff), kept_spec(ROWS, d),
            whole((LAYERS, 4, 8, d)), whole((LAYERS, 8, ff)), whole((LAYERS, 4, 8, d)),
        ],
        out_shape=[
            jax.ShapeDtypeStruct((MB, SEGS, TEXT, d), BF),
            jax.ShapeDtypeStruct(gm0.shape, F32),
            jax.ShapeDtypeStruct((LAYERS, total, 3 * d), BF),
            jax.ShapeDtypeStruct((LAYERS, total, d), BF),
            jax.ShapeDtypeStruct((LAYERS, total, ff), BF),
            jax.ShapeDtypeStruct((LAYERS, total, d), BF),
            jax.ShapeDtypeStruct((LAYERS, 4, 8, d), F32),
            jax.ShapeDtypeStruct((LAYERS, 8, ff), F32),
            jax.ShapeDtypeStruct((LAYERS, 4, 8, d), F32),
        ],
        scratch_shapes=[
            pltpu.VMEM((ROWS, d), F32), pltpu.VMEM(gm0.shape, F32),
            pltpu.VMEM((ROWS, d), F32), pltpu.VMEM((ROWS, d), F32), pltpu.VMEM((ROWS, d), BF),
        ],
        compiler_params=pltpu.CompilerParams(
            dimension_semantics=("arbitrary", "arbitrary"), vmem_limit_bytes=VMEM_LIMIT
        ),
        name="rmt_backward",
    )(counts, lens, cot, gm0, qkv, p_all, gp, xh1, xh2, rs, wqkv, wo, wup, wdn, norm.astype(F32))
    tg, gm = outs[:2]
    small = (outs[6].sum(axis=2), outs[7].sum(axis=1), outs[8].sum(axis=2))
    return tg, gm[:, TEXT - TAIL + MEM :].astype(BF), outs[2:6], small


def weight_grads(kept, grads):
    a, _, _, c, y, g = kept[:6]
    dqkv, dao, du, df = grads

    def product(lhs, rhs):
        dims = (((1,), (1,)), ((0,), (0,)))
        return lax.dot_general(lhs, rhs, dims, preferred_element_type=F32).astype(BF)

    return product(a, dqkv), product(c, dao), product(y, du), product(g, df)


MESH = pl.DeviceIdType.MESH
ZN = 4


def multiple(v, k):
    return v if isinstance(v, int) else pl.multiple_of(v, k)


def span(start, size):
    return pl.ds(multiple(start, size if size % 128 else 128), size)


def where_am_i():
    w, n = lax.axis_index("wide"), lax.axis_index("narrow")
    z, x = lax.div(w, 2), lax.rem(w, 2)
    y, c = lax.div(n, 2), lax.rem(n, 2)
    links = {
        "p": {"wide": w, "narrow": n + 1 - 2 * c},
        "x": {"wide": w + 1 - 2 * x, "narrow": n},
        "y": {"wide": w, "narrow": lax.rem(n + 2, 4)},
        "up": {"wide": w + 2, "narrow": n},
        "down": {"wide": w - 2, "narrow": n},
    }
    return w, n, z, x, y, c, links


def enter(z, links):
    barrier = pltpu.get_barrier_semaphore()
    for name in ("p", "x", "y"):
        pl.semaphore_signal(barrier, inc=1, device_id=links[name], device_id_type=MESH)

    @pl.when(z < ZN - 1)
    def _():
        pl.semaphore_signal(barrier, inc=1, device_id=links["up"], device_id_type=MESH)

    @pl.when(z > 0)
    def _():
        pl.semaphore_signal(barrier, inc=1, device_id=links["down"], device_id_type=MESH)

    pl.semaphore_wait(barrier, 3 + jnp.minimum(z, 1) + jnp.minimum(ZN - 1 - z, 1))


class Net:
    def __init__(self, ssem, rsem, links):
        self.ssem, self.rsem, self.links = ssem, rsem, links
        self.next_send, self.next_recv = 0, 0

    def sends(self, count):
        base, self.next_send = self.next_send, self.next_send + count
        return base

    def recvs(self, count):
        base, self.next_recv = self.next_recv, self.next_recv + count
        return base

    def copy(self, link, src, dst, s, r):
        return pltpu.make_async_remote_copy(
            src_ref=src, dst_ref=dst, send_sem=self.ssem.at[s], recv_sem=self.rsem.at[r],
            device_id=self.links[link], device_id_type=MESH,
        )


def gather_kernel(
    q_in, o_in, u_in, d_in, s_in, Q, O, U, D, S,
    tq, to, tu, td, aq, ao, au, ad, ssem, rsem, lsem,
):
    w, n, z, x, y, c, links = where_am_i()
    mine, other = c, 1 - c
    net = Net(ssem, rsem, links)
    rw, cn = aq.shape[1], aq.shape[2]
    rd, cu = ad.shape[0], au.shape[1]
    half = cu // 2
    enter(z, links)

    first = [net.copy("p", src, dst, net.sends(1), net.recvs(1)) for src, dst in (
        (q_in.at[other], tq), (o_in.at[other], to), (u_in.at[other], tu), (d_in.at[other], td),
        (s_in, S.at[z, x, y, c]),
    )]
    for cp in first:
        cp.start()
    own_small = pltpu.make_async_copy(s_in, S.at[z, x, y, c], lsem.at[4])
    own_small.start()

    def join(own, got):
        a, b = own.astype(F32), got.astype(F32)
        lo, hi = jnp.where(c == 0, a, b), jnp.where(c == 0, b, a)
        return jnp.concatenate([lo, hi], axis=-1).astype(BF)

    outs = (
        (au, U.at[mine, span(rw * w, rw), span(cu * y, cu)]),
        (aq, Q.at[mine, :, span(rw * w, rw), span(cn * y, cn)]),
        (ao, O.at[mine, span(rw * w, rw), span(cn * y, cn)]),
        (ad, D.at[mine, span(rd * w, rd), span(cn * y, cn)]),
    )
    first[2].wait()
    au[...] = join(u_in[mine], tu[...])
    first[0].wait()
    for j in range(3):
        aq[j] = join(q_in[mine, j], tq[j])
    first[1].wait()
    ao[...] = join(o_in[mine], to[...])
    first[3].wait()
    ad[...] = join(d_in[mine], td[...])
    first[4].wait()
    own_small.wait()
    local = [pltpu.make_async_copy(src, dst, lsem.at[k]) for k, (src, dst) in enumerate(outs)]
    for cp in local:
        cp.start()
    for cp in local:
        cp.wait()

    def rows_a(zp):
        return span(2 * rw * zp, 2 * rw)

    def reg_a(zp, yp, layer):
        return [Q.at[layer, :, rows_a(zp), span(cn * yp, cn)], O.at[layer, rows_a(zp), span(cn * yp, cn)]]

    def blk_a(wp, yp, layer):
        rows = span(rw * wp, rw)
        return [Q.at[layer, :, rows, span(cn * yp, cn)], O.at[layer, rows, span(cn * yp, cn)]]

    def reg_d(zp, xp, layer):
        return [D.at[layer, span(rd * (2 * zp + xp), rd), :]]

    def blk_d(wp, yp, layer):
        return [D.at[layer, span(rd * wp, rd), span(cn * yp, cn)]]

    def blk_u(zp, xp, yp, layer):
        return [U.at[layer, span(rw * (2 * zp + xp), rw), span(cu * yp, cu)]]

    def blk_u1(zp, xp, yp, layer):
        return [U.at[layer, span(rw * (2 * zp + xp), rw), span(cu * yp, half)]]

    def blk_u2(zp, xp, yp, layer):
        return [U.at[layer, span(rw * (2 * zp + xp), rw), span(cu * yp + half, half)]]

    def pair_u1(zp, yp, layer):
        return [U.at[layer, rows_a(zp), span(cu * yp, half)]]

    def pair_u2(zp, xp, layer):
        return blk_u2(zp, xp, 0, layer) + blk_u2(zp, xp, 1, layer)

    class Lane:
        def __init__(self, link, sent, got, parts):
            self.link, self.sent, self.got, self.parts = link, sent, got, parts
            self.s = [net.sends(ZN) for _ in range(parts)]
            self.r = [net.recvs(ZN) for _ in range(parts)]

        def send(self, zp):
            for k, ref in enumerate(self.sent(zp)):
                net.copy(self.link, ref, ref, self.s[k] + zp, self.r[k] + zp).start()

        def recv(self, zp):
            for k, ref in enumerate(self.got(zp)):
                net.copy(self.link, ref, ref, self.s[k] + zp, self.r[k] + zp).wait_recv()

        def drain(self, zp):
            for k, ref in enumerate(self.sent(zp)):
                net.copy(self.link, ref, ref, self.s[k] + zp, self.r[k] + zp).wait_send()

    class Line:
        def __init__(self, region, parts):
            self.region, self.parts = region, parts
            self.su = [net.sends(ZN) for _ in range(parts)]
            self.sd = [net.sends(ZN) for _ in range(parts)]
            self.r = [net.recvs(ZN) for _ in range(parts)]

        def each(self, link, sems, zp, what):
            for k, ref in enumerate(self.region(zp)):
                getattr(net.copy(link, ref, ref, sems[k] + zp, self.r[k] + zp), what)()

        def own(self, what="start"):
            @pl.when(z < ZN - 1)
            def _():
                self.each("up", self.su, z, what)

            @pl.when(z > 0)
            def _():
                self.each("down", self.sd, z, what)

        def relay(self, t, what="start"):
            @pl.when(jnp.minimum(z - t, ZN - 2 - z) >= 0)
            def _():
                self.each("up", self.su, z - t, what)

            @pl.when(jnp.minimum(ZN - 1 - t - z, z - 1) >= 0)
            def _():
                self.each("down", self.sd, z + t, what)

        def recv(self, zp):
            self.each("up", self.su, zp, "wait_recv")

    line_a = Line(lambda zp: reg_a(zp, y, mine), 2)
    line_d = Line(lambda zp: reg_d(zp, x, mine), 1)
    line_u = Line(lambda zp: blk_u(zp, x, y, mine), 1)
    x1 = Lane("x", lambda zp: blk_a(w, y, mine), lambda zp: blk_a(w + 1 - 2 * x, y, mine), 2)
    y1 = Lane("y", lambda zp: blk_d(w, y, mine), lambda zp: blk_d(w, 1 - y, mine), 1)
    x_u1 = Lane("x", lambda zp: blk_u1(zp, x, y, mine), lambda zp: blk_u1(zp, 1 - x, y, mine), 1)
    y_u2 = Lane("y", lambda zp: blk_u2(zp, x, y, mine), lambda zp: blk_u2(zp, x, 1 - y, mine), 1)
    y_a = Lane("y", lambda zp: reg_a(zp, y, mine), lambda zp: reg_a(zp, 1 - y, mine), 2)
    x_d = Lane("x", lambda zp: reg_d(zp, x, mine), lambda zp: reg_d(zp, 1 - x, mine), 1)
    y_u1 = Lane("y", lambda zp: pair_u1(zp, y, mine), lambda zp: pair_u1(zp, 1 - y, mine), 1)
    x_u2 = Lane("x", lambda zp: pair_u2(zp, x, mine), lambda zp: pair_u2(zp, 1 - x, mine), 2)

    def to_partner(make, parts):
        return Lane("p", lambda zp: make(zp, mine), lambda zp: make(zp, other), parts)

    p_a = to_partner(lambda zp, l: reg_a(zp, y, l), 2)
    p_a2 = to_partner(lambda zp, l: reg_a(zp, 1 - y, l), 2)
    p_d = to_partner(lambda zp, l: reg_d(zp, x, l), 1)
    p_d2 = to_partner(lambda zp, l: reg_d(zp, 1 - x, l), 1)
    p_u1 = to_partner(lambda zp, l: pair_u1(zp, y, l), 1)
    p_u1b = to_partner(lambda zp, l: pair_u1(zp, 1 - y, l), 1)
    p_u2 = to_partner(lambda zp, l: pair_u2(zp, x, l), 2)
    p_u2b = to_partner(lambda zp, l: pair_u2(zp, 1 - x, l), 2)

    small_x = Lane("x", lambda zp: [S.at[z, x, y]], lambda zp: [S.at[z, 1 - x, y]], 1)
    small_y = Lane("y", lambda zp: [S.at[z, :, y]], lambda zp: [S.at[z, :, 1 - y]], 1)
    line_s = Line(lambda zp: [S.at[zp]], 1)

    line_u.own()
    x1.send(0)
    y1.send(0)
    small_x.send(0)
    x_u1.send(z)
    y_u2.send(z)
    small_x.recv(0)
    small_y.send(0)
    x1.recv(0)
    line_a.own()
    y_a.send(z)
    p_a.send(z)
    y1.recv(0)
    line_d.own()
    x_d.send(z)
    p_d.send(z)
    small_y.recv(0)
    line_s.own()

    def second(zp):
        x_u1.recv(zp)
        y_u1.send(zp)
        p_u1.send(zp)
        y_u2.recv(zp)
        x_u2.send(zp)
        p_u2.send(zp)

    def third(zp):
        y_a.recv(zp)
        p_a2.send(zp)
        x_d.recv(zp)
        p_d2.send(zp)
        y_u1.recv(zp)
        p_u1b.send(zp)
        x_u2.recv(zp)
        p_u2b.send(zp)

    def both_ways(t, make):
        @pl.when(z >= t)
        def _():
            make(z - t)

        @pl.when(z < ZN - t)
        def _():
            make(z + t)

    def take(line, t, *lanes):
        both_ways(t, line.recv)
        line.relay(t)
        for lane in lanes:
            both_ways(t, lane.send)

    second(z)
    for t in range(1, ZN):
        take(line_u, t, x_u1, y_u2)
        take(line_a, t, y_a, p_a)
        if t == 1:
            third(z)
        else:
            both_ways(t - 1, third)
        take(line_d, t, x_d, p_d)
        both_ways(t, second)
        take(line_s, t)
    both_ways(ZN - 1, third)

    partner = (p_a, p_a2, p_d, p_d2, p_u1, p_u1b, p_u2, p_u2b)
    for zp in range(ZN):
        for lane in partner:
            lane.recv(zp)
    for zp in range(ZN):
        for lane in partner + (x_u1, y_u2, y_a, x_d, y_u1, x_u2):
            lane.drain(zp)
    for lane in (x1, y1, small_x, small_y):
        lane.drain(0)
    for line in (line_u, line_a, line_d, line_s):
        line.own("wait_send")
        for t in range(1, ZN):
            line.relay(t, "wait_send")
    assert net.next_send <= ssem.shape[0] and net.next_recv <= rsem.shape[0]


def gather_fast(pieces):
    wqkv, wo, wup, wdn, bias, ubias, norm = pieces
    _, _, rw, cn = wqkv.shape
    rd, cu = wdn.shape[1], wup.shape[2]
    d, ff = rw * 8, rd * 8
    small = jnp.concatenate([bias[:, 0], norm[:, 0], ubias, jnp.zeros_like(ubias)], axis=0).astype(F32)
    small = jnp.pad(small, ((0, 0), (0, 128 - rw)))
    hbm = pl.BlockSpec(memory_space=pl.ANY)
    vmem = pl.BlockSpec(memory_space=pltpu.VMEM)
    Q, O, U, D, S = pl.pallas_call(
        gather_kernel,
        in_specs=[vmem] * 5,
        out_specs=[hbm] * 5,
        out_shape=[
            jax.ShapeDtypeStruct((LAYERS, 3, d, d), BF),
            jax.ShapeDtypeStruct((LAYERS, d, d), BF),
            jax.ShapeDtypeStruct((LAYERS, d, ff), BF),
            jax.ShapeDtypeStruct((LAYERS, ff, d), BF),
            jax.ShapeDtypeStruct((ZN, 2, 2, 2, 8, 128), F32),
        ],
        scratch_shapes=[
            pltpu.VMEM((3, rw, cn), BF), pltpu.VMEM((rw, cn), BF), pltpu.VMEM((rw, cu), BF), pltpu.VMEM((rd, cn), BF),
            pltpu.VMEM((3, rw, 2 * cn), BF), pltpu.VMEM((rw, 2 * cn), BF),
            pltpu.VMEM((rw, 2 * cu), BF), pltpu.VMEM((rd, 2 * cn), BF),
            pltpu.SemaphoreType.DMA((160,)), pltpu.SemaphoreType.DMA((160,)), pltpu.SemaphoreType.DMA((5,)),
        ],
        compiler_params=pltpu.CompilerParams(collective_id=1, has_side_effects=True),
        name="weight_gather",
    )(wqkv, wo, wup, wdn, small)
    S = S.reshape(8, 4, 8, 128)[..., :rw]
    rows = jnp.transpose(S, (2, 1, 0, 3)).reshape(8, 4, d)
    ub = jnp.transpose(S[:, :, 4:6], (2, 0, 1, 3)).reshape(2, ff)
    return Q, O, U, D, rows[0:2], ub, rows[2:4]


def accumulate(dst, src, rows, step=48):
    def body(i, carry):
        r = pl.ds(pl.multiple_of(i * step, 16), step)
        dst[r, :] = dst[r, :] + src[r, :]
        return carry

    lax.fori_loop(0, rows // step, body, 0)


def scatter_kernel(
    gq, go, gu, gd, sm_in, oq, oo, ou, od, sm_out,
    AQ, AO, AU, AD, PQ, PO, PU, PD, FA, FO, FD, F1, F2, S1, S2, ZA, ZO, ZD, ZU, TA, TO, TD,
    hq, ho, hu, hd, s_p, s_x, s_y, s_below, s_above, s_a, s_b, s_sum, s_up, s_down, ssem, rsem, lsem,
):
    w, n, z, x, y, c, links = where_am_i()
    mine, other = c, 1 - c
    net = Net(ssem, rsem, links)
    d, ff = AO.shape[1], AU.shape[1]
    rw, cn = d // 8, d // 2
    rd, cu = ff // 8, ff // 2
    half = cu // 2
    enter(z, links)

    class Hop:
        def __init__(self, link, pairs, parts):
            self.link, self.pairs = link, pairs
            self.s = [net.sends(ZN) for _ in range(parts)]
            self.r = [net.recvs(ZN) for _ in range(parts)]

        def each(self, zp, what):
            for k, (src, dst) in enumerate(self.pairs(zp)):
                getattr(net.copy(self.link, src, dst, self.s[k] + zp, self.r[k] + zp), what)()

        def send(self, zp):
            self.each(zp, "start")

        def recv(self, zp):
            self.each(zp, "wait_recv")

        def drain(self, zp):
            self.each(zp, "wait_send")

    def rows_a(zp):
        return span(2 * rw * zp, 2 * rw)

    def slab(zp, layer, q, o, u, dn):
        rows = rows_a(zp)
        down = span(2 * rd * zp, 2 * rd)
        return [(gq.at[layer, rows, j * d : (j + 1) * d], q.at[j, rows, :]) for j in range(3)] + [
            (go.at[layer, rows, :], o.at[rows, :]),
            (gd.at[layer, down, :], dn.at[down, :]),
            (gu.at[layer, rows, :], u.at[rows, :]),
        ]

    def own_loads(zp):
        return [
            pltpu.make_async_copy(src, dst, lsem.at[k * ZN + zp])
            for k, (src, dst) in enumerate(slab(zp, mine, AQ, AO, AU, AD))
        ]

    swap = Hop("p", lambda zp: slab(zp, other, PQ, PO, PU, PD), 6)

    def cols_a(yp):
        return span(cn * yp, cn)

    def rows_x(zp, xp):
        return span(rw * (2 * zp + xp), rw)

    def rows_d(zp, xp):
        return span(rd * (2 * zp + xp), rd)

    def reg_a(zp, yp):
        return AQ.at[:, rows_a(zp), cols_a(yp)], AO.at[rows_a(zp), cols_a(yp)]

    def reg_d(zp, xp):
        return AD.at[rows_d(zp, xp), :]

    def u1(zp, yp):
        return AU.at[rows_a(zp), span(cu * yp, half)]

    def u1_part(zp, xp, yp):
        return AU.at[rows_x(zp, xp), span(cu * yp, half)]

    def u2(zp, xp, yp):
        return AU.at[rows_x(zp, xp), span(cu * yp + half, half)]

    def blk_u(zp):
        return AU.at[rows_x(zp, x), span(cu * y, cu)]

    y_a = Hop("y", lambda zp: list(zip(reg_a(zp, 1 - y), (FA.at[zp], FO.at[zp]))), 2)
    x_d = Hop("x", lambda zp: [(reg_d(zp, 1 - x), FD.at[zp])], 1)
    y_u1 = Hop("y", lambda zp: [(u1(zp, 1 - y), F1.at[zp])], 1)
    x_u2 = Hop("x", lambda zp: [(u2(zp, 1 - x, yp), F2.at[yp, zp]) for yp in range(2)], 2)
    x_u1 = Hop("x", lambda zp: [(u1_part(zp, 1 - x, y), S1.at[zp])], 1)
    y_u2 = Hop("y", lambda zp: [(u2(zp, x, 1 - y), S2.at[zp])], 1)
    last_a = Hop("x", lambda zp: [
        (AQ.at[:, rows_x(z, 1 - x), cols_a(y)], TA), (AO.at[rows_x(z, 1 - x), cols_a(y)], TO)
    ], 2)
    last_d = Hop("y", lambda zp: [(AD.at[rows_d(z, x), cols_a(1 - y)], TD)], 1)

    class Line:
        def __init__(self, region, bufs):
            self.region, self.bufs = region, bufs
            self.su = [net.sends(ZN) for _ in bufs]
            self.sd = [net.sends(ZN) for _ in bufs]
            self.r = [net.recvs(ZN + 1) for _ in bufs]

        def up(self, zp, what):
            slot = jnp.where(zp == z + 1, ZN, zp)

            @pl.when(zp > z)
            def _():
                for k, (src, buf) in enumerate(zip(self.region(zp), self.bufs)):
                    getattr(net.copy("up", src, buf.at[slot], self.su[k] + zp, self.r[k] + slot), what)()

        def down(self, zp, what):
            @pl.when(zp < z)
            def _():
                for k, (src, buf) in enumerate(zip(self.region(zp), self.bufs)):
                    getattr(net.copy("down", src, buf.at[zp], self.sd[k] + zp, self.r[k] + zp), what)()

        def take(self, zp, slot):
            for k, (dst, buf) in enumerate(zip(self.region(zp), self.bufs)):
                net.copy("up", dst, buf.at[slot], self.su[k] + zp, self.r[k] + slot).wait_recv()
                self.add(dst, buf.at[slot])

        def add(self, dst, src):
            if len(src.shape) == 3:
                for j in range(src.shape[0]):
                    accumulate(dst.at[j], src.at[j], src.shape[1])
            else:
                accumulate(dst, src, src.shape[0])

        def go(self, zp):
            @pl.when(jnp.minimum(z - zp, ZN - 2 - z) >= 0)
            def _():
                self.take(zp, zp)

            @pl.when(jnp.minimum(zp - z, z - 1) >= 0)
            def _():
                self.take(zp, jnp.where(zp == z, ZN, zp))

            self.up(zp, "start")
            self.down(zp, "start")

        def drain(self, zp):
            self.up(zp, "wait_send")
            self.down(zp, "wait_send")

    line_a = Line(lambda zp: reg_a(zp, y), (ZA, ZO))
    line_d = Line(lambda zp: (reg_d(zp, x),), (ZD,))
    line_u = Line(lambda zp: (blk_u(zp),), (ZU,))

    table = ((3, 3, 0, 0), (2, 0, 3, 1), (1, 2, 1, 2), (0, 1, 2, 3))
    order = [jnp.where(z == 0, t[0], jnp.where(z == 1, t[1], jnp.where(z == 2, t[2], t[3]))) for t in table]

    small = [
        net.copy(link, src, dst, net.sends(1), net.recvs(1))
        for link, src, dst in (("p", sm_in, s_p), ("x", s_a, s_x), ("y", s_b, s_y))
    ]
    small_up = net.copy("up", s_up, s_below, net.sends(1), net.recvs(1))
    small_down = net.copy("down", s_down, s_above, net.sends(1), net.recvs(1))

    small[0].start()
    for zp in order:
        for cp in own_loads(zp):
            cp.start()
        swap.send(zp)

    def open_slab(zp):
        for cp in own_loads(zp):
            cp.wait()
        swap.recv(zp)
        rows = rows_a(zp)
        for j in range(3):
            accumulate(AQ.at[j, rows, :], PQ.at[j, rows, :], 2 * rw)
        accumulate(AO.at[rows, :], PO.at[rows, :], 2 * rw)
        y_a.send(zp)
        down = span(2 * rd * zp, 2 * rd)
        accumulate(AD.at[down, :], PD.at[down, :], 2 * rd)
        x_d.send(zp)
        accumulate(AU.at[rows, :], PU.at[rows, :], 2 * rw, 16)
        y_u1.send(zp)
        x_u2.send(zp)

    def middle(zp):
        y_a.recv(zp)
        qa, oa = reg_a(zp, y)
        for j in range(3):
            accumulate(qa.at[j], FA.at[zp, j], 2 * rw)
        accumulate(oa, FO.at[zp], 2 * rw)
        line_a.go(zp)
        x_d.recv(zp)
        accumulate(reg_d(zp, x), FD.at[zp], rd)
        line_d.go(zp)
        y_u1.recv(zp)
        accumulate(u1(zp, y), F1.at[zp], 2 * rw)
        x_u1.send(zp)
        x_u2.recv(zp)
        for yp in range(2):
            accumulate(u2(zp, x, yp), F2.at[yp, zp], rw)
        y_u2.send(zp)

    def close(zp):
        x_u1.recv(zp)
        accumulate(u1_part(zp, x, y), S1.at[zp], rw)
        y_u2.recv(zp)
        accumulate(u2(zp, x, y), S2.at[zp], rw)
        line_u.go(zp)

    open_slab(order[0])
    small[0].wait()
    s_a[...] = sm_in[...] + s_p[...]
    small[1].start()
    open_slab(order[1])
    middle(order[0])
    small[1].wait()
    s_b[...] = s_a[...] + s_x[...]
    small[2].start()
    open_slab(order[2])
    close(order[0])
    middle(order[1])
    small[2].wait()
    s_sum[...] = s_b[...] + s_y[...]
    open_slab(order[3])
    close(order[1])
    middle(order[2])

    @pl.when(z > 0)
    def _():
        small_up.wait_recv()

    @pl.when(z == 0)
    def _():
        s_below[...] = jnp.zeros_like(s_below)

    @pl.when(z < ZN - 1)
    def _():
        s_up[...] = s_sum[...] + s_below[...]
        small_up.start()

    close(order[2])
    middle(order[3])
    last_a.send(0)
    last_d.send(0)

    @pl.when(z < ZN - 1)
    def _():
        small_down.wait_recv()

    @pl.when(z == ZN - 1)
    def _():
        s_above[...] = jnp.zeros_like(s_above)

    @pl.when(z > 0)
    def _():
        s_down[...] = s_sum[...] + s_above[...]
        small_down.start()

    sm_out[...] = s_sum[...] + s_below[...] + s_above[...]
    close(order[3])

    def pick(v, k):
        lo, hi = v[..., :k], v[..., k:]
        return jnp.where(c == 0, lo, hi), jnp.where(c == 0, hi, lo)

    out = [
        net.copy("p", src, dst.at[mine], net.sends(1), net.recvs(1))
        for src, dst in ((hu, ou), (hq, oq), (ho, oo), (hd, od))
    ]
    rows = rows_x(z, x)
    ou[mine] = AU[rows, span(cu * y + half * c, half)].astype(F32)
    hu[...] = AU[rows, span(cu * y + half * (1 - c), half)].astype(F32)
    out[0].start()
    last_a.recv(0)
    for j in range(3):
        keep, give = pick(AQ[j, rows, cols_a(y)].astype(F32) + TA[j].astype(F32), cn // 2)
        oq[mine, j] = keep
        hq[j] = give
    out[1].start()
    keep, give = pick(AO[rows, cols_a(y)].astype(F32) + TO[...].astype(F32), cn // 2)
    oo[mine] = keep
    ho[...] = give
    out[2].start()
    last_d.recv(0)
    for k in range(rd // rw):
        part = pl.ds(k * rw, rw)
        here = span(rd * w + k * rw, rw)
        keep, give = pick(AD[here, cols_a(y)].astype(F32) + TD[part, :].astype(F32), cn // 2)
        od[mine, part, :] = keep
        hd[part, :] = give
    out[3].start()

    for zp in range(ZN):
        for hop in (swap, y_a, x_d, y_u1, x_u2, x_u1, y_u2):
            hop.drain(zp)
        for line in (line_a, line_d, line_u):
            line.drain(zp)
    last_a.drain(0)
    last_d.drain(0)

    @pl.when(z < ZN - 1)
    def _():
        small_up.wait_send()

    @pl.when(z > 0)
    def _():
        small_down.wait_send()

    for cp in out:
        cp.wait()
    assert net.next_send <= ssem.shape[0] and net.next_recv <= rsem.shape[0]


def scatter_fast(big, small):
    gq, go, gup, gdn = big
    gb, gub, gn = small
    d, ff = gup.shape[1:]
    rw, cn, rd, cu = d // 8, d // 2, ff // 8, ff // 2
    pack = jnp.concatenate([gb.reshape(-1, d), gub.reshape(-1, d), gn.reshape(-1, d)], axis=0)
    hbm = pl.BlockSpec(memory_space=pl.ANY)
    vmem = pl.BlockSpec(memory_space=pltpu.VMEM)

    def buf(*shape):
        return pltpu.VMEM(shape, BF)

    def wide(*shape):
        return pltpu.VMEM(shape, F32)

    outs = [(3, rw, cn // 2), (rw, cn // 2), (rw, cu // 2), (rd, cn // 2)]
    full = [buf(3, d, d), buf(d, d), buf(d, ff), buf(ff, d)]
    oq, oo, ou, od, total = pl.pallas_call(
        scatter_kernel,
        in_specs=[hbm] * 4 + [vmem],
        out_specs=[vmem] * 5,
        out_shape=[jax.ShapeDtypeStruct((LAYERS,) + s, F32) for s in outs] + [jax.ShapeDtypeStruct(pack.shape, F32)],
        scratch_shapes=full + full + [
            buf(ZN, 3, 2 * rw, cn), buf(ZN, 2 * rw, cn), buf(ZN, rd, d), buf(ZN, 2 * rw, cu // 2),
            buf(2, ZN, rw, cu // 2), buf(ZN, rw, cu // 2), buf(ZN, rw, cu // 2),
            buf(ZN + 1, 3, 2 * rw, cn), buf(ZN + 1, 2 * rw, cn), buf(ZN + 1, rd, d), buf(ZN + 1, rw, cu),
            buf(3, rw, cn), buf(rw, cn), buf(rd, cn),
        ] + [wide(*s) for s in outs] + [wide(*pack.shape)] * 10 + [
            pltpu.SemaphoreType.DMA((140,)), pltpu.SemaphoreType.DMA((120,)), pltpu.SemaphoreType.DMA((6 * ZN,)),
        ],
        compiler_params=pltpu.CompilerParams(collective_id=2, has_side_effects=True, vmem_limit_bytes=VMEM_LIMIT),
        name="gradient_scatter",
    )(gq, go, gup, gdn, pack)
    w, n = lax.axis_index("wide"), lax.axis_index("narrow")
    gb = lax.dynamic_slice(total[0:8].reshape(2, 4, d), (0, n, w * rw), (2, 1, rw))
    gn = lax.dynamic_slice(total[16:24].reshape(2, 4, d), (0, n, w * rw), (2, 1, rw))
    gub = lax.dynamic_slice(total[8:16].reshape(2, ff), (0, (4 * w + n) * rw), (2, rw))
    return oq, oo, ou, od, gb, gub, gn


def gather_weights(pieces):
    wqkv, wo, wup, wdn, bias, ubias, norm = pieces
    narrow = [(wqkv, 3), (wo, 2), (wup, 2), (wdn, 2), (bias, 1), (norm, 1)]
    wqkv, wo, wup, wdn, bias, norm = (lax.all_gather(w, "narrow", axis=k, tiled=True) for w, k in narrow)
    wide = [(wqkv, 2), (wo, 1), (wup, 1), (wdn, 1), (bias, 2), (norm, 2)]
    wqkv, wo, wup, wdn, bias, norm = (lax.all_gather(w, "wide", axis=k, tiled=True) for w, k in wide)
    ubias = lax.all_gather(ubias, ("wide", "narrow"), axis=1, tiled=True)
    return wqkv, wo, wup, wdn, bias, ubias, norm


def scatter_two(grad, row_axis, col_axis):
    low = lax.psum_scatter(grad.astype(BF), "narrow", scatter_dimension=col_axis, tiled=True)
    return lax.psum_scatter(low.astype(F32), "wide", scatter_dimension=row_axis, tiled=True)


def scatter_grads(big, small):
    gq, go, gup, gdn = big
    gq = jnp.moveaxis(gq.reshape(gq.shape[:2] + (3, -1)), 2, 1)
    gb, gub, gn = small
    big = (scatter_two(gq, 2, 3), scatter_two(go, 1, 2), scatter_two(gup, 1, 2), scatter_two(gdn, 1, 2))
    gub = lax.psum_scatter(gub, ("wide", "narrow"), scatter_dimension=1, tiled=True)

    def small_two(g):
        return lax.psum_scatter(
            lax.psum_scatter(g, "narrow", scatter_dimension=1, tiled=True), "wide", scatter_dimension=2, tiled=True
        )

    return big + (small_two(gb), gub, small_two(gn))


def shards(
    near, text_in, memory_in, counts, last_len, cot_text, cot_memory,
    qkv_weight, out_weight, up_weight, down_weight, biases, up_bias, norm_params,
):
    text, cot = text_in[:, 0], cot_text[:, 0]
    mem, cot_mem = memory_in[:, 0], cot_memory[:, 0]
    cnt, lens = counts[:, 0], last_len[:, 0]
    gather = gather_fast if near else gather_weights
    weights = gather((qkv_weight, out_weight, up_weight, down_weight, biases, up_bias, norm_params))
    text_out, mem_out, kept = forward_local(text, mem, cnt, lens, weights)
    text_grad, mem_grad, grads, small = backward_local(cot, cot_mem, cnt, lens, kept, weights)
    scatter = scatter_fast if near else scatter_grads
    grads = scatter(weight_grads(kept, grads), small)
    return (text_out[:, None], mem_out[:, None], text_grad[:, None], mem_grad[:, None]) + grads


def solution(mesh):
    items = ("wide", "narrow")
    act5 = P(None, items, None, None, None)
    act4 = P(None, items, None, None)
    ids = P(None, items)
    split = P(None, "wide", "narrow")
    small = P(None, "narrow", "wide")
    params = (P(None, None, "wide", "narrow"), split, split, split, small, ids, small)
    near = (mesh.shape["wide"], mesh.shape["narrow"]) == (2 * ZN, 4)
    return jax.shard_map(
        functools.partial(shards, near),
        mesh=mesh,
        in_specs=(act5, act4, ids, ids, act5, act4) + params,
        out_specs=(act5, act4, act5, act4) + params,
        check_vma=False,
    )
```

```python
import functools

import jax
import jax.numpy as jnp
from jax import lax
from jax.experimental import pallas as pl
from jax.experimental.pallas import tpu as pltpu
from jax.sharding import PartitionSpec as P

HEADS = 12
HD = 64
MEM = 10
TEXT = 108
SEGS = 4
MB = 2
LAYERS = 2
SEG = TEXT + 2 * MEM
TAIL = 104
ROWS = MB * SEG
EPS = 1e-12
BF = jnp.bfloat16
F32 = jnp.float32
NEG = -1e30
RSQRT2 = 0.7071067811865476
RSQRT2PI = 0.3989422804014327
VMEM_LIMIT = 66_000_000
CHUNK = 32
GROUP_F = 6
GROUP_B = 6


def dot(a, b):
    return lax.dot_general(a, b, (((1,), (0,)), ((), ())), preferred_element_type=F32)


def dot_rt(a, b):
    return lax.dot_general(a, b, (((1,), (1,)), ((), ())), preferred_element_type=F32)


def dot_lt(a, b):
    return lax.dot_general(a, b, (((0,), (0,)), ((), ())), preferred_element_type=F32)


def row_ids(shape):
    return lax.broadcasted_iota(jnp.int32, shape, 0)


def lane_ids(shape):
    return lax.broadcasted_iota(jnp.int32, shape, 1)


def valid_rows(seg, count, length):
    return jnp.where(seg < count - 1, TEXT, jnp.where(seg == count - 1, length, 0))


def colsum(v):
    rows, cols = v.shape
    return jnp.sum(v.reshape(rows // 8, 8, cols), axis=0)


class Loads:
    def __init__(self, pairs, sems, first, order):
        self.pairs, self.sems, self.first, self.order = pairs, sems, first, order

    def each(self, layer, what):
        for k, (src, dst) in enumerate(self.pairs):
            getattr(pltpu.make_async_copy(src.at[layer], dst.at[layer], self.sems.at[layer, k]), what)()

    def start(self):
        self.each(self.order[0], "start")

    def need(self, step):
        @pl.when(self.first & (step == 0))
        def _():
            self.each(self.order[0], "wait")
            self.each(self.order[1], "start")

        @pl.when(self.first & (step == 1))
        def _():
            self.each(self.order[1], "wait")


def fwd_kernel(
    counts, lens, text, mem0, wqkv_hbm, wo_hbm, wup_hbm, wdn_hbm, bias, ubias, norm,
    text_out, mem_out, a_out, qkv_out, p_out, c_out, y_out, g_out, gp_out, xh1_out, xh2_out, rs_out,
    x_ref, mem_ref, y_ref, acc_ref, wqkv, wo, wup, wdn, wsem,
):
    seg = pl.program_id(0)
    layer = pl.program_id(1)
    d = x_ref.shape[-1]
    loads = Loads(((wqkv_hbm, wqkv), (wo_hbm, wo), (wup_hbm, wup), (wdn_hbm, wdn)), wsem, seg == 0, (0, 1))

    @pl.when((seg == 0) & (layer == 0))
    def _():
        loads.start()
        mem_ref[...] = mem0[...]

    @pl.when(layer == 0)
    def _():
        for i in range(MB):
            x_ref[i * SEG : i * SEG + TEXT, :] = text[i, 0].astype(F32)
            tail = slice(i * SEG + TAIL, (i + 1) * SEG)
            now = x_ref[tail, :]
            x_ref[tail, :] = jnp.where(row_ids(now.shape) < TEXT - TAIL, now, mem_ref[i])

    loads.need(layer)
    xb = x_ref[...].astype(BF)
    a_out[0] = xb
    qkv_out[0, :, 0:d] = (dot(xb, wqkv[layer, 0]) + bias[layer, 0:1, :]).astype(BF)
    qkv_out[0, :, d : 2 * d] = dot(xb, wqkv[layer, 1]).astype(BF)
    qkv_out[0, :, 2 * d : 3 * d] = (dot(xb, wqkv[layer, 2]) + bias[layer, 1:2, :]).astype(BF)

    low_half = lane_ids((SEG, 128)) < HD
    lanes = lane_ids((1, SEG))

    def heads_of(v):
        zero = jnp.zeros_like(v)
        return jnp.concatenate([jnp.where(low_half, v, zero), jnp.where(low_half, zero, v)], axis=0)

    for i in range(MB):
        vr = valid_rows(seg, counts[i], lens[i])
        keep = (lanes < vr) | (lanes >= TEXT)
        r0 = i * SEG
        for g0 in range(0, HEADS // 2, GROUP_F):
            pairs = range(g0, g0 + GROUP_F)

            def part(j, pair):
                return qkv_out[0, r0 : r0 + SEG, j * d + pair * 128 : j * d + pair * 128 + 128]

            s_all = [dot_rt(heads_of(part(0, p) * (HD ** -0.5)), part(1, p)) for p in pairs]
            s_all = [jnp.where(keep, s, NEG) for s in s_all]
            e_all = [jnp.exp(s - jnp.max(s, axis=-1, keepdims=True)) for s in s_all]
            p_all = [(e * (1.0 / jnp.sum(e, axis=-1, keepdims=True))).astype(BF) for e in e_all]
            c_all = [dot(pv, part(2, p)) for pv, p in zip(p_all, pairs)]
            for p, pv, c2 in zip(pairs, p_all, c_all):
                u0 = (i * (HEADS // 2) + p) * 2 * SEG
                p_out[0, u0 : u0 + 2 * SEG, :] = pv
                c_out[0, r0 : r0 + SEG, p * 128 : p * 128 + 128] = jnp.where(low_half, c2[:SEG], c2[SEG:]).astype(BF)

    def norm_to(base_ref, gain, shift, add, xh_out, rs_index, to_ref, low_out):
        for k in range(0, ROWS, CHUNK):
            rows = slice(k, k + CHUNK)
            h = base_ref[rows, :] + (acc_ref[rows, :] + add)
            center = h - jnp.mean(h, axis=-1, keepdims=True)
            rs = lax.rsqrt(jnp.mean(center * center, axis=-1, keepdims=True) + EPS)
            xh = center * rs
            xh_out[0, rows, :] = xh
            rs_out[0, rs_index, rows, :] = jnp.broadcast_to(rs, (CHUNK, 128))
            out = xh * gain + shift
            to_ref[rows, :] = out
            if low_out is not None:
                low_out[0, rows, :] = out.astype(BF)

    acc_ref[...] = dot(c_out[0], wo[layer])
    norm_to(x_ref, norm[layer, 0:1, :], norm[layer, 1:2, :], bias[layer, 2:3, :], xh1_out, 0, y_ref, y_out)

    ff = wup.shape[-1]

    def ffn_step():
        cols = slice(0, ff)
        u = dot(y_out[0], wup[layer, :, cols]) + ubias[layer, :, cols]
        cdf = 0.5 * (1.0 + lax.erf(u * RSQRT2))
        g_out[0, :, cols] = (u * cdf).astype(BF)
        gp_out[0, :, cols] = (cdf + u * (jnp.exp(-0.5 * (u * u)) * RSQRT2PI)).astype(BF)

    ffn_step()
    acc_ref[...] = dot(g_out[0], wdn[layer])
    norm_to(y_ref, norm[layer, 2:3, :], norm[layer, 3:4, :], bias[layer, 3:4, :], xh2_out, 1, x_ref, None)

    @pl.when(layer == LAYERS - 1)
    def _():
        for i in range(MB):
            vr = valid_rows(seg, counts[i], lens[i])
            body = x_ref[i * SEG : i * SEG + TEXT, :]
            text_out[i, 0] = jnp.where(row_ids(body.shape) < vr, body, 0.0).astype(BF)
            tail = x_ref[i * SEG + TAIL : (i + 1) * SEG, :]
            both = jnp.where(row_ids(tail.shape) >= TEXT - TAIL + MEM, tail, pltpu.roll(tail, SEG - TAIL - MEM, axis=0))
            mem_ref[i] = jnp.where(seg < counts[i], both, mem_ref[i])
        mem_out[...] = mem_ref[...]


def whole(shape):
    return pl.BlockSpec(shape, lambda *_: (0,) * len(shape), pipeline_mode=pl.Buffered(1))


def saved(rows, cols):
    return pl.BlockSpec((1, rows, cols), lambda s, l: (l, s, 0))


def forward_local(text, mem, counts, lens, weights):
    wqkv, wo, wup, wdn, bias, ubias, norm = weights
    d, ff = wup.shape[1:]
    mem0 = jnp.concatenate([jnp.zeros((MB, TEXT - TAIL, d), F32), mem.astype(F32), mem.astype(F32)], axis=1)
    total = SEGS * ROWS
    units = MB * HEADS * SEG
    smem = pl.BlockSpec(memory_space=pltpu.SMEM)
    hbm = pl.BlockSpec(memory_space=pl.ANY)
    outs = pl.pallas_call(
        fwd_kernel,
        grid=(SEGS, LAYERS),
        in_specs=[
            smem, smem,
            pl.BlockSpec((MB, 1, TEXT, d), lambda s, l: (0, s, 0, 0)),
            whole(mem0.shape), hbm, hbm, hbm, hbm,
            whole(bias.shape), whole((LAYERS, 1, ff)), whole(norm.shape),
        ],
        out_specs=[
            pl.BlockSpec((MB, 1, TEXT, d), lambda s, l: (0, s, 0, 0)),
            whole(mem0.shape),
            saved(ROWS, d), saved(ROWS, 3 * d), saved(units, 128), saved(ROWS, d), saved(ROWS, d),
            saved(ROWS, ff), saved(ROWS, ff), saved(ROWS, d), saved(ROWS, d),
            pl.BlockSpec((1, 2, ROWS, 128), lambda s, l: (l, 0, s, 0)),
        ],
        out_shape=[
            jax.ShapeDtypeStruct((MB, SEGS, TEXT, d), BF),
            jax.ShapeDtypeStruct(mem0.shape, F32),
            jax.ShapeDtypeStruct((LAYERS, total, d), BF),
            jax.ShapeDtypeStruct((LAYERS, total, 3 * d), BF),
            jax.ShapeDtypeStruct((LAYERS, SEGS * units, 128), BF),
            jax.ShapeDtypeStruct((LAYERS, total, d), BF),
            jax.ShapeDtypeStruct((LAYERS, total, d), BF),
            jax.ShapeDtypeStruct((LAYERS, total, ff), BF),
            jax.ShapeDtypeStruct((LAYERS, total, ff), BF),
            jax.ShapeDtypeStruct((LAYERS, total, d), F32),
            jax.ShapeDtypeStruct((LAYERS, total, d), F32),
            jax.ShapeDtypeStruct((LAYERS, 2, total, 128), F32),
        ],
        scratch_shapes=[
            pltpu.VMEM((ROWS, d), F32), pltpu.VMEM(mem0.shape, F32),
            pltpu.VMEM((ROWS, d), F32), pltpu.VMEM((ROWS, d), F32),
            pltpu.VMEM(wqkv.shape, BF), pltpu.VMEM(wo.shape, BF), pltpu.VMEM(wup.shape, BF), pltpu.VMEM(wdn.shape, BF),
            pltpu.SemaphoreType.DMA((LAYERS, 4)),
        ],
        compiler_params=pltpu.CompilerParams(
            dimension_semantics=("arbitrary", "arbitrary"), vmem_limit_bytes=VMEM_LIMIT
        ),
        name="rmt_forward",
    )(counts, lens, text, mem0, wqkv, wo, wup, wdn, bias.astype(F32), ubias.astype(F32)[:, None, :], norm.astype(F32))
    text_out, mem_end = outs[:2]
    return text_out, mem_end[:, TEXT - TAIL + MEM :].astype(BF), outs[2:]


def bwd_kernel(
    counts, lens, cot, gm0, qkv, p_in, gp_in, xh1_in, xh2_in, rs_in, wqkv_hbm, wo_hbm, wup_hbm, wdn_hbm, norm,
    tg_out, gm_out, dqkv_out, dao_out, du_out, df_out, gb_out, gub_out, gn_out,
    g_ref, gm_ref, t_ref, acc_ref, dc_ref, wqkv, wo, wup, wdn, wsem,
):
    seg = SEGS - 1 - pl.program_id(0)
    step = pl.program_id(1)
    layer = LAYERS - 1 - step
    loads = Loads(((wqkv_hbm, wqkv), (wo_hbm, wo), (wup_hbm, wup), (wdn_hbm, wdn)), wsem, seg == SEGS - 1, (1, 0))
    d = g_ref.shape[-1]

    @pl.when((seg == SEGS - 1) & (step == 0))
    def _():
        loads.start()
        gm_ref[...] = gm0[...]
        gb_out[...] = jnp.zeros_like(gb_out)
        gub_out[...] = jnp.zeros_like(gub_out)
        gn_out[...] = jnp.zeros_like(gn_out)

    @pl.when(step == 0)
    def _():
        for i in range(MB):
            vr = valid_rows(seg, counts[i], lens[i])
            ct = cot[i, 0].astype(F32)
            g_ref[i * SEG : i * SEG + TEXT, :] = jnp.where(row_ids(ct.shape) < vr, ct, 0.0)
            tail = slice(i * SEG + TAIL, (i + 1) * SEG)
            now = g_ref[tail, :]
            rows = row_ids(now.shape)
            mem_part = jnp.where((rows >= TEXT - TAIL + MEM) & (seg < counts[i]), gm_ref[i], 0.0)
            g_ref[tail, :] = jnp.where(rows < TEXT - TAIL, now, mem_part)

    loads.need(step)

    def norm_back(base_ref, add_ref, xh_in, rs_slot, gain, slot, low_out, low_slot):
        sums = [jnp.zeros((8, d), F32) for _ in range(3)]
        for k in range(0, ROWS, CHUNK):
            rows = slice(k, k + CHUNK)
            gout = base_ref[rows, :]
            if add_ref is not None:
                gout = gout + add_ref[rows, :]
            xh = xh_in[0, rows, :]
            gx = gout * xh
            t = gout * gain
            inner = jnp.mean(gx * gain, axis=-1, keepdims=True)
            dh = rs_in[0, rs_slot, rows, :][:, :1] * (t - jnp.mean(t, axis=-1, keepdims=True) - xh * inner)
            t_ref[rows, :] = dh
            low = dh.astype(BF)
            low_out[0, rows, :] = low
            sums = [v + colsum(w) for v, w in zip(sums, (gx, gout, low.astype(F32)))]
        gn_out[layer, slot] += sums[0]
        gn_out[layer, slot + 1] += sums[1]
        gb_out[layer, low_slot] += sums[2]

    norm_back(g_ref, None, xh2_in, 1, norm[layer, 2:3, :], 2, df_out, 3)
    ff = wup.shape[-1]

    def ffn_step():
        cols = slice(0, ff)
        dg = dot_rt(df_out[0], wdn[layer, cols, :])
        du = (dg * gp_in[0, :, cols].astype(F32)).astype(BF)
        du_out[0, :, cols] = du
        gub_out[layer, :, cols] += colsum(du.astype(F32))

    ffn_step()
    acc_ref[...] = dot_rt(du_out[0], wup[layer])
    norm_back(t_ref, acc_ref, xh1_in, 0, norm[layer, 0:1, :], 0, dao_out, 2)
    dc_ref[...] = dot_rt(dao_out[0], wo[layer]).astype(BF)

    low_half = lane_ids((SEG, 128)) < HD
    scale = HD ** -0.5

    def heads_of(v):
        zero = jnp.zeros_like(v)
        return jnp.concatenate([jnp.where(low_half, v, zero), jnp.where(low_half, zero, v)], axis=0)

    for i in range(MB):
        r0 = i * SEG
        for g0 in range(0, HEADS // 2, GROUP_B):
            pairs = range(g0, g0 + GROUP_B)

            def part(j, pair):
                return qkv[0, r0 : r0 + SEG, j * d + pair * 128 : j * d + pair * 128 + 128]

            def probs(pair):
                u0 = (i * (HEADS // 2) + pair) * 2 * SEG
                return p_in[0, u0 : u0 + 2 * SEG, :]

            def out(j, pair, v):
                dqkv_out[0, r0 : r0 + SEG, j * d + pair * 128 : j * d + pair * 128 + 128] = v.astype(BF)

            dc2 = [heads_of(dc_ref[r0 : r0 + SEG, p * 128 : p * 128 + 128]) for p in pairs]
            dp = [dot_rt(v, part(2, p)) for v, p in zip(dc2, pairs)]
            for p, v in zip(pairs, dc2):
                out(2, p, dot_lt(probs(p), v))
            pdp = [probs(p).astype(F32) * v for p, v in zip(pairs, dp)]
            ds = [
                (v - probs(p).astype(F32) * jnp.sum(v, axis=-1, keepdims=True)).astype(BF) for p, v in zip(pairs, pdp)
            ]
            dq2 = [dot(v, part(1, p)) for v, p in zip(ds, pairs)]
            dk = [dot_lt(v, heads_of(part(0, p))) for v, p in zip(ds, pairs)]
            for p, a, b in zip(pairs, dq2, dk):
                out(0, p, jnp.where(low_half, a[:SEG], a[SEG:]) * scale)
                out(1, p, b * scale)

    gb_out[layer, 0] += colsum(dqkv_out[0, :, 0:d].astype(F32))
    gb_out[layer, 1] += colsum(dqkv_out[0, :, 2 * d : 3 * d].astype(F32))
    g_ref[...] = (
        t_ref[...]
        + dot_rt(dqkv_out[0, :, 0:d], wqkv[layer, 0])
        + dot_rt(dqkv_out[0, :, d : 2 * d], wqkv[layer, 1])
        + dot_rt(dqkv_out[0, :, 2 * d : 3 * d], wqkv[layer, 2])
    )

    @pl.when(layer == 0)
    def _():
        for i in range(MB):
            tg_out[i, 0] = g_ref[i * SEG : i * SEG + TEXT, :].astype(BF)
            tail = g_ref[i * SEG + TAIL : (i + 1) * SEG, :]
            back = tail + pltpu.roll(tail, MEM, axis=0)
            gm_ref[i] = jnp.where(seg < counts[i], 0.0, gm_ref[i]) + back
        gm_out[...] = gm_ref[...]


def backward_local(cot, cot_mem, counts, lens, kept, weights):
    wqkv, wo, wup, wdn, _, _, norm = weights
    _, qkv, p_all, _, _, _, gp, xh1, xh2, rs = kept
    d, ff = wup.shape[1:]
    gm0 = jnp.concatenate([jnp.zeros((MB, TEXT - TAIL + MEM, d), F32), cot_mem.astype(F32)], axis=1)
    total = SEGS * ROWS
    units = MB * HEADS * SEG
    smem = pl.BlockSpec(memory_space=pltpu.SMEM)
    hbm = pl.BlockSpec(memory_space=pl.ANY)

    def kept_spec(rows, cols):
        return pl.BlockSpec((1, rows, cols), lambda s, l: (LAYERS - 1 - l, SEGS - 1 - s, 0))

    outs = pl.pallas_call(
        bwd_kernel,
        grid=(SEGS, LAYERS),
        in_specs=[
            smem, smem,
            pl.BlockSpec((MB, 1, TEXT, d), lambda s, l: (0, SEGS - 1 - s, 0, 0)),
            whole(gm0.shape),
            kept_spec(ROWS, 3 * d), kept_spec(units, 128), kept_spec(ROWS, ff), kept_spec(ROWS, d), kept_spec(ROWS, d),
            pl.BlockSpec((1, 2, ROWS, 128), lambda s, l: (LAYERS - 1 - l, 0, SEGS - 1 - s, 0)),
            hbm, hbm, hbm, hbm, whole(norm.shape),
        ],
        out_specs=[
            pl.BlockSpec((MB, 1, TEXT, d), lambda s, l: (0, SEGS - 1 - s, 0, 0)),
            whole(gm0.shape),
            kept_spec(ROWS, 3 * d), kept_spec(ROWS, d), kept_spec(ROWS, ff), kept_spec(ROWS, d),
            whole((LAYERS, 4, 8, d)), whole((LAYERS, 8, ff)), whole((LAYERS, 4, 8, d)),
        ],
        out_shape=[
            jax.ShapeDtypeStruct((MB, SEGS, TEXT, d), BF),
            jax.ShapeDtypeStruct(gm0.shape, F32),
            jax.ShapeDtypeStruct((LAYERS, total, 3 * d), BF),
            jax.ShapeDtypeStruct((LAYERS, total, d), BF),
            jax.ShapeDtypeStruct((LAYERS, total, ff), BF),
            jax.ShapeDtypeStruct((LAYERS, total, d), BF),
            jax.ShapeDtypeStruct((LAYERS, 4, 8, d), F32),
            jax.ShapeDtypeStruct((LAYERS, 8, ff), F32),
            jax.ShapeDtypeStruct((LAYERS, 4, 8, d), F32),
        ],
        scratch_shapes=[
            pltpu.VMEM((ROWS, d), F32), pltpu.VMEM(gm0.shape, F32),
            pltpu.VMEM((ROWS, d), F32), pltpu.VMEM((ROWS, d), F32), pltpu.VMEM((ROWS, d), BF),
            pltpu.VMEM(wqkv.shape, BF), pltpu.VMEM(wo.shape, BF), pltpu.VMEM(wup.shape, BF), pltpu.VMEM(wdn.shape, BF),
            pltpu.SemaphoreType.DMA((LAYERS, 4)),
        ],
        compiler_params=pltpu.CompilerParams(
            dimension_semantics=("arbitrary", "arbitrary"), vmem_limit_bytes=VMEM_LIMIT
        ),
        name="rmt_backward",
    )(counts, lens, cot, gm0, qkv, p_all, gp, xh1, xh2, rs, wqkv, wo, wup, wdn, norm.astype(F32))
    tg, gm = outs[:2]
    small = (outs[6].sum(axis=2), outs[7].sum(axis=1), outs[8].sum(axis=2))
    return tg, gm[:, TEXT - TAIL + MEM :].astype(BF), outs[2:6], small


def weight_grads(kept, grads):
    a, _, _, c, y, g = kept[:6]
    dqkv, dao, du, df = grads

    def product(lhs, rhs):
        dims = (((1,), (1,)), ((0,), (0,)))
        return lax.dot_general(lhs, rhs, dims, preferred_element_type=F32).astype(BF)

    return product(a, dqkv), product(c, dao), product(y, du), product(g, df)


MESH = pl.DeviceIdType.MESH
ZN = 4


def multiple(v, k):
    return v if isinstance(v, int) else pl.multiple_of(v, k)


def span(start, size):
    return pl.ds(multiple(start, size if size % 128 else 128), size)


def where_am_i():
    w, n = lax.axis_index("wide"), lax.axis_index("narrow")
    z, x = lax.div(w, 2), lax.rem(w, 2)
    y, c = lax.div(n, 2), lax.rem(n, 2)
    links = {
        "p": {"wide": w, "narrow": n + 1 - 2 * c},
        "x": {"wide": w + 1 - 2 * x, "narrow": n},
        "y": {"wide": w, "narrow": lax.rem(n + 2, 4)},
        "up": {"wide": w + 2, "narrow": n},
        "down": {"wide": w - 2, "narrow": n},
    }
    return w, n, z, x, y, c, links


def enter(z, links):
    barrier = pltpu.get_barrier_semaphore()
    for name in ("p", "x", "y"):
        pl.semaphore_signal(barrier, inc=1, device_id=links[name], device_id_type=MESH)

    @pl.when(z < ZN - 1)
    def _():
        pl.semaphore_signal(barrier, inc=1, device_id=links["up"], device_id_type=MESH)

    @pl.when(z > 0)
    def _():
        pl.semaphore_signal(barrier, inc=1, device_id=links["down"], device_id_type=MESH)

    pl.semaphore_wait(barrier, 3 + jnp.minimum(z, 1) + jnp.minimum(ZN - 1 - z, 1))


class Net:
    def __init__(self, ssem, rsem, links):
        self.ssem, self.rsem, self.links = ssem, rsem, links
        self.next_send, self.next_recv = 0, 0

    def sends(self, count):
        base, self.next_send = self.next_send, self.next_send + count
        return base

    def recvs(self, count):
        base, self.next_recv = self.next_recv, self.next_recv + count
        return base

    def copy(self, link, src, dst, s, r):
        return pltpu.make_async_remote_copy(
            src_ref=src, dst_ref=dst, send_sem=self.ssem.at[s], recv_sem=self.rsem.at[r],
            device_id=self.links[link], device_id_type=MESH,
        )


def gather_kernel(
    q_in, o_in, u_in, d_in, s_in, Q, O, U, D, S,
    tq, to, tu, td, aq, ao, au, ad, ssem, rsem, lsem,
):
    w, n, z, x, y, c, links = where_am_i()
    mine, other = c, 1 - c
    net = Net(ssem, rsem, links)
    rw, cn = aq.shape[1], aq.shape[2]
    rd, cu = ad.shape[0], au.shape[1]
    half = cu // 2
    enter(z, links)

    first = [net.copy("p", src, dst, net.sends(1), net.recvs(1)) for src, dst in (
        (q_in.at[other], tq), (o_in.at[other], to), (u_in.at[other], tu), (d_in.at[other], td),
        (s_in, S.at[z, x, y, c]),
    )]
    for cp in first:
        cp.start()
    own_small = pltpu.make_async_copy(s_in, S.at[z, x, y, c], lsem.at[4])
    own_small.start()

    def join(own, got):
        a, b = own.astype(F32), got.astype(F32)
        lo, hi = jnp.where(c == 0, a, b), jnp.where(c == 0, b, a)
        return jnp.concatenate([lo, hi], axis=-1).astype(BF)

    outs = (
        (au, U.at[mine, span(rw * w, rw), span(cu * y, cu)]),
        (aq, Q.at[mine, :, span(rw * w, rw), span(cn * y, cn)]),
        (ao, O.at[mine, span(rw * w, rw), span(cn * y, cn)]),
        (ad, D.at[mine, span(rd * w, rd), span(cn * y, cn)]),
    )
    first[2].wait()
    au[...] = join(u_in[mine], tu[...])
    first[0].wait()
    for j in range(3):
        aq[j] = join(q_in[mine, j], tq[j])
    first[1].wait()
    ao[...] = join(o_in[mine], to[...])
    first[3].wait()
    ad[...] = join(d_in[mine], td[...])
    first[4].wait()
    own_small.wait()
    local = [pltpu.make_async_copy(src, dst, lsem.at[k]) for k, (src, dst) in enumerate(outs)]
    for cp in local:
        cp.start()
    for cp in local:
        cp.wait()

    def rows_a(zp):
        return span(2 * rw * zp, 2 * rw)

    def reg_a(zp, yp, layer):
        return [Q.at[layer, :, rows_a(zp), span(cn * yp, cn)], O.at[layer, rows_a(zp), span(cn * yp, cn)]]

    def blk_a(wp, yp, layer):
        rows = span(rw * wp, rw)
        return [Q.at[layer, :, rows, span(cn * yp, cn)], O.at[layer, rows, span(cn * yp, cn)]]

    def reg_d(zp, xp, layer):
        return [D.at[layer, span(rd * (2 * zp + xp), rd), :]]

    def blk_d(wp, yp, layer):
        return [D.at[layer, span(rd * wp, rd), span(cn * yp, cn)]]

    def blk_u(zp, xp, yp, layer):
        return [U.at[layer, span(rw * (2 * zp + xp), rw), span(cu * yp, cu)]]

    def blk_u1(zp, xp, yp, layer):
        return [U.at[layer, span(rw * (2 * zp + xp), rw), span(cu * yp, half)]]

    def blk_u2(zp, xp, yp, layer):
        return [U.at[layer, span(rw * (2 * zp + xp), rw), span(cu * yp + half, half)]]

    def pair_u1(zp, yp, layer):
        return [U.at[layer, rows_a(zp), span(cu * yp, half)]]

    def pair_u2(zp, xp, layer):
        return blk_u2(zp, xp, 0, layer) + blk_u2(zp, xp, 1, layer)

    class Lane:
        def __init__(self, link, sent, got, parts):
            self.link, self.sent, self.got, self.parts = link, sent, got, parts
            self.s = [net.sends(ZN) for _ in range(parts)]
            self.r = [net.recvs(ZN) for _ in range(parts)]

        def send(self, zp):
            for k, ref in enumerate(self.sent(zp)):
                net.copy(self.link, ref, ref, self.s[k] + zp, self.r[k] + zp).start()

        def recv(self, zp):
            for k, ref in enumerate(self.got(zp)):
                net.copy(self.link, ref, ref, self.s[k] + zp, self.r[k] + zp).wait_recv()

        def drain(self, zp):
            for k, ref in enumerate(self.sent(zp)):
                net.copy(self.link, ref, ref, self.s[k] + zp, self.r[k] + zp).wait_send()

    class Line:
        def __init__(self, region, parts):
            self.region, self.parts = region, parts
            self.su = [net.sends(ZN) for _ in range(parts)]
            self.sd = [net.sends(ZN) for _ in range(parts)]
            self.r = [net.recvs(ZN) for _ in range(parts)]

        def each(self, link, sems, zp, what):
            for k, ref in enumerate(self.region(zp)):
                getattr(net.copy(link, ref, ref, sems[k] + zp, self.r[k] + zp), what)()

        def own(self, what="start"):
            @pl.when(z < ZN - 1)
            def _():
                self.each("up", self.su, z, what)

            @pl.when(z > 0)
            def _():
                self.each("down", self.sd, z, what)

        def relay(self, t, what="start"):
            @pl.when(jnp.minimum(z - t, ZN - 2 - z) >= 0)
            def _():
                self.each("up", self.su, z - t, what)

            @pl.when(jnp.minimum(ZN - 1 - t - z, z - 1) >= 0)
            def _():
                self.each("down", self.sd, z + t, what)

        def recv(self, zp):
            self.each("up", self.su, zp, "wait_recv")

    line_a = Line(lambda zp: reg_a(zp, y, mine), 2)
    line_d = Line(lambda zp: reg_d(zp, x, mine), 1)
    line_u = Line(lambda zp: blk_u(zp, x, y, mine), 1)
    x1 = Lane("x", lambda zp: blk_a(w, y, mine), lambda zp: blk_a(w + 1 - 2 * x, y, mine), 2)
    y1 = Lane("y", lambda zp: blk_d(w, y, mine), lambda zp: blk_d(w, 1 - y, mine), 1)
    x_u1 = Lane("x", lambda zp: blk_u1(zp, x, y, mine), lambda zp: blk_u1(zp, 1 - x, y, mine), 1)
    y_u2 = Lane("y", lambda zp: blk_u2(zp, x, y, mine), lambda zp: blk_u2(zp, x, 1 - y, mine), 1)
    y_a = Lane("y", lambda zp: reg_a(zp, y, mine), lambda zp: reg_a(zp, 1 - y, mine), 2)
    x_d = Lane("x", lambda zp: reg_d(zp, x, mine), lambda zp: reg_d(zp, 1 - x, mine), 1)
    y_u1 = Lane("y", lambda zp: pair_u1(zp, y, mine), lambda zp: pair_u1(zp, 1 - y, mine), 1)
    x_u2 = Lane("x", lambda zp: pair_u2(zp, x, mine), lambda zp: pair_u2(zp, 1 - x, mine), 2)

    def to_partner(make, parts):
        return Lane("p", lambda zp: make(zp, mine), lambda zp: make(zp, other), parts)

    p_a = to_partner(lambda zp, l: reg_a(zp, y, l), 2)
    p_a2 = to_partner(lambda zp, l: reg_a(zp, 1 - y, l), 2)
    p_d = to_partner(lambda zp, l: reg_d(zp, x, l), 1)
    p_d2 = to_partner(lambda zp, l: reg_d(zp, 1 - x, l), 1)
    p_u1 = to_partner(lambda zp, l: pair_u1(zp, y, l), 1)
    p_u1b = to_partner(lambda zp, l: pair_u1(zp, 1 - y, l), 1)
    p_u2 = to_partner(lambda zp, l: pair_u2(zp, x, l), 2)
    p_u2b = to_partner(lambda zp, l: pair_u2(zp, 1 - x, l), 2)

    small_x = Lane("x", lambda zp: [S.at[z, x, y]], lambda zp: [S.at[z, 1 - x, y]], 1)
    small_y = Lane("y", lambda zp: [S.at[z, :, y]], lambda zp: [S.at[z, :, 1 - y]], 1)
    line_s = Line(lambda zp: [S.at[zp]], 1)

    line_u.own()
    x1.send(0)
    y1.send(0)
    small_x.send(0)
    x_u1.send(z)
    y_u2.send(z)
    small_x.recv(0)
    small_y.send(0)
    x1.recv(0)
    line_a.own()
    y_a.send(z)
    p_a.send(z)
    y1.recv(0)
    line_d.own()
    x_d.send(z)
    p_d.send(z)
    small_y.recv(0)
    line_s.own()

    def second(zp):
        x_u1.recv(zp)
        y_u1.send(zp)
        p_u1.send(zp)
        y_u2.recv(zp)
        x_u2.send(zp)
        p_u2.send(zp)

    def third(zp):
        y_a.recv(zp)
        p_a2.send(zp)
        x_d.recv(zp)
        p_d2.send(zp)
        y_u1.recv(zp)
        p_u1b.send(zp)
        x_u2.recv(zp)
        p_u2b.send(zp)

    def both_ways(t, make):
        @pl.when(z >= t)
        def _():
            make(z - t)

        @pl.when(z < ZN - t)
        def _():
            make(z + t)

    def take(line, t, *lanes):
        both_ways(t, line.recv)
        line.relay(t)
        for lane in lanes:
            both_ways(t, lane.send)

    second(z)
    for t in range(1, ZN):
        take(line_u, t, x_u1, y_u2)
        take(line_a, t, y_a, p_a)
        if t == 1:
            third(z)
        else:
            both_ways(t - 1, third)
        take(line_d, t, x_d, p_d)
        both_ways(t, second)
        take(line_s, t)
    both_ways(ZN - 1, third)

    partner = (p_a, p_a2, p_d, p_d2, p_u1, p_u1b, p_u2, p_u2b)
    for zp in range(ZN):
        for lane in partner:
            lane.recv(zp)
    for zp in range(ZN):
        for lane in partner + (x_u1, y_u2, y_a, x_d, y_u1, x_u2):
            lane.drain(zp)
    for lane in (x1, y1, small_x, small_y):
        lane.drain(0)
    for line in (line_u, line_a, line_d, line_s):
        line.own("wait_send")
        for t in range(1, ZN):
            line.relay(t, "wait_send")
    assert net.next_send <= ssem.shape[0] and net.next_recv <= rsem.shape[0]


def gather_fast(pieces):
    wqkv, wo, wup, wdn, bias, ubias, norm = pieces
    _, _, rw, cn = wqkv.shape
    rd, cu = wdn.shape[1], wup.shape[2]
    d, ff = rw * 8, rd * 8
    small = jnp.concatenate([bias[:, 0], norm[:, 0], ubias, jnp.zeros_like(ubias)], axis=0).astype(F32)
    small = jnp.pad(small, ((0, 0), (0, 128 - rw)))
    hbm = pl.BlockSpec(memory_space=pl.ANY)
    vmem = pl.BlockSpec(memory_space=pltpu.VMEM)
    Q, O, U, D, S = pl.pallas_call(
        gather_kernel,
        in_specs=[vmem] * 5,
        out_specs=[hbm] * 5,
        out_shape=[
            jax.ShapeDtypeStruct((LAYERS, 3, d, d), BF),
            jax.ShapeDtypeStruct((LAYERS, d, d), BF),
            jax.ShapeDtypeStruct((LAYERS, d, ff), BF),
            jax.ShapeDtypeStruct((LAYERS, ff, d), BF),
            jax.ShapeDtypeStruct((ZN, 2, 2, 2, 8, 128), F32),
        ],
        scratch_shapes=[
            pltpu.VMEM((3, rw, cn), BF), pltpu.VMEM((rw, cn), BF), pltpu.VMEM((rw, cu), BF), pltpu.VMEM((rd, cn), BF),
            pltpu.VMEM((3, rw, 2 * cn), BF), pltpu.VMEM((rw, 2 * cn), BF),
            pltpu.VMEM((rw, 2 * cu), BF), pltpu.VMEM((rd, 2 * cn), BF),
            pltpu.SemaphoreType.DMA((160,)), pltpu.SemaphoreType.DMA((160,)), pltpu.SemaphoreType.DMA((5,)),
        ],
        compiler_params=pltpu.CompilerParams(collective_id=1, has_side_effects=True),
        name="weight_gather",
    )(wqkv, wo, wup, wdn, small)
    S = S.reshape(8, 4, 8, 128)[..., :rw]
    rows = jnp.transpose(S, (2, 1, 0, 3)).reshape(8, 4, d)
    ub = jnp.transpose(S[:, :, 4:6], (2, 0, 1, 3)).reshape(2, ff)
    return Q, O, U, D, rows[0:2], ub, rows[2:4]


def accumulate(dst, src, rows, step=48):
    def body(i, carry):
        r = pl.ds(pl.multiple_of(i * step, 16), step)
        dst[r, :] = dst[r, :] + src[r, :]
        return carry

    lax.fori_loop(0, rows // step, body, 0)


def scatter_kernel(
    gq, go, gu, gd, sm_in, oq, oo, ou, od, sm_out,
    AQ, AO, AU, AD, PQ, PO, PU, PD, FA, FO, FD, F1, F2, S1, S2, ZA, ZO, ZD, ZU, TA, TO, TD,
    hq, ho, hu, hd, s_p, s_x, s_y, s_below, s_above, s_a, s_b, s_sum, s_up, s_down, ssem, rsem, lsem,
):
    w, n, z, x, y, c, links = where_am_i()
    mine, other = c, 1 - c
    net = Net(ssem, rsem, links)
    d, ff = AO.shape[1], AU.shape[1]
    rw, cn = d // 8, d // 2
    rd, cu = ff // 8, ff // 2
    half = cu // 2
    enter(z, links)

    class Hop:
        def __init__(self, link, pairs, parts):
            self.link, self.pairs = link, pairs
            self.s = [net.sends(ZN) for _ in range(parts)]
            self.r = [net.recvs(ZN) for _ in range(parts)]

        def each(self, zp, what):
            for k, (src, dst) in enumerate(self.pairs(zp)):
                getattr(net.copy(self.link, src, dst, self.s[k] + zp, self.r[k] + zp), what)()

        def send(self, zp):
            self.each(zp, "start")

        def recv(self, zp):
            self.each(zp, "wait_recv")

        def drain(self, zp):
            self.each(zp, "wait_send")

    def rows_a(zp):
        return span(2 * rw * zp, 2 * rw)

    def slab(zp, layer, q, o, u, dn):
        rows = rows_a(zp)
        down = span(2 * rd * zp, 2 * rd)
        return [(gq.at[layer, rows, j * d : (j + 1) * d], q.at[j, rows, :]) for j in range(3)] + [
            (go.at[layer, rows, :], o.at[rows, :]),
            (gd.at[layer, down, :], dn.at[down, :]),
            (gu.at[layer, rows, :], u.at[rows, :]),
        ]

    def own_loads(zp):
        return [
            pltpu.make_async_copy(src, dst, lsem.at[k * ZN + zp])
            for k, (src, dst) in enumerate(slab(zp, mine, AQ, AO, AU, AD))
        ]

    swap = Hop("p", lambda zp: slab(zp, other, PQ, PO, PU, PD), 6)

    def cols_a(yp):
        return span(cn * yp, cn)

    def rows_x(zp, xp):
        return span(rw * (2 * zp + xp), rw)

    def rows_d(zp, xp):
        return span(rd * (2 * zp + xp), rd)

    def reg_a(zp, yp):
        return AQ.at[:, rows_a(zp), cols_a(yp)], AO.at[rows_a(zp), cols_a(yp)]

    def reg_d(zp, xp):
        return AD.at[rows_d(zp, xp), :]

    def u1(zp, yp):
        return AU.at[rows_a(zp), span(cu * yp, half)]

    def u1_part(zp, xp, yp):
        return AU.at[rows_x(zp, xp), span(cu * yp, half)]

    def u2(zp, xp, yp):
        return AU.at[rows_x(zp, xp), span(cu * yp + half, half)]

    def blk_u(zp):
        return AU.at[rows_x(zp, x), span(cu * y, cu)]

    y_a = Hop("y", lambda zp: list(zip(reg_a(zp, 1 - y), (FA.at[zp], FO.at[zp]))), 2)
    x_d = Hop("x", lambda zp: [(reg_d(zp, 1 - x), FD.at[zp])], 1)
    y_u1 = Hop("y", lambda zp: [(u1(zp, 1 - y), F1.at[zp])], 1)
    x_u2 = Hop("x", lambda zp: [(u2(zp, 1 - x, yp), F2.at[yp, zp]) for yp in range(2)], 2)
    x_u1 = Hop("x", lambda zp: [(u1_part(zp, 1 - x, y), S1.at[zp])], 1)
    y_u2 = Hop("y", lambda zp: [(u2(zp, x, 1 - y), S2.at[zp])], 1)
    last_a = Hop("x", lambda zp: [
        (AQ.at[:, rows_x(z, 1 - x), cols_a(y)], TA), (AO.at[rows_x(z, 1 - x), cols_a(y)], TO)
    ], 2)
    last_d = Hop("y", lambda zp: [(AD.at[rows_d(z, x), cols_a(1 - y)], TD)], 1)

    class Line:
        def __init__(self, region, bufs):
            self.region, self.bufs = region, bufs
            self.su = [net.sends(ZN) for _ in bufs]
            self.sd = [net.sends(ZN) for _ in bufs]
            self.r = [net.recvs(ZN + 1) for _ in bufs]

        def up(self, zp, what):
            slot = jnp.where(zp == z + 1, ZN, zp)

            @pl.when(zp > z)
            def _():
                for k, (src, buf) in enumerate(zip(self.region(zp), self.bufs)):
                    getattr(net.copy("up", src, buf.at[slot], self.su[k] + zp, self.r[k] + slot), what)()

        def down(self, zp, what):
            @pl.when(zp < z)
            def _():
                for k, (src, buf) in enumerate(zip(self.region(zp), self.bufs)):
                    getattr(net.copy("down", src, buf.at[zp], self.sd[k] + zp, self.r[k] + zp), what)()

        def take(self, zp, slot):
            for k, (dst, buf) in enumerate(zip(self.region(zp), self.bufs)):
                net.copy("up", dst, buf.at[slot], self.su[k] + zp, self.r[k] + slot).wait_recv()
                self.add(dst, buf.at[slot])

        def add(self, dst, src):
            if len(src.shape) == 3:
                for j in range(src.shape[0]):
                    accumulate(dst.at[j], src.at[j], src.shape[1])
            else:
                accumulate(dst, src, src.shape[0])

        def go(self, zp):
            @pl.when(jnp.minimum(z - zp, ZN - 2 - z) >= 0)
            def _():
                self.take(zp, zp)

            @pl.when(jnp.minimum(zp - z, z - 1) >= 0)
            def _():
                self.take(zp, jnp.where(zp == z, ZN, zp))

            self.up(zp, "start")
            self.down(zp, "start")

        def drain(self, zp):
            self.up(zp, "wait_send")
            self.down(zp, "wait_send")

    line_a = Line(lambda zp: reg_a(zp, y), (ZA, ZO))
    line_d = Line(lambda zp: (reg_d(zp, x),), (ZD,))
    line_u = Line(lambda zp: (blk_u(zp),), (ZU,))

    table = ((3, 3, 0, 0), (2, 0, 3, 1), (1, 2, 1, 2), (0, 1, 2, 3))
    order = [jnp.where(z == 0, t[0], jnp.where(z == 1, t[1], jnp.where(z == 2, t[2], t[3]))) for t in table]

    small = [
        net.copy(link, src, dst, net.sends(1), net.recvs(1))
        for link, src, dst in (("p", sm_in, s_p), ("x", s_a, s_x), ("y", s_b, s_y))
    ]
    small_up = net.copy("up", s_up, s_below, net.sends(1), net.recvs(1))
    small_down = net.copy("down", s_down, s_above, net.sends(1), net.recvs(1))

    small[0].start()
    for zp in order:
        for cp in own_loads(zp):
            cp.start()
        swap.send(zp)

    def open_slab(zp):
        for cp in own_loads(zp):
            cp.wait()
        swap.recv(zp)
        rows = rows_a(zp)
        for j in range(3):
            accumulate(AQ.at[j, rows, :], PQ.at[j, rows, :], 2 * rw)
        accumulate(AO.at[rows, :], PO.at[rows, :], 2 * rw)
        y_a.send(zp)
        down = span(2 * rd * zp, 2 * rd)
        accumulate(AD.at[down, :], PD.at[down, :], 2 * rd)
        x_d.send(zp)
        accumulate(AU.at[rows, :], PU.at[rows, :], 2 * rw, 16)
        y_u1.send(zp)
        x_u2.send(zp)

    def middle(zp):
        y_a.recv(zp)
        qa, oa = reg_a(zp, y)
        for j in range(3):
            accumulate(qa.at[j], FA.at[zp, j], 2 * rw)
        accumulate(oa, FO.at[zp], 2 * rw)
        line_a.go(zp)
        x_d.recv(zp)
        accumulate(reg_d(zp, x), FD.at[zp], rd)
        line_d.go(zp)
        y_u1.recv(zp)
        accumulate(u1(zp, y), F1.at[zp], 2 * rw)
        x_u1.send(zp)
        x_u2.recv(zp)
        for yp in range(2):
            accumulate(u2(zp, x, yp), F2.at[yp, zp], rw)
        y_u2.send(zp)

    def close(zp):
        x_u1.recv(zp)
        accumulate(u1_part(zp, x, y), S1.at[zp], rw)
        y_u2.recv(zp)
        accumulate(u2(zp, x, y), S2.at[zp], rw)
        line_u.go(zp)

    open_slab(order[0])
    small[0].wait()
    s_a[...] = sm_in[...] + s_p[...]
    small[1].start()
    open_slab(order[1])
    middle(order[0])
    small[1].wait()
    s_b[...] = s_a[...] + s_x[...]
    small[2].start()
    open_slab(order[2])
    close(order[0])
    middle(order[1])
    small[2].wait()
    s_sum[...] = s_b[...] + s_y[...]
    open_slab(order[3])
    close(order[1])
    middle(order[2])

    @pl.when(z > 0)
    def _():
        small_up.wait_recv()

    @pl.when(z == 0)
    def _():
        s_below[...] = jnp.zeros_like(s_below)

    @pl.when(z < ZN - 1)
    def _():
        s_up[...] = s_sum[...] + s_below[...]
        small_up.start()

    close(order[2])
    middle(order[3])
    last_a.send(0)
    last_d.send(0)

    @pl.when(z < ZN - 1)
    def _():
        small_down.wait_recv()

    @pl.when(z == ZN - 1)
    def _():
        s_above[...] = jnp.zeros_like(s_above)

    @pl.when(z > 0)
    def _():
        s_down[...] = s_sum[...] + s_above[...]
        small_down.start()

    sm_out[...] = s_sum[...] + s_below[...] + s_above[...]
    close(order[3])

    def pick(v, k):
        lo, hi = v[..., :k], v[..., k:]
        return jnp.where(c == 0, lo, hi), jnp.where(c == 0, hi, lo)

    out = [
        net.copy("p", src, dst.at[mine], net.sends(1), net.recvs(1))
        for src, dst in ((hu, ou), (hq, oq), (ho, oo), (hd, od))
    ]
    rows = rows_x(z, x)
    ou[mine] = AU[rows, span(cu * y + half * c, half)].astype(F32)
    hu[...] = AU[rows, span(cu * y + half * (1 - c), half)].astype(F32)
    out[0].start()
    last_a.recv(0)
    for j in range(3):
        keep, give = pick(AQ[j, rows, cols_a(y)].astype(F32) + TA[j].astype(F32), cn // 2)
        oq[mine, j] = keep
        hq[j] = give
    out[1].start()
    keep, give = pick(AO[rows, cols_a(y)].astype(F32) + TO[...].astype(F32), cn // 2)
    oo[mine] = keep
    ho[...] = give
    out[2].start()
    last_d.recv(0)
    for k in range(rd // rw):
        part = pl.ds(k * rw, rw)
        here = span(rd * w + k * rw, rw)
        keep, give = pick(AD[here, cols_a(y)].astype(F32) + TD[part, :].astype(F32), cn // 2)
        od[mine, part, :] = keep
        hd[part, :] = give
    out[3].start()

    for zp in range(ZN):
        for hop in (swap, y_a, x_d, y_u1, x_u2, x_u1, y_u2):
            hop.drain(zp)
        for line in (line_a, line_d, line_u):
            line.drain(zp)
    last_a.drain(0)
    last_d.drain(0)

    @pl.when(z < ZN - 1)
    def _():
        small_up.wait_send()

    @pl.when(z > 0)
    def _():
        small_down.wait_send()

    for cp in out:
        cp.wait()
    assert net.next_send <= ssem.shape[0] and net.next_recv <= rsem.shape[0]


def scatter_fast(big, small):
    gq, go, gup, gdn = big
    gb, gub, gn = small
    d, ff = gup.shape[1:]
    rw, cn, rd, cu = d // 8, d // 2, ff // 8, ff // 2
    pack = jnp.concatenate([gb.reshape(-1, d), gub.reshape(-1, d), gn.reshape(-1, d)], axis=0)
    hbm = pl.BlockSpec(memory_space=pl.ANY)
    vmem = pl.BlockSpec(memory_space=pltpu.VMEM)

    def buf(*shape):
        return pltpu.VMEM(shape, BF)

    def wide(*shape):
        return pltpu.VMEM(shape, F32)

    outs = [(3, rw, cn // 2), (rw, cn // 2), (rw, cu // 2), (rd, cn // 2)]
    full = [buf(3, d, d), buf(d, d), buf(d, ff), buf(ff, d)]
    oq, oo, ou, od, total = pl.pallas_call(
        scatter_kernel,
        in_specs=[hbm] * 4 + [vmem],
        out_specs=[vmem] * 5,
        out_shape=[jax.ShapeDtypeStruct((LAYERS,) + s, F32) for s in outs] + [jax.ShapeDtypeStruct(pack.shape, F32)],
        scratch_shapes=full + full + [
            buf(ZN, 3, 2 * rw, cn), buf(ZN, 2 * rw, cn), buf(ZN, rd, d), buf(ZN, 2 * rw, cu // 2),
            buf(2, ZN, rw, cu // 2), buf(ZN, rw, cu // 2), buf(ZN, rw, cu // 2),
            buf(ZN + 1, 3, 2 * rw, cn), buf(ZN + 1, 2 * rw, cn), buf(ZN + 1, rd, d), buf(ZN + 1, rw, cu),
            buf(3, rw, cn), buf(rw, cn), buf(rd, cn),
        ] + [wide(*s) for s in outs] + [wide(*pack.shape)] * 10 + [
            pltpu.SemaphoreType.DMA((140,)), pltpu.SemaphoreType.DMA((120,)), pltpu.SemaphoreType.DMA((6 * ZN,)),
        ],
        compiler_params=pltpu.CompilerParams(collective_id=2, has_side_effects=True, vmem_limit_bytes=VMEM_LIMIT),
        name="gradient_scatter",
    )(gq, go, gup, gdn, pack)
    w, n = lax.axis_index("wide"), lax.axis_index("narrow")
    gb = lax.dynamic_slice(total[0:8].reshape(2, 4, d), (0, n, w * rw), (2, 1, rw))
    gn = lax.dynamic_slice(total[16:24].reshape(2, 4, d), (0, n, w * rw), (2, 1, rw))
    gub = lax.dynamic_slice(total[8:16].reshape(2, ff), (0, (4 * w + n) * rw), (2, rw))
    return oq, oo, ou, od, gb, gub, gn


def gather_weights(pieces):
    wqkv, wo, wup, wdn, bias, ubias, norm = pieces
    narrow = [(wqkv, 3), (wo, 2), (wup, 2), (wdn, 2), (bias, 1), (norm, 1)]
    wqkv, wo, wup, wdn, bias, norm = (lax.all_gather(w, "narrow", axis=k, tiled=True) for w, k in narrow)
    wide = [(wqkv, 2), (wo, 1), (wup, 1), (wdn, 1), (bias, 2), (norm, 2)]
    wqkv, wo, wup, wdn, bias, norm = (lax.all_gather(w, "wide", axis=k, tiled=True) for w, k in wide)
    ubias = lax.all_gather(ubias, ("wide", "narrow"), axis=1, tiled=True)
    return wqkv, wo, wup, wdn, bias, ubias, norm


def scatter_two(grad, row_axis, col_axis):
    low = lax.psum_scatter(grad.astype(BF), "narrow", scatter_dimension=col_axis, tiled=True)
    return lax.psum_scatter(low.astype(F32), "wide", scatter_dimension=row_axis, tiled=True)


def scatter_grads(big, small):
    gq, go, gup, gdn = big
    gq = jnp.moveaxis(gq.reshape(gq.shape[:2] + (3, -1)), 2, 1)
    gb, gub, gn = small
    big = (scatter_two(gq, 2, 3), scatter_two(go, 1, 2), scatter_two(gup, 1, 2), scatter_two(gdn, 1, 2))
    gub = lax.psum_scatter(gub, ("wide", "narrow"), scatter_dimension=1, tiled=True)

    def small_two(g):
        return lax.psum_scatter(
            lax.psum_scatter(g, "narrow", scatter_dimension=1, tiled=True), "wide", scatter_dimension=2, tiled=True
        )

    return big + (small_two(gb), gub, small_two(gn))


def shards(
    near, text_in, memory_in, counts, last_len, cot_text, cot_memory,
    qkv_weight, out_weight, up_weight, down_weight, biases, up_bias, norm_params,
):
    text, cot = text_in[:, 0], cot_text[:, 0]
    mem, cot_mem = memory_in[:, 0], cot_memory[:, 0]
    cnt, lens = counts[:, 0], last_len[:, 0]
    gather = gather_fast if near else gather_weights
    weights = gather((qkv_weight, out_weight, up_weight, down_weight, biases, up_bias, norm_params))
    text_out, mem_out, kept = forward_local(text, mem, cnt, lens, weights)
    text_grad, mem_grad, grads, small = backward_local(cot, cot_mem, cnt, lens, kept, weights)
    scatter = scatter_fast if near else scatter_grads
    grads = scatter(weight_grads(kept, grads), small)
    return (text_out[:, None], mem_out[:, None], text_grad[:, None], mem_grad[:, None]) + grads


def solution(mesh):
    items = ("wide", "narrow")
    act5 = P(None, items, None, None, None)
    act4 = P(None, items, None, None)
    ids = P(None, items)
    split = P(None, "wide", "narrow")
    small = P(None, "narrow", "wide")
    params = (P(None, None, "wide", "narrow"), split, split, split, small, ids, small)
    near = (mesh.shape["wide"], mesh.shape["narrow"]) == (2 * ZN, 4)
    return jax.shard_map(
        functools.partial(shards, near),
        mesh=mesh,
        in_specs=(act5, act4, ids, ids, act5, act4) + params,
        out_specs=(act5, act4, act5, act4) + params,
        check_vma=False,
    )
```

```python
import functools

import jax
import jax.numpy as jnp
from jax import lax
from jax.experimental import pallas as pl
from jax.experimental.pallas import tpu as pltpu
from jax.sharding import PartitionSpec as P

HEADS = 12
HD = 64
MEM = 10
TEXT = 108
SEGS = 4
MB = 2
LAYERS = 2
SEG = TEXT + 2 * MEM
TAIL = 104
ROWS = MB * SEG
EPS = 1e-12
BF = jnp.bfloat16
F32 = jnp.float32
NEG = -1e30
RSQRT2 = 0.7071067811865476
RSQRT2PI = 0.3989422804014327
VMEM_LIMIT = 66_000_000
CHUNK = 32
GROUP_F = 6
GROUP_B = 6


def dot(a, b):
    return lax.dot_general(a, b, (((1,), (0,)), ((), ())), preferred_element_type=F32)


def dot_rt(a, b):
    return lax.dot_general(a, b, (((1,), (1,)), ((), ())), preferred_element_type=F32)


def dot_lt(a, b):
    return lax.dot_general(a, b, (((0,), (0,)), ((), ())), preferred_element_type=F32)


def row_ids(shape):
    return lax.broadcasted_iota(jnp.int32, shape, 0)


def lane_ids(shape):
    return lax.broadcasted_iota(jnp.int32, shape, 1)


def valid_rows(seg, count, length):
    return jnp.where(seg < count - 1, TEXT, jnp.where(seg == count - 1, length, 0))


def colsum(v):
    rows, cols = v.shape
    return jnp.sum(v.reshape(rows // 8, 8, cols), axis=0)


class Loads:
    def __init__(self, pairs, sems, first, order):
        self.pairs, self.sems, self.first, self.order = pairs, sems, first, order

    def each(self, layer, what):
        for k, (src, dst) in enumerate(self.pairs):
            getattr(pltpu.make_async_copy(src.at[layer], dst.at[layer], self.sems.at[layer, k]), what)()

    def start(self):
        self.each(self.order[0], "start")

    def need(self, step):
        @pl.when(self.first & (step == 0))
        def _():
            self.each(self.order[0], "wait")
            self.each(self.order[1], "start")

        @pl.when(self.first & (step == 1))
        def _():
            self.each(self.order[1], "wait")


def fwd_kernel(
    counts, lens, text, mem0, wqkv_hbm, wo_hbm, wup_hbm, wdn_hbm, bias, ubias, norm,
    text_out, mem_out, lhs_out, qkv_out, p_out, gp_out, xh1_out, xh2_out, rs_out,
    x_ref, mem_ref, y_ref, acc_ref, wqkv, wo, wup, wdn, wsem,
):
    seg = pl.program_id(0)
    layer = pl.program_id(1)
    d = x_ref.shape[-1]
    a_out, c_out, y_out = (lhs_out.at[:, :, j * d : (j + 1) * d] for j in range(3))
    g_out = lhs_out.at[:, :, 3 * d :]
    loads = Loads(((wqkv_hbm, wqkv), (wo_hbm, wo), (wup_hbm, wup), (wdn_hbm, wdn)), wsem, seg == 0, (0, 1))

    @pl.when((seg == 0) & (layer == 0))
    def _():
        loads.start()
        mem_ref[...] = mem0[...]

    @pl.when(layer == 0)
    def _():
        for i in range(MB):
            x_ref[i * SEG : i * SEG + TEXT, :] = text[i, 0].astype(F32)
            tail = slice(i * SEG + TAIL, (i + 1) * SEG)
            now = x_ref[tail, :]
            x_ref[tail, :] = jnp.where(row_ids(now.shape) < TEXT - TAIL, now, mem_ref[i])

    loads.need(layer)
    xb = x_ref[...].astype(BF)
    a_out[0] = xb
    qkv_out[0, :, 0:d] = (dot(xb, wqkv[layer, 0]) + bias[layer, 0:1, :]).astype(BF)
    qkv_out[0, :, d : 2 * d] = dot(xb, wqkv[layer, 1]).astype(BF)
    qkv_out[0, :, 2 * d : 3 * d] = (dot(xb, wqkv[layer, 2]) + bias[layer, 1:2, :]).astype(BF)

    low_half = lane_ids((SEG, 128)) < HD
    lanes = lane_ids((1, SEG))

    def heads_of(v):
        zero = jnp.zeros_like(v)
        return jnp.concatenate([jnp.where(low_half, v, zero), jnp.where(low_half, zero, v)], axis=0)

    for i in range(MB):
        vr = valid_rows(seg, counts[i], lens[i])
        keep = (lanes < vr) | (lanes >= TEXT)
        r0 = i * SEG
        for g0 in range(0, HEADS // 2, GROUP_F):
            pairs = range(g0, g0 + GROUP_F)

            def part(j, pair):
                return qkv_out[0, r0 : r0 + SEG, j * d + pair * 128 : j * d + pair * 128 + 128]

            s_all = [dot_rt(heads_of(part(0, p) * (HD ** -0.5)), part(1, p)) for p in pairs]
            s_all = [jnp.where(keep, s, NEG) for s in s_all]
            e_all = [jnp.exp(s - jnp.max(s, axis=-1, keepdims=True)) for s in s_all]
            p_all = [(e * (1.0 / jnp.sum(e, axis=-1, keepdims=True))).astype(BF) for e in e_all]
            c_all = [dot(pv, part(2, p)) for pv, p in zip(p_all, pairs)]
            for p, pv, c2 in zip(pairs, p_all, c_all):
                u0 = (i * (HEADS // 2) + p) * 2 * SEG
                p_out[0, u0 : u0 + 2 * SEG, :] = pv
                c_out[0, r0 : r0 + SEG, p * 128 : p * 128 + 128] = jnp.where(low_half, c2[:SEG], c2[SEG:]).astype(BF)

    def norm_to(base_ref, gain, shift, add, xh_out, rs_index, to_ref, low_out):
        for k in range(0, ROWS, CHUNK):
            rows = slice(k, k + CHUNK)
            h = base_ref[rows, :] + (acc_ref[rows, :] + add)
            center = h - jnp.mean(h, axis=-1, keepdims=True)
            rs = lax.rsqrt(jnp.mean(center * center, axis=-1, keepdims=True) + EPS)
            xh = center * rs
            xh_out[0, rows, :] = xh
            rs_out[0, rs_index, rows, :] = jnp.broadcast_to(rs, (CHUNK, 128))
            out = xh * gain + shift
            to_ref[rows, :] = out
            if low_out is not None:
                low_out[0, rows, :] = out.astype(BF)

    acc_ref[...] = dot(c_out[0], wo[layer])
    norm_to(x_ref, norm[layer, 0:1, :], norm[layer, 1:2, :], bias[layer, 2:3, :], xh1_out, 0, y_ref, y_out)

    ff = wup.shape[-1]

    def ffn_step():
        cols = slice(0, ff)
        u = dot(y_out[0], wup[layer, :, cols]) + ubias[layer, :, cols]
        cdf = 0.5 * (1.0 + lax.erf(u * RSQRT2))
        g_out[0, :, cols] = (u * cdf).astype(BF)
        gp_out[0, :, cols] = (cdf + u * (jnp.exp(-0.5 * (u * u)) * RSQRT2PI)).astype(BF)

    ffn_step()
    acc_ref[...] = dot(g_out[0], wdn[layer])
    norm_to(y_ref, norm[layer, 2:3, :], norm[layer, 3:4, :], bias[layer, 3:4, :], xh2_out, 1, x_ref, None)

    @pl.when(layer == LAYERS - 1)
    def _():
        for i in range(MB):
            vr = valid_rows(seg, counts[i], lens[i])
            body = x_ref[i * SEG : i * SEG + TEXT, :]
            text_out[i, 0] = jnp.where(row_ids(body.shape) < vr, body, 0.0).astype(BF)
            tail = x_ref[i * SEG + TAIL : (i + 1) * SEG, :]
            both = jnp.where(row_ids(tail.shape) >= TEXT - TAIL + MEM, tail, pltpu.roll(tail, SEG - TAIL - MEM, axis=0))
            mem_ref[i] = jnp.where(seg < counts[i], both, mem_ref[i])
        mem_out[...] = mem_ref[...]


def whole(shape):
    return pl.BlockSpec(shape, lambda *_: (0,) * len(shape), pipeline_mode=pl.Buffered(1))


def saved(rows, cols):
    return pl.BlockSpec((1, rows, cols), lambda s, l: (l, s, 0))


def forward_local(text, mem, counts, lens, weights):
    wqkv, wo, wup, wdn, bias, ubias, norm = weights
    d, ff = wup.shape[1:]
    mem0 = jnp.concatenate([jnp.zeros((MB, TEXT - TAIL, d), F32), mem.astype(F32), mem.astype(F32)], axis=1)
    total = SEGS * ROWS
    units = MB * HEADS * SEG
    smem = pl.BlockSpec(memory_space=pltpu.SMEM)
    hbm = pl.BlockSpec(memory_space=pl.ANY)
    outs = pl.pallas_call(
        fwd_kernel,
        grid=(SEGS, LAYERS),
        in_specs=[
            smem, smem,
            pl.BlockSpec((MB, 1, TEXT, d), lambda s, l: (0, s, 0, 0)),
            whole(mem0.shape), hbm, hbm, hbm, hbm,
            whole(bias.shape), whole((LAYERS, 1, ff)), whole(norm.shape),
        ],
        out_specs=[
            pl.BlockSpec((MB, 1, TEXT, d), lambda s, l: (0, s, 0, 0)),
            whole(mem0.shape),
            saved(ROWS, 3 * d + ff), saved(ROWS, 3 * d), saved(units, 128),
            saved(ROWS, ff), saved(ROWS, d), saved(ROWS, d),
            pl.BlockSpec((1, 2, ROWS, 128), lambda s, l: (l, 0, s, 0)),
        ],
        out_shape=[
            jax.ShapeDtypeStruct((MB, SEGS, TEXT, d), BF),
            jax.ShapeDtypeStruct(mem0.shape, F32),
            jax.ShapeDtypeStruct((LAYERS, total, 3 * d + ff), BF),
            jax.ShapeDtypeStruct((LAYERS, total, 3 * d), BF),
            jax.ShapeDtypeStruct((LAYERS, SEGS * units, 128), BF),
            jax.ShapeDtypeStruct((LAYERS, total, ff), BF),
            jax.ShapeDtypeStruct((LAYERS, total, d), F32),
            jax.ShapeDtypeStruct((LAYERS, total, d), F32),
            jax.ShapeDtypeStruct((LAYERS, 2, total, 128), F32),
        ],
        scratch_shapes=[
            pltpu.VMEM((ROWS, d), F32), pltpu.VMEM(mem0.shape, F32),
            pltpu.VMEM((ROWS, d), F32), pltpu.VMEM((ROWS, d), F32),
            pltpu.VMEM(wqkv.shape, BF), pltpu.VMEM(wo.shape, BF), pltpu.VMEM(wup.shape, BF), pltpu.VMEM(wdn.shape, BF),
            pltpu.SemaphoreType.DMA((LAYERS, 4)),
        ],
        compiler_params=pltpu.CompilerParams(
            dimension_semantics=("arbitrary", "arbitrary"), vmem_limit_bytes=VMEM_LIMIT
        ),
        name="rmt_forward",
    )(counts, lens, text, mem0, wqkv, wo, wup, wdn, bias.astype(F32), ubias.astype(F32)[:, None, :], norm.astype(F32))
    text_out, mem_end = outs[:2]
    return text_out, mem_end[:, TEXT - TAIL + MEM :].astype(BF), outs[2:]


def bwd_kernel(
    counts, lens, cot, gm0, qkv, p_in, gp_in, xh1_in, xh2_in, rs_in, wqkv_hbm, wo_hbm, wup_hbm, wdn_hbm, norm,
    tg_out, gm_out, rhs_out, small_out,
    g_ref, gm_ref, t_ref, acc_ref, dc_ref, wqkv, wo, wup, wdn, wsem, gb_out, gub_out, gn_out,
):
    seg = SEGS - 1 - pl.program_id(0)
    step = pl.program_id(1)
    layer = LAYERS - 1 - step
    loads = Loads(((wqkv_hbm, wqkv), (wo_hbm, wo), (wup_hbm, wup), (wdn_hbm, wdn)), wsem, seg == SEGS - 1, (1, 0))
    d = g_ref.shape[-1]
    ff = wup.shape[-1]
    dqkv_out, dao_out = rhs_out.at[:, :, 0 : 3 * d], rhs_out.at[:, :, 3 * d : 4 * d]
    du_out, df_out = rhs_out.at[:, :, 4 * d : 4 * d + ff], rhs_out.at[:, :, 4 * d + ff :]

    @pl.when((seg == SEGS - 1) & (step == 0))
    def _():
        loads.start()
        gm_ref[...] = gm0[...]
        gb_out[...] = jnp.zeros_like(gb_out)
        gub_out[...] = jnp.zeros_like(gub_out)
        gn_out[...] = jnp.zeros_like(gn_out)

    @pl.when(step == 0)
    def _():
        for i in range(MB):
            vr = valid_rows(seg, counts[i], lens[i])
            ct = cot[i, 0].astype(F32)
            g_ref[i * SEG : i * SEG + TEXT, :] = jnp.where(row_ids(ct.shape) < vr, ct, 0.0)
            tail = slice(i * SEG + TAIL, (i + 1) * SEG)
            now = g_ref[tail, :]
            rows = row_ids(now.shape)
            mem_part = jnp.where((rows >= TEXT - TAIL + MEM) & (seg < counts[i]), gm_ref[i], 0.0)
            g_ref[tail, :] = jnp.where(rows < TEXT - TAIL, now, mem_part)

    loads.need(step)

    def norm_back(base_ref, add_ref, xh_in, rs_slot, gain, slot, low_out, low_slot):
        sums = [jnp.zeros((8, d), F32) for _ in range(3)]
        for k in range(0, ROWS, CHUNK):
            rows = slice(k, k + CHUNK)
            gout = base_ref[rows, :]
            if add_ref is not None:
                gout = gout + add_ref[rows, :]
            xh = xh_in[0, rows, :]
            gx = gout * xh
            t = gout * gain
            inner = jnp.mean(gx * gain, axis=-1, keepdims=True)
            dh = rs_in[0, rs_slot, rows, :][:, :1] * (t - jnp.mean(t, axis=-1, keepdims=True) - xh * inner)
            t_ref[rows, :] = dh
            low = dh.astype(BF)
            low_out[0, rows, :] = low
            sums = [v + colsum(w) for v, w in zip(sums, (gx, gout, low.astype(F32)))]
        gn_out[layer, slot] += sums[0]
        gn_out[layer, slot + 1] += sums[1]
        gb_out[layer, low_slot] += sums[2]

    norm_back(g_ref, None, xh2_in, 1, norm[layer, 2:3, :], 2, df_out, 3)

    def ffn_step():
        cols = slice(0, ff)
        dg = dot_rt(df_out[0], wdn[layer, cols, :])
        du = (dg * gp_in[0, :, cols].astype(F32)).astype(BF)
        du_out[0, :, cols] = du
        gub_out[layer, :, cols] += colsum(du.astype(F32))

    ffn_step()
    acc_ref[...] = dot_rt(du_out[0], wup[layer])
    norm_back(t_ref, acc_ref, xh1_in, 0, norm[layer, 0:1, :], 0, dao_out, 2)
    dc_ref[...] = dot_rt(dao_out[0], wo[layer]).astype(BF)

    low_half = lane_ids((SEG, 128)) < HD
    scale = HD ** -0.5

    def heads_of(v):
        zero = jnp.zeros_like(v)
        return jnp.concatenate([jnp.where(low_half, v, zero), jnp.where(low_half, zero, v)], axis=0)

    for i in range(MB):
        r0 = i * SEG
        for g0 in range(0, HEADS // 2, GROUP_B):
            pairs = range(g0, g0 + GROUP_B)

            def part(j, pair):
                return qkv[0, r0 : r0 + SEG, j * d + pair * 128 : j * d + pair * 128 + 128]

            def probs(pair):
                u0 = (i * (HEADS // 2) + pair) * 2 * SEG
                return p_in[0, u0 : u0 + 2 * SEG, :]

            def out(j, pair, v):
                dqkv_out[0, r0 : r0 + SEG, j * d + pair * 128 : j * d + pair * 128 + 128] = v.astype(BF)

            dc2 = [heads_of(dc_ref[r0 : r0 + SEG, p * 128 : p * 128 + 128]) for p in pairs]
            dp = [dot_rt(v, part(2, p)) for v, p in zip(dc2, pairs)]
            for p, v in zip(pairs, dc2):
                out(2, p, dot_lt(probs(p), v))
            pdp = [probs(p).astype(F32) * v for p, v in zip(pairs, dp)]
            ds = [
                (v - probs(p).astype(F32) * jnp.sum(v, axis=-1, keepdims=True)).astype(BF) for p, v in zip(pairs, pdp)
            ]
            dq2 = [dot(v, part(1, p)) for v, p in zip(ds, pairs)]
            dk = [dot_lt(v, heads_of(part(0, p))) for v, p in zip(ds, pairs)]
            for p, a, b in zip(pairs, dq2, dk):
                out(0, p, jnp.where(low_half, a[:SEG], a[SEG:]) * scale)
                out(1, p, b * scale)

    gb_out[layer, 0] += colsum(dqkv_out[0, :, 0:d].astype(F32))
    gb_out[layer, 1] += colsum(dqkv_out[0, :, 2 * d : 3 * d].astype(F32))
    g_ref[...] = (
        t_ref[...]
        + dot_rt(dqkv_out[0, :, 0:d], wqkv[layer, 0])
        + dot_rt(dqkv_out[0, :, d : 2 * d], wqkv[layer, 1])
        + dot_rt(dqkv_out[0, :, 2 * d : 3 * d], wqkv[layer, 2])
    )

    @pl.when(layer == 0)
    def _():
        for i in range(MB):
            tg_out[i, 0] = g_ref[i * SEG : i * SEG + TEXT, :].astype(BF)
            tail = g_ref[i * SEG + TAIL : (i + 1) * SEG, :]
            back = tail + pltpu.roll(tail, MEM, axis=0)
            gm_ref[i] = jnp.where(seg < counts[i], 0.0, gm_ref[i]) + back
        gm_out[...] = gm_ref[...]

    @pl.when((seg == 0) & (layer == 0))
    def _():
        for l in range(LAYERS):
            for k in range(4):
                parts = (gb_out[l, k], gub_out[l, :, k * d : (k + 1) * d], gn_out[l, k])
                for base, part in zip((0, 8, 16), parts):
                    row = base + 4 * l + k
                    small_out[row : row + 1, :] = jnp.sum(part, axis=0, keepdims=True)


def backward_local(cot, cot_mem, counts, lens, kept, weights):
    wqkv, wo, wup, wdn, _, _, norm = weights
    _, qkv, p_all, gp, xh1, xh2, rs = kept
    d, ff = wup.shape[1:]
    gm0 = jnp.concatenate([jnp.zeros((MB, TEXT - TAIL + MEM, d), F32), cot_mem.astype(F32)], axis=1)
    total = SEGS * ROWS
    units = MB * HEADS * SEG
    smem = pl.BlockSpec(memory_space=pltpu.SMEM)
    hbm = pl.BlockSpec(memory_space=pl.ANY)

    def kept_spec(rows, cols):
        return pl.BlockSpec((1, rows, cols), lambda s, l: (LAYERS - 1 - l, SEGS - 1 - s, 0))

    outs = pl.pallas_call(
        bwd_kernel,
        grid=(SEGS, LAYERS),
        in_specs=[
            smem, smem,
            pl.BlockSpec((MB, 1, TEXT, d), lambda s, l: (0, SEGS - 1 - s, 0, 0)),
            whole(gm0.shape),
            kept_spec(ROWS, 3 * d), kept_spec(units, 128), kept_spec(ROWS, ff), kept_spec(ROWS, d), kept_spec(ROWS, d),
            pl.BlockSpec((1, 2, ROWS, 128), lambda s, l: (LAYERS - 1 - l, 0, SEGS - 1 - s, 0)),
            hbm, hbm, hbm, hbm, whole(norm.shape),
        ],
        out_specs=[
            pl.BlockSpec((MB, 1, TEXT, d), lambda s, l: (0, SEGS - 1 - s, 0, 0)),
            whole(gm0.shape),
            kept_spec(ROWS, 5 * d + ff), whole((24, d)),
        ],
        out_shape=[
            jax.ShapeDtypeStruct((MB, SEGS, TEXT, d), BF),
            jax.ShapeDtypeStruct(gm0.shape, F32),
            jax.ShapeDtypeStruct((LAYERS, total, 5 * d + ff), BF),
            jax.ShapeDtypeStruct((24, d), F32),
        ],
        scratch_shapes=[
            pltpu.VMEM((ROWS, d), F32), pltpu.VMEM(gm0.shape, F32),
            pltpu.VMEM((ROWS, d), F32), pltpu.VMEM((ROWS, d), F32), pltpu.VMEM((ROWS, d), BF),
            pltpu.VMEM(wqkv.shape, BF), pltpu.VMEM(wo.shape, BF), pltpu.VMEM(wup.shape, BF), pltpu.VMEM(wdn.shape, BF),
            pltpu.SemaphoreType.DMA((LAYERS, 4)),
            pltpu.VMEM((LAYERS, 4, 8, d), F32), pltpu.VMEM((LAYERS, 8, ff), F32), pltpu.VMEM((LAYERS, 4, 8, d), F32),
        ],
        compiler_params=pltpu.CompilerParams(
            dimension_semantics=("arbitrary", "arbitrary"), vmem_limit_bytes=VMEM_LIMIT
        ),
        name="rmt_backward",
    )(counts, lens, cot, gm0, qkv, p_all, gp, xh1, xh2, rs, wqkv, wo, wup, wdn, norm.astype(F32))
    tg, gm = outs[:2]
    return tg, gm[:, TEXT - TAIL + MEM :].astype(BF), outs[2], outs[3]


TILES = 12


def product_kernel(lhs, rhs, out):
    out[0, 0] = dot_lt(lhs[0], rhs[0]).astype(BF)


def weight_grads(lhs, rhs):
    d = rhs.shape[-1] // 9
    total = lhs.shape[1]

    def left(l, t):
        return (l, 0, jnp.where(t < 3, 0, jnp.where(t < 4, 1, jnp.where(t < 8, 2, t - 5))))

    return pl.pallas_call(
        product_kernel,
        grid=(LAYERS, TILES),
        in_specs=[
            pl.BlockSpec((1, total, d), left),
            pl.BlockSpec((1, total, d), lambda l, t: (l, 0, jnp.minimum(t, 8))),
        ],
        out_specs=pl.BlockSpec((1, 1, d, d), lambda l, t: (l, t, 0, 0)),
        out_shape=jax.ShapeDtypeStruct((LAYERS, TILES, d, d), BF),
        compiler_params=pltpu.CompilerParams(
            dimension_semantics=("arbitrary", "arbitrary"), vmem_limit_bytes=VMEM_LIMIT
        ),
        name="weight_products",
    )(lhs, rhs)


MESH = pl.DeviceIdType.MESH
ZN = 4


def multiple(v, k):
    return v if isinstance(v, int) else pl.multiple_of(v, k)


def span(start, size):
    return pl.ds(multiple(start, size if size % 128 else 128), size)


def where_am_i():
    w, n = lax.axis_index("wide"), lax.axis_index("narrow")
    z, x = lax.div(w, 2), lax.rem(w, 2)
    y, c = lax.div(n, 2), lax.rem(n, 2)
    links = {
        "p": {"wide": w, "narrow": n + 1 - 2 * c},
        "x": {"wide": w + 1 - 2 * x, "narrow": n},
        "y": {"wide": w, "narrow": lax.rem(n + 2, 4)},
        "up": {"wide": w + 2, "narrow": n},
        "down": {"wide": w - 2, "narrow": n},
    }
    return w, n, z, x, y, c, links


def enter(z, links):
    barrier = pltpu.get_barrier_semaphore()
    for name in ("p", "x", "y"):
        pl.semaphore_signal(barrier, inc=1, device_id=links[name], device_id_type=MESH)

    @pl.when(z < ZN - 1)
    def _():
        pl.semaphore_signal(barrier, inc=1, device_id=links["up"], device_id_type=MESH)

    @pl.when(z > 0)
    def _():
        pl.semaphore_signal(barrier, inc=1, device_id=links["down"], device_id_type=MESH)

    pl.semaphore_wait(barrier, 3 + jnp.minimum(z, 1) + jnp.minimum(ZN - 1 - z, 1))


class Net:
    def __init__(self, ssem, rsem, links):
        self.ssem, self.rsem, self.links = ssem, rsem, links
        self.next_send, self.next_recv = 0, 0

    def sends(self, count):
        base, self.next_send = self.next_send, self.next_send + count
        return base

    def recvs(self, count):
        base, self.next_recv = self.next_recv, self.next_recv + count
        return base

    def copy(self, link, src, dst, s, r):
        return pltpu.make_async_remote_copy(
            src_ref=src, dst_ref=dst, send_sem=self.ssem.at[s], recv_sem=self.rsem.at[r],
            device_id=self.links[link], device_id_type=MESH,
        )


def gather_kernel(
    q_in, o_in, u_in, d_in, s_in, Q, O, U, D, S,
    tq, to, tu, td, aq, ao, au, ad, ssem, rsem, lsem,
):
    w, n, z, x, y, c, links = where_am_i()
    mine, other = c, 1 - c
    net = Net(ssem, rsem, links)
    rw, cn = aq.shape[1], aq.shape[2]
    rd, cu = ad.shape[0], au.shape[1]
    half = cu // 2
    enter(z, links)

    first = [net.copy("p", src, dst, net.sends(1), net.recvs(1)) for src, dst in (
        (q_in.at[other], tq), (o_in.at[other], to), (u_in.at[other], tu), (d_in.at[other], td),
        (s_in, S.at[z, x, y, c]),
    )]
    for cp in first:
        cp.start()
    own_small = pltpu.make_async_copy(s_in, S.at[z, x, y, c], lsem.at[4])
    own_small.start()

    def join(own, got):
        a, b = own.astype(F32), got.astype(F32)
        lo, hi = jnp.where(c == 0, a, b), jnp.where(c == 0, b, a)
        return jnp.concatenate([lo, hi], axis=-1).astype(BF)

    outs = (
        (au, U.at[mine, span(rw * w, rw), span(cu * y, cu)]),
        (aq, Q.at[mine, :, span(rw * w, rw), span(cn * y, cn)]),
        (ao, O.at[mine, span(rw * w, rw), span(cn * y, cn)]),
        (ad, D.at[mine, span(rd * w, rd), span(cn * y, cn)]),
    )
    first[2].wait()
    au[...] = join(u_in[mine], tu[...])
    first[0].wait()
    for j in range(3):
        aq[j] = join(q_in[mine, j], tq[j])
    first[1].wait()
    ao[...] = join(o_in[mine], to[...])
    first[3].wait()
    ad[...] = join(d_in[mine], td[...])
    first[4].wait()
    own_small.wait()
    local = [pltpu.make_async_copy(src, dst, lsem.at[k]) for k, (src, dst) in enumerate(outs)]
    for cp in local:
        cp.start()
    for cp in local:
        cp.wait()

    main = rd - rw

    def rows_a(zp):
        return span(2 * rw * zp, 2 * rw)

    def rows_x(zp, xp):
        return span(rw * (2 * zp + xp), rw)

    def rows_d(zp, xp):
        return pl.ds(pl.multiple_of(rd * (2 * zp + xp), rw), main)

    def rows_v(zp, xp):
        return pl.ds(pl.multiple_of(rd * (2 * zp + xp) + main, rw), rw)

    def cols(yp):
        return span(cn * yp, cn)

    def blk_a(zp, xp, yp):
        return [Q.at[mine, :, rows_x(zp, xp), cols(yp)]]

    def blk_d(zp, xp, yp):
        return [D.at[mine, rows_d(zp, xp), cols(yp)]]

    def reg_a(zp, yp, layer):
        return [Q.at[layer, :, rows_a(zp), cols(yp)]]

    def reg_d(zp, xp, layer):
        return [D.at[layer, rows_d(zp, xp), :]]

    def u_cols(zp, xp, start, size):
        return U.at[mine, rows_x(zp, xp), span(start, size)]

    def blk_u(zp, xp, yp):
        return [
            u_cols(zp, xp, cu * yp, cu), O.at[mine, rows_x(zp, xp), cols(yp)], D.at[mine, rows_v(zp, xp), cols(yp)]
        ]

    def blk_u1(zp, xp, yp):
        return [u_cols(zp, xp, cu * yp, half), O.at[mine, rows_x(zp, xp), cols(yp)]]

    def blk_u2(zp, xp, yp):
        return [u_cols(zp, xp, cu * yp + half, half), D.at[mine, rows_v(zp, xp), cols(yp)]]

    def pair_u1(zp, yp, layer):
        return [U.at[layer, rows_a(zp), span(cu * yp, half)], O.at[layer, rows_a(zp), cols(yp)]]

    def pair_u2(zp, xp, layer):
        rows = rows_x(zp, xp)
        return [U.at[layer, rows, span(cu * yp + half, half)] for yp in range(2)] + [D.at[layer, rows_v(zp, xp), :]]

    class Lane:
        def __init__(self, link, sent, got, parts):
            self.link, self.sent, self.got, self.parts = link, sent, got, parts
            self.s = [net.sends(ZN) for _ in range(parts)]
            self.r = [net.recvs(ZN) for _ in range(parts)]

        def send(self, zp):
            for k, ref in enumerate(self.sent(zp)):
                net.copy(self.link, ref, ref, self.s[k] + zp, self.r[k] + zp).start()

        def recv(self, zp):
            for k, ref in enumerate(self.got(zp)):
                net.copy(self.link, ref, ref, self.s[k] + zp, self.r[k] + zp).wait_recv()

        def drain(self, zp):
            for k, ref in enumerate(self.sent(zp)):
                net.copy(self.link, ref, ref, self.s[k] + zp, self.r[k] + zp).wait_send()

    class Line:
        def __init__(self, region, parts):
            self.region, self.parts = region, parts
            self.su = [net.sends(ZN) for _ in range(parts)]
            self.sd = [net.sends(ZN) for _ in range(parts)]
            self.r = [net.recvs(ZN) for _ in range(parts)]

        def each(self, link, sems, zp, what):
            for k, ref in enumerate(self.region(zp)):
                getattr(net.copy(link, ref, ref, sems[k] + zp, self.r[k] + zp), what)()

        def own(self, what="start"):
            @pl.when(z < ZN - 1)
            def _():
                self.each("up", self.su, z, what)

            @pl.when(z > 0)
            def _():
                self.each("down", self.sd, z, what)

        def relay(self, t, what="start"):
            @pl.when(jnp.minimum(z - t, ZN - 2 - z) >= 0)
            def _():
                self.each("up", self.su, z - t, what)

            @pl.when(jnp.minimum(ZN - 1 - t - z, z - 1) >= 0)
            def _():
                self.each("down", self.sd, z + t, what)

        def recv(self, zp):
            self.each("up", self.su, zp, "wait_recv")

    line_a = [Line(lambda zp, xp=xp: blk_a(zp, xp, y), 1) for xp in (x, 1 - x)]
    line_d = [Line(lambda zp, yp=yp: blk_d(zp, x, yp), 1) for yp in (y, 1 - y)]
    line_u = Line(lambda zp: blk_u(zp, x, y), 3)
    x1 = Lane("x", lambda zp: blk_a(z, x, y), lambda zp: blk_a(z, 1 - x, y), 1)
    y1 = Lane("y", lambda zp: blk_d(z, x, y), lambda zp: blk_d(z, x, 1 - y), 1)
    x_u1 = Lane("x", lambda zp: blk_u1(zp, x, y), lambda zp: blk_u1(zp, 1 - x, y), 2)
    y_u2 = Lane("y", lambda zp: blk_u2(zp, x, y), lambda zp: blk_u2(zp, x, 1 - y), 2)
    y_a = [
        Lane("y", lambda zp, xp=xp: blk_a(zp, xp, y), lambda zp, xp=xp: blk_a(zp, xp, 1 - y), 1) for xp in (x, 1 - x)
    ]
    x_d = [
        Lane("x", lambda zp, yp=yp: blk_d(zp, x, yp), lambda zp, yp=yp: blk_d(zp, 1 - x, yp), 1) for yp in (y, 1 - y)
    ]
    y_u1 = Lane("y", lambda zp: pair_u1(zp, y, mine), lambda zp: pair_u1(zp, 1 - y, mine), 2)
    x_u2 = Lane("x", lambda zp: pair_u2(zp, x, mine), lambda zp: pair_u2(zp, 1 - x, mine), 3)

    def to_partner(make, parts):
        return Lane("p", lambda zp: make(zp, mine), lambda zp: make(zp, other), parts)

    p_a = to_partner(lambda zp, l: reg_a(zp, y, l), 1)
    p_a2 = to_partner(lambda zp, l: reg_a(zp, 1 - y, l), 1)
    p_d = to_partner(lambda zp, l: reg_d(zp, x, l), 1)
    p_d2 = to_partner(lambda zp, l: reg_d(zp, 1 - x, l), 1)
    p_u1 = to_partner(lambda zp, l: pair_u1(zp, y, l), 2)
    p_u1b = to_partner(lambda zp, l: pair_u1(zp, 1 - y, l), 2)
    p_u2 = to_partner(lambda zp, l: pair_u2(zp, x, l), 3)
    p_u2b = to_partner(lambda zp, l: pair_u2(zp, 1 - x, l), 3)

    small_x = Lane("x", lambda zp: [S.at[z, x, y]], lambda zp: [S.at[z, 1 - x, y]], 1)
    small_y = Lane("y", lambda zp: [S.at[z, :, y]], lambda zp: [S.at[z, :, 1 - y]], 1)
    line_s = Line(lambda zp: [S.at[zp]], 1)

    small_x.send(0)
    x1.send(0)
    y1.send(0)
    x_u1.send(z)
    y_u2.send(z)
    line_a[0].own()
    line_d[0].own()
    line_u.own()
    y_a[0].send(z)
    x_d[0].send(z)
    small_x.recv(0)
    small_y.send(0)
    x1.recv(0)
    line_a[1].own()
    y_a[1].send(z)
    p_a.send(z)
    y1.recv(0)
    line_d[1].own()
    x_d[1].send(z)
    p_d.send(z)
    small_y.recv(0)
    line_s.own()

    def second(zp):
        x_u1.recv(zp)
        y_u1.send(zp)
        p_u1.send(zp)
        y_u2.recv(zp)
        x_u2.send(zp)
        p_u2.send(zp)

    def third(zp):
        for lane in y_a:
            lane.recv(zp)
        p_a2.send(zp)
        for lane in x_d:
            lane.recv(zp)
        p_d2.send(zp)
        y_u1.recv(zp)
        p_u1b.send(zp)
        x_u2.recv(zp)
        p_u2b.send(zp)

    def both_ways(t, make):
        @pl.when(z >= t)
        def _():
            make(z - t)

        @pl.when(z < ZN - t)
        def _():
            make(z + t)

    def take(line, t, *lanes):
        both_ways(t, line.recv)
        line.relay(t)
        for lane in lanes:
            both_ways(t, lane.send)

    second(z)
    for t in range(1, ZN):
        take(line_a[0], t, y_a[0])
        take(line_d[0], t, x_d[0])
        take(line_u, t, x_u1, y_u2)
        take(line_a[1], t, y_a[1], p_a)
        if t == 1:
            third(z)
        else:
            both_ways(t - 1, third)
        take(line_d[1], t, x_d[1], p_d)
        both_ways(t, second)
        take(line_s, t)
    both_ways(ZN - 1, third)

    partner = (p_a, p_a2, p_d, p_d2, p_u1, p_u1b, p_u2, p_u2b)
    for zp in range(ZN):
        for lane in partner:
            lane.recv(zp)
    for zp in range(ZN):
        for lane in partner + (x_u1, y_u2, *y_a, *x_d, y_u1, x_u2):
            lane.drain(zp)
    for lane in (x1, y1, small_x, small_y):
        lane.drain(0)
    for line in (line_u, *line_a, *line_d, line_s):
        line.own("wait_send")
        for t in range(1, ZN):
            line.relay(t, "wait_send")
    assert net.next_send <= ssem.shape[0] and net.next_recv <= rsem.shape[0]


def gather_fast(pieces):
    wqkv, wo, wup, wdn, bias, ubias, norm = pieces
    _, _, rw, cn = wqkv.shape
    rd, cu = wdn.shape[1], wup.shape[2]
    d, ff = rw * 8, rd * 8
    small = jnp.concatenate([bias[:, 0], norm[:, 0], ubias, jnp.zeros_like(ubias)], axis=0).astype(F32)
    small = jnp.pad(small, ((0, 0), (0, 128 - rw)))
    hbm = pl.BlockSpec(memory_space=pl.ANY)
    vmem = pl.BlockSpec(memory_space=pltpu.VMEM)
    Q, O, U, D, S = pl.pallas_call(
        gather_kernel,
        in_specs=[vmem] * 5,
        out_specs=[hbm] * 5,
        out_shape=[
            jax.ShapeDtypeStruct((LAYERS, 3, d, d), BF),
            jax.ShapeDtypeStruct((LAYERS, d, d), BF),
            jax.ShapeDtypeStruct((LAYERS, d, ff), BF),
            jax.ShapeDtypeStruct((LAYERS, ff, d), BF),
            jax.ShapeDtypeStruct((ZN, 2, 2, 2, 8, 128), F32),
        ],
        scratch_shapes=[
            pltpu.VMEM((3, rw, cn), BF), pltpu.VMEM((rw, cn), BF), pltpu.VMEM((rw, cu), BF), pltpu.VMEM((rd, cn), BF),
            pltpu.VMEM((3, rw, 2 * cn), BF), pltpu.VMEM((rw, 2 * cn), BF),
            pltpu.VMEM((rw, 2 * cu), BF), pltpu.VMEM((rd, 2 * cn), BF),
            pltpu.SemaphoreType.DMA((200,)), pltpu.SemaphoreType.DMA((200,)), pltpu.SemaphoreType.DMA((5,)),
        ],
        compiler_params=pltpu.CompilerParams(collective_id=1, has_side_effects=True),
        name="weight_gather",
    )(wqkv, wo, wup, wdn, small)
    S = S.reshape(8, 4, 8, 128)[..., :rw]
    rows = jnp.transpose(S, (2, 1, 0, 3)).reshape(8, 4, d)
    ub = jnp.transpose(S[:, :, 4:6], (2, 0, 1, 3)).reshape(2, ff)
    return Q, O, U, D, rows[0:2], ub, rows[2:4]


def accumulate(dst, src, rows, step=48):
    def body(i, carry):
        r = pl.ds(pl.multiple_of(i * step, 16), step)
        dst[r, :] = dst[r, :] + src[r, :]
        return carry

    lax.fori_loop(0, rows // step, body, 0)


def scatter_kernel(
    gw, sm_in, oq, oo, ou, od, sm_out,
    AQ, AO, AU, AD, PQ, PO, PU, PD, FA, FD, F1, FO, F2, FV, S1, SO, S2, SV, ZA, ZD, ZU, ZO, ZV, TA, TD,
    hq, ho, hu, hd, s_p, s_x, s_y, s_below, s_above, s_a, s_b, s_sum, s_up, s_down, ssem, rsem, lsem,
):
    w, n, z, x, y, c, links = where_am_i()
    mine, other = c, 1 - c
    net = Net(ssem, rsem, links)
    d, ff = AO.shape[1], AU.shape[1]
    rw, cn = d // 8, d // 2
    rd, cu = ff // 8, ff // 2
    half = cu // 2
    enter(z, links)

    class Hop:
        def __init__(self, link, pairs, parts):
            self.link, self.pairs = link, pairs
            self.s = [net.sends(ZN) for _ in range(parts)]
            self.r = [net.recvs(ZN) for _ in range(parts)]

        def each(self, zp, what):
            for k, (src, dst) in enumerate(self.pairs(zp)):
                getattr(net.copy(self.link, src, dst, self.s[k] + zp, self.r[k] + zp), what)()

        def send(self, zp):
            self.each(zp, "start")

        def recv(self, zp):
            self.each(zp, "wait_recv")

        def drain(self, zp):
            self.each(zp, "wait_send")

    def rows_a(zp):
        return span(2 * rw * zp, 2 * rw)

    main = rd - rw

    def slab(zp, layer, q, o, u, dn):
        rows = rows_a(zp)
        down = span(2 * rd * zp, 2 * rd)
        return [
            [(gw.at[layer, j, rows, :], q.at[j, rows, :]) for j in range(3)],
            [(gw.at[layer, 8 + zp], dn.at[down, :])],
            [(gw.at[layer, 3, rows, :], o.at[rows, :])]
            + [(gw.at[layer, 4 + j, rows, :], u.at[rows, j * d : (j + 1) * d]) for j in range(4)],
        ]

    def own_loads(zp, part):
        return [
            pltpu.make_async_copy(src, dst, lsem.at[((0, 3, 4)[part] + k) * ZN + zp])
            for k, (src, dst) in enumerate(slab(zp, mine, AQ, AO, AU, AD)[part])
        ]

    swap = [Hop("p", lambda zp, p=p: slab(zp, other, PQ, PO, PU, PD)[p], (3, 1, 5)[p]) for p in range(3)]

    def cols_a(yp):
        return span(cn * yp, cn)

    def rows_x(zp, xp):
        return span(rw * (2 * zp + xp), rw)

    def rows_d(zp, xp):
        return pl.ds(pl.multiple_of(rd * (2 * zp + xp), rw), main)

    def rows_v(zp, xp):
        return pl.ds(pl.multiple_of(rd * (2 * zp + xp) + main, rw), rw)

    def reg_a(zp, yp):
        return AQ.at[:, rows_a(zp), cols_a(yp)]

    def reg_d(zp, xp):
        return AD.at[rows_d(zp, xp), :]

    def u1(zp, yp):
        return [AU.at[rows_a(zp), span(cu * yp, half)], AO.at[rows_a(zp), cols_a(yp)]]

    def u1_part(zp, xp, yp):
        return [AU.at[rows_x(zp, xp), span(cu * yp, half)], AO.at[rows_x(zp, xp), cols_a(yp)]]

    def u2(zp, xp):
        rows = rows_x(zp, xp)
        return [AU.at[rows, span(cu * yp + half, half)] for yp in range(2)] + [AD.at[rows_v(zp, xp), :]]

    def u2_part(zp, xp, yp):
        return [AU.at[rows_x(zp, xp), span(cu * yp + half, half)], AD.at[rows_v(zp, xp), cols_a(yp)]]

    def blk_u(zp):
        rows = rows_x(zp, x)
        return [AU.at[rows, span(cu * y, cu)], AO.at[rows, cols_a(y)], AD.at[rows_v(zp, x), cols_a(y)]]

    def bufs_u1(zp):
        return [F1.at[zp], FO.at[zp]]

    def bufs_u2(zp):
        return [F2.at[0, zp], F2.at[1, zp], FV.at[zp]]

    def bufs_s1(zp):
        return [S1.at[zp], SO.at[zp]]

    def bufs_s2(zp):
        return [S2.at[zp], SV.at[zp]]

    y_a = Hop("y", lambda zp: [(reg_a(zp, 1 - y), FA.at[zp])], 1)
    x_d = Hop("x", lambda zp: [(reg_d(zp, 1 - x), FD.at[zp])], 1)
    y_u1 = Hop("y", lambda zp: list(zip(u1(zp, 1 - y), bufs_u1(zp))), 2)
    x_u2 = Hop("x", lambda zp: list(zip(u2(zp, 1 - x), bufs_u2(zp))), 3)
    x_u1 = Hop("x", lambda zp: list(zip(u1_part(zp, 1 - x, y), bufs_s1(zp))), 2)
    y_u2 = Hop("y", lambda zp: list(zip(u2_part(zp, x, 1 - y), bufs_s2(zp))), 2)
    last_a = Hop("x", lambda zp: [(AQ.at[:, rows_x(z, 1 - x), cols_a(y)], TA)], 1)
    last_d = Hop("y", lambda zp: [(AD.at[rows_d(z, x), cols_a(1 - y)], TD)], 1)

    def add_all(dsts, srcs):
        for dst, src in zip(dsts, srcs):
            accumulate(dst, src, src.shape[0])

    class Line:
        def __init__(self, region, bufs):
            self.region, self.bufs = region, bufs
            self.su = [net.sends(ZN) for _ in bufs]
            self.sd = [net.sends(ZN) for _ in bufs]
            self.r = [net.recvs(ZN + 1) for _ in bufs]

        def up(self, zp, what):
            slot = jnp.where(zp == z + 1, ZN, zp)

            @pl.when(zp > z)
            def _():
                for k, (src, buf) in enumerate(zip(self.region(zp), self.bufs)):
                    getattr(net.copy("up", src, buf.at[slot], self.su[k] + zp, self.r[k] + slot), what)()

        def down(self, zp, what):
            @pl.when(zp < z)
            def _():
                for k, (src, buf) in enumerate(zip(self.region(zp), self.bufs)):
                    getattr(net.copy("down", src, buf.at[zp], self.sd[k] + zp, self.r[k] + zp), what)()

        def take(self, zp, slot):
            for k, (dst, buf) in enumerate(zip(self.region(zp), self.bufs)):
                net.copy("up", dst, buf.at[slot], self.su[k] + zp, self.r[k] + slot).wait_recv()
                self.add(dst, buf.at[slot])

        def add(self, dst, src):
            if len(src.shape) == 3:
                for j in range(src.shape[0]):
                    accumulate(dst.at[j], src.at[j], src.shape[1])
            else:
                accumulate(dst, src, src.shape[0])

        def go(self, zp):
            @pl.when(jnp.minimum(z - zp, ZN - 2 - z) >= 0)
            def _():
                self.take(zp, zp)

            @pl.when(jnp.minimum(zp - z, z - 1) >= 0)
            def _():
                self.take(zp, jnp.where(zp == z, ZN, zp))

            self.up(zp, "start")
            self.down(zp, "start")

        def drain(self, zp):
            self.up(zp, "wait_send")
            self.down(zp, "wait_send")

    line_a = Line(lambda zp: (reg_a(zp, y),), (ZA,))
    line_d = Line(lambda zp: (reg_d(zp, x),), (ZD,))
    line_u = Line(blk_u, (ZU, ZO, ZV))

    table = ((3, 3, 0, 0), (2, 0, 3, 1), (1, 2, 1, 2), (0, 1, 2, 3))
    order = [jnp.where(z == 0, t[0], jnp.where(z == 1, t[1], jnp.where(z == 2, t[2], t[3]))) for t in table]

    small = [
        net.copy(link, src, dst, net.sends(1), net.recvs(1))
        for link, src, dst in (("p", sm_in, s_p), ("x", s_a, s_x), ("y", s_b, s_y))
    ]
    small_up = net.copy("up", s_up, s_below, net.sends(1), net.recvs(1))
    small_down = net.copy("down", s_down, s_above, net.sends(1), net.recvs(1))

    small[0].start()
    for zp in order:
        for part in range(3):
            for cp in own_loads(zp, part):
                cp.start()
            swap[part].send(zp)

    def arrive(zp, part):
        for cp in own_loads(zp, part):
            cp.wait()
        swap[part].recv(zp)

    def open_slab(zp):
        rows = rows_a(zp)
        arrive(zp, 0)
        for j in range(3):
            accumulate(AQ.at[j, rows, :], PQ.at[j, rows, :], 2 * rw)
        y_a.send(zp)
        down = span(2 * rd * zp, 2 * rd)
        arrive(zp, 1)
        accumulate(AD.at[down, :], PD.at[down, :], 2 * rd)
        x_d.send(zp)
        arrive(zp, 2)
        accumulate(AO.at[rows, :], PO.at[rows, :], 2 * rw)
        accumulate(AU.at[rows, :], PU.at[rows, :], 2 * rw, 16)
        y_u1.send(zp)
        x_u2.send(zp)

    def mid_a(zp):
        y_a.recv(zp)
        for j in range(3):
            accumulate(reg_a(zp, y).at[j], FA.at[zp, j], 2 * rw)
        line_a.go(zp)

    def mid_d(zp):
        x_d.recv(zp)
        accumulate(reg_d(zp, x), FD.at[zp], main)
        line_d.go(zp)

    def mid_u(zp):
        y_u1.recv(zp)
        add_all(u1(zp, y), bufs_u1(zp))
        x_u1.send(zp)
        x_u2.recv(zp)
        add_all(u2(zp, x), bufs_u2(zp))
        y_u2.send(zp)

    def close(zp):
        x_u1.recv(zp)
        add_all(u1_part(zp, x, y), bufs_s1(zp))
        y_u2.recv(zp)
        add_all(u2_part(zp, x, y), bufs_s2(zp))
        line_u.go(zp)

    open_slab(order[0])
    mid_a(order[0])
    small[0].wait()
    s_a[...] = sm_in[...] + s_p[...]
    small[1].start()
    open_slab(order[1])
    mid_d(order[0])
    mid_u(order[0])
    small[1].wait()
    s_b[...] = s_a[...] + s_x[...]
    small[2].start()
    open_slab(order[2])
    mid_a(order[1])
    close(order[0])
    mid_d(order[1])
    mid_u(order[1])
    small[2].wait()
    s_sum[...] = s_b[...] + s_y[...]
    open_slab(order[3])
    mid_a(order[2])
    close(order[1])
    mid_d(order[2])
    mid_u(order[2])

    @pl.when(z > 0)
    def _():
        small_up.wait_recv()

    @pl.when(z == 0)
    def _():
        s_below[...] = jnp.zeros_like(s_below)

    @pl.when(z < ZN - 1)
    def _():
        s_up[...] = s_sum[...] + s_below[...]
        small_up.start()

    mid_a(order[3])
    last_a.send(0)
    close(order[2])
    mid_d(order[3])
    last_d.send(0)
    mid_u(order[3])

    @pl.when(z < ZN - 1)
    def _():
        small_down.wait_recv()

    @pl.when(z == ZN - 1)
    def _():
        s_above[...] = jnp.zeros_like(s_above)

    @pl.when(z > 0)
    def _():
        s_down[...] = s_sum[...] + s_above[...]
        small_down.start()

    sm_out[...] = s_sum[...] + s_below[...] + s_above[...]
    close(order[3])

    def pick(v, k):
        lo, hi = v[..., :k], v[..., k:]
        return jnp.where(c == 0, lo, hi), jnp.where(c == 0, hi, lo)

    out = [
        net.copy("p", src, dst.at[mine], net.sends(1), net.recvs(1))
        for src, dst in ((hu, ou), (hq, oq), (ho, oo), (hd, od))
    ]
    rows = rows_x(z, x)
    ou[mine] = AU[rows, span(cu * y + half * c, half)].astype(F32)
    hu[...] = AU[rows, span(cu * y + half * (1 - c), half)].astype(F32)
    out[0].start()
    keep, give = pick(AO[rows, cols_a(y)].astype(F32), cn // 2)
    oo[mine] = keep
    ho[...] = give
    out[2].start()
    last_a.recv(0)
    for j in range(3):
        keep, give = pick(AQ[j, rows, cols_a(y)].astype(F32) + TA[j].astype(F32), cn // 2)
        oq[mine, j] = keep
        hq[j] = give
    out[1].start()
    last_d.recv(0)
    for k in range(rd // rw):
        part = slice(k * rw, (k + 1) * rw)
        here = span(rd * w + k * rw, rw)
        total = AD[here, cols_a(y)].astype(F32)
        if k * rw < main:
            total = total + TD[part, :].astype(F32)
        keep, give = pick(total, cn // 2)
        od[mine, part, :] = keep
        hd[part, :] = give
    out[3].start()

    for zp in range(ZN):
        for hop in (*swap, y_a, x_d, y_u1, x_u2, x_u1, y_u2):
            hop.drain(zp)
        for line in (line_a, line_d, line_u):
            line.drain(zp)
    last_a.drain(0)
    last_d.drain(0)

    @pl.when(z < ZN - 1)
    def _():
        small_up.wait_send()

    @pl.when(z > 0)
    def _():
        small_down.wait_send()

    for cp in out:
        cp.wait()
    assert net.next_send <= ssem.shape[0] and net.next_recv <= rsem.shape[0]


def scatter_fast(gw, pack):
    d = gw.shape[-1]
    ff = 4 * d
    rw, cn, rd, cu = d // 8, d // 2, ff // 8, ff // 2
    hbm = pl.BlockSpec(memory_space=pl.ANY)
    vmem = pl.BlockSpec(memory_space=pltpu.VMEM)

    def buf(*shape):
        return pltpu.VMEM(shape, BF)

    def wide(*shape):
        return pltpu.VMEM(shape, F32)

    outs = [(3, rw, cn // 2), (rw, cn // 2), (rw, cu // 2), (rd, cn // 2)]
    full = [buf(3, d, d), buf(d, d), buf(d, ff), buf(ff, d)]
    oq, oo, ou, od, total = pl.pallas_call(
        scatter_kernel,
        in_specs=[hbm, vmem],
        out_specs=[vmem] * 5,
        out_shape=[jax.ShapeDtypeStruct((LAYERS,) + s, F32) for s in outs] + [jax.ShapeDtypeStruct(pack.shape, F32)],
        scratch_shapes=full + full + [
            buf(ZN, 3, 2 * rw, cn), buf(ZN, rd - rw, d), buf(ZN, 2 * rw, cu // 2), buf(ZN, 2 * rw, cn),
            buf(2, ZN, rw, cu // 2), buf(ZN, rw, d), buf(ZN, rw, cu // 2), buf(ZN, rw, cn),
            buf(ZN, rw, cu // 2), buf(ZN, rw, cn), buf(ZN + 1, 3, 2 * rw, cn), buf(ZN + 1, rd - rw, d),
            buf(ZN + 1, rw, cu), buf(ZN + 1, rw, cn), buf(ZN + 1, rw, cn), buf(3, rw, cn), buf(rd - rw, cn),
        ] + [wide(*s) for s in outs] + [wide(*pack.shape)] * 10 + [
            pltpu.SemaphoreType.DMA((180,)), pltpu.SemaphoreType.DMA((160,)), pltpu.SemaphoreType.DMA((9 * ZN,)),
        ],
        compiler_params=pltpu.CompilerParams(collective_id=2, has_side_effects=True, vmem_limit_bytes=VMEM_LIMIT),
        name="gradient_scatter",
    )(gw, pack)
    w, n = lax.axis_index("wide"), lax.axis_index("narrow")
    gb = lax.dynamic_slice(total[0:8].reshape(2, 4, d), (0, n, w * rw), (2, 1, rw))
    gn = lax.dynamic_slice(total[16:24].reshape(2, 4, d), (0, n, w * rw), (2, 1, rw))
    gub = lax.dynamic_slice(total[8:16].reshape(2, ff), (0, (4 * w + n) * rw), (2, rw))
    return oq, oo, ou, od, gb, gub, gn


def gather_weights(pieces):
    wqkv, wo, wup, wdn, bias, ubias, norm = pieces
    narrow = [(wqkv, 3), (wo, 2), (wup, 2), (wdn, 2), (bias, 1), (norm, 1)]
    wqkv, wo, wup, wdn, bias, norm = (lax.all_gather(w, "narrow", axis=k, tiled=True) for w, k in narrow)
    wide = [(wqkv, 2), (wo, 1), (wup, 1), (wdn, 1), (bias, 2), (norm, 2)]
    wqkv, wo, wup, wdn, bias, norm = (lax.all_gather(w, "wide", axis=k, tiled=True) for w, k in wide)
    ubias = lax.all_gather(ubias, ("wide", "narrow"), axis=1, tiled=True)
    return wqkv, wo, wup, wdn, bias, ubias, norm


def scatter_two(grad, row_axis, col_axis):
    low = lax.psum_scatter(grad.astype(BF), "narrow", scatter_dimension=col_axis, tiled=True)
    return lax.psum_scatter(low.astype(F32), "wide", scatter_dimension=row_axis, tiled=True)


def scatter_grads(gw, pack):
    d = gw.shape[-1]
    gq, go, gdn = gw[:, 0:3], gw[:, 3], gw[:, 8:].reshape(LAYERS, -1, d)
    gup = jnp.moveaxis(gw[:, 4:8], 1, 2).reshape(LAYERS, d, -1)
    gb, gub, gn = pack[0:8].reshape(LAYERS, 4, d), pack[8:16].reshape(LAYERS, -1), pack[16:24].reshape(LAYERS, 4, d)
    big = (scatter_two(gq, 2, 3), scatter_two(go, 1, 2), scatter_two(gup, 1, 2), scatter_two(gdn, 1, 2))
    gub = lax.psum_scatter(gub, ("wide", "narrow"), scatter_dimension=1, tiled=True)

    def small_two(g):
        return lax.psum_scatter(
            lax.psum_scatter(g, "narrow", scatter_dimension=1, tiled=True), "wide", scatter_dimension=2, tiled=True
        )

    return big + (small_two(gb), gub, small_two(gn))


def shards(
    near, text_in, memory_in, counts, last_len, cot_text, cot_memory,
    qkv_weight, out_weight, up_weight, down_weight, biases, up_bias, norm_params,
):
    text, cot = text_in[:, 0], cot_text[:, 0]
    mem, cot_mem = memory_in[:, 0], cot_memory[:, 0]
    cnt, lens = counts[:, 0], last_len[:, 0]
    gather = gather_fast if near else gather_weights
    weights = gather((qkv_weight, out_weight, up_weight, down_weight, biases, up_bias, norm_params))
    text_out, mem_out, kept = forward_local(text, mem, cnt, lens, weights)
    text_grad, mem_grad, rhs, small = backward_local(cot, cot_mem, cnt, lens, kept, weights)
    scatter = scatter_fast if near else scatter_grads
    grads = scatter(weight_grads(kept[0], rhs), small)
    return (text_out[:, None], mem_out[:, None], text_grad[:, None], mem_grad[:, None]) + grads


def solution(mesh):
    items = ("wide", "narrow")
    act5 = P(None, items, None, None, None)
    act4 = P(None, items, None, None)
    ids = P(None, items)
    split = P(None, "wide", "narrow")
    small = P(None, "narrow", "wide")
    params = (P(None, None, "wide", "narrow"), split, split, split, small, ids, small)
    near = (mesh.shape["wide"], mesh.shape["narrow"]) == (2 * ZN, 4)
    return jax.shard_map(
        functools.partial(shards, near),
        mesh=mesh,
        in_specs=(act5, act4, ids, ids, act5, act4) + params,
        out_specs=(act5, act4, act5, act4) + params,
        check_vma=False,
    )
```

```python
import functools

import jax
import jax.numpy as jnp
from jax import lax
from jax.experimental import pallas as pl
from jax.experimental.pallas import tpu as pltpu
from jax.sharding import PartitionSpec as P

HEADS = 12
HD = 64
MEM = 10
TEXT = 108
SEGS = 4
MB = 2
LAYERS = 2
SEG = TEXT + 2 * MEM
TAIL = 104
ROWS = MB * SEG
EPS = 1e-12
BF = jnp.bfloat16
F32 = jnp.float32
NEG = -1e30
RSQRT2 = 0.7071067811865476
RSQRT2PI = 0.3989422804014327
VMEM_LIMIT = 66_000_000
CHUNK = 32
GROUP_F = 6
GROUP_B = 6


def dot(a, b):
    return lax.dot_general(a, b, (((1,), (0,)), ((), ())), preferred_element_type=F32)


def dot_rt(a, b):
    return lax.dot_general(a, b, (((1,), (1,)), ((), ())), preferred_element_type=F32)


def dot_lt(a, b):
    return lax.dot_general(a, b, (((0,), (0,)), ((), ())), preferred_element_type=F32)


def row_ids(shape):
    return lax.broadcasted_iota(jnp.int32, shape, 0)


def lane_ids(shape):
    return lax.broadcasted_iota(jnp.int32, shape, 1)


def valid_rows(seg, count, length):
    return jnp.where(seg < count - 1, TEXT, jnp.where(seg == count - 1, length, 0))


def colsum(v):
    rows, cols = v.shape
    return jnp.sum(v.reshape(rows // 8, 8, cols), axis=0)


class Loads:
    def __init__(self, pairs, sems, first, order):
        self.pairs, self.sems, self.first, self.order = pairs, sems, first, order

    def each(self, layer, what):
        for k, (src, dst) in enumerate(self.pairs):
            getattr(pltpu.make_async_copy(src.at[layer], dst.at[layer], self.sems.at[layer, k]), what)()

    def start(self):
        self.each(self.order[0], "start")

    def need(self, step):
        @pl.when(self.first & (step == 0))
        def _():
            self.each(self.order[0], "wait")
            self.each(self.order[1], "start")

        @pl.when(self.first & (step == 1))
        def _():
            self.each(self.order[1], "wait")


def fwd_kernel(
    counts, lens, text, mem0, wqkv_hbm, wo_hbm, wup_hbm, wdn_hbm, bias, ubias, norm,
    text_out, mem_out, lhs_out, qkv_out, p_out, gp_out, xh1_out, xh2_out, rs_out,
    x_ref, mem_ref, y_ref, acc_ref, wqkv, wo, wup, wdn, wsem,
):
    seg = pl.program_id(0)
    layer = pl.program_id(1)
    d = x_ref.shape[-1]
    a_out, c_out, y_out = (lhs_out.at[:, :, j * d : (j + 1) * d] for j in range(3))
    g_out = lhs_out.at[:, :, 3 * d :]
    loads = Loads(((wqkv_hbm, wqkv), (wo_hbm, wo), (wup_hbm, wup), (wdn_hbm, wdn)), wsem, seg == 0, (0, 1))

    @pl.when((seg == 0) & (layer == 0))
    def _():
        loads.start()
        mem_ref[...] = mem0[...]

    @pl.when(layer == 0)
    def _():
        for i in range(MB):
            x_ref[i * SEG : i * SEG + TEXT, :] = text[i, 0].astype(F32)
            tail = slice(i * SEG + TAIL, (i + 1) * SEG)
            now = x_ref[tail, :]
            x_ref[tail, :] = jnp.where(row_ids(now.shape) < TEXT - TAIL, now, mem_ref[i])

    loads.need(layer)
    xb = x_ref[...].astype(BF)
    a_out[0] = xb
    qkv_out[0, :, 0:d] = (dot(xb, wqkv[layer, 0]) + bias[layer, 0:1, :]).astype(BF)
    qkv_out[0, :, d : 2 * d] = dot(xb, wqkv[layer, 1]).astype(BF)
    qkv_out[0, :, 2 * d : 3 * d] = (dot(xb, wqkv[layer, 2]) + bias[layer, 1:2, :]).astype(BF)

    low_half = lane_ids((SEG, 128)) < HD
    lanes = lane_ids((1, SEG))

    def heads_of(v):
        zero = jnp.zeros_like(v)
        return jnp.concatenate([jnp.where(low_half, v, zero), jnp.where(low_half, zero, v)], axis=0)

    for i in range(MB):
        vr = valid_rows(seg, counts[i], lens[i])
        keep = (lanes < vr) | (lanes >= TEXT)
        r0 = i * SEG
        for g0 in range(0, HEADS // 2, GROUP_F):
            pairs = range(g0, g0 + GROUP_F)

            def part(j, pair):
                return qkv_out[0, r0 : r0 + SEG, j * d + pair * 128 : j * d + pair * 128 + 128]

            s_all = [dot_rt(heads_of(part(0, p) * (HD ** -0.5)), part(1, p)) for p in pairs]
            s_all = [jnp.where(keep, s, NEG) for s in s_all]
            e_all = [jnp.exp(s - jnp.max(s, axis=-1, keepdims=True)) for s in s_all]
            p_all = [(e * (1.0 / jnp.sum(e, axis=-1, keepdims=True))).astype(BF) for e in e_all]
            c_all = [dot(pv, part(2, p)) for pv, p in zip(p_all, pairs)]
            for p, pv, c2 in zip(pairs, p_all, c_all):
                u0 = (i * (HEADS // 2) + p) * 2 * SEG
                p_out[0, u0 : u0 + 2 * SEG, :] = pv
                c_out[0, r0 : r0 + SEG, p * 128 : p * 128 + 128] = jnp.where(low_half, c2[:SEG], c2[SEG:]).astype(BF)

    def norm_to(base_ref, gain, shift, add, xh_out, rs_index, to_ref, low_out):
        for k in range(0, ROWS, CHUNK):
            rows = slice(k, k + CHUNK)
            h = base_ref[rows, :] + (acc_ref[rows, :] + add)
            center = h - jnp.mean(h, axis=-1, keepdims=True)
            rs = lax.rsqrt(jnp.mean(center * center, axis=-1, keepdims=True) + EPS)
            xh = center * rs
            xh_out[0, rows, :] = xh
            rs_out[0, rs_index, rows, :] = jnp.broadcast_to(rs, (CHUNK, 128))
            out = xh * gain + shift
            to_ref[rows, :] = out
            if low_out is not None:
                low_out[0, rows, :] = out.astype(BF)

    acc_ref[...] = dot(c_out[0], wo[layer])
    norm_to(x_ref, norm[layer, 0:1, :], norm[layer, 1:2, :], bias[layer, 2:3, :], xh1_out, 0, y_ref, y_out)

    ff = wup.shape[-1]

    def ffn_step():
        cols = slice(0, ff)
        u = dot(y_out[0], wup[layer, :, cols]) + ubias[layer, :, cols]
        cdf = 0.5 * (1.0 + lax.erf(u * RSQRT2))
        g_out[0, :, cols] = (u * cdf).astype(BF)
        gp_out[0, :, cols] = (cdf + u * (jnp.exp(-0.5 * (u * u)) * RSQRT2PI)).astype(BF)

    ffn_step()
    acc_ref[...] = dot(g_out[0], wdn[layer])
    norm_to(y_ref, norm[layer, 2:3, :], norm[layer, 3:4, :], bias[layer, 3:4, :], xh2_out, 1, x_ref, None)

    @pl.when(layer == LAYERS - 1)
    def _():
        for i in range(MB):
            vr = valid_rows(seg, counts[i], lens[i])
            body = x_ref[i * SEG : i * SEG + TEXT, :]
            text_out[i, 0] = jnp.where(row_ids(body.shape) < vr, body, 0.0).astype(BF)
            tail = x_ref[i * SEG + TAIL : (i + 1) * SEG, :]
            both = jnp.where(row_ids(tail.shape) >= TEXT - TAIL + MEM, tail, pltpu.roll(tail, SEG - TAIL - MEM, axis=0))
            mem_ref[i] = jnp.where(seg < counts[i], both, mem_ref[i])
        mem_out[...] = mem_ref[...]


def whole(shape):
    return pl.BlockSpec(shape, lambda *_: (0,) * len(shape), pipeline_mode=pl.Buffered(1))


def saved(rows, cols):
    return pl.BlockSpec((1, rows, cols), lambda s, l: (l, s, 0))


def forward_local(text, mem, counts, lens, weights):
    wqkv, wo, wup, wdn, bias, ubias, norm = weights
    d, ff = wup.shape[1:]
    mem0 = jnp.concatenate([jnp.zeros((MB, TEXT - TAIL, d), F32), mem.astype(F32), mem.astype(F32)], axis=1)
    total = SEGS * ROWS
    units = MB * HEADS * SEG
    smem = pl.BlockSpec(memory_space=pltpu.SMEM)
    hbm = pl.BlockSpec(memory_space=pl.ANY)
    outs = pl.pallas_call(
        fwd_kernel,
        grid=(SEGS, LAYERS),
        in_specs=[
            smem, smem,
            pl.BlockSpec((MB, 1, TEXT, d), lambda s, l: (0, s, 0, 0)),
            whole(mem0.shape), hbm, hbm, hbm, hbm,
            whole(bias.shape), whole((LAYERS, 1, ff)), whole(norm.shape),
        ],
        out_specs=[
            pl.BlockSpec((MB, 1, TEXT, d), lambda s, l: (0, s, 0, 0)),
            whole(mem0.shape),
            saved(ROWS, 3 * d + ff), saved(ROWS, 3 * d), saved(units, 128),
            saved(ROWS, ff), saved(ROWS, d), saved(ROWS, d),
            pl.BlockSpec((1, 2, ROWS, 128), lambda s, l: (l, 0, s, 0)),
        ],
        out_shape=[
            jax.ShapeDtypeStruct((MB, SEGS, TEXT, d), BF),
            jax.ShapeDtypeStruct(mem0.shape, F32),
            jax.ShapeDtypeStruct((LAYERS, total, 3 * d + ff), BF),
            jax.ShapeDtypeStruct((LAYERS, total, 3 * d), BF),
            jax.ShapeDtypeStruct((LAYERS, SEGS * units, 128), BF),
            jax.ShapeDtypeStruct((LAYERS, total, ff), BF),
            jax.ShapeDtypeStruct((LAYERS, total, d), F32),
            jax.ShapeDtypeStruct((LAYERS, total, d), F32),
            jax.ShapeDtypeStruct((LAYERS, 2, total, 128), F32),
        ],
        scratch_shapes=[
            pltpu.VMEM((ROWS, d), F32), pltpu.VMEM(mem0.shape, F32),
            pltpu.VMEM((ROWS, d), F32), pltpu.VMEM((ROWS, d), F32),
            pltpu.VMEM(wqkv.shape, BF), pltpu.VMEM(wo.shape, BF), pltpu.VMEM(wup.shape, BF), pltpu.VMEM(wdn.shape, BF),
            pltpu.SemaphoreType.DMA((LAYERS, 4)),
        ],
        compiler_params=pltpu.CompilerParams(
            dimension_semantics=("arbitrary", "arbitrary"), vmem_limit_bytes=VMEM_LIMIT
        ),
        name="rmt_forward",
    )(counts, lens, text, mem0, wqkv, wo, wup, wdn, bias.astype(F32), ubias.astype(F32)[:, None, :], norm.astype(F32))
    text_out, mem_end = outs[:2]
    return text_out, mem_end[:, TEXT - TAIL + MEM :].astype(BF), outs[2:]


def bwd_kernel(
    counts, lens, cot, gm0, qkv, p_in, gp_in, xh1_in, xh2_in, rs_in, wqkv_hbm, wo_hbm, wup_hbm, wdn_hbm, norm,
    tg_out, gm_out, rhs_out, small_out,
    g_ref, gm_ref, t_ref, acc_ref, dc_ref, wqkv, wo, wup, wdn, wsem, gb_out, gub_out, gn_out,
):
    seg = SEGS - 1 - pl.program_id(0)
    step = pl.program_id(1)
    layer = LAYERS - 1 - step
    loads = Loads(((wqkv_hbm, wqkv), (wo_hbm, wo), (wup_hbm, wup), (wdn_hbm, wdn)), wsem, seg == SEGS - 1, (1, 0))
    d = g_ref.shape[-1]
    ff = wup.shape[-1]
    dqkv_out, dao_out = rhs_out.at[:, :, 0 : 3 * d], rhs_out.at[:, :, 3 * d : 4 * d]
    du_out, df_out = rhs_out.at[:, :, 4 * d : 4 * d + ff], rhs_out.at[:, :, 4 * d + ff :]

    @pl.when((seg == SEGS - 1) & (step == 0))
    def _():
        loads.start()
        gm_ref[...] = gm0[...]
        gb_out[...] = jnp.zeros_like(gb_out)
        gub_out[...] = jnp.zeros_like(gub_out)
        gn_out[...] = jnp.zeros_like(gn_out)

    @pl.when(step == 0)
    def _():
        for i in range(MB):
            vr = valid_rows(seg, counts[i], lens[i])
            ct = cot[i, 0].astype(F32)
            g_ref[i * SEG : i * SEG + TEXT, :] = jnp.where(row_ids(ct.shape) < vr, ct, 0.0)
            tail = slice(i * SEG + TAIL, (i + 1) * SEG)
            now = g_ref[tail, :]
            rows = row_ids(now.shape)
            mem_part = jnp.where((rows >= TEXT - TAIL + MEM) & (seg < counts[i]), gm_ref[i], 0.0)
            g_ref[tail, :] = jnp.where(rows < TEXT - TAIL, now, mem_part)

    loads.need(step)

    def norm_back(base_ref, add_ref, xh_in, rs_slot, gain, slot, low_out, low_slot):
        sums = [jnp.zeros((8, d), F32) for _ in range(3)]
        for k in range(0, ROWS, CHUNK):
            rows = slice(k, k + CHUNK)
            gout = base_ref[rows, :]
            if add_ref is not None:
                gout = gout + add_ref[rows, :]
            xh = xh_in[0, rows, :]
            gx = gout * xh
            t = gout * gain
            inner = jnp.mean(gx * gain, axis=-1, keepdims=True)
            dh = rs_in[0, rs_slot, rows, :][:, :1] * (t - jnp.mean(t, axis=-1, keepdims=True) - xh * inner)
            t_ref[rows, :] = dh
            low = dh.astype(BF)
            low_out[0, rows, :] = low
            sums = [v + colsum(w) for v, w in zip(sums, (gx, gout, low.astype(F32)))]
        gn_out[layer, slot] += sums[0]
        gn_out[layer, slot + 1] += sums[1]
        gb_out[layer, low_slot] += sums[2]

    norm_back(g_ref, None, xh2_in, 1, norm[layer, 2:3, :], 2, df_out, 3)

    def ffn_step():
        cols = slice(0, ff)
        dg = dot_rt(df_out[0], wdn[layer, cols, :])
        du = (dg * gp_in[0, :, cols].astype(F32)).astype(BF)
        du_out[0, :, cols] = du
        gub_out[layer, :, cols] += colsum(du.astype(F32))

    ffn_step()
    acc_ref[...] = dot_rt(du_out[0], wup[layer])
    norm_back(t_ref, acc_ref, xh1_in, 0, norm[layer, 0:1, :], 0, dao_out, 2)
    dc_ref[...] = dot_rt(dao_out[0], wo[layer]).astype(BF)

    low_half = lane_ids((SEG, 128)) < HD
    scale = HD ** -0.5

    def heads_of(v):
        zero = jnp.zeros_like(v)
        return jnp.concatenate([jnp.where(low_half, v, zero), jnp.where(low_half, zero, v)], axis=0)

    for i in range(MB):
        r0 = i * SEG
        for g0 in range(0, HEADS // 2, GROUP_B):
            pairs = range(g0, g0 + GROUP_B)

            def part(j, pair):
                return qkv[0, r0 : r0 + SEG, j * d + pair * 128 : j * d + pair * 128 + 128]

            def probs(pair):
                u0 = (i * (HEADS // 2) + pair) * 2 * SEG
                return p_in[0, u0 : u0 + 2 * SEG, :]

            def out(j, pair, v):
                dqkv_out[0, r0 : r0 + SEG, j * d + pair * 128 : j * d + pair * 128 + 128] = v.astype(BF)

            dc2 = [heads_of(dc_ref[r0 : r0 + SEG, p * 128 : p * 128 + 128]) for p in pairs]
            dp = [dot_rt(v, part(2, p)) for v, p in zip(dc2, pairs)]
            for p, v in zip(pairs, dc2):
                out(2, p, dot_lt(probs(p), v))
            pdp = [probs(p).astype(F32) * v for p, v in zip(pairs, dp)]
            ds = [
                (v - probs(p).astype(F32) * jnp.sum(v, axis=-1, keepdims=True)).astype(BF) for p, v in zip(pairs, pdp)
            ]
            dq2 = [dot(v, part(1, p)) for v, p in zip(ds, pairs)]
            dk = [dot_lt(v, heads_of(part(0, p))) for v, p in zip(ds, pairs)]
            for p, a, b in zip(pairs, dq2, dk):
                out(0, p, jnp.where(low_half, a[:SEG], a[SEG:]) * scale)
                out(1, p, b * scale)

    gb_out[layer, 0] += colsum(dqkv_out[0, :, 0:d].astype(F32))
    gb_out[layer, 1] += colsum(dqkv_out[0, :, 2 * d : 3 * d].astype(F32))
    g_ref[...] = (
        t_ref[...]
        + dot_rt(dqkv_out[0, :, 0:d], wqkv[layer, 0])
        + dot_rt(dqkv_out[0, :, d : 2 * d], wqkv[layer, 1])
        + dot_rt(dqkv_out[0, :, 2 * d : 3 * d], wqkv[layer, 2])
    )

    @pl.when(layer == 0)
    def _():
        for i in range(MB):
            tg_out[i, 0] = g_ref[i * SEG : i * SEG + TEXT, :].astype(BF)
            tail = g_ref[i * SEG + TAIL : (i + 1) * SEG, :]
            back = tail + pltpu.roll(tail, MEM, axis=0)
            gm_ref[i] = jnp.where(seg < counts[i], 0.0, gm_ref[i]) + back
        gm_out[...] = gm_ref[...]

    @pl.when((seg == 0) & (layer == 0))
    def _():
        for l in range(LAYERS):
            for k in range(4):
                parts = (gb_out[l, k], gub_out[l, :, k * d : (k + 1) * d], gn_out[l, k])
                for base, part in zip((0, 8, 16), parts):
                    row = base + 4 * l + k
                    small_out[row : row + 1, :] = jnp.sum(part, axis=0, keepdims=True)


def backward_local(cot, cot_mem, counts, lens, kept, weights):
    wqkv, wo, wup, wdn, _, _, norm = weights
    _, qkv, p_all, gp, xh1, xh2, rs = kept
    d, ff = wup.shape[1:]
    gm0 = jnp.concatenate([jnp.zeros((MB, TEXT - TAIL + MEM, d), F32), cot_mem.astype(F32)], axis=1)
    total = SEGS * ROWS
    units = MB * HEADS * SEG
    smem = pl.BlockSpec(memory_space=pltpu.SMEM)
    hbm = pl.BlockSpec(memory_space=pl.ANY)

    def kept_spec(rows, cols):
        return pl.BlockSpec((1, rows, cols), lambda s, l: (LAYERS - 1 - l, SEGS - 1 - s, 0))

    outs = pl.pallas_call(
        bwd_kernel,
        grid=(SEGS, LAYERS),
        in_specs=[
            smem, smem,
            pl.BlockSpec((MB, 1, TEXT, d), lambda s, l: (0, SEGS - 1 - s, 0, 0)),
            whole(gm0.shape),
            kept_spec(ROWS, 3 * d), kept_spec(units, 128), kept_spec(ROWS, ff), kept_spec(ROWS, d), kept_spec(ROWS, d),
            pl.BlockSpec((1, 2, ROWS, 128), lambda s, l: (LAYERS - 1 - l, 0, SEGS - 1 - s, 0)),
            hbm, hbm, hbm, hbm, whole(norm.shape),
        ],
        out_specs=[
            pl.BlockSpec((MB, 1, TEXT, d), lambda s, l: (0, SEGS - 1 - s, 0, 0)),
            whole(gm0.shape),
            kept_spec(ROWS, 5 * d + ff), whole((24, d)),
        ],
        out_shape=[
            jax.ShapeDtypeStruct((MB, SEGS, TEXT, d), BF),
            jax.ShapeDtypeStruct(gm0.shape, F32),
            jax.ShapeDtypeStruct((LAYERS, total, 5 * d + ff), BF),
            jax.ShapeDtypeStruct((24, d), F32),
        ],
        scratch_shapes=[
            pltpu.VMEM((ROWS, d), F32), pltpu.VMEM(gm0.shape, F32),
            pltpu.VMEM((ROWS, d), F32), pltpu.VMEM((ROWS, d), F32), pltpu.VMEM((ROWS, d), BF),
            pltpu.VMEM(wqkv.shape, BF), pltpu.VMEM(wo.shape, BF), pltpu.VMEM(wup.shape, BF), pltpu.VMEM(wdn.shape, BF),
            pltpu.SemaphoreType.DMA((LAYERS, 4)),
            pltpu.VMEM((LAYERS, 4, 8, d), F32), pltpu.VMEM((LAYERS, 8, ff), F32), pltpu.VMEM((LAYERS, 4, 8, d), F32),
        ],
        compiler_params=pltpu.CompilerParams(
            dimension_semantics=("arbitrary", "arbitrary"), vmem_limit_bytes=VMEM_LIMIT
        ),
        name="rmt_backward",
    )(counts, lens, cot, gm0, qkv, p_all, gp, xh1, xh2, rs, wqkv, wo, wup, wdn, norm.astype(F32))
    tg, gm = outs[:2]
    return tg, gm[:, TEXT - TAIL + MEM :].astype(BF), outs[2], outs[3]


TILES = 12


def product_kernel(ids, lhs, rhs, out):
    out[0, 0] = dot_lt(lhs[0], rhs[0]).astype(BF)


def weight_grads(lhs, rhs, layers):
    d = rhs.shape[-1] // 9
    total = lhs.shape[1]
    count = layers.shape[0]

    def left(l, t, ids):
        return (ids[l], 0, jnp.where(t < 3, 0, jnp.where(t < 4, 1, jnp.where(t < 8, 2, t - 5))))

    return pl.pallas_call(
        product_kernel,
        grid_spec=pltpu.PrefetchScalarGridSpec(
            num_scalar_prefetch=1,
            grid=(count, TILES),
            in_specs=[
                pl.BlockSpec((1, total, d), left),
                pl.BlockSpec((1, total, d), lambda l, t, ids: (ids[l], 0, jnp.minimum(t, 8))),
            ],
            out_specs=pl.BlockSpec((1, 1, d, d), lambda l, t, ids: (l, t, 0, 0)),
        ),
        out_shape=jax.ShapeDtypeStruct((count, TILES, d, d), BF),
        compiler_params=pltpu.CompilerParams(
            dimension_semantics=("arbitrary", "arbitrary"), vmem_limit_bytes=VMEM_LIMIT
        ),
        name="weight_products",
    )(layers, lhs, rhs)


MESH = pl.DeviceIdType.MESH
ZN = 4


def multiple(v, k):
    return v if isinstance(v, int) else pl.multiple_of(v, k)


def span(start, size):
    return pl.ds(multiple(start, size if size % 128 else 128), size)


def where_am_i():
    w, n = lax.axis_index("wide"), lax.axis_index("narrow")
    z, x = lax.div(w, 2), lax.rem(w, 2)
    y, c = lax.div(n, 2), lax.rem(n, 2)
    links = {
        "p": {"wide": w, "narrow": n + 1 - 2 * c},
        "x": {"wide": w + 1 - 2 * x, "narrow": n},
        "y": {"wide": w, "narrow": lax.rem(n + 2, 4)},
        "up": {"wide": w + 2, "narrow": n},
        "down": {"wide": w - 2, "narrow": n},
    }
    return w, n, z, x, y, c, links


def enter(z, links):
    barrier = pltpu.get_barrier_semaphore()
    for name in ("p", "x", "y"):
        pl.semaphore_signal(barrier, inc=1, device_id=links[name], device_id_type=MESH)

    @pl.when(z < ZN - 1)
    def _():
        pl.semaphore_signal(barrier, inc=1, device_id=links["up"], device_id_type=MESH)

    @pl.when(z > 0)
    def _():
        pl.semaphore_signal(barrier, inc=1, device_id=links["down"], device_id_type=MESH)

    pl.semaphore_wait(barrier, 3 + jnp.minimum(z, 1) + jnp.minimum(ZN - 1 - z, 1))


class Net:
    def __init__(self, ssem, rsem, links):
        self.ssem, self.rsem, self.links = ssem, rsem, links
        self.next_send, self.next_recv = 0, 0

    def sends(self, count):
        base, self.next_send = self.next_send, self.next_send + count
        return base

    def recvs(self, count):
        base, self.next_recv = self.next_recv, self.next_recv + count
        return base

    def copy(self, link, src, dst, s, r):
        return pltpu.make_async_remote_copy(
            src_ref=src, dst_ref=dst, send_sem=self.ssem.at[s], recv_sem=self.rsem.at[r],
            device_id=self.links[link], device_id_type=MESH,
        )


def gather_kernel(
    q_in, o_in, u_in, d_in, s_in, Q, O, U, D, S,
    tq, to, tu, td, aq, ao, au, ad, ssem, rsem, lsem,
):
    w, n, z, x, y, c, links = where_am_i()
    mine, other = c, 1 - c
    net = Net(ssem, rsem, links)
    rw, cn = aq.shape[1], aq.shape[2]
    rd, cu = ad.shape[0], au.shape[1]
    half = cu // 2
    enter(z, links)

    first = [net.copy("p", src, dst, net.sends(1), net.recvs(1)) for src, dst in (
        (q_in.at[other], tq), (o_in.at[other], to), (u_in.at[other], tu), (d_in.at[other], td),
        (s_in, S.at[z, x, y, c]),
    )]
    for cp in first:
        cp.start()
    own_small = pltpu.make_async_copy(s_in, S.at[z, x, y, c], lsem.at[4])
    own_small.start()

    def join(own, got):
        a, b = own.astype(F32), got.astype(F32)
        lo, hi = jnp.where(c == 0, a, b), jnp.where(c == 0, b, a)
        return jnp.concatenate([lo, hi], axis=-1).astype(BF)

    outs = (
        (au, U.at[mine, span(rw * w, rw), span(cu * y, cu)]),
        (aq, Q.at[mine, :, span(rw * w, rw), span(cn * y, cn)]),
        (ao, O.at[mine, span(rw * w, rw), span(cn * y, cn)]),
        (ad, D.at[mine, span(rd * w, rd), span(cn * y, cn)]),
    )
    first[2].wait()
    au[...] = join(u_in[mine], tu[...])
    first[0].wait()
    for j in range(3):
        aq[j] = join(q_in[mine, j], tq[j])
    first[1].wait()
    ao[...] = join(o_in[mine], to[...])
    first[3].wait()
    ad[...] = join(d_in[mine], td[...])
    first[4].wait()
    own_small.wait()
    local = [pltpu.make_async_copy(src, dst, lsem.at[k]) for k, (src, dst) in enumerate(outs)]
    for cp in local:
        cp.start()
    for cp in local:
        cp.wait()

    main = rd - rw

    def rows_a(zp):
        return span(2 * rw * zp, 2 * rw)

    def rows_x(zp, xp):
        return span(rw * (2 * zp + xp), rw)

    def rows_d(zp, xp):
        return pl.ds(pl.multiple_of(rd * (2 * zp + xp), rw), main)

    def rows_v(zp, xp):
        return pl.ds(pl.multiple_of(rd * (2 * zp + xp) + main, rw), rw)

    def cols(yp):
        return span(cn * yp, cn)

    def blk_a(zp, xp, yp):
        return [Q.at[mine, :, rows_x(zp, xp), cols(yp)]]

    def blk_d(zp, xp, yp):
        return [D.at[mine, rows_d(zp, xp), cols(yp)]]

    def reg_a(zp, yp, layer):
        return [Q.at[layer, :, rows_a(zp), cols(yp)]]

    def reg_d(zp, xp, layer):
        return [D.at[layer, rows_d(zp, xp), :]]

    def u_cols(zp, xp, start, size):
        return U.at[mine, rows_x(zp, xp), span(start, size)]

    def blk_u(zp, xp, yp):
        return [
            u_cols(zp, xp, cu * yp, cu), O.at[mine, rows_x(zp, xp), cols(yp)], D.at[mine, rows_v(zp, xp), cols(yp)]
        ]

    def blk_u1(zp, xp, yp):
        return [u_cols(zp, xp, cu * yp, half), O.at[mine, rows_x(zp, xp), cols(yp)]]

    def blk_u2(zp, xp, yp):
        return [u_cols(zp, xp, cu * yp + half, half), D.at[mine, rows_v(zp, xp), cols(yp)]]

    def pair_u1(zp, yp, layer):
        return [U.at[layer, rows_a(zp), span(cu * yp, half)], O.at[layer, rows_a(zp), cols(yp)]]

    def pair_u2(zp, xp, layer):
        rows = rows_x(zp, xp)
        return [U.at[layer, rows, span(cu * yp + half, half)] for yp in range(2)] + [D.at[layer, rows_v(zp, xp), :]]

    class Lane:
        def __init__(self, link, sent, got, parts):
            self.link, self.sent, self.got, self.parts = link, sent, got, parts
            self.s = [net.sends(ZN) for _ in range(parts)]
            self.r = [net.recvs(ZN) for _ in range(parts)]

        def send(self, zp):
            for k, ref in enumerate(self.sent(zp)):
                net.copy(self.link, ref, ref, self.s[k] + zp, self.r[k] + zp).start()

        def recv(self, zp):
            for k, ref in enumerate(self.got(zp)):
                net.copy(self.link, ref, ref, self.s[k] + zp, self.r[k] + zp).wait_recv()

        def drain(self, zp):
            for k, ref in enumerate(self.sent(zp)):
                net.copy(self.link, ref, ref, self.s[k] + zp, self.r[k] + zp).wait_send()

    class Line:
        def __init__(self, region, parts):
            self.region, self.parts = region, parts
            self.su = [net.sends(ZN) for _ in range(parts)]
            self.sd = [net.sends(ZN) for _ in range(parts)]
            self.r = [net.recvs(ZN) for _ in range(parts)]

        def each(self, link, sems, zp, what):
            for k, ref in enumerate(self.region(zp)):
                getattr(net.copy(link, ref, ref, sems[k] + zp, self.r[k] + zp), what)()

        def own(self, what="start"):
            @pl.when(z < ZN - 1)
            def _():
                self.each("up", self.su, z, what)

            @pl.when(z > 0)
            def _():
                self.each("down", self.sd, z, what)

        def relay(self, t, what="start"):
            @pl.when(jnp.minimum(z - t, ZN - 2 - z) >= 0)
            def _():
                self.each("up", self.su, z - t, what)

            @pl.when(jnp.minimum(ZN - 1 - t - z, z - 1) >= 0)
            def _():
                self.each("down", self.sd, z + t, what)

        def recv(self, zp):
            self.each("up", self.su, zp, "wait_recv")

    line_a = [Line(lambda zp, xp=xp: blk_a(zp, xp, y), 1) for xp in (x, 1 - x)]
    line_d = [Line(lambda zp, yp=yp: blk_d(zp, x, yp), 1) for yp in (y, 1 - y)]
    line_u = Line(lambda zp: blk_u(zp, x, y), 3)
    x1 = Lane("x", lambda zp: blk_a(z, x, y), lambda zp: blk_a(z, 1 - x, y), 1)
    y1 = Lane("y", lambda zp: blk_d(z, x, y), lambda zp: blk_d(z, x, 1 - y), 1)
    x_u1 = Lane("x", lambda zp: blk_u1(zp, x, y), lambda zp: blk_u1(zp, 1 - x, y), 2)
    y_u2 = Lane("y", lambda zp: blk_u2(zp, x, y), lambda zp: blk_u2(zp, x, 1 - y), 2)
    y_a = [
        Lane("y", lambda zp, xp=xp: blk_a(zp, xp, y), lambda zp, xp=xp: blk_a(zp, xp, 1 - y), 1) for xp in (x, 1 - x)
    ]
    x_d = [
        Lane("x", lambda zp, yp=yp: blk_d(zp, x, yp), lambda zp, yp=yp: blk_d(zp, 1 - x, yp), 1) for yp in (y, 1 - y)
    ]
    y_u1 = Lane("y", lambda zp: pair_u1(zp, y, mine), lambda zp: pair_u1(zp, 1 - y, mine), 2)
    x_u2 = Lane("x", lambda zp: pair_u2(zp, x, mine), lambda zp: pair_u2(zp, 1 - x, mine), 3)

    def to_partner(make, parts):
        return Lane("p", lambda zp: make(zp, mine), lambda zp: make(zp, other), parts)

    p_a = to_partner(lambda zp, l: reg_a(zp, y, l), 1)
    p_a2 = to_partner(lambda zp, l: reg_a(zp, 1 - y, l), 1)
    p_d = to_partner(lambda zp, l: reg_d(zp, x, l), 1)
    p_d2 = to_partner(lambda zp, l: reg_d(zp, 1 - x, l), 1)
    p_u1 = to_partner(lambda zp, l: pair_u1(zp, y, l), 2)
    p_u1b = to_partner(lambda zp, l: pair_u1(zp, 1 - y, l), 2)
    p_u2 = to_partner(lambda zp, l: pair_u2(zp, x, l), 3)
    p_u2b = to_partner(lambda zp, l: pair_u2(zp, 1 - x, l), 3)

    small_x = Lane("x", lambda zp: [S.at[z, x, y]], lambda zp: [S.at[z, 1 - x, y]], 1)
    small_y = Lane("y", lambda zp: [S.at[z, :, y]], lambda zp: [S.at[z, :, 1 - y]], 1)
    line_s = Line(lambda zp: [S.at[zp]], 1)

    small_x.send(0)
    x1.send(0)
    y1.send(0)
    x_u1.send(z)
    y_u2.send(z)
    line_a[0].own()
    line_d[0].own()
    line_u.own()
    y_a[0].send(z)
    x_d[0].send(z)
    small_x.recv(0)
    small_y.send(0)
    x1.recv(0)
    line_a[1].own()
    y_a[1].send(z)
    p_a.send(z)
    y1.recv(0)
    line_d[1].own()
    x_d[1].send(z)
    p_d.send(z)
    small_y.recv(0)
    line_s.own()

    def second(zp):
        x_u1.recv(zp)
        y_u1.send(zp)
        p_u1.send(zp)
        y_u2.recv(zp)
        x_u2.send(zp)
        p_u2.send(zp)

    def third(zp):
        for lane in y_a:
            lane.recv(zp)
        p_a2.send(zp)
        for lane in x_d:
            lane.recv(zp)
        p_d2.send(zp)
        y_u1.recv(zp)
        p_u1b.send(zp)
        x_u2.recv(zp)
        p_u2b.send(zp)

    def both_ways(t, make):
        @pl.when(z >= t)
        def _():
            make(z - t)

        @pl.when(z < ZN - t)
        def _():
            make(z + t)

    def take(line, t, *lanes):
        both_ways(t, line.recv)
        line.relay(t)
        for lane in lanes:
            both_ways(t, lane.send)

    second(z)
    for t in range(1, ZN):
        take(line_a[0], t, y_a[0])
        take(line_d[0], t, x_d[0])
        take(line_u, t, x_u1, y_u2)
        take(line_a[1], t, y_a[1], p_a)
        if t == 1:
            third(z)
        else:
            both_ways(t - 1, third)
        take(line_d[1], t, x_d[1], p_d)
        both_ways(t, second)
        take(line_s, t)
    both_ways(ZN - 1, third)

    partner = (p_a, p_a2, p_d, p_d2, p_u1, p_u1b, p_u2, p_u2b)
    for zp in range(ZN):
        for lane in partner:
            lane.recv(zp)
    for zp in range(ZN):
        for lane in partner + (x_u1, y_u2, *y_a, *x_d, y_u1, x_u2):
            lane.drain(zp)
    for lane in (x1, y1, small_x, small_y):
        lane.drain(0)
    for line in (line_u, *line_a, *line_d, line_s):
        line.own("wait_send")
        for t in range(1, ZN):
            line.relay(t, "wait_send")
    assert net.next_send <= ssem.shape[0] and net.next_recv <= rsem.shape[0]


def gather_fast(pieces):
    wqkv, wo, wup, wdn, bias, ubias, norm = pieces
    _, _, rw, cn = wqkv.shape
    rd, cu = wdn.shape[1], wup.shape[2]
    d, ff = rw * 8, rd * 8
    small = jnp.concatenate([bias[:, 0], norm[:, 0], ubias, jnp.zeros_like(ubias)], axis=0).astype(F32)
    small = jnp.pad(small, ((0, 0), (0, 128 - rw)))
    hbm = pl.BlockSpec(memory_space=pl.ANY)
    vmem = pl.BlockSpec(memory_space=pltpu.VMEM)
    Q, O, U, D, S = pl.pallas_call(
        gather_kernel,
        in_specs=[vmem] * 5,
        out_specs=[hbm] * 5,
        out_shape=[
            jax.ShapeDtypeStruct((LAYERS, 3, d, d), BF),
            jax.ShapeDtypeStruct((LAYERS, d, d), BF),
            jax.ShapeDtypeStruct((LAYERS, d, ff), BF),
            jax.ShapeDtypeStruct((LAYERS, ff, d), BF),
            jax.ShapeDtypeStruct((ZN, 2, 2, 2, 8, 128), F32),
        ],
        scratch_shapes=[
            pltpu.VMEM((3, rw, cn), BF), pltpu.VMEM((rw, cn), BF), pltpu.VMEM((rw, cu), BF), pltpu.VMEM((rd, cn), BF),
            pltpu.VMEM((3, rw, 2 * cn), BF), pltpu.VMEM((rw, 2 * cn), BF),
            pltpu.VMEM((rw, 2 * cu), BF), pltpu.VMEM((rd, 2 * cn), BF),
            pltpu.SemaphoreType.DMA((200,)), pltpu.SemaphoreType.DMA((200,)), pltpu.SemaphoreType.DMA((5,)),
        ],
        compiler_params=pltpu.CompilerParams(collective_id=1, has_side_effects=True),
        name="weight_gather",
    )(wqkv, wo, wup, wdn, small)
    S = S.reshape(8, 4, 8, 128)[..., :rw]
    rows = jnp.transpose(S, (2, 1, 0, 3)).reshape(8, 4, d)
    ub = jnp.transpose(S[:, :, 4:6], (2, 0, 1, 3)).reshape(2, ff)
    return Q, O, U, D, rows[0:2], ub, rows[2:4]


def accumulate(dst, src, rows, step=48):
    def body(i, carry):
        r = pl.ds(pl.multiple_of(i * step, 16), step)
        dst[r, :] = dst[r, :] + src[r, :]
        return carry

    lax.fori_loop(0, rows // step, body, 0)


def scatter_kernel(
    gw, lhs, rhs, sm_in, oq, oo, ou, od, sm_out,
    AT, AD, RH, LT, LB, FA, FD, F1, FO, F2, FV, S1, SO, S2, SV, ZA, ZD, ZU, ZO, ZV, TA, TD,
    hq, ho, hu, hd, s_p, s_x, s_y, s_below, s_above, s_a, s_b, s_sum, s_up, s_down, ssem, rsem, lsem,
):
    w, n, z, x, y, c, links = where_am_i()
    mine, other = c, 1 - c
    net = Net(ssem, rsem, links)
    d, ff = AT.shape[2], AD.shape[0]
    rw, cn = d // 8, d // 2
    rd, cu = ff // 8, ff // 2
    half = cu // 2
    enter(z, links)

    class Hop:
        def __init__(self, link, pairs, parts):
            self.link, self.pairs = link, pairs
            self.s = [net.sends(ZN) for _ in range(parts)]
            self.r = [net.recvs(ZN) for _ in range(parts)]

        def each(self, zp, what):
            for k, (src, dst) in enumerate(self.pairs(zp)):
                getattr(net.copy(self.link, src, dst, self.s[k] + zp, self.r[k] + zp), what)()

        def send(self, zp):
            self.each(zp, "start")

        def recv(self, zp):
            self.each(zp, "wait_recv")

        def drain(self, zp):
            self.each(zp, "wait_send")

    def rows_a(zp):
        return span(2 * rw * zp, 2 * rw)

    main = rd - rw

    def down(zp):
        return span(d * zp, d)

    swap = [
        Hop("p", lambda zp: [(gw.at[0, 0:3, rows_a(zp), :], AT.at[0:3, rows_a(zp), :])], 1),
        Hop("p", lambda zp: [(gw.at[0, 8 + zp], AD.at[down(zp), :])], 1),
        Hop("p", lambda zp: [(gw.at[0, 3:8, rows_a(zp), :], AT.at[3:8, rows_a(zp), :])], 1),
    ]

    def right(t):
        return pltpu.make_async_copy(rhs.at[mine, :, t * d : (t + 1) * d], RH.at[t], lsem.at[t])

    def left(j):
        return pltpu.make_async_copy(lhs.at[mine, :, j * d : (j + 1) * d], LB.at[j], lsem.at[9 + j])

    def left_g(v, zp):
        slot = (v + 3) % 4
        return pltpu.make_async_copy(lhs.at[mine, :, span(d * (3 + zp), d)], LB.at[slot], lsem.at[12 + v])

    def turn(j):
        step = 256

        def body(k, carry):
            part = pl.ds(pl.multiple_of(k * step, step), step)
            LT[j, :, part] = LB[j, part, :].T
            return carry

        lax.fori_loop(0, LB.shape[1] // step, body, 0)

    def products(first, last, zp):
        rows = rows_a(zp)

        def body(t, carry):
            j = jnp.where(t < 3, 0, jnp.where(t < 4, 1, 2))
            AT[t, rows, :] = (AT[t, rows, :].astype(F32) + dot(LT[j, rows, :], RH[t])).astype(BF)
            return carry

        lax.fori_loop(first, last, body, 0)

    def products_down(v, zp):
        rows = down(zp)

        def body(k, carry):
            cols = pl.ds(pl.multiple_of(k * cn, cn), cn)
            AD[rows, cols] = (AD[rows, cols].astype(F32) + dot_lt(LB[(v + 3) % 4], RH[8, :, cols])).astype(BF)
            return carry

        lax.fori_loop(0, 2, body, 0)

    def cols_a(yp):
        return span(cn * yp, cn)

    def rows_x(zp, xp):
        return span(rw * (2 * zp + xp), rw)

    def rows_d(zp, xp):
        return pl.ds(pl.multiple_of(rd * (2 * zp + xp), rw), main)

    def rows_v(zp, xp):
        return pl.ds(pl.multiple_of(rd * (2 * zp + xp) + main, rw), rw)

    def reg_a(zp, yp):
        return AT.at[0:3, rows_a(zp), cols_a(yp)]

    def reg_d(zp, xp):
        return AD.at[rows_d(zp, xp), :]

    def u1(zp, yp):
        return [AT.at[4 + 2 * yp, rows_a(zp), :], AT.at[3, rows_a(zp), cols_a(yp)]]

    def u1_part(zp, xp, yp):
        return [AT.at[4 + 2 * yp, rows_x(zp, xp), :], AT.at[3, rows_x(zp, xp), cols_a(yp)]]

    def u2(zp, xp):
        rows = rows_x(zp, xp)
        return [AT.at[5 + 2 * yp, rows, :] for yp in range(2)] + [AD.at[rows_v(zp, xp), :]]

    def u2_part(zp, xp, yp):
        return [AT.at[5 + 2 * yp, rows_x(zp, xp), :], AD.at[rows_v(zp, xp), cols_a(yp)]]

    def blk_u(zp):
        rows = rows_x(zp, x)
        return [AT.at[pl.ds(4 + 2 * y, 2), rows, :], AT.at[3, rows, cols_a(y)], AD.at[rows_v(zp, x), cols_a(y)]]

    def bufs_u1(zp):
        return [F1.at[zp], FO.at[zp]]

    def bufs_u2(zp):
        return [F2.at[0, zp], F2.at[1, zp], FV.at[zp]]

    def bufs_s1(zp):
        return [S1.at[zp], SO.at[zp]]

    def bufs_s2(zp):
        return [S2.at[zp], SV.at[zp]]

    y_a = Hop("y", lambda zp: [(reg_a(zp, 1 - y), FA.at[zp])], 1)
    x_d = Hop("x", lambda zp: [(reg_d(zp, 1 - x), FD.at[zp])], 1)
    y_u1 = Hop("y", lambda zp: list(zip(u1(zp, 1 - y), bufs_u1(zp))), 2)
    x_u2 = Hop("x", lambda zp: list(zip(u2(zp, 1 - x), bufs_u2(zp))), 3)
    x_u1 = Hop("x", lambda zp: list(zip(u1_part(zp, 1 - x, y), bufs_s1(zp))), 2)
    y_u2 = Hop("y", lambda zp: list(zip(u2_part(zp, x, 1 - y), bufs_s2(zp))), 2)
    last_a = Hop("x", lambda zp: [(AT.at[0:3, rows_x(z, 1 - x), cols_a(y)], TA)], 1)
    last_d = Hop("y", lambda zp: [(AD.at[rows_d(z, x), cols_a(1 - y)], TD)], 1)

    def add_all(dsts, srcs):
        for dst, src in zip(dsts, srcs):
            accumulate(dst, src, src.shape[0])

    class Line:
        def __init__(self, region, bufs):
            self.region, self.bufs = region, bufs
            self.su = [net.sends(ZN) for _ in bufs]
            self.sd = [net.sends(ZN) for _ in bufs]
            self.r = [net.recvs(ZN + 1) for _ in bufs]

        def up(self, zp, what):
            slot = jnp.where(zp == z + 1, ZN, zp)

            @pl.when(zp > z)
            def _():
                for k, (src, buf) in enumerate(zip(self.region(zp), self.bufs)):
                    getattr(net.copy("up", src, buf.at[slot], self.su[k] + zp, self.r[k] + slot), what)()

        def down(self, zp, what):
            @pl.when(zp < z)
            def _():
                for k, (src, buf) in enumerate(zip(self.region(zp), self.bufs)):
                    getattr(net.copy("down", src, buf.at[zp], self.sd[k] + zp, self.r[k] + zp), what)()

        def take(self, zp, slot):
            for k, (dst, buf) in enumerate(zip(self.region(zp), self.bufs)):
                net.copy("up", dst, buf.at[slot], self.su[k] + zp, self.r[k] + slot).wait_recv()
                self.add(dst, buf.at[slot])

        def add(self, dst, src):
            if len(src.shape) == 3:
                for j in range(src.shape[0]):
                    accumulate(dst.at[j], src.at[j], src.shape[1])
            else:
                accumulate(dst, src, src.shape[0])

        def go(self, zp):
            @pl.when(jnp.minimum(z - zp, ZN - 2 - z) >= 0)
            def _():
                self.take(zp, zp)

            @pl.when(jnp.minimum(zp - z, z - 1) >= 0)
            def _():
                self.take(zp, jnp.where(zp == z, ZN, zp))

            self.up(zp, "start")
            self.down(zp, "start")

        def drain(self, zp):
            self.up(zp, "wait_send")
            self.down(zp, "wait_send")

    line_a = Line(lambda zp: (reg_a(zp, y),), (ZA,))
    line_d = Line(lambda zp: (reg_d(zp, x),), (ZD,))
    line_u = Line(blk_u, (ZU, ZO, ZV))

    table = ((3, 3, 0, 0), (2, 0, 3, 1), (1, 2, 1, 2), (0, 1, 2, 3))
    order = [jnp.where(z == 0, t[0], jnp.where(z == 1, t[1], jnp.where(z == 2, t[2], t[3]))) for t in table]

    small = [
        net.copy(link, src, dst, net.sends(1), net.recvs(1))
        for link, src, dst in (("p", sm_in, s_p), ("x", s_a, s_x), ("y", s_b, s_y))
    ]
    small_up = net.copy("up", s_up, s_below, net.sends(1), net.recvs(1))
    small_down = net.copy("down", s_down, s_above, net.sends(1), net.recvs(1))

    small[0].start()
    left(0).start()
    for t in range(3):
        right(t).start()
    left_g(0, order[0]).start()
    right(8).start()
    for j in (1, 2):
        left(j).start()
    for t in range(3, 8):
        right(t).start()
    for zp in order:
        for part in swap:
            part.send(zp)

    def open_slab(v):
        zp = order[v]
        if v == 0:
            left(0).wait()
            turn(0)
            for t in range(3):
                right(t).wait()
        swap[0].recv(zp)
        products(0, 3, zp)
        y_a.send(zp)
        left_g(v, zp).wait()
        if v == 0:
            right(8).wait()
        swap[1].recv(zp)
        products_down(v, zp)
        x_d.send(zp)
        if v == 0:
            left_g(1, order[1]).start()
            for j in (1, 2):
                left(j).wait()
                turn(j)
                left_g(j + 1, order[j + 1]).start()
            for t in range(3, 8):
                right(t).wait()
        swap[2].recv(zp)
        products(3, 8, zp)
        y_u1.send(zp)
        x_u2.send(zp)

    def mid_a(zp):
        y_a.recv(zp)
        for j in range(3):
            accumulate(reg_a(zp, y).at[j], FA.at[zp, j], 2 * rw)
        line_a.go(zp)

    def mid_d(zp):
        x_d.recv(zp)
        accumulate(reg_d(zp, x), FD.at[zp], main)
        line_d.go(zp)

    def mid_u(zp):
        y_u1.recv(zp)
        add_all(u1(zp, y), bufs_u1(zp))
        x_u1.send(zp)
        x_u2.recv(zp)
        add_all(u2(zp, x), bufs_u2(zp))
        y_u2.send(zp)

    def close(zp):
        x_u1.recv(zp)
        add_all(u1_part(zp, x, y), bufs_s1(zp))
        y_u2.recv(zp)
        add_all(u2_part(zp, x, y), bufs_s2(zp))
        line_u.go(zp)

    open_slab(0)
    mid_a(order[0])
    small[0].wait()
    s_a[...] = sm_in[...] + s_p[...]
    small[1].start()
    open_slab(1)
    mid_d(order[0])
    mid_u(order[0])
    small[1].wait()
    s_b[...] = s_a[...] + s_x[...]
    small[2].start()
    open_slab(2)
    mid_a(order[1])
    close(order[0])
    mid_d(order[1])
    mid_u(order[1])
    small[2].wait()
    s_sum[...] = s_b[...] + s_y[...]
    open_slab(3)
    mid_a(order[2])
    close(order[1])
    mid_d(order[2])
    mid_u(order[2])

    @pl.when(z > 0)
    def _():
        small_up.wait_recv()

    @pl.when(z == 0)
    def _():
        s_below[...] = jnp.zeros_like(s_below)

    @pl.when(z < ZN - 1)
    def _():
        s_up[...] = s_sum[...] + s_below[...]
        small_up.start()

    mid_a(order[3])
    last_a.send(0)
    close(order[2])
    mid_d(order[3])
    last_d.send(0)
    mid_u(order[3])

    @pl.when(z < ZN - 1)
    def _():
        small_down.wait_recv()

    @pl.when(z == ZN - 1)
    def _():
        s_above[...] = jnp.zeros_like(s_above)

    @pl.when(z > 0)
    def _():
        s_down[...] = s_sum[...] + s_above[...]
        small_down.start()

    sm_out[...] = s_sum[...] + s_below[...] + s_above[...]
    close(order[3])

    def pick(v, k):
        lo, hi = v[..., :k], v[..., k:]
        return jnp.where(c == 0, lo, hi), jnp.where(c == 0, hi, lo)

    out = [
        net.copy("p", src, dst.at[mine], net.sends(1), net.recvs(1))
        for src, dst in ((hu, ou), (hq, oq), (ho, oo), (hd, od))
    ]
    rows = rows_x(z, x)
    ou[mine] = AT[4 + 2 * y + c, rows, :].astype(F32)
    hu[...] = AT[5 + 2 * y - c, rows, :].astype(F32)
    out[0].start()
    keep, give = pick(AT[3, rows, cols_a(y)].astype(F32), cn // 2)
    oo[mine] = keep
    ho[...] = give
    out[2].start()
    last_a.recv(0)
    for j in range(3):
        keep, give = pick(AT[j, rows, cols_a(y)].astype(F32) + TA[j].astype(F32), cn // 2)
        oq[mine, j] = keep
        hq[j] = give
    out[1].start()
    last_d.recv(0)
    for k in range(rd // rw):
        part = slice(k * rw, (k + 1) * rw)
        here = span(rd * w + k * rw, rw)
        total = AD[here, cols_a(y)].astype(F32)
        if k * rw < main:
            total = total + TD[part, :].astype(F32)
        keep, give = pick(total, cn // 2)
        od[mine, part, :] = keep
        hd[part, :] = give
    out[3].start()

    for zp in range(ZN):
        for hop in (*swap, y_a, x_d, y_u1, x_u2, x_u1, y_u2):
            hop.drain(zp)
        for line in (line_a, line_d, line_u):
            line.drain(zp)
    last_a.drain(0)
    last_d.drain(0)

    @pl.when(z < ZN - 1)
    def _():
        small_up.wait_send()

    @pl.when(z > 0)
    def _():
        small_down.wait_send()

    for cp in out:
        cp.wait()
    assert net.next_send <= ssem.shape[0] and net.next_recv <= rsem.shape[0]


def scatter_fast(gw, lhs, rhs, pack):
    d = gw.shape[-1]
    ff = 4 * d
    rw, cn, rd, cu = d // 8, d // 2, ff // 8, ff // 2
    hbm = pl.BlockSpec(memory_space=pl.ANY)
    vmem = pl.BlockSpec(memory_space=pltpu.VMEM)

    def buf(*shape):
        return pltpu.VMEM(shape, BF)

    def wide(*shape):
        return pltpu.VMEM(shape, F32)

    outs = [(3, rw, cn // 2), (rw, cn // 2), (rw, cu // 2), (rd, cn // 2)]
    total = lhs.shape[1]
    full = [buf(8, d, d), buf(ff, d), buf(9, total, d), buf(3, d, total), buf(4, total, d)]
    oq, oo, ou, od, summed = pl.pallas_call(
        scatter_kernel,
        in_specs=[hbm, hbm, hbm, vmem],
        out_specs=[vmem] * 5,
        out_shape=[jax.ShapeDtypeStruct((LAYERS,) + s, F32) for s in outs] + [jax.ShapeDtypeStruct(pack.shape, F32)],
        scratch_shapes=full + [
            buf(ZN, 3, 2 * rw, cn), buf(ZN, rd - rw, d), buf(ZN, 2 * rw, cu // 2), buf(ZN, 2 * rw, cn),
            buf(2, ZN, rw, cu // 2), buf(ZN, rw, d), buf(ZN, rw, cu // 2), buf(ZN, rw, cn),
            buf(ZN, rw, cu // 2), buf(ZN, rw, cn), buf(ZN + 1, 3, 2 * rw, cn), buf(ZN + 1, rd - rw, d),
            buf(ZN + 1, 2, rw, cu // 2), buf(ZN + 1, rw, cn), buf(ZN + 1, rw, cn), buf(3, rw, cn), buf(rd - rw, cn),
        ] + [wide(*s) for s in outs] + [wide(*pack.shape)] * 10 + [
            pltpu.SemaphoreType.DMA((180,)), pltpu.SemaphoreType.DMA((160,)), pltpu.SemaphoreType.DMA((16,)),
        ],
        compiler_params=pltpu.CompilerParams(collective_id=2, has_side_effects=True, vmem_limit_bytes=VMEM_LIMIT),
        name="gradient_scatter",
    )(gw, lhs, rhs, pack)
    w, n = lax.axis_index("wide"), lax.axis_index("narrow")
    gb = lax.dynamic_slice(summed[0:8].reshape(2, 4, d), (0, n, w * rw), (2, 1, rw))
    gn = lax.dynamic_slice(summed[16:24].reshape(2, 4, d), (0, n, w * rw), (2, 1, rw))
    gub = lax.dynamic_slice(summed[8:16].reshape(2, ff), (0, (4 * w + n) * rw), (2, rw))
    return oq, oo, ou, od, gb, gub, gn


def gather_weights(pieces):
    wqkv, wo, wup, wdn, bias, ubias, norm = pieces
    narrow = [(wqkv, 3), (wo, 2), (wup, 2), (wdn, 2), (bias, 1), (norm, 1)]
    wqkv, wo, wup, wdn, bias, norm = (lax.all_gather(w, "narrow", axis=k, tiled=True) for w, k in narrow)
    wide = [(wqkv, 2), (wo, 1), (wup, 1), (wdn, 1), (bias, 2), (norm, 2)]
    wqkv, wo, wup, wdn, bias, norm = (lax.all_gather(w, "wide", axis=k, tiled=True) for w, k in wide)
    ubias = lax.all_gather(ubias, ("wide", "narrow"), axis=1, tiled=True)
    return wqkv, wo, wup, wdn, bias, ubias, norm


def scatter_two(grad, row_axis, col_axis):
    low = lax.psum_scatter(grad.astype(BF), "narrow", scatter_dimension=col_axis, tiled=True)
    return lax.psum_scatter(low.astype(F32), "wide", scatter_dimension=row_axis, tiled=True)


def scatter_grads(gw, pack):
    d = gw.shape[-1]
    gq, go, gdn = gw[:, 0:3], gw[:, 3], gw[:, 8:].reshape(LAYERS, -1, d)
    gup = jnp.moveaxis(gw[:, 4:8], 1, 2).reshape(LAYERS, d, -1)
    gb, gub, gn = pack[0:8].reshape(LAYERS, 4, d), pack[8:16].reshape(LAYERS, -1), pack[16:24].reshape(LAYERS, 4, d)
    big = (scatter_two(gq, 2, 3), scatter_two(go, 1, 2), scatter_two(gup, 1, 2), scatter_two(gdn, 1, 2))
    gub = lax.psum_scatter(gub, ("wide", "narrow"), scatter_dimension=1, tiled=True)

    def small_two(g):
        return lax.psum_scatter(
            lax.psum_scatter(g, "narrow", scatter_dimension=1, tiled=True), "wide", scatter_dimension=2, tiled=True
        )

    return big + (small_two(gb), gub, small_two(gn))


def shards(
    near, text_in, memory_in, counts, last_len, cot_text, cot_memory,
    qkv_weight, out_weight, up_weight, down_weight, biases, up_bias, norm_params,
):
    text, cot = text_in[:, 0], cot_text[:, 0]
    mem, cot_mem = memory_in[:, 0], cot_memory[:, 0]
    cnt, lens = counts[:, 0], last_len[:, 0]
    gather = gather_fast if near else gather_weights
    weights = gather((qkv_weight, out_weight, up_weight, down_weight, biases, up_bias, norm_params))
    text_out, mem_out, kept = forward_local(text, mem, cnt, lens, weights)
    text_grad, mem_grad, rhs, small = backward_local(cot, cot_mem, cnt, lens, kept, weights)
    if near:
        other = 1 - lax.rem(lax.axis_index("narrow"), 2)
        grads = scatter_fast(weight_grads(kept[0], rhs, other[None]), kept[0], rhs, small)
    else:
        grads = scatter_grads(weight_grads(kept[0], rhs, jnp.arange(LAYERS, dtype=jnp.int32)), small)
    return (text_out[:, None], mem_out[:, None], text_grad[:, None], mem_grad[:, None]) + grads


def solution(mesh):
    items = ("wide", "narrow")
    act5 = P(None, items, None, None, None)
    act4 = P(None, items, None, None)
    ids = P(None, items)
    split = P(None, "wide", "narrow")
    small = P(None, "narrow", "wide")
    params = (P(None, None, "wide", "narrow"), split, split, split, small, ids, small)
    near = (mesh.shape["wide"], mesh.shape["narrow"]) == (2 * ZN, 4)
    return jax.shard_map(
        functools.partial(shards, near),
        mesh=mesh,
        in_specs=(act5, act4, ids, ids, act5, act4) + params,
        out_specs=(act5, act4, act5, act4) + params,
        check_vma=False,
    )
```

```python
import functools

import jax
import jax.numpy as jnp
from jax import lax
from jax.experimental import pallas as pl
from jax.experimental.pallas import tpu as pltpu
from jax.sharding import PartitionSpec as P

HEADS = 12
HD = 64
MEM = 10
TEXT = 108
SEGS = 4
MB = 2
LAYERS = 2
SEG = TEXT + 2 * MEM
TAIL = 104
ROWS = MB * SEG
EPS = 1e-12
BF = jnp.bfloat16
F32 = jnp.float32
NEG = -1e30
RSQRT2 = 0.7071067811865476
RSQRT2PI = 0.3989422804014327
VMEM_LIMIT = 66_000_000
CHUNK = 32
GROUP_F = 6
GROUP_B = 6


def dot(a, b):
    return lax.dot_general(a, b, (((1,), (0,)), ((), ())), preferred_element_type=F32)


def dot_rt(a, b):
    return lax.dot_general(a, b, (((1,), (1,)), ((), ())), preferred_element_type=F32)


def dot_lt(a, b):
    return lax.dot_general(a, b, (((0,), (0,)), ((), ())), preferred_element_type=F32)


def row_ids(shape):
    return lax.broadcasted_iota(jnp.int32, shape, 0)


def lane_ids(shape):
    return lax.broadcasted_iota(jnp.int32, shape, 1)


def valid_rows(seg, count, length):
    return jnp.where(seg < count - 1, TEXT, jnp.where(seg == count - 1, length, 0))


def colsum(v):
    rows, cols = v.shape
    return jnp.sum(v.reshape(rows // 8, 8, cols), axis=0)


class Loads:
    def __init__(self, pairs, sems, first, order):
        self.pairs, self.sems, self.first, self.order = pairs, sems, first, order

    def each(self, layer, what):
        for k, (src, dst) in enumerate(self.pairs):
            getattr(pltpu.make_async_copy(src.at[layer], dst.at[layer], self.sems.at[layer, k]), what)()

    def start(self):
        self.each(self.order[0], "start")

    def need(self, step):
        @pl.when(self.first & (step == 0))
        def _():
            self.each(self.order[0], "wait")
            self.each(self.order[1], "start")

        @pl.when(self.first & (step == 1))
        def _():
            self.each(self.order[1], "wait")


def fwd_kernel(
    counts, lens, text, mem0, wqkv_hbm, wo_hbm, wup_hbm, wdn_hbm, bias, ubias, norm,
    text_out, mem_out, lhs_out, qkv_out, p_out, gp_out, xh1_out, xh2_out, rs_out,
    x_ref, mem_ref, y_ref, acc_ref, wqkv, wo, wup, wdn, wsem,
):
    seg = pl.program_id(0)
    layer = pl.program_id(1)
    d = x_ref.shape[-1]
    a_out, c_out, y_out = (lhs_out.at[:, :, j * d : (j + 1) * d] for j in range(3))
    g_out = lhs_out.at[:, :, 3 * d :]
    loads = Loads(((wqkv_hbm, wqkv), (wo_hbm, wo), (wup_hbm, wup), (wdn_hbm, wdn)), wsem, seg == 0, (0, 1))

    @pl.when((seg == 0) & (layer == 0))
    def _():
        loads.start()
        mem_ref[...] = mem0[...]

    @pl.when(layer == 0)
    def _():
        for i in range(MB):
            x_ref[i * SEG : i * SEG + TEXT, :] = text[i, 0].astype(F32)
            tail = slice(i * SEG + TAIL, (i + 1) * SEG)
            now = x_ref[tail, :]
            x_ref[tail, :] = jnp.where(row_ids(now.shape) < TEXT - TAIL, now, mem_ref[i])

    loads.need(layer)
    xb = x_ref[...].astype(BF)
    a_out[0] = xb
    qkv_out[0, :, 0:d] = (dot(xb, wqkv[layer, 0]) + bias[layer, 0:1, :]).astype(BF)
    qkv_out[0, :, d : 2 * d] = dot(xb, wqkv[layer, 1]).astype(BF)
    qkv_out[0, :, 2 * d : 3 * d] = (dot(xb, wqkv[layer, 2]) + bias[layer, 1:2, :]).astype(BF)

    low_half = lane_ids((SEG, 128)) < HD
    lanes = lane_ids((1, SEG))

    def heads_of(v):
        zero = jnp.zeros_like(v)
        return jnp.concatenate([jnp.where(low_half, v, zero), jnp.where(low_half, zero, v)], axis=0)

    for i in range(MB):
        vr = valid_rows(seg, counts[i], lens[i])
        keep = (lanes < vr) | (lanes >= TEXT)
        r0 = i * SEG
        for g0 in range(0, HEADS // 2, GROUP_F):
            pairs = range(g0, g0 + GROUP_F)

            def part(j, pair):
                return qkv_out[0, r0 : r0 + SEG, j * d + pair * 128 : j * d + pair * 128 + 128]

            s_all = [dot_rt(heads_of(part(0, p) * (HD ** -0.5)), part(1, p)) for p in pairs]
            s_all = [jnp.where(keep, s, NEG) for s in s_all]
            e_all = [jnp.exp(s - jnp.max(s, axis=-1, keepdims=True)) for s in s_all]
            p_all = [(e * (1.0 / jnp.sum(e, axis=-1, keepdims=True))).astype(BF) for e in e_all]
            c_all = [dot(pv, part(2, p)) for pv, p in zip(p_all, pairs)]
            for p, pv, c2 in zip(pairs, p_all, c_all):
                u0 = (i * (HEADS // 2) + p) * 2 * SEG
                p_out[0, u0 : u0 + 2 * SEG, :] = pv
                c_out[0, r0 : r0 + SEG, p * 128 : p * 128 + 128] = jnp.where(low_half, c2[:SEG], c2[SEG:]).astype(BF)

    def norm_to(base_ref, gain, shift, add, xh_out, rs_index, to_ref, low_out):
        for k in range(0, ROWS, CHUNK):
            rows = slice(k, k + CHUNK)
            h = base_ref[rows, :] + (acc_ref[rows, :] + add)
            center = h - jnp.mean(h, axis=-1, keepdims=True)
            rs = lax.rsqrt(jnp.mean(center * center, axis=-1, keepdims=True) + EPS)
            xh = center * rs
            xh_out[0, rows, :] = xh
            rs_out[0, rs_index, rows, :] = jnp.broadcast_to(rs, (CHUNK, 128))
            out = xh * gain + shift
            to_ref[rows, :] = out
            if low_out is not None:
                low_out[0, rows, :] = out.astype(BF)

    acc_ref[...] = dot(c_out[0], wo[layer])
    norm_to(x_ref, norm[layer, 0:1, :], norm[layer, 1:2, :], bias[layer, 2:3, :], xh1_out, 0, y_ref, y_out)

    ff = wup.shape[-1]

    def ffn_step():
        cols = slice(0, ff)
        u = dot(y_out[0], wup[layer, :, cols]) + ubias[layer, :, cols]
        cdf = 0.5 * (1.0 + lax.erf(u * RSQRT2))
        g_out[0, :, cols] = (u * cdf).astype(BF)
        gp_out[0, :, cols] = (cdf + u * (jnp.exp(-0.5 * (u * u)) * RSQRT2PI)).astype(BF)

    ffn_step()
    acc_ref[...] = dot(g_out[0], wdn[layer])
    norm_to(y_ref, norm[layer, 2:3, :], norm[layer, 3:4, :], bias[layer, 3:4, :], xh2_out, 1, x_ref, None)

    @pl.when(layer == LAYERS - 1)
    def _():
        for i in range(MB):
            vr = valid_rows(seg, counts[i], lens[i])
            body = x_ref[i * SEG : i * SEG + TEXT, :]
            text_out[i, 0] = jnp.where(row_ids(body.shape) < vr, body, 0.0).astype(BF)
            tail = x_ref[i * SEG + TAIL : (i + 1) * SEG, :]
            both = jnp.where(row_ids(tail.shape) >= TEXT - TAIL + MEM, tail, pltpu.roll(tail, SEG - TAIL - MEM, axis=0))
            mem_ref[i] = jnp.where(seg < counts[i], both, mem_ref[i])
        mem_out[...] = mem_ref[...]


def whole(shape):
    return pl.BlockSpec(shape, lambda *_: (0,) * len(shape), pipeline_mode=pl.Buffered(1))


def saved(rows, cols):
    return pl.BlockSpec((1, rows, cols), lambda s, l: (l, s, 0))


def forward_local(text, mem, counts, lens, weights):
    wqkv, wo, wup, wdn, bias, ubias, norm = weights
    d, ff = wup.shape[1:]
    mem0 = jnp.concatenate([jnp.zeros((MB, TEXT - TAIL, d), F32), mem.astype(F32), mem.astype(F32)], axis=1)
    total = SEGS * ROWS
    units = MB * HEADS * SEG
    smem = pl.BlockSpec(memory_space=pltpu.SMEM)
    hbm = pl.BlockSpec(memory_space=pl.ANY)
    outs = pl.pallas_call(
        fwd_kernel,
        grid=(SEGS, LAYERS),
        in_specs=[
            smem, smem,
            pl.BlockSpec((MB, 1, TEXT, d), lambda s, l: (0, s, 0, 0)),
            whole(mem0.shape), hbm, hbm, hbm, hbm,
            whole(bias.shape), whole((LAYERS, 1, ff)), whole(norm.shape),
        ],
        out_specs=[
            pl.BlockSpec((MB, 1, TEXT, d), lambda s, l: (0, s, 0, 0)),
            whole(mem0.shape),
            saved(ROWS, 3 * d + ff), saved(ROWS, 3 * d), saved(units, 128),
            saved(ROWS, ff), saved(ROWS, d), saved(ROWS, d),
            pl.BlockSpec((1, 2, ROWS, 128), lambda s, l: (l, 0, s, 0)),
        ],
        out_shape=[
            jax.ShapeDtypeStruct((MB, SEGS, TEXT, d), BF),
            jax.ShapeDtypeStruct(mem0.shape, F32),
            jax.ShapeDtypeStruct((LAYERS, total, 3 * d + ff), BF),
            jax.ShapeDtypeStruct((LAYERS, total, 3 * d), BF),
            jax.ShapeDtypeStruct((LAYERS, SEGS * units, 128), BF),
            jax.ShapeDtypeStruct((LAYERS, total, ff), BF),
            jax.ShapeDtypeStruct((LAYERS, total, d), F32),
            jax.ShapeDtypeStruct((LAYERS, total, d), F32),
            jax.ShapeDtypeStruct((LAYERS, 2, total, 128), F32),
        ],
        scratch_shapes=[
            pltpu.VMEM((ROWS, d), F32), pltpu.VMEM(mem0.shape, F32),
            pltpu.VMEM((ROWS, d), F32), pltpu.VMEM((ROWS, d), F32),
            pltpu.VMEM(wqkv.shape, BF), pltpu.VMEM(wo.shape, BF), pltpu.VMEM(wup.shape, BF), pltpu.VMEM(wdn.shape, BF),
            pltpu.SemaphoreType.DMA((LAYERS, 4)),
        ],
        compiler_params=pltpu.CompilerParams(
            dimension_semantics=("arbitrary", "arbitrary"), vmem_limit_bytes=VMEM_LIMIT
        ),
        name="rmt_forward",
    )(counts, lens, text, mem0, wqkv, wo, wup, wdn, bias.astype(F32), ubias.astype(F32)[:, None, :], norm.astype(F32))
    text_out, mem_end = outs[:2]
    return text_out, mem_end[:, TEXT - TAIL + MEM :].astype(BF), outs[2:]


def bwd_kernel(
    counts, lens, cot, gm0, qkv, p_in, gp_in, xh1_in, xh2_in, rs_in, wqkv_hbm, wo_hbm, wup_hbm, wdn_hbm, norm,
    tg_out, gm_out, rhs_out, small_out,
    g_ref, gm_ref, t_ref, acc_ref, dc_ref, wqkv, wo, wup, wdn, wsem, gb_out, gub_out, gn_out,
):
    seg = SEGS - 1 - pl.program_id(0)
    step = pl.program_id(1)
    layer = LAYERS - 1 - step
    loads = Loads(((wqkv_hbm, wqkv), (wo_hbm, wo), (wup_hbm, wup), (wdn_hbm, wdn)), wsem, seg == SEGS - 1, (1, 0))
    d = g_ref.shape[-1]
    ff = wup.shape[-1]
    dqkv_out, dao_out = rhs_out.at[:, :, 0 : 3 * d], rhs_out.at[:, :, 3 * d : 4 * d]
    du_out, df_out = rhs_out.at[:, :, 4 * d : 4 * d + ff], rhs_out.at[:, :, 4 * d + ff :]

    @pl.when((seg == SEGS - 1) & (step == 0))
    def _():
        loads.start()
        gm_ref[...] = gm0[...]
        gb_out[...] = jnp.zeros_like(gb_out)
        gub_out[...] = jnp.zeros_like(gub_out)
        gn_out[...] = jnp.zeros_like(gn_out)

    @pl.when(step == 0)
    def _():
        for i in range(MB):
            vr = valid_rows(seg, counts[i], lens[i])
            ct = cot[i, 0].astype(F32)
            g_ref[i * SEG : i * SEG + TEXT, :] = jnp.where(row_ids(ct.shape) < vr, ct, 0.0)
            tail = slice(i * SEG + TAIL, (i + 1) * SEG)
            now = g_ref[tail, :]
            rows = row_ids(now.shape)
            mem_part = jnp.where((rows >= TEXT - TAIL + MEM) & (seg < counts[i]), gm_ref[i], 0.0)
            g_ref[tail, :] = jnp.where(rows < TEXT - TAIL, now, mem_part)

    loads.need(step)

    def norm_back(base_ref, add_ref, xh_in, rs_slot, gain, slot, low_out, low_slot):
        sums = [jnp.zeros((8, d), F32) for _ in range(3)]
        for k in range(0, ROWS, CHUNK):
            rows = slice(k, k + CHUNK)
            gout = base_ref[rows, :]
            if add_ref is not None:
                gout = gout + add_ref[rows, :]
            xh = xh_in[0, rows, :]
            gx = gout * xh
            t = gout * gain
            inner = jnp.mean(gx * gain, axis=-1, keepdims=True)
            dh = rs_in[0, rs_slot, rows, :][:, :1] * (t - jnp.mean(t, axis=-1, keepdims=True) - xh * inner)
            t_ref[rows, :] = dh
            low = dh.astype(BF)
            low_out[0, rows, :] = low
            sums = [v + colsum(w) for v, w in zip(sums, (gx, gout, low.astype(F32)))]
        gn_out[layer, slot] += sums[0]
        gn_out[layer, slot + 1] += sums[1]
        gb_out[layer, low_slot] += sums[2]

    norm_back(g_ref, None, xh2_in, 1, norm[layer, 2:3, :], 2, df_out, 3)

    def ffn_step():
        cols = slice(0, ff)
        dg = dot_rt(df_out[0], wdn[layer, cols, :])
        du = (dg * gp_in[0, :, cols].astype(F32)).astype(BF)
        du_out[0, :, cols] = du
        gub_out[layer, :, cols] += colsum(du.astype(F32))

    ffn_step()
    acc_ref[...] = dot_rt(du_out[0], wup[layer])
    norm_back(t_ref, acc_ref, xh1_in, 0, norm[layer, 0:1, :], 0, dao_out, 2)
    dc_ref[...] = dot_rt(dao_out[0], wo[layer]).astype(BF)

    low_half = lane_ids((SEG, 128)) < HD
    scale = HD ** -0.5

    def heads_of(v):
        zero = jnp.zeros_like(v)
        return jnp.concatenate([jnp.where(low_half, v, zero), jnp.where(low_half, zero, v)], axis=0)

    for i in range(MB):
        r0 = i * SEG
        for g0 in range(0, HEADS // 2, GROUP_B):
            pairs = range(g0, g0 + GROUP_B)

            def part(j, pair):
                return qkv[0, r0 : r0 + SEG, j * d + pair * 128 : j * d + pair * 128 + 128]

            def probs(pair):
                u0 = (i * (HEADS // 2) + pair) * 2 * SEG
                return p_in[0, u0 : u0 + 2 * SEG, :]

            def out(j, pair, v):
                dqkv_out[0, r0 : r0 + SEG, j * d + pair * 128 : j * d + pair * 128 + 128] = v.astype(BF)

            dc2 = [heads_of(dc_ref[r0 : r0 + SEG, p * 128 : p * 128 + 128]) for p in pairs]
            dp = [dot_rt(v, part(2, p)) for v, p in zip(dc2, pairs)]
            for p, v in zip(pairs, dc2):
                out(2, p, dot_lt(probs(p), v))
            pdp = [probs(p).astype(F32) * v for p, v in zip(pairs, dp)]
            ds = [
                (v - probs(p).astype(F32) * jnp.sum(v, axis=-1, keepdims=True)).astype(BF) for p, v in zip(pairs, pdp)
            ]
            dq2 = [dot(v, part(1, p)) for v, p in zip(ds, pairs)]
            dk = [dot_lt(v, heads_of(part(0, p))) for v, p in zip(ds, pairs)]
            for p, a, b in zip(pairs, dq2, dk):
                out(0, p, jnp.where(low_half, a[:SEG], a[SEG:]) * scale)
                out(1, p, b * scale)

    gb_out[layer, 0] += colsum(dqkv_out[0, :, 0:d].astype(F32))
    gb_out[layer, 1] += colsum(dqkv_out[0, :, 2 * d : 3 * d].astype(F32))
    g_ref[...] = (
        t_ref[...]
        + dot_rt(dqkv_out[0, :, 0:d], wqkv[layer, 0])
        + dot_rt(dqkv_out[0, :, d : 2 * d], wqkv[layer, 1])
        + dot_rt(dqkv_out[0, :, 2 * d : 3 * d], wqkv[layer, 2])
    )

    @pl.when(layer == 0)
    def _():
        for i in range(MB):
            tg_out[i, 0] = g_ref[i * SEG : i * SEG + TEXT, :].astype(BF)
            tail = g_ref[i * SEG + TAIL : (i + 1) * SEG, :]
            back = tail + pltpu.roll(tail, MEM, axis=0)
            gm_ref[i] = jnp.where(seg < counts[i], 0.0, gm_ref[i]) + back
        gm_out[...] = gm_ref[...]

    @pl.when((seg == 0) & (layer == 0))
    def _():
        for l in range(LAYERS):
            for k in range(4):
                parts = (gb_out[l, k], gub_out[l, :, k * d : (k + 1) * d], gn_out[l, k])
                for base, part in zip((0, 8, 16), parts):
                    row = base + 4 * l + k
                    small_out[row : row + 1, :] = jnp.sum(part, axis=0, keepdims=True)


def backward_local(cot, cot_mem, counts, lens, kept, weights):
    wqkv, wo, wup, wdn, _, _, norm = weights
    _, qkv, p_all, gp, xh1, xh2, rs = kept
    d, ff = wup.shape[1:]
    gm0 = jnp.concatenate([jnp.zeros((MB, TEXT - TAIL + MEM, d), F32), cot_mem.astype(F32)], axis=1)
    total = SEGS * ROWS
    units = MB * HEADS * SEG
    smem = pl.BlockSpec(memory_space=pltpu.SMEM)
    hbm = pl.BlockSpec(memory_space=pl.ANY)

    def kept_spec(rows, cols):
        return pl.BlockSpec((1, rows, cols), lambda s, l: (LAYERS - 1 - l, SEGS - 1 - s, 0))

    outs = pl.pallas_call(
        bwd_kernel,
        grid=(SEGS, LAYERS),
        in_specs=[
            smem, smem,
            pl.BlockSpec((MB, 1, TEXT, d), lambda s, l: (0, SEGS - 1 - s, 0, 0)),
            whole(gm0.shape),
            kept_spec(ROWS, 3 * d), kept_spec(units, 128), kept_spec(ROWS, ff), kept_spec(ROWS, d), kept_spec(ROWS, d),
            pl.BlockSpec((1, 2, ROWS, 128), lambda s, l: (LAYERS - 1 - l, 0, SEGS - 1 - s, 0)),
            hbm, hbm, hbm, hbm, whole(norm.shape),
        ],
        out_specs=[
            pl.BlockSpec((MB, 1, TEXT, d), lambda s, l: (0, SEGS - 1 - s, 0, 0)),
            whole(gm0.shape),
            kept_spec(ROWS, 5 * d + ff), whole((24, d)),
        ],
        out_shape=[
            jax.ShapeDtypeStruct((MB, SEGS, TEXT, d), BF),
            jax.ShapeDtypeStruct(gm0.shape, F32),
            jax.ShapeDtypeStruct((LAYERS, total, 5 * d + ff), BF),
            jax.ShapeDtypeStruct((24, d), F32),
        ],
        scratch_shapes=[
            pltpu.VMEM((ROWS, d), F32), pltpu.VMEM(gm0.shape, F32),
            pltpu.VMEM((ROWS, d), F32), pltpu.VMEM((ROWS, d), F32), pltpu.VMEM((ROWS, d), BF),
            pltpu.VMEM(wqkv.shape, BF), pltpu.VMEM(wo.shape, BF), pltpu.VMEM(wup.shape, BF), pltpu.VMEM(wdn.shape, BF),
            pltpu.SemaphoreType.DMA((LAYERS, 4)),
            pltpu.VMEM((LAYERS, 4, 8, d), F32), pltpu.VMEM((LAYERS, 8, ff), F32), pltpu.VMEM((LAYERS, 4, 8, d), F32),
        ],
        compiler_params=pltpu.CompilerParams(
            dimension_semantics=("arbitrary", "arbitrary"), vmem_limit_bytes=VMEM_LIMIT
        ),
        name="rmt_backward",
    )(counts, lens, cot, gm0, qkv, p_all, gp, xh1, xh2, rs, wqkv, wo, wup, wdn, norm.astype(F32))
    tg, gm = outs[:2]
    return tg, gm[:, TEXT - TAIL + MEM :].astype(BF), outs[2], outs[3]


TILES = 12


def product_kernel(ids, lhs, rhs, out):
    out[0, 0] = dot_lt(lhs[0], rhs[0]).astype(BF)


def weight_grads(lhs, rhs, layers):
    d = rhs.shape[-1] // 9
    total = lhs.shape[1]
    count = layers.shape[0]

    def left(l, t, ids):
        return (ids[l], 0, jnp.where(t < 3, 0, jnp.where(t < 4, 1, jnp.where(t < 8, 2, t - 5))))

    return pl.pallas_call(
        product_kernel,
        grid_spec=pltpu.PrefetchScalarGridSpec(
            num_scalar_prefetch=1,
            grid=(count, TILES),
            in_specs=[
                pl.BlockSpec((1, total, d), left),
                pl.BlockSpec((1, total, d), lambda l, t, ids: (ids[l], 0, jnp.minimum(t, 8))),
            ],
            out_specs=pl.BlockSpec((1, 1, d, d), lambda l, t, ids: (l, t, 0, 0)),
        ),
        out_shape=jax.ShapeDtypeStruct((count, TILES, d, d), BF),
        compiler_params=pltpu.CompilerParams(
            dimension_semantics=("arbitrary", "arbitrary"), vmem_limit_bytes=VMEM_LIMIT
        ),
        name="weight_products",
    )(layers, lhs, rhs)


MESH = pl.DeviceIdType.MESH
ZN = 4


def multiple(v, k):
    return v if isinstance(v, int) else pl.multiple_of(v, k)


def span(start, size):
    return pl.ds(multiple(start, size if size % 128 else 128), size)


def where_am_i():
    w, n = lax.axis_index("wide"), lax.axis_index("narrow")
    z, x = lax.div(w, 2), lax.rem(w, 2)
    y, c = lax.div(n, 2), lax.rem(n, 2)
    links = {
        "p": {"wide": w, "narrow": n + 1 - 2 * c},
        "x": {"wide": w + 1 - 2 * x, "narrow": n},
        "y": {"wide": w, "narrow": lax.rem(n + 2, 4)},
        "up": {"wide": w + 2, "narrow": n},
        "down": {"wide": w - 2, "narrow": n},
    }
    return w, n, z, x, y, c, links


def enter(z, links):
    barrier = pltpu.get_barrier_semaphore()
    for name in ("p", "x", "y"):
        pl.semaphore_signal(barrier, inc=1, device_id=links[name], device_id_type=MESH)

    @pl.when(z < ZN - 1)
    def _():
        pl.semaphore_signal(barrier, inc=1, device_id=links["up"], device_id_type=MESH)

    @pl.when(z > 0)
    def _():
        pl.semaphore_signal(barrier, inc=1, device_id=links["down"], device_id_type=MESH)

    pl.semaphore_wait(barrier, 3 + jnp.minimum(z, 1) + jnp.minimum(ZN - 1 - z, 1))


class Net:
    def __init__(self, ssem, rsem, links):
        self.ssem, self.rsem, self.links = ssem, rsem, links
        self.next_send, self.next_recv = 0, 0

    def sends(self, count):
        base, self.next_send = self.next_send, self.next_send + count
        return base

    def recvs(self, count):
        base, self.next_recv = self.next_recv, self.next_recv + count
        return base

    def copy(self, link, src, dst, s, r):
        return pltpu.make_async_remote_copy(
            src_ref=src, dst_ref=dst, send_sem=self.ssem.at[s], recv_sem=self.rsem.at[r],
            device_id=self.links[link], device_id_type=MESH,
        )


def gather_kernel(
    q_in, o_in, u_in, d_in, s_in, Q, O, U, D, S,
    tq, to, tu, td, aq, ao, au, ad, ssem, rsem, lsem,
):
    w, n, z, x, y, c, links = where_am_i()
    mine, other = c, 1 - c
    net = Net(ssem, rsem, links)
    rw, cn = aq.shape[1], aq.shape[2]
    rd, cu = ad.shape[0], au.shape[1]
    half = cu // 2
    enter(z, links)

    first = [net.copy("p", src, dst, net.sends(1), net.recvs(1)) for src, dst in (
        (q_in.at[other], tq), (d_in.at[other], td), (u_in.at[other], tu), (o_in.at[other], to),
        (s_in, S.at[z, x, y, c]),
    )]
    for cp in first:
        cp.start()
    own_small = pltpu.make_async_copy(s_in, S.at[z, x, y, c], lsem.at[4])
    own_small.start()

    def join(own, got):
        a, b = own.astype(F32), got.astype(F32)
        lo, hi = jnp.where(c == 0, a, b), jnp.where(c == 0, b, a)
        return jnp.concatenate([lo, hi], axis=-1).astype(BF)

    places = (
        (aq, Q.at[mine, :, span(rw * w, rw), span(cn * y, cn)]),
        (ad, D.at[mine, span(rd * w, rd), span(cn * y, cn)]),
        (au, U.at[mine, span(rw * w, rw), span(cu * y, cu)]),
        (ao, O.at[mine, span(rw * w, rw), span(cn * y, cn)]),
    )

    def put(*which):
        local = [pltpu.make_async_copy(*places[k], lsem.at[k]) for k in which]
        for cp in local:
            cp.start()
        for cp in local:
            cp.wait()

    main = rd - rw

    def rows_a(zp):
        return span(2 * rw * zp, 2 * rw)

    def rows_x(zp, xp):
        return span(rw * (2 * zp + xp), rw)

    def rows_d(zp, xp):
        return pl.ds(pl.multiple_of(rd * (2 * zp + xp), rw), main)

    def rows_v(zp, xp):
        return pl.ds(pl.multiple_of(rd * (2 * zp + xp) + main, rw), rw)

    def cols(yp):
        return span(cn * yp, cn)

    def blk_a(zp, xp, yp):
        return [Q.at[mine, :, rows_x(zp, xp), cols(yp)]]

    def blk_d(zp, xp, yp):
        return [D.at[mine, rows_d(zp, xp), cols(yp)]]

    def reg_a(zp, yp, layer):
        return [Q.at[layer, :, rows_a(zp), cols(yp)]]

    def reg_d(zp, xp, layer):
        return [D.at[layer, rows_d(zp, xp), :]]

    def u_cols(zp, xp, start, size):
        return U.at[mine, rows_x(zp, xp), span(start, size)]

    def blk_u(zp, xp, yp):
        return [
            u_cols(zp, xp, cu * yp, cu), O.at[mine, rows_x(zp, xp), cols(yp)], D.at[mine, rows_v(zp, xp), cols(yp)]
        ]

    def blk_u1(zp, xp, yp):
        return [u_cols(zp, xp, cu * yp, half), O.at[mine, rows_x(zp, xp), cols(yp)]]

    def blk_u2(zp, xp, yp):
        return [u_cols(zp, xp, cu * yp + half, half), D.at[mine, rows_v(zp, xp), cols(yp)]]

    def pair_u1(zp, yp, layer):
        return [U.at[layer, rows_a(zp), span(cu * yp, half)], O.at[layer, rows_a(zp), cols(yp)]]

    def pair_u2(zp, xp, layer):
        rows = rows_x(zp, xp)
        return [U.at[layer, rows, span(cu * yp + half, half)] for yp in range(2)] + [D.at[layer, rows_v(zp, xp), :]]

    class Lane:
        def __init__(self, link, sent, got, parts):
            self.link, self.sent, self.got, self.parts = link, sent, got, parts
            self.s = [net.sends(ZN) for _ in range(parts)]
            self.r = [net.recvs(ZN) for _ in range(parts)]

        def send(self, zp):
            for k, ref in enumerate(self.sent(zp)):
                net.copy(self.link, ref, ref, self.s[k] + zp, self.r[k] + zp).start()

        def recv(self, zp):
            for k, ref in enumerate(self.got(zp)):
                net.copy(self.link, ref, ref, self.s[k] + zp, self.r[k] + zp).wait_recv()

        def drain(self, zp):
            for k, ref in enumerate(self.sent(zp)):
                net.copy(self.link, ref, ref, self.s[k] + zp, self.r[k] + zp).wait_send()

    class Line:
        def __init__(self, region, parts):
            self.region, self.parts = region, parts
            self.su = [net.sends(ZN) for _ in range(parts)]
            self.sd = [net.sends(ZN) for _ in range(parts)]
            self.r = [net.recvs(ZN) for _ in range(parts)]

        def each(self, link, sems, zp, what):
            for k, ref in enumerate(self.region(zp)):
                getattr(net.copy(link, ref, ref, sems[k] + zp, self.r[k] + zp), what)()

        def own(self, what="start"):
            @pl.when(z < ZN - 1)
            def _():
                self.each("up", self.su, z, what)

            @pl.when(z > 0)
            def _():
                self.each("down", self.sd, z, what)

        def relay(self, t, what="start"):
            @pl.when(jnp.minimum(z - t, ZN - 2 - z) >= 0)
            def _():
                self.each("up", self.su, z - t, what)

            @pl.when(jnp.minimum(ZN - 1 - t - z, z - 1) >= 0)
            def _():
                self.each("down", self.sd, z + t, what)

        def recv(self, zp):
            self.each("up", self.su, zp, "wait_recv")

    line_a = [Line(lambda zp, xp=xp: blk_a(zp, xp, y), 1) for xp in (x, 1 - x)]
    line_d = [Line(lambda zp, yp=yp: blk_d(zp, x, yp), 1) for yp in (y, 1 - y)]
    line_u = Line(lambda zp: blk_u(zp, x, y), 3)
    x1 = Lane("x", lambda zp: blk_a(z, x, y), lambda zp: blk_a(z, 1 - x, y), 1)
    y1 = Lane("y", lambda zp: blk_d(z, x, y), lambda zp: blk_d(z, x, 1 - y), 1)
    x_u1 = Lane("x", lambda zp: blk_u1(zp, x, y), lambda zp: blk_u1(zp, 1 - x, y), 2)
    y_u2 = Lane("y", lambda zp: blk_u2(zp, x, y), lambda zp: blk_u2(zp, x, 1 - y), 2)
    y_a = [
        Lane("y", lambda zp, xp=xp: blk_a(zp, xp, y), lambda zp, xp=xp: blk_a(zp, xp, 1 - y), 1) for xp in (x, 1 - x)
    ]
    x_d = [
        Lane("x", lambda zp, yp=yp: blk_d(zp, x, yp), lambda zp, yp=yp: blk_d(zp, 1 - x, yp), 1) for yp in (y, 1 - y)
    ]
    y_u1 = Lane("y", lambda zp: pair_u1(zp, y, mine), lambda zp: pair_u1(zp, 1 - y, mine), 2)
    x_u2 = Lane("x", lambda zp: pair_u2(zp, x, mine), lambda zp: pair_u2(zp, 1 - x, mine), 3)

    def to_partner(make, parts):
        return Lane("p", lambda zp: make(zp, mine), lambda zp: make(zp, other), parts)

    p_a = to_partner(lambda zp, l: reg_a(zp, y, l), 1)
    p_a2 = to_partner(lambda zp, l: reg_a(zp, 1 - y, l), 1)
    p_d = to_partner(lambda zp, l: reg_d(zp, x, l), 1)
    p_d2 = to_partner(lambda zp, l: reg_d(zp, 1 - x, l), 1)
    p_u1 = to_partner(lambda zp, l: pair_u1(zp, y, l), 2)
    p_u1b = to_partner(lambda zp, l: pair_u1(zp, 1 - y, l), 2)
    p_u2 = to_partner(lambda zp, l: pair_u2(zp, x, l), 3)
    p_u2b = to_partner(lambda zp, l: pair_u2(zp, 1 - x, l), 3)

    small_x = Lane("x", lambda zp: [S.at[z, x, y]], lambda zp: [S.at[z, 1 - x, y]], 1)
    small_y = Lane("y", lambda zp: [S.at[z, :, y]], lambda zp: [S.at[z, :, 1 - y]], 1)
    line_s = Line(lambda zp: [S.at[zp]], 1)

    first[0].wait()
    for j in range(3):
        aq[j] = join(q_in[mine, j], tq[j])
    put(0)
    x1.send(0)
    line_a[0].own()
    first[1].wait()
    ad[...] = join(d_in[mine], td[...])
    put(1)
    y1.send(0)
    line_d[0].own()
    first[2].wait()
    au[...] = join(u_in[mine], tu[...])
    first[3].wait()
    ao[...] = join(o_in[mine], to[...])
    put(2, 3)
    first[4].wait()
    own_small.wait()
    small_x.send(0)
    x_u1.send(z)
    y_u2.send(z)
    line_u.own()
    y_a[0].send(z)
    x_d[0].send(z)
    small_x.recv(0)
    small_y.send(0)
    x1.recv(0)
    line_a[1].own()
    y_a[1].send(z)
    p_a.send(z)
    y1.recv(0)
    line_d[1].own()
    x_d[1].send(z)
    p_d.send(z)
    small_y.recv(0)
    line_s.own()

    def second(zp):
        x_u1.recv(zp)
        y_u1.send(zp)
        p_u1.send(zp)
        y_u2.recv(zp)
        x_u2.send(zp)
        p_u2.send(zp)

    def third(zp):
        for lane in y_a:
            lane.recv(zp)
        p_a2.send(zp)
        for lane in x_d:
            lane.recv(zp)
        p_d2.send(zp)
        y_u1.recv(zp)
        p_u1b.send(zp)
        x_u2.recv(zp)
        p_u2b.send(zp)

    def both_ways(t, make):
        @pl.when(z >= t)
        def _():
            make(z - t)

        @pl.when(z < ZN - t)
        def _():
            make(z + t)

    def take(line, t, *lanes):
        both_ways(t, line.recv)
        line.relay(t)
        for lane in lanes:
            both_ways(t, lane.send)

    second(z)
    for t in range(1, ZN):
        take(line_a[0], t, y_a[0])
        take(line_d[0], t, x_d[0])
        take(line_u, t, x_u1, y_u2)
        take(line_a[1], t, y_a[1], p_a)
        if t == 1:
            third(z)
        else:
            both_ways(t - 1, third)
        take(line_d[1], t, x_d[1], p_d)
        both_ways(t, second)
        take(line_s, t)
    both_ways(ZN - 1, third)

    partner = (p_a, p_a2, p_d, p_d2, p_u1, p_u1b, p_u2, p_u2b)
    for zp in range(ZN):
        for lane in partner:
            lane.recv(zp)
    for zp in range(ZN):
        for lane in partner + (x_u1, y_u2, *y_a, *x_d, y_u1, x_u2):
            lane.drain(zp)
    for lane in (x1, y1, small_x, small_y):
        lane.drain(0)
    for line in (line_u, *line_a, *line_d, line_s):
        line.own("wait_send")
        for t in range(1, ZN):
            line.relay(t, "wait_send")
    assert net.next_send <= ssem.shape[0] and net.next_recv <= rsem.shape[0]


def gather_fast(pieces):
    wqkv, wo, wup, wdn, bias, ubias, norm = pieces
    _, _, rw, cn = wqkv.shape
    rd, cu = wdn.shape[1], wup.shape[2]
    d, ff = rw * 8, rd * 8
    small = jnp.concatenate([bias[:, 0], norm[:, 0], ubias, jnp.zeros_like(ubias)], axis=0).astype(F32)
    small = jnp.pad(small, ((0, 0), (0, 128 - rw)))
    hbm = pl.BlockSpec(memory_space=pl.ANY)
    vmem = pl.BlockSpec(memory_space=pltpu.VMEM)
    Q, O, U, D, S = pl.pallas_call(
        gather_kernel,
        in_specs=[vmem] * 5,
        out_specs=[hbm] * 5,
        out_shape=[
            jax.ShapeDtypeStruct((LAYERS, 3, d, d), BF),
            jax.ShapeDtypeStruct((LAYERS, d, d), BF),
            jax.ShapeDtypeStruct((LAYERS, d, ff), BF),
            jax.ShapeDtypeStruct((LAYERS, ff, d), BF),
            jax.ShapeDtypeStruct((ZN, 2, 2, 2, 8, 128), F32),
        ],
        scratch_shapes=[
            pltpu.VMEM((3, rw, cn), BF), pltpu.VMEM((rw, cn), BF), pltpu.VMEM((rw, cu), BF), pltpu.VMEM((rd, cn), BF),
            pltpu.VMEM((3, rw, 2 * cn), BF), pltpu.VMEM((rw, 2 * cn), BF),
            pltpu.VMEM((rw, 2 * cu), BF), pltpu.VMEM((rd, 2 * cn), BF),
            pltpu.SemaphoreType.DMA((200,)), pltpu.SemaphoreType.DMA((200,)), pltpu.SemaphoreType.DMA((5,)),
        ],
        compiler_params=pltpu.CompilerParams(collective_id=1, has_side_effects=True),
        name="weight_gather",
    )(wqkv, wo, wup, wdn, small)
    S = S.reshape(8, 4, 8, 128)[..., :rw]
    rows = jnp.transpose(S, (2, 1, 0, 3)).reshape(8, 4, d)
    ub = jnp.transpose(S[:, :, 4:6], (2, 0, 1, 3)).reshape(2, ff)
    return Q, O, U, D, rows[0:2], ub, rows[2:4]


def accumulate(dst, src, rows, step=48):
    def body(i, carry):
        r = pl.ds(pl.multiple_of(i * step, 16), step)
        dst[r, :] = dst[r, :] + src[r, :]
        return carry

    lax.fori_loop(0, rows // step, body, 0)


def scatter_kernel(
    gw, lhs, rhs, sm_in, oq, oo, ou, od, sm_out,
    AT, AD, RH, LT, LB, FA, FD, F1, FO, F2, FV, S1, SO, S2, SV, ZA, ZD, ZU, ZO, ZV, TA, TD,
    hq, ho, hu, hd, s_p, s_x, s_y, s_below, s_above, s_a, s_b, s_sum, s_up, s_down, ssem, rsem, lsem,
):
    w, n, z, x, y, c, links = where_am_i()
    mine, other = c, 1 - c
    net = Net(ssem, rsem, links)
    d, ff = AT.shape[2], AD.shape[0]
    rw, cn = d // 8, d // 2
    rd, cu = ff // 8, ff // 2
    half = cu // 2
    enter(z, links)

    class Hop:
        def __init__(self, link, pairs, parts):
            self.link, self.pairs = link, pairs
            self.s = [net.sends(ZN) for _ in range(parts)]
            self.r = [net.recvs(ZN) for _ in range(parts)]

        def each(self, zp, what):
            for k, (src, dst) in enumerate(self.pairs(zp)):
                getattr(net.copy(self.link, src, dst, self.s[k] + zp, self.r[k] + zp), what)()

        def send(self, zp):
            self.each(zp, "start")

        def recv(self, zp):
            self.each(zp, "wait_recv")

        def drain(self, zp):
            self.each(zp, "wait_send")

    def rows_a(zp):
        return span(2 * rw * zp, 2 * rw)

    main = rd - rw

    def down(zp):
        return span(d * zp, d)

    swap = [
        Hop("p", lambda zp: [(gw.at[0, 0:3, rows_a(zp), :], AT.at[0:3, rows_a(zp), :])], 1),
        Hop("p", lambda zp: [(gw.at[0, 8 + zp], AD.at[down(zp), :])], 1),
        Hop("p", lambda zp: [(gw.at[0, 3:8, rows_a(zp), :], AT.at[3:8, rows_a(zp), :])], 1),
    ]

    def right(t):
        return pltpu.make_async_copy(rhs.at[mine, :, t * d : (t + 1) * d], RH.at[t], lsem.at[t])

    def left(j):
        return pltpu.make_async_copy(lhs.at[mine, :, j * d : (j + 1) * d], LB.at[j], lsem.at[9 + j])

    def left_g(v, zp):
        slot = (v + 3) % 4
        return pltpu.make_async_copy(lhs.at[mine, :, span(d * (3 + zp), d)], LB.at[slot], lsem.at[12 + v])

    def turn(j):
        step = 256

        def body(k, carry):
            part = pl.ds(pl.multiple_of(k * step, step), step)
            LT[j, :, part] = LB[j, part, :].T
            return carry

        lax.fori_loop(0, LB.shape[1] // step, body, 0)

    def products(first, last, zp):
        rows = rows_a(zp)

        def body(t, carry):
            j = jnp.where(t < 3, 0, jnp.where(t < 4, 1, 2))
            AT[t, rows, :] = (AT[t, rows, :].astype(F32) + dot(LT[j, rows, :], RH[t])).astype(BF)
            return carry

        lax.fori_loop(first, last, body, 0)

    def products_down(v, zp):
        rows = down(zp)

        def body(k, carry):
            cols = pl.ds(pl.multiple_of(k * cn, cn), cn)
            AD[rows, cols] = (AD[rows, cols].astype(F32) + dot_lt(LB[(v + 3) % 4], RH[8, :, cols])).astype(BF)
            return carry

        lax.fori_loop(0, 2, body, 0)

    def cols_a(yp):
        return span(cn * yp, cn)

    def rows_x(zp, xp):
        return span(rw * (2 * zp + xp), rw)

    def rows_d(zp, xp):
        return pl.ds(pl.multiple_of(rd * (2 * zp + xp), rw), main)

    def rows_v(zp, xp):
        return pl.ds(pl.multiple_of(rd * (2 * zp + xp) + main, rw), rw)

    def reg_a(zp, yp):
        return AT.at[0:3, rows_a(zp), cols_a(yp)]

    def reg_d(zp, xp):
        return AD.at[rows_d(zp, xp), :]

    def u1(zp, yp):
        return [AT.at[4 + 2 * yp, rows_a(zp), :], AT.at[3, rows_a(zp), cols_a(yp)]]

    def u1_part(zp, xp, yp):
        return [AT.at[4 + 2 * yp, rows_x(zp, xp), :], AT.at[3, rows_x(zp, xp), cols_a(yp)]]

    def u2(zp, xp):
        rows = rows_x(zp, xp)
        return [AT.at[5 + 2 * yp, rows, :] for yp in range(2)] + [AD.at[rows_v(zp, xp), :]]

    def u2_part(zp, xp, yp):
        return [AT.at[5 + 2 * yp, rows_x(zp, xp), :], AD.at[rows_v(zp, xp), cols_a(yp)]]

    def blk_u(zp):
        rows = rows_x(zp, x)
        return [AT.at[pl.ds(4 + 2 * y, 2), rows, :], AT.at[3, rows, cols_a(y)], AD.at[rows_v(zp, x), cols_a(y)]]

    def bufs_u1(zp):
        return [F1.at[zp], FO.at[zp]]

    def bufs_u2(zp):
        return [F2.at[0, zp], F2.at[1, zp], FV.at[zp]]

    def bufs_s1(zp):
        return [S1.at[zp], SO.at[zp]]

    def bufs_s2(zp):
        return [S2.at[zp], SV.at[zp]]

    y_a = Hop("y", lambda zp: [(reg_a(zp, 1 - y), FA.at[zp])], 1)
    x_d = Hop("x", lambda zp: [(reg_d(zp, 1 - x), FD.at[zp])], 1)
    y_u1 = Hop("y", lambda zp: list(zip(u1(zp, 1 - y), bufs_u1(zp))), 2)
    x_u2 = Hop("x", lambda zp: list(zip(u2(zp, 1 - x), bufs_u2(zp))), 3)
    x_u1 = Hop("x", lambda zp: list(zip(u1_part(zp, 1 - x, y), bufs_s1(zp))), 2)
    y_u2 = Hop("y", lambda zp: list(zip(u2_part(zp, x, 1 - y), bufs_s2(zp))), 2)
    last_a = Hop("x", lambda zp: [(AT.at[0:3, rows_x(z, 1 - x), cols_a(y)], TA)], 1)
    last_d = Hop("y", lambda zp: [(AD.at[rows_d(z, x), cols_a(1 - y)], TD)], 1)

    def add_all(dsts, srcs):
        for dst, src in zip(dsts, srcs):
            accumulate(dst, src, src.shape[0])

    class Line:
        def __init__(self, region, bufs):
            self.region, self.bufs = region, bufs
            self.su = [net.sends(ZN) for _ in bufs]
            self.sd = [net.sends(ZN) for _ in bufs]
            self.r = [net.recvs(ZN + 1) for _ in bufs]

        def up(self, zp, what):
            slot = jnp.where(zp == z + 1, ZN, zp)

            @pl.when(zp > z)
            def _():
                for k, (src, buf) in enumerate(zip(self.region(zp), self.bufs)):
                    getattr(net.copy("up", src, buf.at[slot], self.su[k] + zp, self.r[k] + slot), what)()

        def down(self, zp, what):
            @pl.when(zp < z)
            def _():
                for k, (src, buf) in enumerate(zip(self.region(zp), self.bufs)):
                    getattr(net.copy("down", src, buf.at[zp], self.sd[k] + zp, self.r[k] + zp), what)()

        def take(self, zp, slot):
            for k, (dst, buf) in enumerate(zip(self.region(zp), self.bufs)):
                net.copy("up", dst, buf.at[slot], self.su[k] + zp, self.r[k] + slot).wait_recv()
                self.add(dst, buf.at[slot])

        def add(self, dst, src):
            if len(src.shape) == 3:
                for j in range(src.shape[0]):
                    accumulate(dst.at[j], src.at[j], src.shape[1])
            else:
                accumulate(dst, src, src.shape[0])

        def go(self, zp):
            @pl.when(jnp.minimum(z - zp, ZN - 2 - z) >= 0)
            def _():
                self.take(zp, zp)

            @pl.when(jnp.minimum(zp - z, z - 1) >= 0)
            def _():
                self.take(zp, jnp.where(zp == z, ZN, zp))

            self.up(zp, "start")
            self.down(zp, "start")

        def drain(self, zp):
            self.up(zp, "wait_send")
            self.down(zp, "wait_send")

    line_a = Line(lambda zp: (reg_a(zp, y),), (ZA,))
    line_d = Line(lambda zp: (reg_d(zp, x),), (ZD,))
    line_u = Line(blk_u, (ZU, ZO, ZV))

    table = ((3, 3, 0, 0), (2, 0, 3, 1), (1, 2, 1, 2), (0, 1, 2, 3))
    order = [jnp.where(z == 0, t[0], jnp.where(z == 1, t[1], jnp.where(z == 2, t[2], t[3]))) for t in table]

    small = [
        net.copy(link, src, dst, net.sends(1), net.recvs(1))
        for link, src, dst in (("p", sm_in, s_p), ("x", s_a, s_x), ("y", s_b, s_y))
    ]
    small_up = net.copy("up", s_up, s_below, net.sends(1), net.recvs(1))
    small_down = net.copy("down", s_down, s_above, net.sends(1), net.recvs(1))

    small[0].start()
    left(0).start()
    for t in range(3):
        right(t).start()
    left_g(0, order[0]).start()
    right(8).start()
    for j in (1, 2):
        left(j).start()
    for t in range(3, 8):
        right(t).start()
    for zp in order:
        for part in swap:
            part.send(zp)

    def open_q(v):
        zp = order[v]
        if v == 0:
            left(0).wait()
            turn(0)
            for t in range(3):
                right(t).wait()
        swap[0].recv(zp)
        products(0, 3, zp)
        y_a.send(zp)

    def open_d(v):
        zp = order[v]
        left_g(v, zp).wait()
        if v == 0:
            right(8).wait()
        swap[1].recv(zp)
        products_down(v, zp)
        x_d.send(zp)

    def open_u(v):
        zp = order[v]
        if v == 0:
            left_g(1, order[1]).start()
            for j in (1, 2):
                left(j).wait()
                turn(j)
                left_g(j + 1, order[j + 1]).start()
            for t in range(3, 8):
                right(t).wait()
        swap[2].recv(zp)
        products(3, 8, zp)
        y_u1.send(zp)
        x_u2.send(zp)

    def mid_a(zp):
        y_a.recv(zp)
        for j in range(3):
            accumulate(reg_a(zp, y).at[j], FA.at[zp, j], 2 * rw)
        line_a.go(zp)

    def mid_d(zp):
        x_d.recv(zp)
        accumulate(reg_d(zp, x), FD.at[zp], main)
        line_d.go(zp)

    def mid_u(zp):
        y_u1.recv(zp)
        add_all(u1(zp, y), bufs_u1(zp))
        x_u1.send(zp)
        x_u2.recv(zp)
        add_all(u2(zp, x), bufs_u2(zp))
        y_u2.send(zp)

    def close(zp):
        x_u1.recv(zp)
        add_all(u1_part(zp, x, y), bufs_s1(zp))
        y_u2.recv(zp)
        add_all(u2_part(zp, x, y), bufs_s2(zp))
        line_u.go(zp)

    open_q(0)
    open_d(0)
    open_u(0)
    mid_a(order[0])
    small[0].wait()
    s_a[...] = sm_in[...] + s_p[...]
    small[1].start()
    open_q(1)
    open_d(1)
    mid_d(order[0])
    open_u(1)
    mid_u(order[0])
    small[1].wait()
    s_b[...] = s_a[...] + s_x[...]
    small[2].start()
    open_q(2)
    open_d(2)
    mid_a(order[1])
    open_u(2)
    close(order[0])
    mid_d(order[1])
    mid_u(order[1])
    small[2].wait()
    s_sum[...] = s_b[...] + s_y[...]
    open_q(3)
    open_d(3)
    mid_a(order[2])
    open_u(3)
    close(order[1])
    mid_d(order[2])
    mid_u(order[2])

    @pl.when(z > 0)
    def _():
        small_up.wait_recv()

    @pl.when(z == 0)
    def _():
        s_below[...] = jnp.zeros_like(s_below)

    @pl.when(z < ZN - 1)
    def _():
        s_up[...] = s_sum[...] + s_below[...]
        small_up.start()

    mid_a(order[3])
    last_a.send(0)
    close(order[2])
    mid_d(order[3])
    last_d.send(0)
    mid_u(order[3])

    @pl.when(z < ZN - 1)
    def _():
        small_down.wait_recv()

    @pl.when(z == ZN - 1)
    def _():
        s_above[...] = jnp.zeros_like(s_above)

    @pl.when(z > 0)
    def _():
        s_down[...] = s_sum[...] + s_above[...]
        small_down.start()

    sm_out[...] = s_sum[...] + s_below[...] + s_above[...]
    close(order[3])

    def pick(v, k):
        lo, hi = v[..., :k], v[..., k:]
        return jnp.where(c == 0, lo, hi), jnp.where(c == 0, hi, lo)

    out = [
        net.copy("p", src, dst.at[mine], net.sends(1), net.recvs(1))
        for src, dst in ((hu, ou), (hq, oq), (ho, oo), (hd, od))
    ]
    rows = rows_x(z, x)
    ou[mine] = AT[4 + 2 * y + c, rows, :].astype(F32)
    hu[...] = AT[5 + 2 * y - c, rows, :].astype(F32)
    out[0].start()
    keep, give = pick(AT[3, rows, cols_a(y)].astype(F32), cn // 2)
    oo[mine] = keep
    ho[...] = give
    out[2].start()
    last_a.recv(0)
    for j in range(3):
        keep, give = pick(AT[j, rows, cols_a(y)].astype(F32) + TA[j].astype(F32), cn // 2)
        oq[mine, j] = keep
        hq[j] = give
    out[1].start()
    last_d.recv(0)
    for k in range(rd // rw):
        part = slice(k * rw, (k + 1) * rw)
        here = span(rd * w + k * rw, rw)
        total = AD[here, cols_a(y)].astype(F32)
        if k * rw < main:
            total = total + TD[part, :].astype(F32)
        keep, give = pick(total, cn // 2)
        od[mine, part, :] = keep
        hd[part, :] = give
    out[3].start()

    for zp in range(ZN):
        for hop in (*swap, y_a, x_d, y_u1, x_u2, x_u1, y_u2):
            hop.drain(zp)
        for line in (line_a, line_d, line_u):
            line.drain(zp)
    last_a.drain(0)
    last_d.drain(0)

    @pl.when(z < ZN - 1)
    def _():
        small_up.wait_send()

    @pl.when(z > 0)
    def _():
        small_down.wait_send()

    for cp in out:
        cp.wait()
    assert net.next_send <= ssem.shape[0] and net.next_recv <= rsem.shape[0]


def scatter_fast(gw, lhs, rhs, pack):
    d = gw.shape[-1]
    ff = 4 * d
    rw, cn, rd, cu = d // 8, d // 2, ff // 8, ff // 2
    hbm = pl.BlockSpec(memory_space=pl.ANY)
    vmem = pl.BlockSpec(memory_space=pltpu.VMEM)

    def buf(*shape):
        return pltpu.VMEM(shape, BF)

    def wide(*shape):
        return pltpu.VMEM(shape, F32)

    outs = [(3, rw, cn // 2), (rw, cn // 2), (rw, cu // 2), (rd, cn // 2)]
    total = lhs.shape[1]
    full = [buf(8, d, d), buf(ff, d), buf(9, total, d), buf(3, d, total), buf(4, total, d)]
    oq, oo, ou, od, summed = pl.pallas_call(
        scatter_kernel,
        in_specs=[hbm, hbm, hbm, vmem],
        out_specs=[vmem] * 5,
        out_shape=[jax.ShapeDtypeStruct((LAYERS,) + s, F32) for s in outs] + [jax.ShapeDtypeStruct(pack.shape, F32)],
        scratch_shapes=full + [
            buf(ZN, 3, 2 * rw, cn), buf(ZN, rd - rw, d), buf(ZN, 2 * rw, cu // 2), buf(ZN, 2 * rw, cn),
            buf(2, ZN, rw, cu // 2), buf(ZN, rw, d), buf(ZN, rw, cu // 2), buf(ZN, rw, cn),
            buf(ZN, rw, cu // 2), buf(ZN, rw, cn), buf(ZN + 1, 3, 2 * rw, cn), buf(ZN + 1, rd - rw, d),
            buf(ZN + 1, 2, rw, cu // 2), buf(ZN + 1, rw, cn), buf(ZN + 1, rw, cn), buf(3, rw, cn), buf(rd - rw, cn),
        ] + [wide(*s) for s in outs] + [wide(*pack.shape)] * 10 + [
            pltpu.SemaphoreType.DMA((180,)), pltpu.SemaphoreType.DMA((160,)), pltpu.SemaphoreType.DMA((16,)),
        ],
        compiler_params=pltpu.CompilerParams(collective_id=2, has_side_effects=True, vmem_limit_bytes=VMEM_LIMIT),
        name="gradient_scatter",
    )(gw, lhs, rhs, pack)
    w, n = lax.axis_index("wide"), lax.axis_index("narrow")
    gb = lax.dynamic_slice(summed[0:8].reshape(2, 4, d), (0, n, w * rw), (2, 1, rw))
    gn = lax.dynamic_slice(summed[16:24].reshape(2, 4, d), (0, n, w * rw), (2, 1, rw))
    gub = lax.dynamic_slice(summed[8:16].reshape(2, ff), (0, (4 * w + n) * rw), (2, rw))
    return oq, oo, ou, od, gb, gub, gn


def gather_weights(pieces):
    wqkv, wo, wup, wdn, bias, ubias, norm = pieces
    narrow = [(wqkv, 3), (wo, 2), (wup, 2), (wdn, 2), (bias, 1), (norm, 1)]
    wqkv, wo, wup, wdn, bias, norm = (lax.all_gather(w, "narrow", axis=k, tiled=True) for w, k in narrow)
    wide = [(wqkv, 2), (wo, 1), (wup, 1), (wdn, 1), (bias, 2), (norm, 2)]
    wqkv, wo, wup, wdn, bias, norm = (lax.all_gather(w, "wide", axis=k, tiled=True) for w, k in wide)
    ubias = lax.all_gather(ubias, ("wide", "narrow"), axis=1, tiled=True)
    return wqkv, wo, wup, wdn, bias, ubias, norm


def scatter_two(grad, row_axis, col_axis):
    low = lax.psum_scatter(grad.astype(BF), "narrow", scatter_dimension=col_axis, tiled=True)
    return lax.psum_scatter(low.astype(F32), "wide", scatter_dimension=row_axis, tiled=True)


def scatter_grads(gw, pack):
    d = gw.shape[-1]
    gq, go, gdn = gw[:, 0:3], gw[:, 3], gw[:, 8:].reshape(LAYERS, -1, d)
    gup = jnp.moveaxis(gw[:, 4:8], 1, 2).reshape(LAYERS, d, -1)
    gb, gub, gn = pack[0:8].reshape(LAYERS, 4, d), pack[8:16].reshape(LAYERS, -1), pack[16:24].reshape(LAYERS, 4, d)
    big = (scatter_two(gq, 2, 3), scatter_two(go, 1, 2), scatter_two(gup, 1, 2), scatter_two(gdn, 1, 2))
    gub = lax.psum_scatter(gub, ("wide", "narrow"), scatter_dimension=1, tiled=True)

    def small_two(g):
        return lax.psum_scatter(
            lax.psum_scatter(g, "narrow", scatter_dimension=1, tiled=True), "wide", scatter_dimension=2, tiled=True
        )

    return big + (small_two(gb), gub, small_two(gn))


def shards(
    near, text_in, memory_in, counts, last_len, cot_text, cot_memory,
    qkv_weight, out_weight, up_weight, down_weight, biases, up_bias, norm_params,
):
    text, cot = text_in[:, 0], cot_text[:, 0]
    mem, cot_mem = memory_in[:, 0], cot_memory[:, 0]
    cnt, lens = counts[:, 0], last_len[:, 0]
    gather = gather_fast if near else gather_weights
    weights = gather((qkv_weight, out_weight, up_weight, down_weight, biases, up_bias, norm_params))
    text_out, mem_out, kept = forward_local(text, mem, cnt, lens, weights)
    text_grad, mem_grad, rhs, small = backward_local(cot, cot_mem, cnt, lens, kept, weights)
    if near:
        other = 1 - lax.rem(lax.axis_index("narrow"), 2)
        grads = scatter_fast(weight_grads(kept[0], rhs, other[None]), kept[0], rhs, small)
    else:
        grads = scatter_grads(weight_grads(kept[0], rhs, jnp.arange(LAYERS, dtype=jnp.int32)), small)
    return (text_out[:, None], mem_out[:, None], text_grad[:, None], mem_grad[:, None]) + grads


def solution(mesh):
    items = ("wide", "narrow")
    act5 = P(None, items, None, None, None)
    act4 = P(None, items, None, None)
    ids = P(None, items)
    split = P(None, "wide", "narrow")
    small = P(None, "narrow", "wide")
    params = (P(None, None, "wide", "narrow"), split, split, split, small, ids, small)
    near = (mesh.shape["wide"], mesh.shape["narrow"]) == (2 * ZN, 4)
    return jax.shard_map(
        functools.partial(shards, near),
        mesh=mesh,
        in_specs=(act5, act4, ids, ids, act5, act4) + params,
        out_specs=(act5, act4, act5, act4) + params,
        check_vma=False,
    )
```

```python
import functools

import jax
import jax.numpy as jnp
from jax import lax
from jax.experimental import pallas as pl
from jax.experimental.pallas import tpu as pltpu
from jax.sharding import PartitionSpec as P

HEADS = 12
HD = 64
MEM = 10
TEXT = 108
SEGS = 4
MB = 2
LAYERS = 2
SEG = TEXT + 2 * MEM
TAIL = 104
ROWS = MB * SEG
EPS = 1e-12
BF = jnp.bfloat16
F32 = jnp.float32
NEG = -1e30
RSQRT2 = 0.7071067811865476
RSQRT2PI = 0.3989422804014327
VMEM_LIMIT = 66_000_000
CHUNK = 32
GROUP_F = 6
GROUP_B = 6


def dot(a, b):
    return lax.dot_general(a, b, (((1,), (0,)), ((), ())), preferred_element_type=F32)


def dot_rt(a, b):
    return lax.dot_general(a, b, (((1,), (1,)), ((), ())), preferred_element_type=F32)


def dot_lt(a, b):
    return lax.dot_general(a, b, (((0,), (0,)), ((), ())), preferred_element_type=F32)


def row_ids(shape):
    return lax.broadcasted_iota(jnp.int32, shape, 0)


def lane_ids(shape):
    return lax.broadcasted_iota(jnp.int32, shape, 1)


def valid_rows(seg, count, length):
    return jnp.where(seg < count - 1, TEXT, jnp.where(seg == count - 1, length, 0))


def colsum(v):
    rows, cols = v.shape
    return jnp.sum(v.reshape(rows // 8, 8, cols), axis=0)


class Loads:
    def __init__(self, pairs, sems, first, order):
        self.pairs, self.sems, self.first, self.order = pairs, sems, first, order

    def each(self, layer, what):
        for k, (src, dst) in enumerate(self.pairs):
            getattr(pltpu.make_async_copy(src.at[layer], dst.at[layer], self.sems.at[layer, k]), what)()

    def start(self):
        self.each(self.order[0], "start")

    def need(self, step):
        @pl.when(self.first & (step == 0))
        def _():
            self.each(self.order[0], "wait")
            self.each(self.order[1], "start")

        @pl.when(self.first & (step == 1))
        def _():
            self.each(self.order[1], "wait")


def fwd_kernel(
    counts, lens, text, mem0, wqkv_hbm, wo_hbm, wup_hbm, wdn_hbm, par, ubias,
    text_out, mem_out, lhs_out, qkv_out, p_out, gp_out, xh1_out, xh2_out, rs_out,
    x_ref, mem_ref, y_ref, acc_ref, wqkv, wo, wup, wdn, wsem,
):
    seg = pl.program_id(0)
    layer = pl.program_id(1)
    d = x_ref.shape[-1]
    a_out, c_out, y_out = (lhs_out.at[:, :, j * d : (j + 1) * d] for j in range(3))
    g_out = lhs_out.at[:, :, 3 * d :]
    bias, norm = par.at[0:LAYERS], par.at[LAYERS : 2 * LAYERS]
    loads = Loads(((wqkv_hbm, wqkv), (wo_hbm, wo), (wup_hbm, wup), (wdn_hbm, wdn)), wsem, seg == 0, (0, 1))

    @pl.when((seg == 0) & (layer == 0))
    def _():
        loads.start()
        mem_ref[...] = mem0[...]

    @pl.when(layer == 0)
    def _():
        for i in range(MB):
            x_ref[i * SEG : i * SEG + TEXT, :] = text[i, 0].astype(F32)
            tail = slice(i * SEG + TAIL, (i + 1) * SEG)
            now = x_ref[tail, :]
            x_ref[tail, :] = jnp.where(row_ids(now.shape) < TEXT - TAIL, now, mem_ref[i])

    loads.need(layer)
    xb = x_ref[...].astype(BF)
    a_out[0] = xb
    qkv_out[0, :, 0:d] = (dot(xb, wqkv[layer, 0]) + bias[layer, 0:1, :]).astype(BF)
    qkv_out[0, :, d : 2 * d] = dot(xb, wqkv[layer, 1]).astype(BF)
    qkv_out[0, :, 2 * d : 3 * d] = (dot(xb, wqkv[layer, 2]) + bias[layer, 1:2, :]).astype(BF)

    low_half = lane_ids((SEG, 128)) < HD
    lanes = lane_ids((1, SEG))

    def heads_of(v):
        zero = jnp.zeros_like(v)
        return jnp.concatenate([jnp.where(low_half, v, zero), jnp.where(low_half, zero, v)], axis=0)

    for i in range(MB):
        vr = valid_rows(seg, counts[i], lens[i])
        keep = (lanes < vr) | (lanes >= TEXT)
        r0 = i * SEG
        for g0 in range(0, HEADS // 2, GROUP_F):
            pairs = range(g0, g0 + GROUP_F)

            def part(j, pair):
                return qkv_out[0, r0 : r0 + SEG, j * d + pair * 128 : j * d + pair * 128 + 128]

            s_all = [dot_rt(heads_of(part(0, p) * (HD ** -0.5)), part(1, p)) for p in pairs]
            s_all = [jnp.where(keep, s, NEG) for s in s_all]
            e_all = [jnp.exp(s - jnp.max(s, axis=-1, keepdims=True)) for s in s_all]
            p_all = [(e * (1.0 / jnp.sum(e, axis=-1, keepdims=True))).astype(BF) for e in e_all]
            c_all = [dot(pv, part(2, p)) for pv, p in zip(p_all, pairs)]
            for p, pv, c2 in zip(pairs, p_all, c_all):
                u0 = (i * (HEADS // 2) + p) * 2 * SEG
                p_out[0, u0 : u0 + 2 * SEG, :] = pv
                c_out[0, r0 : r0 + SEG, p * 128 : p * 128 + 128] = jnp.where(low_half, c2[:SEG], c2[SEG:]).astype(BF)

    def norm_to(base_ref, gain, shift, add, xh_out, rs_index, to_ref, low_out):
        for k in range(0, ROWS, CHUNK):
            rows = slice(k, k + CHUNK)
            h = base_ref[rows, :] + (acc_ref[rows, :] + add)
            center = h - jnp.mean(h, axis=-1, keepdims=True)
            rs = lax.rsqrt(jnp.mean(center * center, axis=-1, keepdims=True) + EPS)
            xh = center * rs
            xh_out[0, rows, :] = xh
            rs_out[0, rs_index, rows, :] = jnp.broadcast_to(rs, (CHUNK, 128))
            out = xh * gain + shift
            to_ref[rows, :] = out
            if low_out is not None:
                low_out[0, rows, :] = out.astype(BF)

    acc_ref[...] = dot(c_out[0], wo[layer])
    norm_to(x_ref, norm[layer, 0:1, :], norm[layer, 1:2, :], bias[layer, 2:3, :], xh1_out, 0, y_ref, y_out)

    ff = wup.shape[-1]

    def ffn_step():
        cols = slice(0, ff)
        u = dot(y_out[0], wup[layer, :, cols]) + ubias[layer, :, cols]
        cdf = 0.5 * (1.0 + lax.erf(u * RSQRT2))
        g_out[0, :, cols] = (u * cdf).astype(BF)
        gp_out[0, :, cols] = (cdf + u * (jnp.exp(-0.5 * (u * u)) * RSQRT2PI)).astype(BF)

    ffn_step()
    acc_ref[...] = dot(g_out[0], wdn[layer])
    norm_to(y_ref, norm[layer, 2:3, :], norm[layer, 3:4, :], bias[layer, 3:4, :], xh2_out, 1, x_ref, None)

    @pl.when(layer == LAYERS - 1)
    def _():
        for i in range(MB):
            vr = valid_rows(seg, counts[i], lens[i])
            body = x_ref[i * SEG : i * SEG + TEXT, :]
            text_out[i, 0] = jnp.where(row_ids(body.shape) < vr, body, 0.0).astype(BF)
            tail = x_ref[i * SEG + TAIL : (i + 1) * SEG, :]
            both = jnp.where(row_ids(tail.shape) >= TEXT - TAIL + MEM, tail, pltpu.roll(tail, SEG - TAIL - MEM, axis=0))
            mem_ref[i] = jnp.where(seg < counts[i], both, mem_ref[i])
        mem_out[...] = mem_ref[...]


def whole(shape):
    return pl.BlockSpec(shape, lambda *_: (0,) * len(shape), pipeline_mode=pl.Buffered(1))


def saved(rows, cols):
    return pl.BlockSpec((1, rows, cols), lambda s, l: (l, s, 0))


def forward_local(text, mem, counts, lens, weights):
    wqkv, wo, wup, wdn, par, ubias = weights
    d, ff = wup.shape[1:]
    mem0 = jnp.concatenate([jnp.zeros((MB, TEXT - TAIL, d), F32), mem.astype(F32), mem.astype(F32)], axis=1)
    total = SEGS * ROWS
    units = MB * HEADS * SEG
    smem = pl.BlockSpec(memory_space=pltpu.SMEM)
    hbm = pl.BlockSpec(memory_space=pl.ANY)
    outs = pl.pallas_call(
        fwd_kernel,
        grid=(SEGS, LAYERS),
        in_specs=[
            smem, smem,
            pl.BlockSpec((MB, 1, TEXT, d), lambda s, l: (0, s, 0, 0)),
            whole(mem0.shape), hbm, hbm, hbm, hbm,
            whole(par.shape), whole((LAYERS, 1, ff)),
        ],
        out_specs=[
            pl.BlockSpec((MB, 1, TEXT, d), lambda s, l: (0, s, 0, 0)),
            whole(mem0.shape),
            saved(ROWS, 3 * d + ff), saved(ROWS, 3 * d), saved(units, 128),
            saved(ROWS, ff), saved(ROWS, d), saved(ROWS, d),
            pl.BlockSpec((1, 2, ROWS, 128), lambda s, l: (l, 0, s, 0)),
        ],
        out_shape=[
            jax.ShapeDtypeStruct((MB, SEGS, TEXT, d), BF),
            jax.ShapeDtypeStruct(mem0.shape, F32),
            jax.ShapeDtypeStruct((LAYERS, total, 3 * d + ff), BF),
            jax.ShapeDtypeStruct((LAYERS, total, 3 * d), BF),
            jax.ShapeDtypeStruct((LAYERS, SEGS * units, 128), BF),
            jax.ShapeDtypeStruct((LAYERS, total, ff), BF),
            jax.ShapeDtypeStruct((LAYERS, total, d), F32),
            jax.ShapeDtypeStruct((LAYERS, total, d), F32),
            jax.ShapeDtypeStruct((LAYERS, 2, total, 128), F32),
        ],
        scratch_shapes=[
            pltpu.VMEM((ROWS, d), F32), pltpu.VMEM(mem0.shape, F32),
            pltpu.VMEM((ROWS, d), F32), pltpu.VMEM((ROWS, d), F32),
            pltpu.VMEM(wqkv.shape, BF), pltpu.VMEM(wo.shape, BF), pltpu.VMEM(wup.shape, BF), pltpu.VMEM(wdn.shape, BF),
            pltpu.SemaphoreType.DMA((LAYERS, 4)),
        ],
        compiler_params=pltpu.CompilerParams(
            dimension_semantics=("arbitrary", "arbitrary"), vmem_limit_bytes=VMEM_LIMIT
        ),
        name="rmt_forward",
    )(counts, lens, text, mem0, wqkv, wo, wup, wdn, par, ubias.astype(F32)[:, None, :])
    text_out, mem_end = outs[:2]
    return text_out, mem_end[:, TEXT - TAIL + MEM :].astype(BF), outs[2:]


def bwd_kernel(
    counts, lens, cot, gm0, qkv, p_in, gp_in, xh1_in, xh2_in, rs_in, wqkv_hbm, wo_hbm, wup_hbm, wdn_hbm, par,
    tg_out, gm_out, rhs_out, small_out,
    g_ref, gm_ref, t_ref, acc_ref, dc_ref, wqkv, wo, wup, wdn, wsem, gb_out, gub_out, gn_out,
):
    seg = SEGS - 1 - pl.program_id(0)
    step = pl.program_id(1)
    layer = LAYERS - 1 - step
    loads = Loads(((wqkv_hbm, wqkv), (wo_hbm, wo), (wup_hbm, wup), (wdn_hbm, wdn)), wsem, seg == SEGS - 1, (1, 0))
    d = g_ref.shape[-1]
    ff = wup.shape[-1]
    norm = par.at[LAYERS : 2 * LAYERS]
    dqkv_out, dao_out = rhs_out.at[:, :, 0 : 3 * d], rhs_out.at[:, :, 3 * d : 4 * d]
    du_out, df_out = rhs_out.at[:, :, 4 * d : 4 * d + ff], rhs_out.at[:, :, 4 * d + ff :]

    @pl.when((seg == SEGS - 1) & (step == 0))
    def _():
        loads.start()
        gm_ref[...] = gm0[...]
        gb_out[...] = jnp.zeros_like(gb_out)
        gub_out[...] = jnp.zeros_like(gub_out)
        gn_out[...] = jnp.zeros_like(gn_out)

    @pl.when(step == 0)
    def _():
        for i in range(MB):
            vr = valid_rows(seg, counts[i], lens[i])
            ct = cot[i, 0].astype(F32)
            g_ref[i * SEG : i * SEG + TEXT, :] = jnp.where(row_ids(ct.shape) < vr, ct, 0.0)
            tail = slice(i * SEG + TAIL, (i + 1) * SEG)
            now = g_ref[tail, :]
            rows = row_ids(now.shape)
            mem_part = jnp.where((rows >= TEXT - TAIL + MEM) & (seg < counts[i]), gm_ref[i], 0.0)
            g_ref[tail, :] = jnp.where(rows < TEXT - TAIL, now, mem_part)

    loads.need(step)

    def norm_back(base_ref, add_ref, xh_in, rs_slot, gain, slot, low_out, low_slot):
        sums = [jnp.zeros((8, d), F32) for _ in range(3)]
        for k in range(0, ROWS, CHUNK):
            rows = slice(k, k + CHUNK)
            gout = base_ref[rows, :]
            if add_ref is not None:
                gout = gout + add_ref[rows, :]
            xh = xh_in[0, rows, :]
            gx = gout * xh
            t = gout * gain
            inner = jnp.mean(gx * gain, axis=-1, keepdims=True)
            dh = rs_in[0, rs_slot, rows, :][:, :1] * (t - jnp.mean(t, axis=-1, keepdims=True) - xh * inner)
            t_ref[rows, :] = dh
            low = dh.astype(BF)
            low_out[0, rows, :] = low
            sums = [v + colsum(w) for v, w in zip(sums, (gx, gout, low.astype(F32)))]
        gn_out[layer, slot] += sums[0]
        gn_out[layer, slot + 1] += sums[1]
        gb_out[layer, low_slot] += sums[2]

    norm_back(g_ref, None, xh2_in, 1, norm[layer, 2:3, :], 2, df_out, 3)

    def ffn_step():
        cols = slice(0, ff)
        dg = dot_rt(df_out[0], wdn[layer, cols, :])
        du = (dg * gp_in[0, :, cols].astype(F32)).astype(BF)
        du_out[0, :, cols] = du
        gub_out[layer, :, cols] += colsum(du.astype(F32))

    ffn_step()
    acc_ref[...] = dot_rt(du_out[0], wup[layer])
    norm_back(t_ref, acc_ref, xh1_in, 0, norm[layer, 0:1, :], 0, dao_out, 2)
    dc_ref[...] = dot_rt(dao_out[0], wo[layer]).astype(BF)

    low_half = lane_ids((SEG, 128)) < HD
    scale = HD ** -0.5

    def heads_of(v):
        zero = jnp.zeros_like(v)
        return jnp.concatenate([jnp.where(low_half, v, zero), jnp.where(low_half, zero, v)], axis=0)

    for i in range(MB):
        r0 = i * SEG
        for g0 in range(0, HEADS // 2, GROUP_B):
            pairs = range(g0, g0 + GROUP_B)

            def part(j, pair):
                return qkv[0, r0 : r0 + SEG, j * d + pair * 128 : j * d + pair * 128 + 128]

            def probs(pair):
                u0 = (i * (HEADS // 2) + pair) * 2 * SEG
                return p_in[0, u0 : u0 + 2 * SEG, :]

            def out(j, pair, v):
                dqkv_out[0, r0 : r0 + SEG, j * d + pair * 128 : j * d + pair * 128 + 128] = v.astype(BF)

            dc2 = [heads_of(dc_ref[r0 : r0 + SEG, p * 128 : p * 128 + 128]) for p in pairs]
            dp = [dot_rt(v, part(2, p)) for v, p in zip(dc2, pairs)]
            for p, v in zip(pairs, dc2):
                out(2, p, dot_lt(probs(p), v))
            pdp = [probs(p).astype(F32) * v for p, v in zip(pairs, dp)]
            ds = [
                (v - probs(p).astype(F32) * jnp.sum(v, axis=-1, keepdims=True)).astype(BF) for p, v in zip(pairs, pdp)
            ]
            dq2 = [dot(v, part(1, p)) for v, p in zip(ds, pairs)]
            dk = [dot_lt(v, heads_of(part(0, p))) for v, p in zip(ds, pairs)]
            for p, a, b in zip(pairs, dq2, dk):
                out(0, p, jnp.where(low_half, a[:SEG], a[SEG:]) * scale)
                out(1, p, b * scale)

    gb_out[layer, 0] += colsum(dqkv_out[0, :, 0:d].astype(F32))
    gb_out[layer, 1] += colsum(dqkv_out[0, :, 2 * d : 3 * d].astype(F32))
    g_ref[...] = (
        t_ref[...]
        + dot_rt(dqkv_out[0, :, 0:d], wqkv[layer, 0])
        + dot_rt(dqkv_out[0, :, d : 2 * d], wqkv[layer, 1])
        + dot_rt(dqkv_out[0, :, 2 * d : 3 * d], wqkv[layer, 2])
    )

    @pl.when(layer == 0)
    def _():
        for i in range(MB):
            tg_out[i, 0] = g_ref[i * SEG : i * SEG + TEXT, :].astype(BF)
            tail = g_ref[i * SEG + TAIL : (i + 1) * SEG, :]
            back = tail + pltpu.roll(tail, MEM, axis=0)
            gm_ref[i] = jnp.where(seg < counts[i], 0.0, gm_ref[i]) + back
        gm_out[...] = gm_ref[...]

    @pl.when((seg == 0) & (layer == 0))
    def _():
        for l in range(LAYERS):
            for k in range(4):
                parts = (gb_out[l, k], gub_out[l, :, k * d : (k + 1) * d], gn_out[l, k])
                for base, part in zip((0, 8, 16), parts):
                    row = base + 4 * l + k
                    small_out[row : row + 1, :] = jnp.sum(part, axis=0, keepdims=True)


def backward_local(cot, cot_mem, counts, lens, kept, weights):
    wqkv, wo, wup, wdn, par, _ = weights
    _, qkv, p_all, gp, xh1, xh2, rs = kept
    d, ff = wup.shape[1:]
    gm0 = jnp.concatenate([jnp.zeros((MB, TEXT - TAIL + MEM, d), F32), cot_mem.astype(F32)], axis=1)
    total = SEGS * ROWS
    units = MB * HEADS * SEG
    smem = pl.BlockSpec(memory_space=pltpu.SMEM)
    hbm = pl.BlockSpec(memory_space=pl.ANY)

    def kept_spec(rows, cols):
        return pl.BlockSpec((1, rows, cols), lambda s, l: (LAYERS - 1 - l, SEGS - 1 - s, 0))

    outs = pl.pallas_call(
        bwd_kernel,
        grid=(SEGS, LAYERS),
        in_specs=[
            smem, smem,
            pl.BlockSpec((MB, 1, TEXT, d), lambda s, l: (0, SEGS - 1 - s, 0, 0)),
            whole(gm0.shape),
            kept_spec(ROWS, 3 * d), kept_spec(units, 128), kept_spec(ROWS, ff), kept_spec(ROWS, d), kept_spec(ROWS, d),
            pl.BlockSpec((1, 2, ROWS, 128), lambda s, l: (LAYERS - 1 - l, 0, SEGS - 1 - s, 0)),
            hbm, hbm, hbm, hbm, whole(par.shape),
        ],
        out_specs=[
            pl.BlockSpec((MB, 1, TEXT, d), lambda s, l: (0, SEGS - 1 - s, 0, 0)),
            whole(gm0.shape),
            kept_spec(ROWS, 5 * d + ff), whole((24, d)),
        ],
        out_shape=[
            jax.ShapeDtypeStruct((MB, SEGS, TEXT, d), BF),
            jax.ShapeDtypeStruct(gm0.shape, F32),
            jax.ShapeDtypeStruct((LAYERS, total, 5 * d + ff), BF),
            jax.ShapeDtypeStruct((24, d), F32),
        ],
        scratch_shapes=[
            pltpu.VMEM((ROWS, d), F32), pltpu.VMEM(gm0.shape, F32),
            pltpu.VMEM((ROWS, d), F32), pltpu.VMEM((ROWS, d), F32), pltpu.VMEM((ROWS, d), BF),
            pltpu.VMEM(wqkv.shape, BF), pltpu.VMEM(wo.shape, BF), pltpu.VMEM(wup.shape, BF), pltpu.VMEM(wdn.shape, BF),
            pltpu.SemaphoreType.DMA((LAYERS, 4)),
            pltpu.VMEM((LAYERS, 4, 8, d), F32), pltpu.VMEM((LAYERS, 8, ff), F32), pltpu.VMEM((LAYERS, 4, 8, d), F32),
        ],
        compiler_params=pltpu.CompilerParams(
            dimension_semantics=("arbitrary", "arbitrary"), vmem_limit_bytes=VMEM_LIMIT
        ),
        name="rmt_backward",
    )(counts, lens, cot, gm0, qkv, p_all, gp, xh1, xh2, rs, wqkv, wo, wup, wdn, par)
    tg, gm = outs[:2]
    return tg, gm[:, TEXT - TAIL + MEM :].astype(BF), outs[2], outs[3]


TILES = 12


def product_kernel(ids, lhs, rhs, out):
    out[0, 0] = dot_lt(lhs[0], rhs[0]).astype(BF)


def weight_grads(lhs, rhs, layers):
    d = rhs.shape[-1] // 9
    total = lhs.shape[1]
    count = layers.shape[0]

    def left(l, t, ids):
        return (ids[l], 0, jnp.where(t < 3, 0, jnp.where(t < 4, 1, jnp.where(t < 8, 2, t - 5))))

    return pl.pallas_call(
        product_kernel,
        grid_spec=pltpu.PrefetchScalarGridSpec(
            num_scalar_prefetch=1,
            grid=(count, TILES),
            in_specs=[
                pl.BlockSpec((1, total, d), left),
                pl.BlockSpec((1, total, d), lambda l, t, ids: (ids[l], 0, jnp.minimum(t, 8))),
            ],
            out_specs=pl.BlockSpec((1, 1, d, d), lambda l, t, ids: (l, t, 0, 0)),
        ),
        out_shape=jax.ShapeDtypeStruct((count, TILES, d, d), BF),
        compiler_params=pltpu.CompilerParams(
            dimension_semantics=("arbitrary", "arbitrary"), vmem_limit_bytes=VMEM_LIMIT
        ),
        name="weight_products",
    )(layers, lhs, rhs)


MESH = pl.DeviceIdType.MESH
ZN = 4


def multiple(v, k):
    return v if isinstance(v, int) else pl.multiple_of(v, k)


def span(start, size):
    return pl.ds(multiple(start, size if size % 128 else 128), size)


def where_am_i():
    w, n = lax.axis_index("wide"), lax.axis_index("narrow")
    z, x = lax.div(w, 2), lax.rem(w, 2)
    y, c = lax.div(n, 2), lax.rem(n, 2)
    links = {
        "p": {"wide": w, "narrow": n + 1 - 2 * c},
        "x": {"wide": w + 1 - 2 * x, "narrow": n},
        "y": {"wide": w, "narrow": lax.rem(n + 2, 4)},
        "up": {"wide": w + 2, "narrow": n},
        "down": {"wide": w - 2, "narrow": n},
    }
    return w, n, z, x, y, c, links


def enter(z, links):
    barrier = pltpu.get_barrier_semaphore()
    for name in ("p", "x", "y"):
        pl.semaphore_signal(barrier, inc=1, device_id=links[name], device_id_type=MESH)

    @pl.when(z < ZN - 1)
    def _():
        pl.semaphore_signal(barrier, inc=1, device_id=links["up"], device_id_type=MESH)

    @pl.when(z > 0)
    def _():
        pl.semaphore_signal(barrier, inc=1, device_id=links["down"], device_id_type=MESH)

    pl.semaphore_wait(barrier, 3 + jnp.minimum(z, 1) + jnp.minimum(ZN - 1 - z, 1))


class Net:
    def __init__(self, ssem, rsem, links):
        self.ssem, self.rsem, self.links = ssem, rsem, links
        self.next_send, self.next_recv = 0, 0

    def sends(self, count):
        base, self.next_send = self.next_send, self.next_send + count
        return base

    def recvs(self, count):
        base, self.next_recv = self.next_recv, self.next_recv + count
        return base

    def copy(self, link, src, dst, s, r):
        return pltpu.make_async_remote_copy(
            src_ref=src, dst_ref=dst, send_sem=self.ssem.at[s], recv_sem=self.rsem.at[r],
            device_id=self.links[link], device_id_type=MESH,
        )


def gather_kernel(
    q_in, o_in, u_in, d_in, s_in, Q, O, U, D, S,
    tq, to, tu, td, aq, ao, au, ad, ssem, rsem, lsem,
):
    w, n, z, x, y, c, links = where_am_i()
    mine, other = c, 1 - c
    net = Net(ssem, rsem, links)
    rw, cn = aq.shape[1], aq.shape[2]
    rd, cu = ad.shape[0], au.shape[1]
    half = cu // 2
    enter(z, links)

    first = [net.copy("p", src, dst, net.sends(1), net.recvs(1)) for src, dst in (
        (q_in.at[other], tq), (d_in.at[other], td), (u_in.at[other], tu), (o_in.at[other], to),
        (s_in, S.at[z, x, y, c]),
    )]
    for cp in first:
        cp.start()
    own_small = pltpu.make_async_copy(s_in, S.at[z, x, y, c], lsem.at[4])
    own_small.start()

    def join(own, got):
        a, b = own.astype(F32), got.astype(F32)
        lo, hi = jnp.where(c == 0, a, b), jnp.where(c == 0, b, a)
        return jnp.concatenate([lo, hi], axis=-1).astype(BF)

    places = (
        (aq, Q.at[mine, :, span(rw * w, rw), span(cn * y, cn)]),
        (ad, D.at[mine, span(rd * w, rd), span(cn * y, cn)]),
        (au, U.at[mine, span(rw * w, rw), span(cu * y, cu)]),
        (ao, O.at[mine, span(rw * w, rw), span(cn * y, cn)]),
    )

    def put(*which):
        local = [pltpu.make_async_copy(*places[k], lsem.at[k]) for k in which]
        for cp in local:
            cp.start()
        for cp in local:
            cp.wait()

    main = rd - rw

    def rows_a(zp):
        return span(2 * rw * zp, 2 * rw)

    def rows_x(zp, xp):
        return span(rw * (2 * zp + xp), rw)

    def rows_d(zp, xp):
        return pl.ds(pl.multiple_of(rd * (2 * zp + xp), rw), main)

    def rows_v(zp, xp):
        return pl.ds(pl.multiple_of(rd * (2 * zp + xp) + main, rw), rw)

    def cols(yp):
        return span(cn * yp, cn)

    def blk_a(zp, xp, yp):
        return [Q.at[mine, :, rows_x(zp, xp), cols(yp)]]

    def blk_d(zp, xp, yp):
        return [D.at[mine, rows_d(zp, xp), cols(yp)]]

    def reg_a(zp, yp, layer):
        return [Q.at[layer, :, rows_a(zp), cols(yp)]]

    def reg_d(zp, xp, layer):
        return [D.at[layer, rows_d(zp, xp), :]]

    def u_cols(zp, xp, start, size):
        return U.at[mine, rows_x(zp, xp), span(start, size)]

    def blk_u(zp, xp, yp):
        return [
            u_cols(zp, xp, cu * yp, cu), O.at[mine, rows_x(zp, xp), cols(yp)], D.at[mine, rows_v(zp, xp), cols(yp)]
        ]

    def blk_u1(zp, xp, yp):
        return [u_cols(zp, xp, cu * yp, half), O.at[mine, rows_x(zp, xp), cols(yp)]]

    def blk_u2(zp, xp, yp):
        return [u_cols(zp, xp, cu * yp + half, half), D.at[mine, rows_v(zp, xp), cols(yp)]]

    def pair_u1(zp, yp, layer):
        return [U.at[layer, rows_a(zp), span(cu * yp, half)], O.at[layer, rows_a(zp), cols(yp)]]

    def pair_u2(zp, xp, layer):
        rows = rows_x(zp, xp)
        return [U.at[layer, rows, span(cu * yp + half, half)] for yp in range(2)] + [D.at[layer, rows_v(zp, xp), :]]

    class Lane:
        def __init__(self, link, sent, got, parts):
            self.link, self.sent, self.got, self.parts = link, sent, got, parts
            self.s = [net.sends(ZN) for _ in range(parts)]
            self.r = [net.recvs(ZN) for _ in range(parts)]

        def send(self, zp):
            for k, ref in enumerate(self.sent(zp)):
                net.copy(self.link, ref, ref, self.s[k] + zp, self.r[k] + zp).start()

        def recv(self, zp):
            for k, ref in enumerate(self.got(zp)):
                net.copy(self.link, ref, ref, self.s[k] + zp, self.r[k] + zp).wait_recv()

        def drain(self, zp):
            for k, ref in enumerate(self.sent(zp)):
                net.copy(self.link, ref, ref, self.s[k] + zp, self.r[k] + zp).wait_send()

    class Line:
        def __init__(self, region, parts):
            self.region, self.parts = region, parts
            self.su = [net.sends(ZN) for _ in range(parts)]
            self.sd = [net.sends(ZN) for _ in range(parts)]
            self.r = [net.recvs(ZN) for _ in range(parts)]

        def each(self, link, sems, zp, what):
            for k, ref in enumerate(self.region(zp)):
                getattr(net.copy(link, ref, ref, sems[k] + zp, self.r[k] + zp), what)()

        def own(self, what="start"):
            @pl.when(z < ZN - 1)
            def _():
                self.each("up", self.su, z, what)

            @pl.when(z > 0)
            def _():
                self.each("down", self.sd, z, what)

        def relay(self, t, what="start"):
            @pl.when(jnp.minimum(z - t, ZN - 2 - z) >= 0)
            def _():
                self.each("up", self.su, z - t, what)

            @pl.when(jnp.minimum(ZN - 1 - t - z, z - 1) >= 0)
            def _():
                self.each("down", self.sd, z + t, what)

        def recv(self, zp):
            self.each("up", self.su, zp, "wait_recv")

    line_a = [Line(lambda zp, xp=xp: blk_a(zp, xp, y), 1) for xp in (x, 1 - x)]
    line_d = [Line(lambda zp, yp=yp: blk_d(zp, x, yp), 1) for yp in (y, 1 - y)]
    line_u = Line(lambda zp: blk_u(zp, x, y), 3)
    x1 = Lane("x", lambda zp: blk_a(z, x, y), lambda zp: blk_a(z, 1 - x, y), 1)
    y1 = Lane("y", lambda zp: blk_d(z, x, y), lambda zp: blk_d(z, x, 1 - y), 1)
    x_u1 = Lane("x", lambda zp: blk_u1(zp, x, y), lambda zp: blk_u1(zp, 1 - x, y), 2)
    y_u2 = Lane("y", lambda zp: blk_u2(zp, x, y), lambda zp: blk_u2(zp, x, 1 - y), 2)
    y_a = [
        Lane("y", lambda zp, xp=xp: blk_a(zp, xp, y), lambda zp, xp=xp: blk_a(zp, xp, 1 - y), 1) for xp in (x, 1 - x)
    ]
    x_d = [
        Lane("x", lambda zp, yp=yp: blk_d(zp, x, yp), lambda zp, yp=yp: blk_d(zp, 1 - x, yp), 1) for yp in (y, 1 - y)
    ]
    y_u1 = Lane("y", lambda zp: pair_u1(zp, y, mine), lambda zp: pair_u1(zp, 1 - y, mine), 2)
    x_u2 = Lane("x", lambda zp: pair_u2(zp, x, mine), lambda zp: pair_u2(zp, 1 - x, mine), 3)

    def to_partner(make, parts):
        return Lane("p", lambda zp: make(zp, mine), lambda zp: make(zp, other), parts)

    p_a = to_partner(lambda zp, l: reg_a(zp, y, l), 1)
    p_a2 = to_partner(lambda zp, l: reg_a(zp, 1 - y, l), 1)
    p_d = to_partner(lambda zp, l: reg_d(zp, x, l), 1)
    p_d2 = to_partner(lambda zp, l: reg_d(zp, 1 - x, l), 1)
    p_u1 = to_partner(lambda zp, l: pair_u1(zp, y, l), 2)
    p_u1b = to_partner(lambda zp, l: pair_u1(zp, 1 - y, l), 2)
    p_u2 = to_partner(lambda zp, l: pair_u2(zp, x, l), 3)
    p_u2b = to_partner(lambda zp, l: pair_u2(zp, 1 - x, l), 3)

    small_x = Lane("x", lambda zp: [S.at[z, x, y]], lambda zp: [S.at[z, 1 - x, y]], 1)
    small_y = Lane("y", lambda zp: [S.at[z, :, y]], lambda zp: [S.at[z, :, 1 - y]], 1)
    line_s = Line(lambda zp: [S.at[zp]], 1)

    first[0].wait()
    for j in range(3):
        aq[j] = join(q_in[mine, j], tq[j])
    put(0)
    x1.send(0)
    line_a[0].own()
    first[1].wait()
    ad[...] = join(d_in[mine], td[...])
    put(1)
    y1.send(0)
    line_d[0].own()
    first[2].wait()
    au[...] = join(u_in[mine], tu[...])
    first[3].wait()
    ao[...] = join(o_in[mine], to[...])
    put(2, 3)
    first[4].wait()
    own_small.wait()
    small_x.send(0)
    x_u1.send(z)
    y_u2.send(z)
    line_u.own()
    y_a[0].send(z)
    x_d[0].send(z)
    small_x.recv(0)
    small_y.send(0)
    x1.recv(0)
    line_a[1].own()
    y_a[1].send(z)
    p_a.send(z)
    y1.recv(0)
    line_d[1].own()
    x_d[1].send(z)
    p_d.send(z)
    small_y.recv(0)
    line_s.own()

    def second(zp):
        x_u1.recv(zp)
        y_u1.send(zp)
        p_u1.send(zp)
        y_u2.recv(zp)
        x_u2.send(zp)
        p_u2.send(zp)

    def third(zp):
        for lane in y_a:
            lane.recv(zp)
        p_a2.send(zp)
        for lane in x_d:
            lane.recv(zp)
        p_d2.send(zp)
        y_u1.recv(zp)
        p_u1b.send(zp)
        x_u2.recv(zp)
        p_u2b.send(zp)

    def both_ways(t, make):
        @pl.when(z >= t)
        def _():
            make(z - t)

        @pl.when(z < ZN - t)
        def _():
            make(z + t)

    def take(line, t, *lanes):
        both_ways(t, line.recv)
        line.relay(t)
        for lane in lanes:
            both_ways(t, lane.send)

    second(z)
    for t in range(1, ZN):
        take(line_a[0], t, y_a[0])
        take(line_d[0], t, x_d[0])
        take(line_u, t, x_u1, y_u2)
        take(line_a[1], t, y_a[1], p_a)
        if t == 1:
            third(z)
        else:
            both_ways(t - 1, third)
        take(line_d[1], t, x_d[1], p_d)
        both_ways(t, second)
        take(line_s, t)
    both_ways(ZN - 1, third)

    partner = (p_a, p_a2, p_d, p_d2, p_u1, p_u1b, p_u2, p_u2b)
    for zp in range(ZN):
        for lane in partner:
            lane.recv(zp)
    for zp in range(ZN):
        for lane in partner + (x_u1, y_u2, *y_a, *x_d, y_u1, x_u2):
            lane.drain(zp)
    for lane in (x1, y1, small_x, small_y):
        lane.drain(0)
    for line in (line_u, *line_a, *line_d, line_s):
        line.own("wait_send")
        for t in range(1, ZN):
            line.relay(t, "wait_send")
    assert net.next_send <= ssem.shape[0] and net.next_recv <= rsem.shape[0]


def gather_fast(pieces):
    wqkv, wo, wup, wdn, bias, ubias, norm = pieces
    _, _, rw, cn = wqkv.shape
    rd, cu = wdn.shape[1], wup.shape[2]
    d, ff = rw * 8, rd * 8
    small = jnp.concatenate([bias[:, 0], norm[:, 0], ubias, jnp.zeros_like(ubias)], axis=0).astype(F32)
    small = jnp.pad(small, ((0, 0), (0, 128 - rw)))
    hbm = pl.BlockSpec(memory_space=pl.ANY)
    vmem = pl.BlockSpec(memory_space=pltpu.VMEM)
    Q, O, U, D, S = pl.pallas_call(
        gather_kernel,
        in_specs=[vmem] * 5,
        out_specs=[hbm] * 5,
        out_shape=[
            jax.ShapeDtypeStruct((LAYERS, 3, d, d), BF),
            jax.ShapeDtypeStruct((LAYERS, d, d), BF),
            jax.ShapeDtypeStruct((LAYERS, d, ff), BF),
            jax.ShapeDtypeStruct((LAYERS, ff, d), BF),
            jax.ShapeDtypeStruct((ZN, 2, 2, 2, 8, 128), F32),
        ],
        scratch_shapes=[
            pltpu.VMEM((3, rw, cn), BF), pltpu.VMEM((rw, cn), BF), pltpu.VMEM((rw, cu), BF), pltpu.VMEM((rd, cn), BF),
            pltpu.VMEM((3, rw, 2 * cn), BF), pltpu.VMEM((rw, 2 * cn), BF),
            pltpu.VMEM((rw, 2 * cu), BF), pltpu.VMEM((rd, 2 * cn), BF),
            pltpu.SemaphoreType.DMA((200,)), pltpu.SemaphoreType.DMA((200,)), pltpu.SemaphoreType.DMA((5,)),
        ],
        compiler_params=pltpu.CompilerParams(collective_id=1, has_side_effects=True),
        name="weight_gather",
    )(wqkv, wo, wup, wdn, small)
    S = S.reshape(8, 4, 8, 128)[..., :rw]
    rows = jnp.transpose(S, (2, 1, 0, 3)).reshape(8, 4, d)
    ub = jnp.transpose(S[:, :, 4:6], (2, 0, 1, 3)).reshape(2, ff)
    return Q, O, U, D, rows, ub


def accumulate(dst, src, rows, step=48):
    def body(i, carry):
        r = pl.ds(pl.multiple_of(i * step, 16), step)
        dst[r, :] = dst[r, :] + src[r, :]
        return carry

    lax.fori_loop(0, rows // step, body, 0)


def scatter_kernel(
    gw, lhs, rhs, sm_in, oq, oo, ou, od, sm_out,
    AT, AD, RH, LT, LB, FA, FD, F1, FO, F2, FV, S1, SO, S2, SV, ZA, ZD, ZU, ZO, ZV, TA, TD,
    hq, ho, hu, hd, s_p, s_x, s_y, s_below, s_above, s_a, s_b, s_sum, s_up, s_down, ssem, rsem, lsem,
):
    w, n, z, x, y, c, links = where_am_i()
    mine, other = c, 1 - c
    net = Net(ssem, rsem, links)
    d, ff = AT.shape[2], AD.shape[0]
    rw, cn = d // 8, d // 2
    rd, cu = ff // 8, ff // 2
    half = cu // 2
    enter(z, links)

    class Hop:
        def __init__(self, link, pairs, parts):
            self.link, self.pairs = link, pairs
            self.s = [net.sends(ZN) for _ in range(parts)]
            self.r = [net.recvs(ZN) for _ in range(parts)]

        def each(self, zp, what):
            for k, (src, dst) in enumerate(self.pairs(zp)):
                getattr(net.copy(self.link, src, dst, self.s[k] + zp, self.r[k] + zp), what)()

        def send(self, zp):
            self.each(zp, "start")

        def recv(self, zp):
            self.each(zp, "wait_recv")

        def drain(self, zp):
            self.each(zp, "wait_send")

    def rows_a(zp):
        return span(2 * rw * zp, 2 * rw)

    main = rd - rw

    def down(zp):
        return span(d * zp, d)

    swap = [
        Hop("p", lambda zp: [(gw.at[0, 0:3, rows_a(zp), :], AT.at[0:3, rows_a(zp), :])], 1),
        Hop("p", lambda zp: [(gw.at[0, 8 + zp], AD.at[down(zp), :])], 1),
        Hop("p", lambda zp: [(gw.at[0, 3:8, rows_a(zp), :], AT.at[3:8, rows_a(zp), :])], 1),
    ]

    def right(t):
        return pltpu.make_async_copy(rhs.at[mine, :, t * d : (t + 1) * d], RH.at[t], lsem.at[t])

    def left(j):
        return pltpu.make_async_copy(lhs.at[mine, :, j * d : (j + 1) * d], LB.at[j], lsem.at[9 + j])

    def left_g(v, zp):
        slot = (v + 3) % 4
        return pltpu.make_async_copy(lhs.at[mine, :, span(d * (3 + zp), d)], LB.at[slot], lsem.at[12 + v])

    def turn(j):
        step = 256

        def body(k, carry):
            part = pl.ds(pl.multiple_of(k * step, step), step)
            LT[j, :, part] = LB[j, part, :].T
            return carry

        lax.fori_loop(0, LB.shape[1] // step, body, 0)

    def products(first, last, zp):
        rows = rows_a(zp)

        def body(t, carry):
            j = jnp.where(t < 3, 0, jnp.where(t < 4, 1, 2))
            AT[t, rows, :] = (AT[t, rows, :].astype(F32) + dot(LT[j, rows, :], RH[t])).astype(BF)
            return carry

        lax.fori_loop(first, last, body, 0)

    def products_down(v, zp):
        rows = down(zp)

        def body(k, carry):
            cols = pl.ds(pl.multiple_of(k * cn, cn), cn)
            AD[rows, cols] = (AD[rows, cols].astype(F32) + dot_lt(LB[(v + 3) % 4], RH[8, :, cols])).astype(BF)
            return carry

        lax.fori_loop(0, 2, body, 0)

    def cols_a(yp):
        return span(cn * yp, cn)

    def rows_x(zp, xp):
        return span(rw * (2 * zp + xp), rw)

    def rows_d(zp, xp):
        return pl.ds(pl.multiple_of(rd * (2 * zp + xp), rw), main)

    def rows_v(zp, xp):
        return pl.ds(pl.multiple_of(rd * (2 * zp + xp) + main, rw), rw)

    def reg_a(zp, yp):
        return AT.at[0:3, rows_a(zp), cols_a(yp)]

    def reg_d(zp, xp):
        return AD.at[rows_d(zp, xp), :]

    def u1(zp, yp):
        return [AT.at[4 + 2 * yp, rows_a(zp), :], AT.at[3, rows_a(zp), cols_a(yp)]]

    def u1_part(zp, xp, yp):
        return [AT.at[4 + 2 * yp, rows_x(zp, xp), :], AT.at[3, rows_x(zp, xp), cols_a(yp)]]

    def u2(zp, xp):
        rows = rows_x(zp, xp)
        return [AT.at[5 + 2 * yp, rows, :] for yp in range(2)] + [AD.at[rows_v(zp, xp), :]]

    def u2_part(zp, xp, yp):
        return [AT.at[5 + 2 * yp, rows_x(zp, xp), :], AD.at[rows_v(zp, xp), cols_a(yp)]]

    def blk_u(zp):
        rows = rows_x(zp, x)
        return [AT.at[pl.ds(4 + 2 * y, 2), rows, :], AT.at[3, rows, cols_a(y)], AD.at[rows_v(zp, x), cols_a(y)]]

    def bufs_u1(zp):
        return [F1.at[zp], FO.at[zp]]

    def bufs_u2(zp):
        return [F2.at[0, zp], F2.at[1, zp], FV.at[zp]]

    def bufs_s1(zp):
        return [S1.at[zp], SO.at[zp]]

    def bufs_s2(zp):
        return [S2.at[zp], SV.at[zp]]

    y_a = Hop("y", lambda zp: [(reg_a(zp, 1 - y), FA.at[zp])], 1)
    x_d = Hop("x", lambda zp: [(reg_d(zp, 1 - x), FD.at[zp])], 1)
    y_u1 = Hop("y", lambda zp: list(zip(u1(zp, 1 - y), bufs_u1(zp))), 2)
    x_u2 = Hop("x", lambda zp: list(zip(u2(zp, 1 - x), bufs_u2(zp))), 3)
    x_u1 = Hop("x", lambda zp: list(zip(u1_part(zp, 1 - x, y), bufs_s1(zp))), 2)
    y_u2 = Hop("y", lambda zp: list(zip(u2_part(zp, x, 1 - y), bufs_s2(zp))), 2)
    last_a = Hop("x", lambda zp: [(AT.at[0:3, rows_x(z, 1 - x), cols_a(y)], TA)], 1)
    last_d = Hop("y", lambda zp: [(AD.at[rows_d(z, x), cols_a(1 - y)], TD)], 1)

    def add_all(dsts, srcs):
        for dst, src in zip(dsts, srcs):
            accumulate(dst, src, src.shape[0])

    class Line:
        def __init__(self, region, bufs):
            self.region, self.bufs = region, bufs
            self.su = [net.sends(ZN) for _ in bufs]
            self.sd = [net.sends(ZN) for _ in bufs]
            self.r = [net.recvs(ZN + 1) for _ in bufs]

        def up(self, zp, what):
            slot = jnp.where(zp == z + 1, ZN, zp)

            @pl.when(zp > z)
            def _():
                for k, (src, buf) in enumerate(zip(self.region(zp), self.bufs)):
                    getattr(net.copy("up", src, buf.at[slot], self.su[k] + zp, self.r[k] + slot), what)()

        def down(self, zp, what):
            @pl.when(zp < z)
            def _():
                for k, (src, buf) in enumerate(zip(self.region(zp), self.bufs)):
                    getattr(net.copy("down", src, buf.at[zp], self.sd[k] + zp, self.r[k] + zp), what)()

        def take(self, zp, slot):
            for k, (dst, buf) in enumerate(zip(self.region(zp), self.bufs)):
                net.copy("up", dst, buf.at[slot], self.su[k] + zp, self.r[k] + slot).wait_recv()
                self.add(dst, buf.at[slot])

        def add(self, dst, src):
            if len(src.shape) == 3:
                for j in range(src.shape[0]):
                    accumulate(dst.at[j], src.at[j], src.shape[1])
            else:
                accumulate(dst, src, src.shape[0])

        def go(self, zp):
            @pl.when(jnp.minimum(z - zp, ZN - 2 - z) >= 0)
            def _():
                self.take(zp, zp)

            @pl.when(jnp.minimum(zp - z, z - 1) >= 0)
            def _():
                self.take(zp, jnp.where(zp == z, ZN, zp))

            self.up(zp, "start")
            self.down(zp, "start")

        def drain(self, zp):
            self.up(zp, "wait_send")
            self.down(zp, "wait_send")

    line_a = Line(lambda zp: (reg_a(zp, y),), (ZA,))
    line_d = Line(lambda zp: (reg_d(zp, x),), (ZD,))
    line_u = Line(blk_u, (ZU, ZO, ZV))

    table = ((3, 3, 0, 0), (2, 0, 3, 1), (1, 2, 1, 2), (0, 1, 2, 3))
    order = [jnp.where(z == 0, t[0], jnp.where(z == 1, t[1], jnp.where(z == 2, t[2], t[3]))) for t in table]

    small = [
        net.copy(link, src, dst, net.sends(1), net.recvs(1))
        for link, src, dst in (("p", sm_in, s_p), ("x", s_a, s_x), ("y", s_b, s_y))
    ]
    small_up = net.copy("up", s_up, s_below, net.sends(1), net.recvs(1))
    small_down = net.copy("down", s_down, s_above, net.sends(1), net.recvs(1))

    small[0].start()
    left(0).start()
    for t in range(3):
        right(t).start()
    left_g(0, order[0]).start()
    right(8).start()
    for j in (1, 2):
        left(j).start()
    for t in range(3, 8):
        right(t).start()
    for zp in order:
        for part in swap:
            part.send(zp)

    def open_q(v):
        zp = order[v]
        if v == 0:
            left(0).wait()
            turn(0)
            for t in range(3):
                right(t).wait()
        swap[0].recv(zp)
        products(0, 3, zp)
        y_a.send(zp)

    def open_d(v):
        zp = order[v]
        left_g(v, zp).wait()
        if v == 0:
            right(8).wait()
        swap[1].recv(zp)
        products_down(v, zp)
        x_d.send(zp)

    def open_u(v):
        zp = order[v]
        if v == 0:
            left_g(1, order[1]).start()
            for j in (1, 2):
                left(j).wait()
                turn(j)
                left_g(j + 1, order[j + 1]).start()
            for t in range(3, 8):
                right(t).wait()
        swap[2].recv(zp)
        products(3, 8, zp)
        y_u1.send(zp)
        x_u2.send(zp)

    def mid_a(zp):
        y_a.recv(zp)
        for j in range(3):
            accumulate(reg_a(zp, y).at[j], FA.at[zp, j], 2 * rw)
        line_a.go(zp)

    def mid_d(zp):
        x_d.recv(zp)
        accumulate(reg_d(zp, x), FD.at[zp], main)
        line_d.go(zp)

    def mid_u(zp):
        y_u1.recv(zp)
        add_all(u1(zp, y), bufs_u1(zp))
        x_u1.send(zp)
        x_u2.recv(zp)
        add_all(u2(zp, x), bufs_u2(zp))
        y_u2.send(zp)

    def close(zp):
        x_u1.recv(zp)
        add_all(u1_part(zp, x, y), bufs_s1(zp))
        y_u2.recv(zp)
        add_all(u2_part(zp, x, y), bufs_s2(zp))
        line_u.go(zp)

    open_q(0)
    open_d(0)
    open_u(0)
    mid_a(order[0])
    small[0].wait()
    s_a[...] = sm_in[...] + s_p[...]
    small[1].start()
    open_q(1)
    open_d(1)
    mid_d(order[0])
    open_u(1)
    mid_u(order[0])
    small[1].wait()
    s_b[...] = s_a[...] + s_x[...]
    small[2].start()
    open_q(2)
    open_d(2)
    mid_a(order[1])
    open_u(2)
    close(order[0])
    mid_d(order[1])
    mid_u(order[1])
    small[2].wait()
    s_sum[...] = s_b[...] + s_y[...]
    open_q(3)
    open_d(3)
    mid_a(order[2])
    open_u(3)
    close(order[1])
    mid_d(order[2])
    mid_u(order[2])

    @pl.when(z > 0)
    def _():
        small_up.wait_recv()

    @pl.when(z == 0)
    def _():
        s_below[...] = jnp.zeros_like(s_below)

    @pl.when(z < ZN - 1)
    def _():
        s_up[...] = s_sum[...] + s_below[...]
        small_up.start()

    mid_a(order[3])
    last_a.send(0)
    close(order[2])
    mid_d(order[3])
    last_d.send(0)
    mid_u(order[3])

    @pl.when(z < ZN - 1)
    def _():
        small_down.wait_recv()

    @pl.when(z == ZN - 1)
    def _():
        s_above[...] = jnp.zeros_like(s_above)

    @pl.when(z > 0)
    def _():
        s_down[...] = s_sum[...] + s_above[...]
        small_down.start()

    sm_out[...] = s_sum[...] + s_below[...] + s_above[...]
    close(order[3])

    def pick(v, k):
        lo, hi = v[..., :k], v[..., k:]
        return jnp.where(c == 0, lo, hi), jnp.where(c == 0, hi, lo)

    out = [
        net.copy("p", src, dst.at[mine], net.sends(1), net.recvs(1))
        for src, dst in ((hu, ou), (hq, oq), (ho, oo), (hd, od))
    ]
    rows = rows_x(z, x)
    ou[mine] = AT[4 + 2 * y + c, rows, :].astype(F32)
    hu[...] = AT[5 + 2 * y - c, rows, :].astype(F32)
    out[0].start()
    keep, give = pick(AT[3, rows, cols_a(y)].astype(F32), cn // 2)
    oo[mine] = keep
    ho[...] = give
    out[2].start()
    last_a.recv(0)
    for j in range(3):
        keep, give = pick(AT[j, rows, cols_a(y)].astype(F32) + TA[j].astype(F32), cn // 2)
        oq[mine, j] = keep
        hq[j] = give
    out[1].start()
    last_d.recv(0)
    for k in range(rd // rw):
        part = slice(k * rw, (k + 1) * rw)
        here = span(rd * w + k * rw, rw)
        total = AD[here, cols_a(y)].astype(F32)
        if k * rw < main:
            total = total + TD[part, :].astype(F32)
        keep, give = pick(total, cn // 2)
        od[mine, part, :] = keep
        hd[part, :] = give
    out[3].start()

    for zp in range(ZN):
        for hop in (*swap, y_a, x_d, y_u1, x_u2, x_u1, y_u2):
            hop.drain(zp)
        for line in (line_a, line_d, line_u):
            line.drain(zp)
    last_a.drain(0)
    last_d.drain(0)

    @pl.when(z < ZN - 1)
    def _():
        small_up.wait_send()

    @pl.when(z > 0)
    def _():
        small_down.wait_send()

    for cp in out:
        cp.wait()
    assert net.next_send <= ssem.shape[0] and net.next_recv <= rsem.shape[0]


def scatter_fast(gw, lhs, rhs, pack):
    d = gw.shape[-1]
    ff = 4 * d
    rw, cn, rd, cu = d // 8, d // 2, ff // 8, ff // 2
    hbm = pl.BlockSpec(memory_space=pl.ANY)
    vmem = pl.BlockSpec(memory_space=pltpu.VMEM)

    def buf(*shape):
        return pltpu.VMEM(shape, BF)

    def wide(*shape):
        return pltpu.VMEM(shape, F32)

    outs = [(3, rw, cn // 2), (rw, cn // 2), (rw, cu // 2), (rd, cn // 2)]
    total = lhs.shape[1]
    full = [buf(8, d, d), buf(ff, d), buf(9, total, d), buf(3, d, total), buf(4, total, d)]
    oq, oo, ou, od, summed = pl.pallas_call(
        scatter_kernel,
        in_specs=[hbm, hbm, hbm, vmem],
        out_specs=[vmem] * 5,
        out_shape=[jax.ShapeDtypeStruct((LAYERS,) + s, F32) for s in outs] + [jax.ShapeDtypeStruct(pack.shape, F32)],
        scratch_shapes=full + [
            buf(ZN, 3, 2 * rw, cn), buf(ZN, rd - rw, d), buf(ZN, 2 * rw, cu // 2), buf(ZN, 2 * rw, cn),
            buf(2, ZN, rw, cu // 2), buf(ZN, rw, d), buf(ZN, rw, cu // 2), buf(ZN, rw, cn),
            buf(ZN, rw, cu // 2), buf(ZN, rw, cn), buf(ZN + 1, 3, 2 * rw, cn), buf(ZN + 1, rd - rw, d),
            buf(ZN + 1, 2, rw, cu // 2), buf(ZN + 1, rw, cn), buf(ZN + 1, rw, cn), buf(3, rw, cn), buf(rd - rw, cn),
        ] + [wide(*s) for s in outs] + [wide(*pack.shape)] * 10 + [
            pltpu.SemaphoreType.DMA((180,)), pltpu.SemaphoreType.DMA((160,)), pltpu.SemaphoreType.DMA((16,)),
        ],
        compiler_params=pltpu.CompilerParams(collective_id=2, has_side_effects=True, vmem_limit_bytes=VMEM_LIMIT),
        name="gradient_scatter",
    )(gw, lhs, rhs, pack)
    w, n = lax.axis_index("wide"), lax.axis_index("narrow")
    gb = lax.dynamic_slice(summed[0:8].reshape(2, 4, d), (0, n, w * rw), (2, 1, rw))
    gn = lax.dynamic_slice(summed[16:24].reshape(2, 4, d), (0, n, w * rw), (2, 1, rw))
    gub = lax.dynamic_slice(summed[8:16].reshape(2, ff), (0, (4 * w + n) * rw), (2, rw))
    return oq, oo, ou, od, gb, gub, gn


def gather_weights(pieces):
    wqkv, wo, wup, wdn, bias, ubias, norm = pieces
    narrow = [(wqkv, 3), (wo, 2), (wup, 2), (wdn, 2), (bias, 1), (norm, 1)]
    wqkv, wo, wup, wdn, bias, norm = (lax.all_gather(w, "narrow", axis=k, tiled=True) for w, k in narrow)
    wide = [(wqkv, 2), (wo, 1), (wup, 1), (wdn, 1), (bias, 2), (norm, 2)]
    wqkv, wo, wup, wdn, bias, norm = (lax.all_gather(w, "wide", axis=k, tiled=True) for w, k in wide)
    ubias = lax.all_gather(ubias, ("wide", "narrow"), axis=1, tiled=True)
    return wqkv, wo, wup, wdn, jnp.concatenate([bias, norm], axis=0).astype(F32), ubias


def scatter_two(grad, row_axis, col_axis):
    low = lax.psum_scatter(grad.astype(BF), "narrow", scatter_dimension=col_axis, tiled=True)
    return lax.psum_scatter(low.astype(F32), "wide", scatter_dimension=row_axis, tiled=True)


def scatter_grads(gw, pack):
    d = gw.shape[-1]
    gq, go, gdn = gw[:, 0:3], gw[:, 3], gw[:, 8:].reshape(LAYERS, -1, d)
    gup = jnp.moveaxis(gw[:, 4:8], 1, 2).reshape(LAYERS, d, -1)
    gb, gub, gn = pack[0:8].reshape(LAYERS, 4, d), pack[8:16].reshape(LAYERS, -1), pack[16:24].reshape(LAYERS, 4, d)
    big = (scatter_two(gq, 2, 3), scatter_two(go, 1, 2), scatter_two(gup, 1, 2), scatter_two(gdn, 1, 2))
    gub = lax.psum_scatter(gub, ("wide", "narrow"), scatter_dimension=1, tiled=True)

    def small_two(g):
        return lax.psum_scatter(
            lax.psum_scatter(g, "narrow", scatter_dimension=1, tiled=True), "wide", scatter_dimension=2, tiled=True
        )

    return big + (small_two(gb), gub, small_two(gn))


def shards(
    near, text_in, memory_in, counts, last_len, cot_text, cot_memory,
    qkv_weight, out_weight, up_weight, down_weight, biases, up_bias, norm_params,
):
    text, cot = text_in[:, 0], cot_text[:, 0]
    mem, cot_mem = memory_in[:, 0], cot_memory[:, 0]
    cnt, lens = counts[:, 0], last_len[:, 0]
    gather = gather_fast if near else gather_weights
    weights = gather((qkv_weight, out_weight, up_weight, down_weight, biases, up_bias, norm_params))
    text_out, mem_out, kept = forward_local(text, mem, cnt, lens, weights)
    text_grad, mem_grad, rhs, small = backward_local(cot, cot_mem, cnt, lens, kept, weights)
    if near:
        other = 1 - lax.rem(lax.axis_index("narrow"), 2)
        grads = scatter_fast(weight_grads(kept[0], rhs, other[None]), kept[0], rhs, small)
    else:
        grads = scatter_grads(weight_grads(kept[0], rhs, jnp.arange(LAYERS, dtype=jnp.int32)), small)
    return (text_out[:, None], mem_out[:, None], text_grad[:, None], mem_grad[:, None]) + grads


def solution(mesh):
    items = ("wide", "narrow")
    act5 = P(None, items, None, None, None)
    act4 = P(None, items, None, None)
    ids = P(None, items)
    split = P(None, "wide", "narrow")
    small = P(None, "narrow", "wide")
    params = (P(None, None, "wide", "narrow"), split, split, split, small, ids, small)
    near = (mesh.shape["wide"], mesh.shape["narrow"]) == (2 * ZN, 4)
    return jax.shard_map(
        functools.partial(shards, near),
        mesh=mesh,
        in_specs=(act5, act4, ids, ids, act5, act4) + params,
        out_specs=(act5, act4, act5, act4) + params,
        check_vma=False,
    )
```
